32 devices in a mesh: gx: 4 (over y, x), gy: 4 (over z), gz: 2 (over core).
Axes of the slice: x: 2, y: 2, z: 4, core: 2. Of those that a mesh axis runs over, the one named last changes fastest.
Arguments:
- residual: float32 [3, 32, 256, 512], P(None, 'gz', 'gx', 'gy'), may hold values from -32 to 32
- edge_diag: float32 [3, 32, 256, 512], P(None, 'gz', 'gx', 'gy'), may hold values from 6.5 to 9
- node_shift: float32 [32, 256, 512], P('gz', 'gx', 'gy'), may hold values from 0.05 to 3
- coarse_shift: float32 [16, 128, 256], P('gz', 'gx', 'gy'), may hold values from 0.05 to 3
Outputs:
- correction: float32 [3, 32, 256, 512], P(None, 'gz', 'gx', 'gy')
The draws below stay inside these ranges and needn't reach their ends.
All inputs are finite; a program needn't handle non-finite values.
Results may differ from the reference program's by a relative error of at most 0.000021.
Values sent between devices are 32-bit elements; how exact they have to be, the bound alone decides.
No kernel may reach another device: no remote copies, remote signals or barrier semaphores. Data moves between devices by JAX's collectives and lax.ppermute only.
A program may use at most 128 MiB of HBM per device.

```python
import math
import jax
import jax.numpy as jnp

NX = 256
NY = 512
NZ = 32


def draw_residual(key, part):
    second_key = jax.random.fold_in(jax.random.fold_in(key, 11), 1)
    zpos = jnp.arange(NZ, dtype=jnp.float32) / NZ
    xpos = jnp.arange(NX, dtype=jnp.float32) / NX
    ramp = 2.0 * (1.0 + zpos)[:, None, None] * (1.0 + xpos)[None, :, None] * jnp.ones((1, 1, NY), jnp.float32)
    rough = jnp.clip(jax.random.normal(second_key, (3, NZ, NX, NY), jnp.float32), -4.0, 4.0)
    values = ramp[None] * rough
    return values.astype(jnp.float32)


def level_of(own_key, shape, shards, least, top_value):
    loudness = 1.0
    for position, shards_of in shards:
        draws = jax.random.uniform(jax.random.fold_in(jax.random.fold_in(own_key, 6), position), (shards_of,), jnp.float32, least / len(shards), top_value / len(shards))
        loudness = loudness * jnp.repeat(jnp.exp(draws), shape[position] // shards_of).reshape((-1,) + (1,) * (len(shape) - 1 - position))
    return loudness


def setup_inputs(seed: int = 0) -> dict:
    keys = jax.random.split(jax.random.key(seed), 5)
    return {
        "residual": draw_residual(jax.random.fold_in(keys[4], 71), 0),
        "edge_diag": jnp.clip(6.5 + 2.5 * jax.random.uniform(keys[1], (3, NZ, NX, NY), jnp.float32) ** level_of(keys[1], (3, NZ, NX, NY), ((1, 2), (2, 4), (3, 4)), -0.2, 0.2), 6.5, 9.0),
        "node_shift": jnp.clip(jnp.exp(math.log(3.0) - 4.0943445 * jax.random.uniform(keys[2], (NZ, NX, NY), jnp.float32) ** level_of(keys[2], (NZ, NX, NY), ((0, 2), (1, 4), (2, 4)), -0.2, 0.2)), 0.05, 3.0),
        "coarse_shift": jnp.clip(jnp.exp(math.log(3.0) - 4.0943445 * jax.random.uniform(keys[3], (NZ // 2, NX // 2, NY // 2), jnp.float32) ** level_of(keys[3], (NZ // 2, NX // 2, NY // 2), ((0, 2), (1, 4), (2, 4)), -0.2, 0.2)), 0.05, 3.0),
    }


def neighbours(padded):
    total = padded[2:, 1:-1, 1:-1] + padded[:-2, 1:-1, 1:-1]
    total = total + padded[1:-1, 2:, 1:-1] + padded[1:-1, :-2, 1:-1]
    return total + padded[1:-1, 1:-1, 2:] + padded[1:-1, 1:-1, :-2]


def apply_op(field, diagonal):
    return diagonal * field - neighbours(jnp.pad(field, 1))


def reference(residual, edge_diag, node_shift, coarse_shift):
    scaled = residual / edge_diag
    padded = jnp.pad(scaled, ((0, 0), (1, 1), (1, 1), (1, 1)))
    edge_near = jnp.stack([neighbours(padded[component]) for component in range(3)])
    smooth_part = 2.0 * scaled - (edge_diag * scaled - edge_near) / edge_diag
    nodal_rhs = (padded[0, :-2, 1:-1, 1:-1] - scaled[0]) + (padded[1, 1:-1, :-2, 1:-1] - scaled[1]) + (padded[2, 1:-1, 1:-1, :-2] - scaled[2])
    node_diag = 6.0 + node_shift
    first_guess = nodal_rhs / node_diag
    node_res = nodal_rhs - apply_op(first_guess, node_diag)
    sx, sy, sz = node_res.shape
    coarse_rhs = node_res.reshape(sx // 2, 2, sy // 2, 2, sz // 2, 2).sum(axis=(1, 3, 5))
    coarse_diag = 6.0 + coarse_shift
    first_dir = coarse_rhs / coarse_diag
    first_image = apply_op(first_dir, coarse_diag)
    second_dir = first_image / coarse_diag
    second_image = apply_op(second_dir, coarse_diag)
    gone = jnp.sum(first_dir * coarse_rhs)
    gtwo = jnp.sum(second_dir * coarse_rhs)
    hone = jnp.sum(first_dir * first_image)
    hmix = jnp.sum(second_dir * first_image)
    htwo = jnp.sum(second_dir * second_image)
    coef_two = (gtwo - hmix * gone / hone) / (htwo - hmix * hmix / hone)
    coef_one = (gone - hmix * coef_two) / hone
    coarse_sol = coef_one * first_dir + coef_two * second_dir
    spread = jnp.broadcast_to(coarse_sol[:, None, :, None, :, None], (sx // 2, 2, sy // 2, 2, sz // 2, 2)).reshape(sx, sy, sz)
    nodal = first_guess + spread
    final_nodal = nodal + (nodal_rhs - apply_op(nodal, node_diag)) / node_diag
    fpad = jnp.pad(final_nodal, 1)
    grads = jnp.stack([fpad[2:, 1:-1, 1:-1] - final_nodal, fpad[1:-1, 2:, 1:-1] - final_nodal, fpad[1:-1, 1:-1, 2:] - final_nodal])
    return smooth_part + grads
```

```python
import jax
import jax.numpy as jnp
from jax import lax
from jax.experimental import pallas as pl
from jax.experimental.pallas import tpu as pltpu
from jax.sharding import PartitionSpec as P

F32 = jnp.float32
HIGHEST = lax.Precision.HIGHEST
LANES = 128


def lane_ids(rows):
    return lax.broadcasted_iota(jnp.int32, (rows, LANES), 1)


def row_ids(rows):
    return lax.broadcasted_iota(jnp.int32, (rows, LANES), 0)


def shift_lanes(value, amount):
    return pltpu.roll(value, amount % LANES, 1)


def shift_rows(value, amount):
    return pltpu.roll(value, amount % value.shape[0], 0)


def low_of(axis, size, first, second):
    place = lax.axis_index(axis)
    odd = place % 2 == 1
    zero = jnp.zeros_like(first)
    if second is None:
        return jnp.where(odd, first, zero)
    return jnp.where(odd, first, jnp.where(place > 0, second, zero))


def high_of(axis, size, first, second):
    place = lax.axis_index(axis)
    even = place % 2 == 0
    zero = jnp.zeros_like(first)
    if second is None:
        return jnp.where(even, first, zero)
    return jnp.where(even, first, jnp.where(place < size - 1, second, zero))


def from_below(axis, value):
    return jnp.where(lax.axis_index(axis) > 0, value, jnp.zeros_like(value))


def from_above(axis, size, value):
    return jnp.where(lax.axis_index(axis) < size - 1, value, jnp.zeros_like(value))


def ring(value, axis, step):
    size = lax.axis_size(axis)
    return lax.ppermute(value, axis, [(i, (i + step) % size) for i in range(size)])


def swap(values, axis):
    size = lax.axis_size(axis)
    even = [(i, i ^ 1) for i in range(size)]
    out = [lax.ppermute(values[0], axis, even)]
    if len(values) > 1:
        odd = [(i, (i + 1) % size if i % 2 else (i - 1) % size) for i in range(size)]
        out.append(lax.ppermute(values[1], axis, odd))
    return out


def write_sides(axis, refs, up, down):
    even = lax.axis_index(axis) % 2 == 0

    @pl.when(even)
    def _():
        up(refs[0])
        if len(refs) > 1:
            down(refs[1])

    @pl.when(jnp.logical_not(even))
    def _():
        down(refs[0])
        if len(refs) > 1:
            up(refs[1])


def call(body, outs, name, scratch=(), **kwargs):
    return pl.pallas_call(
        body,
        out_shape=[jax.ShapeDtypeStruct(shape, F32) for shape in outs],
        scratch_shapes=[pltpu.VMEM(shape, F32) for shape in scratch],
        name=name,
        **kwargs,
    )


def vmem(count):
    return [pl.BlockSpec(memory_space=pltpu.VMEM)] * count


def edge_stage(residual, edge_diag):
    _, nz, nx, ny = residual.shape
    step = 4
    steps = nz // step

    def body(res, diag, part, up_z, up_x, up_y, low_z, low_x, low_y, last):
        block = pl.program_id(0)
        lane = lane_ids(nx)
        row = row_ids(nx)

        @pl.when(block == 0)
        def _():
            last[...] = jnp.zeros_like(last)
            up_y[...] = jnp.zeros_like(up_y)
            low_y[...] = jnp.zeros_like(low_y)

        before = last[...]
        high = up_y[...]
        low = low_y[...]
        for j in range(step):
            z = block * step + j
            s = [res[k, j] / diag[k, j] for k in range(3)]
            total = before - s[0]
            total += jnp.where(row == 0, 0.0, shift_rows(s[1], 1)) - s[1]
            total += jnp.where(lane == 0, 0.0, shift_lanes(s[2], 1)) - s[2]
            part[j] = total
            before = s[0]
            for k in range(3):
                up_x[pl.ds(k * nz + z, 1), :] = s[k][nx - 1 :, :]
                low_x[pl.ds(k * nz + z, 1), :] = s[k][:1, :]
                spot = k * nz + z
                high = jnp.where(lane == spot, pltpu.roll(s[k], spot + 1, 1), high)
                low = jnp.where(lane == spot, pltpu.roll(s[k], spot, 1), low)
            if j == 0:

                @pl.when(block == 0)
                def _():
                    for k in range(3):
                        low_z[k] = s[k]

            if j == step - 1:

                @pl.when(block == steps - 1)
                def _():
                    for k in range(3):
                        up_z[k] = s[k]

        last[...] = before
        up_y[...] = high
        low_y[...] = low

    whole = lambda *shape: pl.BlockSpec(shape, lambda i: (0,) * len(shape))
    spec = pl.BlockSpec((3, step, nx, ny), lambda i: (0, i, 0, 0))
    faces = [(3, nx, ny), (3 * nz, ny), (nx, LANES)] * 2
    return call(
        body,
        [(nz, nx, ny)] + faces,
        "edge_stage",
        scratch=[(nx, ny)],
        grid=(steps,),
        in_specs=[spec, spec],
        out_specs=[pl.BlockSpec((step, nx, ny), lambda i: (i, 0, 0))] + [whole(*f) for f in faces],
    )(residual, edge_diag)


def plane(values, row_count):
    return jnp.concatenate([values, jnp.zeros((row_count - values.shape[0], LANES), F32)], axis=0)


def nodal_stage(part, node_shift, coarse_shift, got_z, got_x, got_y, low_z, z_count):
    nz, nx, ny = part.shape
    cz, cx, cy = nz // 2, nx // 2, ny // 2
    rows = cx + 8
    sends = 1 if z_count == 2 else 2

    def body(part, shift, coarse, gz, gx, gy, low_z, fg, rhs, xb, yb, w, *rest):
        out, (pair, s_, xl_, yl_, zl_, zh_) = rest[:sends], rest[sends:]
        lane = lane_ids(nx)
        row = row_ids(nx)
        lane_c = lane_ids(rows)
        row_c = row_ids(rows)
        below_z = from_below("gz", gz[0])
        below_y = from_below("gy", gy[...])
        fine = lax.broadcasted_iota(jnp.int32, (ny, 2 * LANES), 0)
        coarse_lane = lax.broadcasted_iota(jnp.int32, (ny, 2 * LANES), 1)
        miss = jnp.where(
            coarse_lane < LANES, fine // 2 - coarse_lane, fine - 2 * (coarse_lane - LANES)
        )
        gather = jnp.where(miss == 0, 1.0, 0.0)
        for c in range(cz):
            both = []
            for z in (2 * c, 2 * c + 1):
                total = part[z]
                if z == 0:
                    total += below_z
                total += jnp.where(row == 0, from_below("gx", gx[nz + z : nz + z + 1, :]), 0.0)
                total += jnp.where(lane == 0, shift_lanes(below_y, -(2 * nz + z)), 0.0)
                guess = total / (6.0 + shift[z])
                fg[z] = guess
                both.append(guess)
            pair[c % 2] = both[0] + both[1]
            low = pair[c % 2, pl.ds(0, cx, 2), :]
            high = pair[c % 2, pl.ds(1, cx, 2), :]
            first = fg[2 * c, pl.ds(0, cx, 2), :] + fg[2 * c, pl.ds(1, cx, 2), :]
            stacked = jnp.concatenate([low + high, low, first], axis=0)
            sums = jnp.dot(stacked, gather, precision=HIGHEST, preferred_element_type=F32)
            s = sums[:cx, :LANES]
            z_low = sums[2 * cx :, :LANES]
            s_[c] = plane(s, rows)
            yl_[c] = plane(sums[:cx, LANES:], rows)
            xl_[c] = plane(sums[cx : 2 * cx, :LANES], rows)
            zl_[c] = plane(z_low, rows)
            zh_[c] = plane(s - z_low, rows)
            w[c] = jnp.zeros((rows, LANES), F32)
            w[c, :cx, :cy] = 1.0 / (6.0 + coarse[c])
        for c in range(cz):
            s, x_low, y_low = s_[c], xl_[c], yl_[c]
            x_high = s - x_low
            y_high = s - y_low
            total = 3.0 * s
            total += shift_rows(x_low, -1) + shift_rows(x_high, 1)
            total += shift_lanes(y_low, -1) + shift_lanes(y_high, 1)
            if c > 0:
                total += zh_[c - 1]
            if c < cz - 1:
                total += zl_[c + 1]
            rhs[c] = total
            xb[c] = jnp.where(row_c < cx // 2, x_low, x_high)
            yb[c] = jnp.where(lane_c < cy // 2, y_low, y_high)
        rhs[cz] = zh_[cz - 1]
        rhs[cz + 1] = jnp.zeros((rows, LANES), F32)
        rhs[cz + 2] = jnp.zeros((rows, LANES), F32)
        rhs[cz + 3] = zl_[0]

        def fill(ref, near, far, half, face):
            planes = [rhs[near], rhs[far], w[near], w[far], half]
            planes += [xb[near], xb[far], yb[near], yb[far]]
            for i, value in enumerate(planes):
                ref[i * rows : (i + 1) * rows, :] = value
            ref[9 * rows : 9 * rows + nx, :] = face

        def up(ref):
            fill(ref, cz - 1, cz - 2, zh_[cz - 1], fg[nz - 1])
            for k in range(3):
                at = 9 * rows + nx + k * nx
                ref[at : at + nx, :] = jnp.zeros((nx, LANES), F32)

        def down(ref):
            fill(ref, 0, 1, zl_[0], fg[0])
            for k in range(3):
                at = 9 * rows + nx + k * nx
                ref[at : at + nx, :] = low_z[k]

        write_sides("gz", out, up, down)

    coarse = (cz, rows, LANES)
    send = (9 * rows + 4 * nx, LANES)
    return call(
        body,
        [(nz, nx, ny), (cz + 4, rows, LANES), coarse, coarse, coarse] + [send] * sends,
        "nodal_stage",
        scratch=[(2, nx, ny), coarse, coarse, coarse, coarse, coarse],
        in_specs=vmem(7),
        out_specs=vmem(5 + sends),
    )(part, node_shift, coarse_shift, got_z, got_x, got_y, low_z)


def x_stage(got, rhs, xb, yb, w, fg, low_x, z_count, x_count):
    planes, rows, _ = rhs.shape
    cz, cx = planes - 4, rows - 8
    nz, nx, _ = fg.shape
    sends = 1 if x_count == 2 else 2
    gots = len(got)

    def body(*refs):
        got = refs[:gots]
        rhs, xb, yb, w, fg, low_x, rhs2, yb2, w2 = refs[gots : gots + 9]
        out, (xb2,) = refs[gots + 9 : gots + 9 + sends], refs[gots + 9 + sends :]

        def take(pick, i):
            at = slice(i * rows, (i + 1) * rows)
            values = [ref[at, :] for ref in got]
            return pick("gz", z_count, values[0], values[1] if gots > 1 else None)

        for c in range(1, cz - 1):
            rhs2[c] = rhs[c]
        rhs2[0] = rhs[0] + take(low_of, 4)
        rhs2[cz - 1] = rhs[cz - 1] + take(high_of, 4)
        rhs2[cz] = rhs[cz] + take(high_of, 0)
        rhs2[cz + 1] = take(high_of, 1)
        rhs2[cz + 2] = take(low_of, 1)
        rhs2[cz + 3] = rhs[cz + 3] + take(low_of, 0)
        for here, there, i in ((w, w2, 2), (xb, xb2, 5), (yb, yb2, 7)):
            for c in range(cz):
                there[c] = here[c]
            there[cz] = take(high_of, i)
            there[cz + 1] = take(high_of, i + 1)
            there[cz + 2] = take(low_of, i + 1)
            there[cz + 3] = take(low_of, i)

        def fill(ref, near, far, fine):
            pieces = [rhs2[:, near, :], rhs2[:, far, :], w2[:, near, :], w2[:, far, :]]
            pieces += [xb2[:, near, :], yb2[:, near, :], yb2[:, far, :]]
            for i, value in enumerate(pieces):
                ref[i * 16 : i * 16 + planes, :] = value
                if planes < 16:
                    ref[i * 16 + planes : i * 16 + 16, :] = jnp.zeros((16 - planes, LANES), F32)
            ref[112 : 112 + nz, :] = fg[:, fine, :]

        def up(ref):
            fill(ref, cx - 1, cx - 2, nx - 1)
            ref[112 + nz : 112 + 4 * nz, :] = jnp.zeros((3 * nz, LANES), F32)

        def down(ref):
            fill(ref, 0, 1, 0)
            ref[112 + nz : 112 + 4 * nz, :] = low_x[...]

        write_sides("gx", out, up, down)

    whole = (planes, rows, LANES)
    return call(
        body,
        [whole, whole, whole] + [(112 + 4 * nz, LANES)] * sends,
        "x_stage",
        scratch=[whole],
        in_specs=vmem(gots + 6),
        out_specs=vmem(3 + sends),
    )(*got, rhs, xb, yb, w, fg, low_x)


def y_stage(got, rhs, yb, w, fg, low_y, x_count, y_count):
    planes, rows, _ = rhs.shape
    cx = rows - 8
    nz, nx, ny = fg.shape
    cy = ny // 2
    sends = 1 if y_count == 2 else 2
    gots = len(got)

    def body(*refs):
        got = refs[:gots]
        rhs, yb, w, fg, low_y, rhs3, w3 = refs[gots : gots + 7]
        out, (yb3, add) = refs[gots + 7 : gots + 7 + sends], refs[gots + 7 + sends :]

        def take(pick, i):
            at = slice(i * 16, i * 16 + planes)
            values = [ref[at, :] for ref in got]
            return pick("gx", x_count, values[0], values[1] if gots > 1 else None)

        add[...] = jnp.zeros_like(add)
        add[:, cx, :] = take(high_of, 0)
        add[:, cx + 1, :] = take(high_of, 1)
        add[:, rows - 1, :] = take(low_of, 0)
        add[:, rows - 2, :] = take(low_of, 1)
        add[:, cx - 1, :] = take(high_of, 4)
        add[:, 0, :] = take(low_of, 4)
        for c in range(planes):
            rhs3[c] = rhs[c] + add[c]
            w3[c] = w[c]
            yb3[c] = yb[c]
        for there, i in ((w3, 2), (yb3, 5)):
            there[:, cx, :] = take(high_of, i)
            there[:, cx + 1, :] = take(high_of, i + 1)
            there[:, rows - 1, :] = take(low_of, i)
            there[:, rows - 2, :] = take(low_of, i + 1)

        lane_c = lane_ids(rows)
        lane = lane_ids(nx)

        def fill(ref, near, far, fine, tail):
            acc = jnp.zeros((rows, LANES), F32)
            jobs = ((rhs3, near), (rhs3, far), (w3, near), (w3, far), (yb3, near))
            for i, (field, at) in enumerate(jobs):
                for z in range(planes):
                    spot = i * planes + z
                    acc = jnp.where(lane_c == spot, shift_lanes(field[z], spot - at), acc)
            acc = plane(acc, nx)
            base = 5 * planes
            for z in range(nz):
                acc = jnp.where(lane == base + z, shift_lanes(fg[z], base + z - fine), acc)
            if tail is not None:
                at = base + nz
                moved = shift_lanes(tail, at)
                acc = jnp.where((lane >= at) & (lane < at + 3 * nz), moved, acc)
            ref[...] = acc

        def up(ref):
            fill(ref, cy - 1, cy - 2, ny - 1, None)

        def down(ref):
            fill(ref, 0, 1, 0, low_y[...])

        write_sides("gy", out, up, down)

    whole = (planes, rows, LANES)
    return call(
        body,
        [whole, whole] + [(nx, LANES)] * sends,
        "y_stage",
        scratch=[whole, whole],
        in_specs=vmem(gots + 5),
        out_specs=vmem(2 + sends),
    )(*got, rhs, yb, w, fg, low_y)


def coarse_stage(got, rhs, w, y_count, devices):
    planes, rows, _ = rhs.shape
    cz, cx = planes - 4, rows - 8
    cy = LANES // 2
    gots = len(got)

    def body(*refs):
        got = refs[:gots]
        rhs, w, v1, v2, sums, tot, inv_, image_ = refs[gots:]
        values = [ref[:rows, :] for ref in got]
        second = values[1] if gots > 1 else None
        low = low_of("gy", y_count, values[0], second)
        high = high_of("gy", y_count, values[0], second)
        lane = lane_ids(rows)
        spots_r = ((cy, high, 0), (cy + 1, high, 1), (LANES - 1, low, 0), (LANES - 2, low, 1))
        spots_r += ((cy - 1, high, 4), (0, low, 4))
        for z in range(planes):
            right = rhs[z]
            for at, source, i in spots_r:
                moved = shift_lanes(source, at - (i * planes + z))
                right += jnp.where(lane == at, moved, 0.0)
            inv = w[z]
            for at, source, i in spots_r[:4]:
                moved = shift_lanes(source, at - ((i + 2) * planes + z))
                inv = jnp.where(lane == at, moved, inv)
            inv_[z] = inv
            tot[z] = right
            v1[z] = right * inv

        def near(field, z):
            here = field[z]
            total = field[(z + 1) % planes] + field[(z - 1) % planes]
            total += shift_rows(here, 1) + shift_rows(here, -1)
            return total + shift_lanes(here, 1) + shift_lanes(here, -1)

        v2[cz + 1] = jnp.zeros((rows, LANES), F32)
        v2[cz + 2] = jnp.zeros((rows, LANES), F32)
        for z in list(range(cz + 1)) + [planes - 1]:
            image = tot[z] - near(v1, z)
            if z < cz:
                image_[z] = image
            v2[z] = image * inv_[z]
        parts = [jnp.zeros((cx, LANES), F32)] * 5
        for z in range(cz):
            first, second_, right, image = v1[z], v2[z], tot[z], image_[z]
            third = image - near(v2, z)
            terms = (first * right, second_ * right, first * image, second_ * image, second_ * third)
            parts = [a + b[:cx, :] for a, b in zip(parts, terms)]
        keep = lane_ids(1) < cy
        lines = [jnp.where(keep, jnp.sum(a, axis=0, keepdims=True), 0.0) for a in parts]
        tile = jnp.concatenate(lines + [jnp.zeros((3, LANES), F32)], axis=0)
        column = jnp.sum(tile, axis=1, keepdims=True)
        spread = jnp.where(lane_ids(8) == row_ids(8), column, 0.0)
        line = jnp.sum(spread, axis=0, keepdims=True)
        sums[...] = jnp.broadcast_to(line[None], (devices, 1, LANES))

    whole = (planes, rows, LANES)
    return call(
        body,
        [whole, whole, (devices, 1, LANES)],
        "coarse_stage",
        scratch=[whole, whole, whole],
        in_specs=vmem(gots + 2),
        out_specs=vmem(3),
    )(*got, rhs, w)


def final_stage(sums, v1, v2, fg, node_shift, got_z, got_x, got_y, counts):
    planes, rows, _ = v1.shape
    cz, cx = planes - 4, rows - 8
    nz, nx, ny = fg.shape
    n_z, n_x, n_y = len(got_z), len(got_x), len(got_y)

    def body(*refs):
        sums, v1, v2, fg, shift = refs[:5]
        gz = refs[5 : 5 + n_z]
        gx = refs[5 + n_z : 5 + n_z + n_x]
        gy = refs[5 + n_z + n_x : 5 + n_z + n_x + n_y]
        fn, down_z, down_x, down_y, dup, inter = refs[5 + n_z + n_x + n_y :]

        def both(refs, axis, size, at):
            values = [ref[at, :] for ref in refs]
            second = values[1] if len(values) > 1 else None
            return low_of(axis, size, values[0], second), high_of(axis, size, values[0], second)

        total = jnp.sum(sums[...], axis=0)
        lane1 = lane_ids(1)
        gone, gtwo, hone, hmix, htwo = [
            jnp.sum(jnp.where(lane1 == i, total, 0.0), axis=1, keepdims=True) for i in range(5)
        ]
        two = (gtwo - hmix * gone / hone) / (htwo - hmix * hmix / hone)
        one = (gone - hmix * two) / hone
        source = lax.broadcasted_iota(jnp.int32, (LANES, 2 * LANES), 0)
        target = lax.broadcasted_iota(jnp.int32, (LANES, 2 * LANES), 1)
        fine = target - LANES
        side = jnp.where(fine % 2 == 1, fine // 2 + 1, (fine // 2 + LANES - 1) % LANES)
        spread = jnp.where(jnp.where(target < LANES, target // 2, side) == source, 1.0, 0.0)
        for z in list(range(cz + 1)) + [planes - 1]:
            sol = one * v1[z] + two * v2[z]
            dup[z] = jnp.dot(sol, spread, precision=HIGHEST, preferred_element_type=F32)

        z_face = slice(9 * rows, 9 * rows + nx)
        z_low, z_high = both(gz, "gz", counts[0], z_face)
        x_low, x_high = both(gx, "gx", counts[1], slice(112, 112 + nz))
        y_low, y_high = both(gy, "gy", counts[2], slice(0, nx))
        lane = lane_ids(nx)
        row = row_ids(nx)
        base = 5 * planes
        acc = jnp.zeros((nx, LANES), F32)
        for z in range(nz):
            c, odd = z // 2, z % 2
            here = dup[c, :, :LANES]
            same = 3.0 * here + dup[c, :, LANES:]
            same += dup[(c + 1 if odd else c - 1) % planes, :, :LANES]
            slot = z % 2
            inter[slot, pl.ds(0, cx, 2), :] = (same + shift_rows(here, 1))[:cx, :]
            inter[slot, pl.ds(1, cx, 2), :] = (same + shift_rows(here, -1))[:cx, :]
            guess = fg[z]
            around = inter[slot]
            around += fg[z - 1] if z > 0 else z_low
            around += fg[z + 1] if z < nz - 1 else z_high
            around += jnp.where(row == 0, x_low[z : z + 1, :], shift_rows(guess, 1))
            around += jnp.where(row == nx - 1, x_high[z : z + 1, :], shift_rows(guess, -1))
            left = shift_lanes(y_low, -(base + z))
            right = shift_lanes(y_high, -(base + z) - 1)
            around += jnp.where(lane == 0, left, shift_lanes(guess, 1))
            around += jnp.where(lane == LANES - 1, right, shift_lanes(guess, -1))
            value = guess + around / (6.0 + shift[z])
            fn[z] = value
            if z == 0:
                down_z[...] = value
            down_x[z : z + 1, :] = value[:1, :]
            acc = jnp.where(lane == z, shift_lanes(value, z), acc)
        down_y[...] = acc

    return call(
        body,
        [(nz, nx, ny), (nx, ny), (nz, ny), (nx, LANES)],
        "final_stage",
        scratch=[(planes, rows, 2 * LANES), (2, nx, LANES)],
        in_specs=vmem(5 + n_z + n_x + n_y),
        out_specs=vmem(4),
    )(sums, v1, v2, fg, node_shift, *got_z, *got_x, *got_y)


def output_stage(residual, edge_diag, fn, above, below, got_z, got_x, got_y, planes, counts):
    _, nz, nx, ny = residual.shape
    n_z, n_x, n_y = len(got_z), len(got_x), len(got_y)
    rows = nx // 2 + 8

    def body(*refs):
        res, diag, fn, fz, fx, fy, lz, lx, ly = refs[:9]
        gz = refs[9 : 9 + n_z]
        gx = refs[9 + n_z : 9 + n_z + n_x]
        gy = refs[9 + n_z + n_x : 9 + n_z + n_x + n_y]
        out, s = refs[9 + n_z + n_x + n_y :]
        k = pl.program_id(0)
        lane = lane_ids(nx)
        row = row_ids(nx)

        def above_of(refs, axis, size, at):
            values = [ref[at, :] for ref in refs]
            return high_of(axis, size, values[0], values[1] if len(values) > 1 else None)

        for z in range(nz):
            s[z] = res[0, z] / diag[0, z]
        z_low = from_below("gz", lz[k])
        z_high = above_of(gz, "gz", counts[0], pl.ds(9 * rows + nx + k * nx, nx))
        x_low = from_below("gx", lx[pl.ds(k * nz, nz), :])
        x_high = above_of(gx, "gx", counts[1], pl.ds(112 + nz + k * nz, nz))
        y_low = pltpu.roll(from_below("gy", ly[...]), (LANES - k * nz) % LANES, 1)
        y_high = above_of(gy, "gy", counts[2], pl.ds(0, nx))
        y_high = pltpu.roll(y_high, (2 * LANES - 5 * planes - nz - k * nz) % LANES, 1)
        for z in range(nz):
            here = s[z]
            around = s[z - 1] if z > 0 else z_low
            around += s[z + 1] if z < nz - 1 else z_high
            around += jnp.where(row == 0, x_low[z : z + 1, :], shift_rows(here, 1))
            around += jnp.where(row == nx - 1, x_high[z : z + 1, :], shift_rows(here, -1))
            left = shift_lanes(y_low, -z)
            right = shift_lanes(y_high, -z - 1)
            around += jnp.where(lane == 0, left, shift_lanes(here, 1))
            around += jnp.where(lane == LANES - 1, right, shift_lanes(here, -1))
            out[0, z] = here + around / diag[0, z] - fn[z]

        @pl.when(k == 0)
        def _():
            for z in range(nz - 1):
                out[0, z] += fn[z + 1]
            out[0, nz - 1] += from_above("gz", counts[0], fz[...])

        @pl.when(k == 1)
        def _():
            face = from_above("gx", counts[1], fx[...])
            for z in range(nz):
                out[0, z] += jnp.where(row == nx - 1, face[z : z + 1, :], shift_rows(fn[z], -1))

        @pl.when(k == 2)
        def _():
            face = from_above("gy", counts[2], fy[...])
            for z in range(nz):
                moved = shift_lanes(face, -z - 1)
                out[0, z] += jnp.where(lane == LANES - 1, moved, shift_lanes(fn[z], -1))

    spec = pl.BlockSpec((1, nz, nx, ny), lambda k: (k, 0, 0, 0))
    args = (fn, *above, *below, *got_z, *got_x, *got_y)
    whole = [pl.BlockSpec(a.shape, lambda k, n=a.ndim: (0,) * n) for a in args]
    return call(
        body,
        [residual.shape],
        "output_stage",
        scratch=[(nz, nx, ny)],
        grid=(3,),
        in_specs=[spec, spec] + whole,
        out_specs=[spec],
    )(residual, edge_diag, *args)[0]


def local(residual, edge_diag, node_shift, coarse_shift):
    axes = ("gz", "gx", "gy")
    counts = tuple(lax.axis_size(a) for a in axes)
    devices = counts[0] * counts[1] * counts[2]
    part, up_z, up_x, up_y, low_z, low_x, low_y = edge_stage(residual, edge_diag)
    below = (ring(up_z, "gz", 1), ring(up_x, "gx", 1), ring(up_y, "gy", 1))
    fg, rhs, xb, yb, w, *send = nodal_stage(part, node_shift, coarse_shift, *below, low_z, counts[0])
    got_z = swap(send, "gz")
    rhs, yb, w, *send = x_stage(got_z, rhs, xb, yb, w, fg, low_x, counts[0], counts[1])
    got_x = swap(send, "gx")
    planes = rhs.shape[0]
    rhs, w, *send = y_stage(got_x, rhs, yb, w, fg, low_y, counts[1], counts[2])
    got_y = swap(send, "gy")
    v1, v2, sums = coarse_stage(got_y, rhs, w, counts[2], devices)
    sums = lax.all_to_all(sums, ("gx", "gy", "gz"), 0, 0)
    fn, down_z, down_x, down_y = final_stage(
        sums, v1, v2, fg, node_shift, got_z, got_x, got_y, counts
    )
    above = (ring(down_z, "gz", -1), ring(down_x, "gx", -1), ring(down_y, "gy", -1))
    return output_stage(
        residual, edge_diag, fn, above, below, got_z, got_x, got_y, planes, counts
    )


def solution(mesh):
    placed = (
        P(None, "gz", "gx", "gy"),
        P(None, "gz", "gx", "gy"),
        P("gz", "gx", "gy"),
        P("gz", "gx", "gy"),
    )
    return jax.shard_map(
        local, mesh=mesh, in_specs=placed, out_specs=P(None, "gz", "gx", "gy"), check_vma=False
    )
```

```python
import jax
import jax.numpy as jnp
from jax import lax
from jax.experimental import pallas as pl
from jax.experimental.pallas import tpu as pltpu
from jax.sharding import PartitionSpec as P

F32 = jnp.float32
HIGHEST = lax.Precision.HIGHEST
LANES = 128


def lane_ids(rows):
    return lax.broadcasted_iota(jnp.int32, (rows, LANES), 1)


def row_ids(rows):
    return lax.broadcasted_iota(jnp.int32, (rows, LANES), 0)


def shift_lanes(value, amount):
    return pltpu.roll(value, amount % LANES, 1)


def shift_rows(value, amount):
    return pltpu.roll(value, amount % value.shape[0], 0)


def low_of(axis, size, first, second):
    place = lax.axis_index(axis)
    odd = place % 2 == 1
    zero = jnp.zeros_like(first)
    if second is None:
        return jnp.where(odd, first, zero)
    return jnp.where(odd, first, jnp.where(place > 0, second, zero))


def high_of(axis, size, first, second):
    place = lax.axis_index(axis)
    even = place % 2 == 0
    zero = jnp.zeros_like(first)
    if second is None:
        return jnp.where(even, first, zero)
    return jnp.where(even, first, jnp.where(place < size - 1, second, zero))


def from_below(axis, value):
    return jnp.where(lax.axis_index(axis) > 0, value, jnp.zeros_like(value))


def from_above(axis, size, value):
    return jnp.where(lax.axis_index(axis) < size - 1, value, jnp.zeros_like(value))


def ring(value, axis, step):
    size = lax.axis_size(axis)
    return lax.ppermute(value, axis, [(i, (i + step) % size) for i in range(size)])


def swap(values, axis):
    size = lax.axis_size(axis)
    even = [(i, i ^ 1) for i in range(size)]
    out = [lax.ppermute(values[0], axis, even)]
    if len(values) > 1:
        odd = [(i, (i + 1) % size if i % 2 else (i - 1) % size) for i in range(size)]
        out.append(lax.ppermute(values[1], axis, odd))
    return out


def write_sides(axis, refs, up, down):
    even = lax.axis_index(axis) % 2 == 0

    @pl.when(even)
    def _():
        up(refs[0])
        if len(refs) > 1:
            down(refs[1])

    @pl.when(jnp.logical_not(even))
    def _():
        down(refs[0])
        if len(refs) > 1:
            up(refs[1])


def call(body, outs, name, scratch=(), far=(), far_out=False, **kwargs):
    kind = jax.ShapeDtypeStruct if far_out else pltpu.VMEM
    run = pl.pallas_call(
        body,
        out_shape=[kind(shape, F32) for shape in outs],
        scratch_shapes=[pltpu.VMEM(shape, F32) for shape in scratch],
        name=name,
        **kwargs,
    )

    def apply(*args):
        near = [
            a if i in far else pltpu.with_memory_space_constraint(a, pltpu.VMEM)
            for i, a in enumerate(args)
        ]
        return run(*near)

    return apply


def vmem(count):
    return [pl.BlockSpec(memory_space=pltpu.VMEM)] * count


def edge_stage(residual, edge_diag):
    _, nz, nx, ny = residual.shape
    step = 4
    steps = nz // step

    def body(res, diag, part, up_z, up_x, up_y, low_z, low_x, low_y, last):
        block = pl.program_id(0)
        lane = lane_ids(nx)
        row = row_ids(nx)

        @pl.when(block == 0)
        def _():
            last[...] = jnp.zeros_like(last)
            up_y[...] = jnp.zeros_like(up_y)
            low_y[...] = jnp.zeros_like(low_y)

        before = last[...]
        high = up_y[...]
        low = low_y[...]
        for j in range(step):
            z = block * step + j
            s = [res[k, j] / diag[k, j] for k in range(3)]
            total = before - s[0]
            total += jnp.where(row == 0, 0.0, shift_rows(s[1], 1)) - s[1]
            total += jnp.where(lane == 0, 0.0, shift_lanes(s[2], 1)) - s[2]
            part[j] = total
            before = s[0]
            for k in range(3):
                up_x[pl.ds(k * nz + z, 1), :] = s[k][nx - 1 :, :]
                low_x[pl.ds(k * nz + z, 1), :] = s[k][:1, :]
                spot = k * nz + z
                high = jnp.where(lane == spot, pltpu.roll(s[k], spot + 1, 1), high)
                low = jnp.where(lane == spot, pltpu.roll(s[k], spot, 1), low)
            if j == 0:

                @pl.when(block == 0)
                def _():
                    for k in range(3):
                        low_z[k] = s[k]

            if j == step - 1:

                @pl.when(block == steps - 1)
                def _():
                    for k in range(3):
                        up_z[k] = s[k]

        last[...] = before
        up_y[...] = high
        low_y[...] = low

    whole = lambda *shape: pl.BlockSpec(shape, lambda i: (0,) * len(shape))
    spec = pl.BlockSpec((3, step, nx, ny), lambda i: (0, i, 0, 0))
    faces = [(3, nx, ny), (3 * nz, ny), (nx, LANES)] * 2
    return call(
        body,
        [(nz, nx, ny)] + faces,
        "edge_stage",
        scratch=[(nx, ny)],
        far=(0, 1),
        grid=(steps,),
        in_specs=[spec, spec],
        out_specs=[pl.BlockSpec((step, nx, ny), lambda i: (i, 0, 0))] + [whole(*f) for f in faces],
    )(residual, edge_diag)


def plane(values, row_count):
    return jnp.concatenate([values, jnp.zeros((row_count - values.shape[0], LANES), F32)], axis=0)


def nodal_stage(part, node_shift, coarse_shift, got_z, got_x, got_y, low_z, z_count):
    nz, nx, ny = part.shape
    cz, cx, cy = nz // 2, nx // 2, ny // 2
    rows = cx + 8
    sends = 1 if z_count == 2 else 2

    def body(part, shift, coarse, gz, gx, gy, low_z, fg, rhs, xb, yb, w, *rest):
        out, (pair, s_, xl_, yl_, zl_, zh_) = rest[:sends], rest[sends:]
        lane = lane_ids(nx)
        row = row_ids(nx)
        lane_c = lane_ids(rows)
        row_c = row_ids(rows)
        below_z = from_below("gz", gz[0])
        below_y = from_below("gy", gy[...])
        fine = lax.broadcasted_iota(jnp.int32, (ny, 2 * LANES), 0)
        coarse_lane = lax.broadcasted_iota(jnp.int32, (ny, 2 * LANES), 1)
        miss = jnp.where(
            coarse_lane < LANES, fine // 2 - coarse_lane, fine - 2 * (coarse_lane - LANES)
        )
        gather = jnp.where(miss == 0, 1.0, 0.0)
        for c in range(cz):
            both = []
            for z in (2 * c, 2 * c + 1):
                total = part[z]
                if z == 0:
                    total += below_z
                total += jnp.where(row == 0, from_below("gx", gx[nz + z : nz + z + 1, :]), 0.0)
                total += jnp.where(lane == 0, shift_lanes(below_y, -(2 * nz + z)), 0.0)
                guess = total / (6.0 + shift[z])
                fg[z] = guess
                both.append(guess)
            pair[c % 2] = both[0] + both[1]
            low = pair[c % 2, pl.ds(0, cx, 2), :]
            high = pair[c % 2, pl.ds(1, cx, 2), :]
            first = fg[2 * c, pl.ds(0, cx, 2), :] + fg[2 * c, pl.ds(1, cx, 2), :]
            stacked = jnp.concatenate([low + high, low, first], axis=0)
            sums = jnp.dot(stacked, gather, precision=HIGHEST, preferred_element_type=F32)
            s = sums[:cx, :LANES]
            z_low = sums[2 * cx :, :LANES]
            s_[c] = plane(s, rows)
            yl_[c] = plane(sums[:cx, LANES:], rows)
            xl_[c] = plane(sums[cx : 2 * cx, :LANES], rows)
            zl_[c] = plane(z_low, rows)
            zh_[c] = plane(s - z_low, rows)
            w[c] = jnp.zeros((rows, LANES), F32)
            w[c, :cx, :cy] = 1.0 / (6.0 + coarse[c])
        for c in range(cz):
            s, x_low, y_low = s_[c], xl_[c], yl_[c]
            x_high = s - x_low
            y_high = s - y_low
            total = 3.0 * s
            total += shift_rows(x_low, -1) + shift_rows(x_high, 1)
            total += shift_lanes(y_low, -1) + shift_lanes(y_high, 1)
            if c > 0:
                total += zh_[c - 1]
            if c < cz - 1:
                total += zl_[c + 1]
            rhs[c] = total
            xb[c] = jnp.where(row_c < cx // 2, x_low, x_high)
            yb[c] = jnp.where(lane_c < cy // 2, y_low, y_high)
        rhs[cz] = zh_[cz - 1]
        rhs[cz + 1] = jnp.zeros((rows, LANES), F32)
        rhs[cz + 2] = jnp.zeros((rows, LANES), F32)
        rhs[cz + 3] = zl_[0]

        def fill(ref, near, far, half, face):
            planes = [rhs[near], rhs[far], w[near], w[far], half]
            planes += [xb[near], xb[far], yb[near], yb[far]]
            for i, value in enumerate(planes):
                ref[i * rows : (i + 1) * rows, :] = value
            ref[9 * rows : 9 * rows + nx, :] = face

        def up(ref):
            fill(ref, cz - 1, cz - 2, zh_[cz - 1], fg[nz - 1])
            for k in range(3):
                at = 9 * rows + nx + k * nx
                ref[at : at + nx, :] = jnp.zeros((nx, LANES), F32)

        def down(ref):
            fill(ref, 0, 1, zl_[0], fg[0])
            for k in range(3):
                at = 9 * rows + nx + k * nx
                ref[at : at + nx, :] = low_z[k]

        write_sides("gz", out, up, down)

    coarse = (cz, rows, LANES)
    send = (9 * rows + 4 * nx, LANES)
    return call(
        body,
        [(nz, nx, ny), (cz + 4, rows, LANES), coarse, coarse, coarse] + [send] * sends,
        "nodal_stage",
        scratch=[(2, nx, ny), coarse, coarse, coarse, coarse, coarse],
        in_specs=vmem(7),
        out_specs=vmem(5 + sends),
    )(part, node_shift, coarse_shift, got_z, got_x, got_y, low_z)


def x_stage(got, rhs, xb, yb, w, fg, low_x, z_count, x_count):
    planes, rows, _ = rhs.shape
    cz, cx = planes - 4, rows - 8
    nz, nx, _ = fg.shape
    sends = 1 if x_count == 2 else 2
    gots = len(got)

    def body(*refs):
        got = refs[:gots]
        rhs, xb, yb, w, fg, low_x, rhs2, yb2, w2 = refs[gots : gots + 9]
        out, (xb2,) = refs[gots + 9 : gots + 9 + sends], refs[gots + 9 + sends :]

        def take(pick, i):
            at = slice(i * rows, (i + 1) * rows)
            values = [ref[at, :] for ref in got]
            return pick("gz", z_count, values[0], values[1] if gots > 1 else None)

        for c in range(1, cz - 1):
            rhs2[c] = rhs[c]
        rhs2[0] = rhs[0] + take(low_of, 4)
        rhs2[cz - 1] = rhs[cz - 1] + take(high_of, 4)
        rhs2[cz] = rhs[cz] + take(high_of, 0)
        rhs2[cz + 1] = take(high_of, 1)
        rhs2[cz + 2] = take(low_of, 1)
        rhs2[cz + 3] = rhs[cz + 3] + take(low_of, 0)
        for here, there, i in ((w, w2, 2), (xb, xb2, 5), (yb, yb2, 7)):
            for c in range(cz):
                there[c] = here[c]
            there[cz] = take(high_of, i)
            there[cz + 1] = take(high_of, i + 1)
            there[cz + 2] = take(low_of, i + 1)
            there[cz + 3] = take(low_of, i)

        def fill(ref, near, far, fine):
            pieces = [rhs2[:, near, :], rhs2[:, far, :], w2[:, near, :], w2[:, far, :]]
            pieces += [xb2[:, near, :], yb2[:, near, :], yb2[:, far, :]]
            for i, value in enumerate(pieces):
                ref[i * 16 : i * 16 + planes, :] = value
                if planes < 16:
                    ref[i * 16 + planes : i * 16 + 16, :] = jnp.zeros((16 - planes, LANES), F32)
            ref[112 : 112 + nz, :] = fg[:, fine, :]

        def up(ref):
            fill(ref, cx - 1, cx - 2, nx - 1)
            ref[112 + nz : 112 + 4 * nz, :] = jnp.zeros((3 * nz, LANES), F32)

        def down(ref):
            fill(ref, 0, 1, 0)
            ref[112 + nz : 112 + 4 * nz, :] = low_x[...]

        write_sides("gx", out, up, down)

    whole = (planes, rows, LANES)
    return call(
        body,
        [whole, whole, whole] + [(112 + 4 * nz, LANES)] * sends,
        "x_stage",
        scratch=[whole],
        in_specs=vmem(gots + 6),
        out_specs=vmem(3 + sends),
    )(*got, rhs, xb, yb, w, fg, low_x)


def y_stage(got, rhs, yb, w, fg, low_y, x_count, y_count):
    planes, rows, _ = rhs.shape
    cx = rows - 8
    nz, nx, ny = fg.shape
    cy = ny // 2
    sends = 1 if y_count == 2 else 2
    gots = len(got)

    def body(*refs):
        got = refs[:gots]
        rhs, yb, w, fg, low_y, rhs3, w3 = refs[gots : gots + 7]
        out, (yb3, add) = refs[gots + 7 : gots + 7 + sends], refs[gots + 7 + sends :]

        def take(pick, i):
            at = slice(i * 16, i * 16 + planes)
            values = [ref[at, :] for ref in got]
            return pick("gx", x_count, values[0], values[1] if gots > 1 else None)

        add[...] = jnp.zeros_like(add)
        add[:, cx, :] = take(high_of, 0)
        add[:, cx + 1, :] = take(high_of, 1)
        add[:, rows - 1, :] = take(low_of, 0)
        add[:, rows - 2, :] = take(low_of, 1)
        add[:, cx - 1, :] = take(high_of, 4)
        add[:, 0, :] = take(low_of, 4)
        for c in range(planes):
            rhs3[c] = rhs[c] + add[c]
            w3[c] = w[c]
            yb3[c] = yb[c]
        for there, i in ((w3, 2), (yb3, 5)):
            there[:, cx, :] = take(high_of, i)
            there[:, cx + 1, :] = take(high_of, i + 1)
            there[:, rows - 1, :] = take(low_of, i)
            there[:, rows - 2, :] = take(low_of, i + 1)

        lane_c = lane_ids(rows)
        lane = lane_ids(nx)

        def fill(ref, near, far, fine, tail):
            acc = jnp.zeros((rows, LANES), F32)
            jobs = ((rhs3, near), (rhs3, far), (w3, near), (w3, far), (yb3, near))
            for i, (field, at) in enumerate(jobs):
                for z in range(planes):
                    spot = i * planes + z
                    acc = jnp.where(lane_c == spot, shift_lanes(field[z], spot - at), acc)
            acc = plane(acc, nx)
            base = 5 * planes
            for z in range(nz):
                acc = jnp.where(lane == base + z, shift_lanes(fg[z], base + z - fine), acc)
            if tail is not None:
                at = base + nz
                moved = shift_lanes(tail, at)
                acc = jnp.where((lane >= at) & (lane < at + 3 * nz), moved, acc)
            ref[...] = acc

        def up(ref):
            fill(ref, cy - 1, cy - 2, ny - 1, None)

        def down(ref):
            fill(ref, 0, 1, 0, low_y[...])

        write_sides("gy", out, up, down)

    whole = (planes, rows, LANES)
    return call(
        body,
        [whole, whole] + [(nx, LANES)] * sends,
        "y_stage",
        scratch=[whole, whole],
        in_specs=vmem(gots + 5),
        out_specs=vmem(2 + sends),
    )(*got, rhs, yb, w, fg, low_y)


def coarse_stage(got, rhs, w, y_count, devices):
    planes, rows, _ = rhs.shape
    cz, cx = planes - 4, rows - 8
    cy = LANES // 2
    gots = len(got)

    def body(*refs):
        got = refs[:gots]
        rhs, w, v1, v2, sums, tot, inv_, image_ = refs[gots:]
        values = [ref[:rows, :] for ref in got]
        second = values[1] if gots > 1 else None
        low = low_of("gy", y_count, values[0], second)
        high = high_of("gy", y_count, values[0], second)
        lane = lane_ids(rows)
        spots_r = ((cy, high, 0), (cy + 1, high, 1), (LANES - 1, low, 0), (LANES - 2, low, 1))
        spots_r += ((cy - 1, high, 4), (0, low, 4))
        for z in range(planes):
            right = rhs[z]
            for at, source, i in spots_r:
                moved = shift_lanes(source, at - (i * planes + z))
                right += jnp.where(lane == at, moved, 0.0)
            inv = w[z]
            for at, source, i in spots_r[:4]:
                moved = shift_lanes(source, at - ((i + 2) * planes + z))
                inv = jnp.where(lane == at, moved, inv)
            inv_[z] = inv
            tot[z] = right
            v1[z] = right * inv

        def near(field, z):
            here = field[z]
            total = field[(z + 1) % planes] + field[(z - 1) % planes]
            total += shift_rows(here, 1) + shift_rows(here, -1)
            return total + shift_lanes(here, 1) + shift_lanes(here, -1)

        v2[cz + 1] = jnp.zeros((rows, LANES), F32)
        v2[cz + 2] = jnp.zeros((rows, LANES), F32)
        for z in list(range(cz + 1)) + [planes - 1]:
            image = tot[z] - near(v1, z)
            if z < cz:
                image_[z] = image
            v2[z] = image * inv_[z]
        parts = [jnp.zeros((cx, LANES), F32)] * 5
        for z in range(cz):
            first, second_, right, image = v1[z], v2[z], tot[z], image_[z]
            third = image - near(v2, z)
            terms = (first * right, second_ * right, first * image, second_ * image, second_ * third)
            parts = [a + b[:cx, :] for a, b in zip(parts, terms)]
        keep = lane_ids(1) < cy
        lines = [jnp.where(keep, jnp.sum(a, axis=0, keepdims=True), 0.0) for a in parts]
        tile = jnp.concatenate(lines + [jnp.zeros((3, LANES), F32)], axis=0)
        column = jnp.sum(tile, axis=1, keepdims=True)
        spread = jnp.where(lane_ids(8) == row_ids(8), column, 0.0)
        line = jnp.sum(spread, axis=0, keepdims=True)
        sums[...] = jnp.broadcast_to(line[None], (devices, 1, LANES))

    whole = (planes, rows, LANES)
    return call(
        body,
        [whole, whole, (devices, 1, LANES)],
        "coarse_stage",
        scratch=[whole, whole, whole],
        in_specs=vmem(gots + 2),
        out_specs=vmem(3),
    )(*got, rhs, w)


def final_stage(sums, v1, v2, fg, node_shift, got_z, got_x, got_y, counts):
    planes, rows, _ = v1.shape
    cz, cx = planes - 4, rows - 8
    nz, nx, ny = fg.shape
    n_z, n_x, n_y = len(got_z), len(got_x), len(got_y)

    def body(*refs):
        sums, v1, v2, fg, shift = refs[:5]
        gz = refs[5 : 5 + n_z]
        gx = refs[5 + n_z : 5 + n_z + n_x]
        gy = refs[5 + n_z + n_x : 5 + n_z + n_x + n_y]
        fn, down_z, down_x, down_y, dup, inter = refs[5 + n_z + n_x + n_y :]

        def both(refs, axis, size, at):
            values = [ref[at, :] for ref in refs]
            second = values[1] if len(values) > 1 else None
            return low_of(axis, size, values[0], second), high_of(axis, size, values[0], second)

        total = jnp.sum(sums[...], axis=0)
        lane1 = lane_ids(1)
        gone, gtwo, hone, hmix, htwo = [
            jnp.sum(jnp.where(lane1 == i, total, 0.0), axis=1, keepdims=True) for i in range(5)
        ]
        two = (gtwo - hmix * gone / hone) / (htwo - hmix * hmix / hone)
        one = (gone - hmix * two) / hone
        source = lax.broadcasted_iota(jnp.int32, (LANES, 2 * LANES), 0)
        target = lax.broadcasted_iota(jnp.int32, (LANES, 2 * LANES), 1)
        fine = target - LANES
        side = jnp.where(fine % 2 == 1, fine // 2 + 1, (fine // 2 + LANES - 1) % LANES)
        spread = jnp.where(jnp.where(target < LANES, target // 2, side) == source, 1.0, 0.0)
        for z in list(range(cz + 1)) + [planes - 1]:
            sol = one * v1[z] + two * v2[z]
            dup[z] = jnp.dot(sol, spread, precision=HIGHEST, preferred_element_type=F32)

        z_face = slice(9 * rows, 9 * rows + nx)
        z_low, z_high = both(gz, "gz", counts[0], z_face)
        x_low, x_high = both(gx, "gx", counts[1], slice(112, 112 + nz))
        y_low, y_high = both(gy, "gy", counts[2], slice(0, nx))
        lane = lane_ids(nx)
        row = row_ids(nx)
        base = 5 * planes
        acc = jnp.zeros((nx, LANES), F32)
        for z in range(nz):
            c, odd = z // 2, z % 2
            here = dup[c, :, :LANES]
            same = 3.0 * here + dup[c, :, LANES:]
            same += dup[(c + 1 if odd else c - 1) % planes, :, :LANES]
            slot = z % 2
            inter[slot, pl.ds(0, cx, 2), :] = (same + shift_rows(here, 1))[:cx, :]
            inter[slot, pl.ds(1, cx, 2), :] = (same + shift_rows(here, -1))[:cx, :]
            guess = fg[z]
            around = inter[slot]
            around += fg[z - 1] if z > 0 else z_low
            around += fg[z + 1] if z < nz - 1 else z_high
            around += jnp.where(row == 0, x_low[z : z + 1, :], shift_rows(guess, 1))
            around += jnp.where(row == nx - 1, x_high[z : z + 1, :], shift_rows(guess, -1))
            left = shift_lanes(y_low, -(base + z))
            right = shift_lanes(y_high, -(base + z) - 1)
            around += jnp.where(lane == 0, left, shift_lanes(guess, 1))
            around += jnp.where(lane == LANES - 1, right, shift_lanes(guess, -1))
            value = guess + around / (6.0 + shift[z])
            fn[z] = value
            if z == 0:
                down_z[...] = value
            down_x[z : z + 1, :] = value[:1, :]
            acc = jnp.where(lane == z, shift_lanes(value, z), acc)
        down_y[...] = acc

    return call(
        body,
        [(nz, nx, ny), (nx, ny), (nz, ny), (nx, LANES)],
        "final_stage",
        scratch=[(planes, rows, 2 * LANES), (2, nx, LANES)],
        in_specs=vmem(5 + n_z + n_x + n_y),
        out_specs=vmem(4),
    )(sums, v1, v2, fg, node_shift, *got_z, *got_x, *got_y)


def output_stage(residual, edge_diag, fn, above, below, got_z, got_x, got_y, planes, counts):
    _, nz, nx, ny = residual.shape
    n_z, n_x, n_y = len(got_z), len(got_x), len(got_y)
    rows = nx // 2 + 8

    def body(*refs):
        res, diag, fn, fz, fx, fy, lz, lx, ly = refs[:9]
        gz = refs[9 : 9 + n_z]
        gx = refs[9 + n_z : 9 + n_z + n_x]
        gy = refs[9 + n_z + n_x : 9 + n_z + n_x + n_y]
        out, s = refs[9 + n_z + n_x + n_y :]
        k = pl.program_id(0)
        lane = lane_ids(nx)
        row = row_ids(nx)

        def above_of(refs, axis, size, at):
            values = [ref[at, :] for ref in refs]
            return high_of(axis, size, values[0], values[1] if len(values) > 1 else None)

        for z in range(nz):
            s[z] = res[0, z] / diag[0, z]
        z_low = from_below("gz", lz[k])
        z_high = above_of(gz, "gz", counts[0], pl.ds(9 * rows + nx + k * nx, nx))
        x_low = from_below("gx", lx[pl.ds(k * nz, nz), :])
        x_high = above_of(gx, "gx", counts[1], pl.ds(112 + nz + k * nz, nz))
        y_low = pltpu.roll(from_below("gy", ly[...]), (LANES - k * nz) % LANES, 1)
        y_high = above_of(gy, "gy", counts[2], pl.ds(0, nx))
        y_high = pltpu.roll(y_high, (2 * LANES - 5 * planes - nz - k * nz) % LANES, 1)
        for z in range(nz):
            here = s[z]
            around = s[z - 1] if z > 0 else z_low
            around += s[z + 1] if z < nz - 1 else z_high
            around += jnp.where(row == 0, x_low[z : z + 1, :], shift_rows(here, 1))
            around += jnp.where(row == nx - 1, x_high[z : z + 1, :], shift_rows(here, -1))
            left = shift_lanes(y_low, -z)
            right = shift_lanes(y_high, -z - 1)
            around += jnp.where(lane == 0, left, shift_lanes(here, 1))
            around += jnp.where(lane == LANES - 1, right, shift_lanes(here, -1))
            out[0, z] = here + around / diag[0, z] - fn[z]

        @pl.when(k == 0)
        def _():
            for z in range(nz - 1):
                out[0, z] += fn[z + 1]
            out[0, nz - 1] += from_above("gz", counts[0], fz[...])

        @pl.when(k == 1)
        def _():
            face = from_above("gx", counts[1], fx[...])
            for z in range(nz):
                out[0, z] += jnp.where(row == nx - 1, face[z : z + 1, :], shift_rows(fn[z], -1))

        @pl.when(k == 2)
        def _():
            face = from_above("gy", counts[2], fy[...])
            for z in range(nz):
                moved = shift_lanes(face, -z - 1)
                out[0, z] += jnp.where(lane == LANES - 1, moved, shift_lanes(fn[z], -1))

    spec = pl.BlockSpec((1, nz, nx, ny), lambda k: (k, 0, 0, 0))
    args = (fn, *above, *below, *got_z, *got_x, *got_y)
    whole = [pl.BlockSpec(a.shape, lambda k, n=a.ndim: (0,) * n) for a in args]
    return call(
        body,
        [residual.shape],
        "output_stage",
        scratch=[(nz, nx, ny)],
        far=(0, 1),
        far_out=True,
        grid=(3,),
        in_specs=[spec, spec] + whole,
        out_specs=[spec],
    )(residual, edge_diag, *args)[0]


def local(residual, edge_diag, node_shift, coarse_shift):
    axes = ("gz", "gx", "gy")
    counts = tuple(lax.axis_size(a) for a in axes)
    devices = counts[0] * counts[1] * counts[2]
    part, up_z, up_x, up_y, low_z, low_x, low_y = edge_stage(residual, edge_diag)
    below = (ring(up_z, "gz", 1), ring(up_x, "gx", 1), ring(up_y, "gy", 1))
    fg, rhs, xb, yb, w, *send = nodal_stage(part, node_shift, coarse_shift, *below, low_z, counts[0])
    got_z = swap(send, "gz")
    rhs, yb, w, *send = x_stage(got_z, rhs, xb, yb, w, fg, low_x, counts[0], counts[1])
    got_x = swap(send, "gx")
    planes = rhs.shape[0]
    rhs, w, *send = y_stage(got_x, rhs, yb, w, fg, low_y, counts[1], counts[2])
    got_y = swap(send, "gy")
    v1, v2, sums = coarse_stage(got_y, rhs, w, counts[2], devices)
    sums = lax.all_to_all(sums, ("gx", "gy", "gz"), 0, 0)
    fn, down_z, down_x, down_y = final_stage(
        sums, v1, v2, fg, node_shift, got_z, got_x, got_y, counts
    )
    above = (ring(down_z, "gz", -1), ring(down_x, "gx", -1), ring(down_y, "gy", -1))
    return output_stage(
        residual, edge_diag, fn, above, below, got_z, got_x, got_y, planes, counts
    )


def solution(mesh):
    placed = (
        P(None, "gz", "gx", "gy"),
        P(None, "gz", "gx", "gy"),
        P("gz", "gx", "gy"),
        P("gz", "gx", "gy"),
    )
    return jax.shard_map(
        local, mesh=mesh, in_specs=placed, out_specs=P(None, "gz", "gx", "gy"), check_vma=False
    )
```

```python
import jax
import jax.numpy as jnp
from jax import lax
from jax.experimental import pallas as pl
from jax.experimental.pallas import tpu as pltpu
from jax.sharding import PartitionSpec as P

F32 = jnp.float32
HIGHEST = lax.Precision.HIGHEST
LANES = 128


def lane_ids(rows):
    return lax.broadcasted_iota(jnp.int32, (rows, LANES), 1)


def row_ids(rows):
    return lax.broadcasted_iota(jnp.int32, (rows, LANES), 0)


def shift_lanes(value, amount):
    return pltpu.roll(value, amount % LANES, 1)


def shift_rows(value, amount):
    return pltpu.roll(value, amount % value.shape[0], 0)


def low_of(axis, size, first, second):
    place = lax.axis_index(axis)
    odd = place % 2 == 1
    zero = jnp.zeros_like(first)
    if second is None:
        return jnp.where(odd, first, zero)
    return jnp.where(odd, first, jnp.where(place > 0, second, zero))


def high_of(axis, size, first, second):
    place = lax.axis_index(axis)
    even = place % 2 == 0
    zero = jnp.zeros_like(first)
    if second is None:
        return jnp.where(even, first, zero)
    return jnp.where(even, first, jnp.where(place < size - 1, second, zero))


def from_below(axis, value):
    return jnp.where(lax.axis_index(axis) > 0, value, jnp.zeros_like(value))


def from_above(axis, size, value):
    return jnp.where(lax.axis_index(axis) < size - 1, value, jnp.zeros_like(value))


def ring(value, axis, step):
    size = lax.axis_size(axis)
    return lax.ppermute(value, axis, [(i, (i + step) % size) for i in range(size)])


def swap(values, axis):
    size = lax.axis_size(axis)
    even = [(i, i ^ 1) for i in range(size)]
    out = [lax.ppermute(values[0], axis, even)]
    if len(values) > 1:
        odd = [(i, (i + 1) % size if i % 2 else (i - 1) % size) for i in range(size)]
        out.append(lax.ppermute(values[1], axis, odd))
    return out


def write_sides(axis, refs, up, down):
    even = lax.axis_index(axis) % 2 == 0

    @pl.when(even)
    def _():
        up(refs[0])
        if len(refs) > 1:
            down(refs[1])

    @pl.when(jnp.logical_not(even))
    def _():
        down(refs[0])
        if len(refs) > 1:
            up(refs[1])


def call(body, outs, name, scratch=(), far=(), far_out=False, **kwargs):
    kind = jax.ShapeDtypeStruct if far_out else pltpu.VMEM
    run = pl.pallas_call(
        body,
        out_shape=[kind(shape, F32) for shape in outs],
        scratch_shapes=[pltpu.VMEM(shape, F32) for shape in scratch],
        name=name,
        compiler_params=pltpu.CompilerParams(vmem_limit_bytes=12 * 2**20),
        **kwargs,
    )

    def apply(*args):
        near = [
            a if i in far else pltpu.with_memory_space_constraint(a, pltpu.VMEM)
            for i, a in enumerate(args)
        ]
        return run(*near)

    return apply


def vmem(count):
    return [pl.BlockSpec(memory_space=pltpu.VMEM)] * count


def edge_stage(residual, edge_diag):
    _, nz, nx, ny = residual.shape
    step = 4
    steps = nz // step

    def body(res, diag, part, up_z, up_x, up_y, low_z, low_x, low_y, last):
        block = pl.program_id(0)
        lane = lane_ids(nx)
        row = row_ids(nx)

        @pl.when(block == 0)
        def _():
            last[...] = jnp.zeros_like(last)
            up_y[...] = jnp.zeros_like(up_y)
            low_y[...] = jnp.zeros_like(low_y)

        before = last[...]
        high = up_y[...]
        low = low_y[...]
        for j in range(step):
            z = block * step + j
            s = [res[k, j] / diag[k, j] for k in range(3)]
            total = before - s[0]
            total += jnp.where(row == 0, 0.0, shift_rows(s[1], 1)) - s[1]
            total += jnp.where(lane == 0, 0.0, shift_lanes(s[2], 1)) - s[2]
            part[j] = total
            before = s[0]
            for k in range(3):
                up_x[pl.ds(k * nz + z, 1), :] = s[k][nx - 1 :, :]
                low_x[pl.ds(k * nz + z, 1), :] = s[k][:1, :]
                spot = k * nz + z
                high = jnp.where(lane == spot, pltpu.roll(s[k], spot + 1, 1), high)
                low = jnp.where(lane == spot, pltpu.roll(s[k], spot, 1), low)
            if j == 0:

                @pl.when(block == 0)
                def _():
                    for k in range(3):
                        low_z[k] = s[k]

            if j == step - 1:

                @pl.when(block == steps - 1)
                def _():
                    for k in range(3):
                        up_z[k] = s[k]

        last[...] = before
        up_y[...] = high
        low_y[...] = low

    whole = lambda *shape: pl.BlockSpec(shape, lambda i: (0,) * len(shape))
    spec = pl.BlockSpec((3, step, nx, ny), lambda i: (0, i, 0, 0))
    faces = [(3, nx, ny), (3 * nz, ny), (nx, LANES)] * 2
    return call(
        body,
        [(nz, nx, ny)] + faces,
        "edge_stage",
        scratch=[(nx, ny)],
        far=(0, 1),
        grid=(steps,),
        in_specs=[spec, spec],
        out_specs=[pl.BlockSpec((step, nx, ny), lambda i: (i, 0, 0))] + [whole(*f) for f in faces],
    )(residual, edge_diag)


def plane(values, row_count):
    return jnp.concatenate([values, jnp.zeros((row_count - values.shape[0], LANES), F32)], axis=0)


def nodal_stage(part, node_shift, coarse_shift, got_z, got_x, got_y, low_z, z_count):
    nz, nx, ny = part.shape
    cz, cx, cy = nz // 2, nx // 2, ny // 2
    rows = cx + 8
    sends = 1 if z_count == 2 else 2

    def body(part, shift, coarse, gz, gx, gy, low_z, fg, rhs, xb, yb, w, *rest):
        out, (pair, s_, xl_, yl_, zl_, zh_) = rest[:sends], rest[sends:]
        lane = lane_ids(nx)
        row = row_ids(nx)
        lane_c = lane_ids(rows)
        row_c = row_ids(rows)
        below_z = from_below("gz", gz[0])
        below_y = from_below("gy", gy[...])
        fine = lax.broadcasted_iota(jnp.int32, (ny, 2 * LANES), 0)
        coarse_lane = lax.broadcasted_iota(jnp.int32, (ny, 2 * LANES), 1)
        miss = jnp.where(
            coarse_lane < LANES, fine // 2 - coarse_lane, fine - 2 * (coarse_lane - LANES)
        )
        gather = jnp.where(miss == 0, 1.0, 0.0)
        for c in range(cz):
            both = []
            for z in (2 * c, 2 * c + 1):
                total = part[z]
                if z == 0:
                    total += below_z
                total += jnp.where(row == 0, from_below("gx", gx[nz + z : nz + z + 1, :]), 0.0)
                total += jnp.where(lane == 0, shift_lanes(below_y, -(2 * nz + z)), 0.0)
                guess = total / (6.0 + shift[z])
                fg[z] = guess
                both.append(guess)
            pair[c % 2] = both[0] + both[1]
            low = pair[c % 2, pl.ds(0, cx, 2), :]
            high = pair[c % 2, pl.ds(1, cx, 2), :]
            first = fg[2 * c, pl.ds(0, cx, 2), :] + fg[2 * c, pl.ds(1, cx, 2), :]
            stacked = jnp.concatenate([low + high, low, first], axis=0)
            sums = jnp.dot(stacked, gather, precision=HIGHEST, preferred_element_type=F32)
            s = sums[:cx, :LANES]
            z_low = sums[2 * cx :, :LANES]
            s_[c] = plane(s, rows)
            yl_[c] = plane(sums[:cx, LANES:], rows)
            xl_[c] = plane(sums[cx : 2 * cx, :LANES], rows)
            zl_[c] = plane(z_low, rows)
            zh_[c] = plane(s - z_low, rows)
            w[c] = jnp.zeros((rows, LANES), F32)
            w[c, :cx, :cy] = 1.0 / (6.0 + coarse[c])
        for c in range(cz):
            s, x_low, y_low = s_[c], xl_[c], yl_[c]
            x_high = s - x_low
            y_high = s - y_low
            total = 3.0 * s
            total += shift_rows(x_low, -1) + shift_rows(x_high, 1)
            total += shift_lanes(y_low, -1) + shift_lanes(y_high, 1)
            if c > 0:
                total += zh_[c - 1]
            if c < cz - 1:
                total += zl_[c + 1]
            rhs[c] = total
            xb[c] = jnp.where(row_c < cx // 2, x_low, x_high)
            yb[c] = jnp.where(lane_c < cy // 2, y_low, y_high)
        rhs[cz] = zh_[cz - 1]
        rhs[cz + 1] = jnp.zeros((rows, LANES), F32)
        rhs[cz + 2] = jnp.zeros((rows, LANES), F32)
        rhs[cz + 3] = zl_[0]

        def fill(ref, near, far, half, face):
            planes = [rhs[near], rhs[far], w[near], w[far], half]
            planes += [xb[near], xb[far], yb[near], yb[far]]
            for i, value in enumerate(planes):
                ref[i * rows : (i + 1) * rows, :] = value
            ref[9 * rows : 9 * rows + nx, :] = face

        def up(ref):
            fill(ref, cz - 1, cz - 2, zh_[cz - 1], fg[nz - 1])
            for k in range(3):
                at = 9 * rows + nx + k * nx
                ref[at : at + nx, :] = jnp.zeros((nx, LANES), F32)

        def down(ref):
            fill(ref, 0, 1, zl_[0], fg[0])
            for k in range(3):
                at = 9 * rows + nx + k * nx
                ref[at : at + nx, :] = low_z[k]

        write_sides("gz", out, up, down)

    coarse = (cz, rows, LANES)
    send = (9 * rows + 4 * nx, LANES)
    return call(
        body,
        [(nz, nx, ny), (cz + 4, rows, LANES), coarse, coarse, coarse] + [send] * sends,
        "nodal_stage",
        scratch=[(2, nx, ny), coarse, coarse, coarse, coarse, coarse],
        in_specs=vmem(7),
        out_specs=vmem(5 + sends),
    )(part, node_shift, coarse_shift, got_z, got_x, got_y, low_z)


def x_stage(got, rhs, xb, yb, w, fg, low_x, z_count, x_count):
    planes, rows, _ = rhs.shape
    cz, cx = planes - 4, rows - 8
    nz, nx, _ = fg.shape
    sends = 1 if x_count == 2 else 2
    gots = len(got)

    def body(*refs):
        got = refs[:gots]
        rhs, xb, yb, w, fg, low_x, rhs2, yb2, w2 = refs[gots : gots + 9]
        out, (xb2,) = refs[gots + 9 : gots + 9 + sends], refs[gots + 9 + sends :]

        def take(pick, i):
            at = slice(i * rows, (i + 1) * rows)
            values = [ref[at, :] for ref in got]
            return pick("gz", z_count, values[0], values[1] if gots > 1 else None)

        for c in range(1, cz - 1):
            rhs2[c] = rhs[c]
        rhs2[0] = rhs[0] + take(low_of, 4)
        rhs2[cz - 1] = rhs[cz - 1] + take(high_of, 4)
        rhs2[cz] = rhs[cz] + take(high_of, 0)
        rhs2[cz + 1] = take(high_of, 1)
        rhs2[cz + 2] = take(low_of, 1)
        rhs2[cz + 3] = rhs[cz + 3] + take(low_of, 0)
        for here, there, i in ((w, w2, 2), (xb, xb2, 5), (yb, yb2, 7)):
            for c in range(cz):
                there[c] = here[c]
            there[cz] = take(high_of, i)
            there[cz + 1] = take(high_of, i + 1)
            there[cz + 2] = take(low_of, i + 1)
            there[cz + 3] = take(low_of, i)

        def fill(ref, near, far, fine):
            pieces = [rhs2[:, near, :], rhs2[:, far, :], w2[:, near, :], w2[:, far, :]]
            pieces += [xb2[:, near, :], yb2[:, near, :], yb2[:, far, :]]
            for i, value in enumerate(pieces):
                ref[i * 16 : i * 16 + planes, :] = value
                if planes < 16:
                    ref[i * 16 + planes : i * 16 + 16, :] = jnp.zeros((16 - planes, LANES), F32)
            ref[112 : 112 + nz, :] = fg[:, fine, :]

        def up(ref):
            fill(ref, cx - 1, cx - 2, nx - 1)
            ref[112 + nz : 112 + 4 * nz, :] = jnp.zeros((3 * nz, LANES), F32)

        def down(ref):
            fill(ref, 0, 1, 0)
            ref[112 + nz : 112 + 4 * nz, :] = low_x[...]

        write_sides("gx", out, up, down)

    whole = (planes, rows, LANES)
    return call(
        body,
        [whole, whole, whole] + [(112 + 4 * nz, LANES)] * sends,
        "x_stage",
        scratch=[whole],
        in_specs=vmem(gots + 6),
        out_specs=vmem(3 + sends),
    )(*got, rhs, xb, yb, w, fg, low_x)


def y_stage(got, rhs, yb, w, fg, low_y, x_count, y_count):
    planes, rows, _ = rhs.shape
    cx = rows - 8
    nz, nx, ny = fg.shape
    cy = ny // 2
    sends = 1 if y_count == 2 else 2
    gots = len(got)

    def body(*refs):
        got = refs[:gots]
        rhs, yb, w, fg, low_y, rhs3, w3 = refs[gots : gots + 7]
        out, (yb3, add) = refs[gots + 7 : gots + 7 + sends], refs[gots + 7 + sends :]

        def take(pick, i):
            at = slice(i * 16, i * 16 + planes)
            values = [ref[at, :] for ref in got]
            return pick("gx", x_count, values[0], values[1] if gots > 1 else None)

        add[...] = jnp.zeros_like(add)
        add[:, cx, :] = take(high_of, 0)
        add[:, cx + 1, :] = take(high_of, 1)
        add[:, rows - 1, :] = take(low_of, 0)
        add[:, rows - 2, :] = take(low_of, 1)
        add[:, cx - 1, :] = take(high_of, 4)
        add[:, 0, :] = take(low_of, 4)
        for c in range(planes):
            rhs3[c] = rhs[c] + add[c]
            w3[c] = w[c]
            yb3[c] = yb[c]
        for there, i in ((w3, 2), (yb3, 5)):
            there[:, cx, :] = take(high_of, i)
            there[:, cx + 1, :] = take(high_of, i + 1)
            there[:, rows - 1, :] = take(low_of, i)
            there[:, rows - 2, :] = take(low_of, i + 1)

        lane_c = lane_ids(rows)
        lane = lane_ids(nx)

        def fill(ref, near, far, fine, tail):
            acc = jnp.zeros((rows, LANES), F32)
            jobs = ((rhs3, near), (rhs3, far), (w3, near), (w3, far), (yb3, near))
            for i, (field, at) in enumerate(jobs):
                for z in range(planes):
                    spot = i * planes + z
                    acc = jnp.where(lane_c == spot, shift_lanes(field[z], spot - at), acc)
            acc = plane(acc, nx)
            base = 5 * planes
            for z in range(nz):
                acc = jnp.where(lane == base + z, shift_lanes(fg[z], base + z - fine), acc)
            if tail is not None:
                at = base + nz
                moved = shift_lanes(tail, at)
                acc = jnp.where((lane >= at) & (lane < at + 3 * nz), moved, acc)
            ref[...] = acc

        def up(ref):
            fill(ref, cy - 1, cy - 2, ny - 1, None)

        def down(ref):
            fill(ref, 0, 1, 0, low_y[...])

        write_sides("gy", out, up, down)

    whole = (planes, rows, LANES)
    return call(
        body,
        [whole, whole] + [(nx, LANES)] * sends,
        "y_stage",
        scratch=[whole, whole],
        in_specs=vmem(gots + 5),
        out_specs=vmem(2 + sends),
    )(*got, rhs, yb, w, fg, low_y)


def coarse_stage(got, rhs, w, y_count, devices):
    planes, rows, _ = rhs.shape
    cz, cx = planes - 4, rows - 8
    cy = LANES // 2
    gots = len(got)

    def body(*refs):
        got = refs[:gots]
        rhs, w, v1, v2, sums, tot, inv_, image_ = refs[gots:]
        values = [ref[:rows, :] for ref in got]
        second = values[1] if gots > 1 else None
        low = low_of("gy", y_count, values[0], second)
        high = high_of("gy", y_count, values[0], second)
        lane = lane_ids(rows)
        spots_r = ((cy, high, 0), (cy + 1, high, 1), (LANES - 1, low, 0), (LANES - 2, low, 1))
        spots_r += ((cy - 1, high, 4), (0, low, 4))
        for z in range(planes):
            right = rhs[z]
            for at, source, i in spots_r:
                moved = shift_lanes(source, at - (i * planes + z))
                right += jnp.where(lane == at, moved, 0.0)
            inv = w[z]
            for at, source, i in spots_r[:4]:
                moved = shift_lanes(source, at - ((i + 2) * planes + z))
                inv = jnp.where(lane == at, moved, inv)
            inv_[z] = inv
            tot[z] = right
            v1[z] = right * inv

        def near(field, z):
            here = field[z]
            total = field[(z + 1) % planes] + field[(z - 1) % planes]
            total += shift_rows(here, 1) + shift_rows(here, -1)
            return total + shift_lanes(here, 1) + shift_lanes(here, -1)

        v2[cz + 1] = jnp.zeros((rows, LANES), F32)
        v2[cz + 2] = jnp.zeros((rows, LANES), F32)
        for z in list(range(cz + 1)) + [planes - 1]:
            image = tot[z] - near(v1, z)
            if z < cz:
                image_[z] = image
            v2[z] = image * inv_[z]
        parts = [jnp.zeros((cx, LANES), F32)] * 5
        for z in range(cz):
            first, second_, right, image = v1[z], v2[z], tot[z], image_[z]
            third = image - near(v2, z)
            terms = (first * right, second_ * right, first * image, second_ * image, second_ * third)
            parts = [a + b[:cx, :] for a, b in zip(parts, terms)]
        keep = lane_ids(1) < cy
        lines = [jnp.where(keep, jnp.sum(a, axis=0, keepdims=True), 0.0) for a in parts]
        tile = jnp.concatenate(lines + [jnp.zeros((3, LANES), F32)], axis=0)
        column = jnp.sum(tile, axis=1, keepdims=True)
        spread = jnp.where(lane_ids(8) == row_ids(8), column, 0.0)
        line = jnp.sum(spread, axis=0, keepdims=True)
        sums[...] = jnp.broadcast_to(line[None], (devices, 1, LANES))

    whole = (planes, rows, LANES)
    return call(
        body,
        [whole, whole, (devices, 1, LANES)],
        "coarse_stage",
        scratch=[whole, whole, whole],
        in_specs=vmem(gots + 2),
        out_specs=vmem(3),
    )(*got, rhs, w)


def final_stage(sums, v1, v2, fg, node_shift, got_z, got_x, got_y, counts):
    planes, rows, _ = v1.shape
    cz, cx = planes - 4, rows - 8
    nz, nx, ny = fg.shape
    n_z, n_x, n_y = len(got_z), len(got_x), len(got_y)

    def body(*refs):
        sums, v1, v2, fg, shift = refs[:5]
        gz = refs[5 : 5 + n_z]
        gx = refs[5 + n_z : 5 + n_z + n_x]
        gy = refs[5 + n_z + n_x : 5 + n_z + n_x + n_y]
        fn, down_z, down_x, down_y, dup, inter = refs[5 + n_z + n_x + n_y :]

        def both(refs, axis, size, at):
            values = [ref[at, :] for ref in refs]
            second = values[1] if len(values) > 1 else None
            return low_of(axis, size, values[0], second), high_of(axis, size, values[0], second)

        total = jnp.sum(sums[...], axis=0)
        lane1 = lane_ids(1)
        gone, gtwo, hone, hmix, htwo = [
            jnp.sum(jnp.where(lane1 == i, total, 0.0), axis=1, keepdims=True) for i in range(5)
        ]
        two = (gtwo - hmix * gone / hone) / (htwo - hmix * hmix / hone)
        one = (gone - hmix * two) / hone
        source = lax.broadcasted_iota(jnp.int32, (LANES, 2 * LANES), 0)
        target = lax.broadcasted_iota(jnp.int32, (LANES, 2 * LANES), 1)
        fine = target - LANES
        side = jnp.where(fine % 2 == 1, fine // 2 + 1, (fine // 2 + LANES - 1) % LANES)
        spread = jnp.where(jnp.where(target < LANES, target // 2, side) == source, 1.0, 0.0)
        for z in list(range(cz + 1)) + [planes - 1]:
            sol = one * v1[z] + two * v2[z]
            dup[z] = jnp.dot(sol, spread, precision=HIGHEST, preferred_element_type=F32)

        z_face = slice(9 * rows, 9 * rows + nx)
        z_low, z_high = both(gz, "gz", counts[0], z_face)
        x_low, x_high = both(gx, "gx", counts[1], slice(112, 112 + nz))
        y_low, y_high = both(gy, "gy", counts[2], slice(0, nx))
        lane = lane_ids(nx)
        row = row_ids(nx)
        base = 5 * planes
        acc = jnp.zeros((nx, LANES), F32)
        for z in range(nz):
            c, odd = z // 2, z % 2
            here = dup[c, :, :LANES]
            same = 3.0 * here + dup[c, :, LANES:]
            same += dup[(c + 1 if odd else c - 1) % planes, :, :LANES]
            slot = z % 2
            inter[slot, pl.ds(0, cx, 2), :] = (same + shift_rows(here, 1))[:cx, :]
            inter[slot, pl.ds(1, cx, 2), :] = (same + shift_rows(here, -1))[:cx, :]
            guess = fg[z]
            around = inter[slot]
            around += fg[z - 1] if z > 0 else z_low
            around += fg[z + 1] if z < nz - 1 else z_high
            around += jnp.where(row == 0, x_low[z : z + 1, :], shift_rows(guess, 1))
            around += jnp.where(row == nx - 1, x_high[z : z + 1, :], shift_rows(guess, -1))
            left = shift_lanes(y_low, -(base + z))
            right = shift_lanes(y_high, -(base + z) - 1)
            around += jnp.where(lane == 0, left, shift_lanes(guess, 1))
            around += jnp.where(lane == LANES - 1, right, shift_lanes(guess, -1))
            value = guess + around / (6.0 + shift[z])
            fn[z] = value
            if z == 0:
                down_z[...] = value
            down_x[z : z + 1, :] = value[:1, :]
            acc = jnp.where(lane == z, shift_lanes(value, z), acc)
        down_y[...] = acc

    return call(
        body,
        [(nz, nx, ny), (nx, ny), (nz, ny), (nx, LANES)],
        "final_stage",
        scratch=[(planes, rows, 2 * LANES), (2, nx, LANES)],
        in_specs=vmem(5 + n_z + n_x + n_y),
        out_specs=vmem(4),
    )(sums, v1, v2, fg, node_shift, *got_z, *got_x, *got_y)


def output_stage(residual, edge_diag, fn, above, below, got_z, got_x, got_y, planes, counts):
    _, nz, nx, ny = residual.shape
    n_z, n_x, n_y = len(got_z), len(got_x), len(got_y)
    rows = nx // 2 + 8

    def body(*refs):
        res, diag, fn, fz, fx, fy, lz, lx, ly = refs[:9]
        gz = refs[9 : 9 + n_z]
        gx = refs[9 + n_z : 9 + n_z + n_x]
        gy = refs[9 + n_z + n_x : 9 + n_z + n_x + n_y]
        out, s = refs[9 + n_z + n_x + n_y :]
        k = pl.program_id(0)
        lane = lane_ids(nx)
        row = row_ids(nx)

        def above_of(refs, axis, size, at):
            values = [ref[at, :] for ref in refs]
            return high_of(axis, size, values[0], values[1] if len(values) > 1 else None)

        for z in range(nz):
            s[z] = res[0, z] / diag[0, z]
        z_low = from_below("gz", lz[k])
        z_high = above_of(gz, "gz", counts[0], pl.ds(9 * rows + nx + k * nx, nx))
        x_low = from_below("gx", lx[pl.ds(k * nz, nz), :])
        x_high = above_of(gx, "gx", counts[1], pl.ds(112 + nz + k * nz, nz))
        y_low = pltpu.roll(from_below("gy", ly[...]), (LANES - k * nz) % LANES, 1)
        y_high = above_of(gy, "gy", counts[2], pl.ds(0, nx))
        y_high = pltpu.roll(y_high, (2 * LANES - 5 * planes - nz - k * nz) % LANES, 1)
        for z in range(nz):
            here = s[z]
            around = s[z - 1] if z > 0 else z_low
            around += s[z + 1] if z < nz - 1 else z_high
            around += jnp.where(row == 0, x_low[z : z + 1, :], shift_rows(here, 1))
            around += jnp.where(row == nx - 1, x_high[z : z + 1, :], shift_rows(here, -1))
            left = shift_lanes(y_low, -z)
            right = shift_lanes(y_high, -z - 1)
            around += jnp.where(lane == 0, left, shift_lanes(here, 1))
            around += jnp.where(lane == LANES - 1, right, shift_lanes(here, -1))
            out[0, z] = here + around / diag[0, z] - fn[z]

        @pl.when(k == 0)
        def _():
            for z in range(nz - 1):
                out[0, z] += fn[z + 1]
            out[0, nz - 1] += from_above("gz", counts[0], fz[...])

        @pl.when(k == 1)
        def _():
            face = from_above("gx", counts[1], fx[...])
            for z in range(nz):
                out[0, z] += jnp.where(row == nx - 1, face[z : z + 1, :], shift_rows(fn[z], -1))

        @pl.when(k == 2)
        def _():
            face = from_above("gy", counts[2], fy[...])
            for z in range(nz):
                moved = shift_lanes(face, -z - 1)
                out[0, z] += jnp.where(lane == LANES - 1, moved, shift_lanes(fn[z], -1))

    spec = pl.BlockSpec((1, nz, nx, ny), lambda k: (k, 0, 0, 0))
    args = (fn, *above, *below, *got_z, *got_x, *got_y)
    whole = [pl.BlockSpec(a.shape, lambda k, n=a.ndim: (0,) * n) for a in args]
    return call(
        body,
        [residual.shape],
        "output_stage",
        scratch=[(nz, nx, ny)],
        far=(0, 1),
        far_out=True,
        grid=(3,),
        in_specs=[spec, spec] + whole,
        out_specs=[spec],
    )(residual, edge_diag, *args)[0]


def local(residual, edge_diag, node_shift, coarse_shift):
    axes = ("gz", "gx", "gy")
    counts = tuple(lax.axis_size(a) for a in axes)
    devices = counts[0] * counts[1] * counts[2]
    part, up_z, up_x, up_y, low_z, low_x, low_y = edge_stage(residual, edge_diag)
    below = (ring(up_z, "gz", 1), ring(up_x, "gx", 1), ring(up_y, "gy", 1))
    fg, rhs, xb, yb, w, *send = nodal_stage(part, node_shift, coarse_shift, *below, low_z, counts[0])
    got_z = swap(send, "gz")
    rhs, yb, w, *send = x_stage(got_z, rhs, xb, yb, w, fg, low_x, counts[0], counts[1])
    got_x = swap(send, "gx")
    planes = rhs.shape[0]
    rhs, w, *send = y_stage(got_x, rhs, yb, w, fg, low_y, counts[1], counts[2])
    got_y = swap(send, "gy")
    v1, v2, sums = coarse_stage(got_y, rhs, w, counts[2], devices)
    sums = lax.all_to_all(sums, ("gx", "gy", "gz"), 0, 0)
    fn, down_z, down_x, down_y = final_stage(
        sums, v1, v2, fg, node_shift, got_z, got_x, got_y, counts
    )
    above = (ring(down_z, "gz", -1), ring(down_x, "gx", -1), ring(down_y, "gy", -1))
    return output_stage(
        residual, edge_diag, fn, above, below, got_z, got_x, got_y, planes, counts
    )


def solution(mesh):
    placed = (
        P(None, "gz", "gx", "gy"),
        P(None, "gz", "gx", "gy"),
        P("gz", "gx", "gy"),
        P("gz", "gx", "gy"),
    )
    return jax.shard_map(
        local, mesh=mesh, in_specs=placed, out_specs=P(None, "gz", "gx", "gy"), check_vma=False
    )
```

```python
import jax
import jax.numpy as jnp
from jax import lax
from jax.experimental import pallas as pl
from jax.experimental.pallas import tpu as pltpu
from jax.sharding import PartitionSpec as P

F32 = jnp.float32
HIGHEST = lax.Precision.HIGHEST
LANES = 128


def lane_ids(rows):
    return lax.broadcasted_iota(jnp.int32, (rows, LANES), 1)


def row_ids(rows):
    return lax.broadcasted_iota(jnp.int32, (rows, LANES), 0)


def shift_lanes(value, amount):
    return pltpu.roll(value, amount % LANES, 1)


def shift_rows(value, amount):
    return pltpu.roll(value, amount % value.shape[0], 0)


def low_of(axis, size, first, second):
    place = lax.axis_index(axis)
    odd = place % 2 == 1
    zero = jnp.zeros_like(first)
    if second is None:
        return jnp.where(odd, first, zero)
    return jnp.where(odd, first, jnp.where(place > 0, second, zero))


def high_of(axis, size, first, second):
    place = lax.axis_index(axis)
    even = place % 2 == 0
    zero = jnp.zeros_like(first)
    if second is None:
        return jnp.where(even, first, zero)
    return jnp.where(even, first, jnp.where(place < size - 1, second, zero))


def from_below(axis, value):
    return jnp.where(lax.axis_index(axis) > 0, value, jnp.zeros_like(value))


def from_above(axis, size, value):
    return jnp.where(lax.axis_index(axis) < size - 1, value, jnp.zeros_like(value))


def ring(value, axis, step):
    size = lax.axis_size(axis)
    return lax.ppermute(value, axis, [(i, (i + step) % size) for i in range(size)])


def swap(values, axis):
    size = lax.axis_size(axis)
    even = [(i, i ^ 1) for i in range(size)]
    out = [lax.ppermute(values[0], axis, even)]
    if len(values) > 1:
        odd = [(i, (i + 1) % size if i % 2 else (i - 1) % size) for i in range(size)]
        out.append(lax.ppermute(values[1], axis, odd))
    return out


def write_sides(axis, refs, up, down):
    even = lax.axis_index(axis) % 2 == 0

    @pl.when(even)
    def _():
        up(refs[0])
        if len(refs) > 1:
            down(refs[1])

    @pl.when(jnp.logical_not(even))
    def _():
        down(refs[0])
        if len(refs) > 1:
            up(refs[1])


def call(body, outs, name, scratch=(), far=(), free=(), far_out=False, **kwargs):
    kind = jax.ShapeDtypeStruct if far_out else pltpu.VMEM
    run = pl.pallas_call(
        body,
        out_shape=[kind(shape, F32) for shape in outs],
        scratch_shapes=[pltpu.VMEM(s, F32) if isinstance(s, tuple) else s for s in scratch],
        name=name,
        compiler_params=pltpu.CompilerParams(vmem_limit_bytes=12 * 2**20),
        **kwargs,
    )

    def apply(*args):
        spaces = [pltpu.HBM if i in far else pltpu.VMEM for i in range(len(args))]
        return run(
            *(
                a if i in free else pltpu.with_memory_space_constraint(a, space)
                for i, (a, space) in enumerate(zip(args, spaces))
            )
        )

    return apply


def vmem(count):
    return [pl.BlockSpec(memory_space=pltpu.VMEM)] * count


def edge_stage(residual, edge_diag):
    _, nz, nx, ny = residual.shape
    step = 4
    steps = nz // step

    def body(res, diag, part, up_z, up_x, up_y, low_z, low_x, low_y, last):
        block = pl.program_id(0)
        lane = lane_ids(nx)
        row = row_ids(nx)

        @pl.when(block == 0)
        def _():
            last[...] = jnp.zeros_like(last)
            up_y[...] = jnp.zeros_like(up_y)
            low_y[...] = jnp.zeros_like(low_y)

        before = last[...]
        high = up_y[...]
        low = low_y[...]
        for j in range(step):
            z = block * step + j
            s = [res[k, j] / diag[k, j] for k in range(3)]
            total = before - s[0]
            total += jnp.where(row == 0, 0.0, shift_rows(s[1], 1)) - s[1]
            total += jnp.where(lane == 0, 0.0, shift_lanes(s[2], 1)) - s[2]
            part[j] = total
            before = s[0]
            for k in range(3):
                up_x[pl.ds(k * nz + z, 1), :] = s[k][nx - 1 :, :]
                low_x[pl.ds(k * nz + z, 1), :] = s[k][:1, :]
                spot = k * nz + z
                high = jnp.where(lane == spot, pltpu.roll(s[k], spot + 1, 1), high)
                low = jnp.where(lane == spot, pltpu.roll(s[k], spot, 1), low)
            if j == 0:

                @pl.when(block == 0)
                def _():
                    for k in range(3):
                        low_z[k] = s[k]

            if j == step - 1:

                @pl.when(block == steps - 1)
                def _():
                    for k in range(3):
                        up_z[k] = s[k]

        last[...] = before
        up_y[...] = high
        low_y[...] = low

    whole = lambda *shape: pl.BlockSpec(shape, lambda i: (0,) * len(shape))
    spec = pl.BlockSpec((3, step, nx, ny), lambda i: (0, i, 0, 0))
    faces = [(3, nx, ny), (3 * nz, ny), (nx, LANES)] * 2
    return call(
        body,
        [(nz, nx, ny)] + faces,
        "edge_stage",
        scratch=[(nx, ny)],
        far=(0, 1),
        grid=(steps,),
        in_specs=[spec, spec],
        out_specs=[pl.BlockSpec((step, nx, ny), lambda i: (i, 0, 0))] + [whole(*f) for f in faces],
    )(residual, edge_diag)


def plane(values, row_count):
    return jnp.concatenate([values, jnp.zeros((row_count - values.shape[0], LANES), F32)], axis=0)


def nodal_stage(part, node_shift, coarse_shift, got_z, got_x, got_y, low_z, z_count):
    nz, nx, ny = part.shape
    cz, cx, cy = nz // 2, nx // 2, ny // 2
    rows = cx + 8
    sends = 1 if z_count == 2 else 2

    def body(part, shift, coarse, gz, gx, gy, low_z, fg, rhs, xb, yb, w, *rest):
        out, (pair, s_, xl_, yl_, zl_, zh_) = rest[:sends], rest[sends:]
        lane = lane_ids(nx)
        row = row_ids(nx)
        lane_c = lane_ids(rows)
        row_c = row_ids(rows)
        below_z = from_below("gz", gz[0])
        below_y = from_below("gy", gy[...])
        fine = lax.broadcasted_iota(jnp.int32, (ny, 2 * LANES), 0)
        coarse_lane = lax.broadcasted_iota(jnp.int32, (ny, 2 * LANES), 1)
        miss = jnp.where(
            coarse_lane < LANES, fine // 2 - coarse_lane, fine - 2 * (coarse_lane - LANES)
        )
        gather = jnp.where(miss == 0, 1.0, 0.0)
        for c in range(cz):
            both = []
            for z in (2 * c, 2 * c + 1):
                total = part[z]
                if z == 0:
                    total += below_z
                total += jnp.where(row == 0, from_below("gx", gx[nz + z : nz + z + 1, :]), 0.0)
                total += jnp.where(lane == 0, shift_lanes(below_y, -(2 * nz + z)), 0.0)
                guess = total / (6.0 + shift[z])
                fg[z] = guess
                both.append(guess)
            pair[c % 2] = both[0] + both[1]
            low = pair[c % 2, pl.ds(0, cx, 2), :]
            high = pair[c % 2, pl.ds(1, cx, 2), :]
            first = fg[2 * c, pl.ds(0, cx, 2), :] + fg[2 * c, pl.ds(1, cx, 2), :]
            stacked = jnp.concatenate([low + high, low, first], axis=0)
            sums = jnp.dot(stacked, gather, precision=HIGHEST, preferred_element_type=F32)
            s = sums[:cx, :LANES]
            z_low = sums[2 * cx :, :LANES]
            s_[c] = plane(s, rows)
            yl_[c] = plane(sums[:cx, LANES:], rows)
            xl_[c] = plane(sums[cx : 2 * cx, :LANES], rows)
            zl_[c] = plane(z_low, rows)
            zh_[c] = plane(s - z_low, rows)
            w[c] = jnp.zeros((rows, LANES), F32)
            w[c, :cx, :cy] = 1.0 / (6.0 + coarse[c])
        for c in range(cz):
            s, x_low, y_low = s_[c], xl_[c], yl_[c]
            x_high = s - x_low
            y_high = s - y_low
            total = 3.0 * s
            total += shift_rows(x_low, -1) + shift_rows(x_high, 1)
            total += shift_lanes(y_low, -1) + shift_lanes(y_high, 1)
            if c > 0:
                total += zh_[c - 1]
            if c < cz - 1:
                total += zl_[c + 1]
            rhs[c] = total
            xb[c] = jnp.where(row_c < cx // 2, x_low, x_high)
            yb[c] = jnp.where(lane_c < cy // 2, y_low, y_high)
        rhs[cz] = zh_[cz - 1]
        rhs[cz + 1] = jnp.zeros((rows, LANES), F32)
        rhs[cz + 2] = jnp.zeros((rows, LANES), F32)
        rhs[cz + 3] = zl_[0]

        def fill(ref, near, far, half, face):
            planes = [rhs[near], rhs[far], w[near], w[far], half]
            planes += [xb[near], xb[far], yb[near], yb[far]]
            for i, value in enumerate(planes):
                ref[i * rows : (i + 1) * rows, :] = value
            ref[9 * rows : 9 * rows + nx, :] = face

        def tail(ref, values):
            for i, value in enumerate(values):
                at = 9 * rows + nx + i * nx
                ref[at : at + nx, :] = value

        def up(ref):
            fill(ref, cz - 1, cz - 2, zh_[cz - 1], fg[nz - 1])
            tail(ref, [jnp.zeros((nx, LANES), F32)] * 5)

        def down(ref):
            fill(ref, 0, 1, zl_[0], fg[0])
            here = fg[0]
            around = fg[1] + jnp.where(row == 0, 0.0, shift_rows(here, 1))
            around += jnp.where(row == nx - 1, 0.0, shift_rows(here, -1))
            around += jnp.where(lane == 0, 0.0, shift_lanes(here, 1))
            around += jnp.where(lane == ny - 1, 0.0, shift_lanes(here, -1))
            inverse = 1.0 / (6.0 + shift[0])
            tail(ref, [low_z[0], low_z[1], low_z[2], here + inverse * around, inverse])

        write_sides("gz", out, up, down)

    coarse = (cz, rows, LANES)
    send = (9 * rows + 6 * nx, LANES)
    return call(
        body,
        [(nz, nx, ny), (cz + 4, rows, LANES), coarse, coarse, coarse] + [send] * sends,
        "nodal_stage",
        scratch=[(2, nx, ny), coarse, coarse, coarse, coarse, coarse],
        in_specs=vmem(7),
        out_specs=vmem(5 + sends),
    )(part, node_shift, coarse_shift, got_z, got_x, got_y, low_z)


def x_stage(got, rhs, xb, yb, w, fg, low_x, node_shift, z_count, x_count):
    planes, rows, _ = rhs.shape
    cz, cx = planes - 4, rows - 8
    nz, nx, ny = fg.shape
    cy = ny // 2
    sends = 1 if x_count == 2 else 2
    gots = len(got)

    def body(*refs):
        got = refs[:gots]
        rhs, xb, yb, w, fg, low_x, shift, rhs2, yb2, w2 = refs[gots : gots + 10]
        out, (xb2,) = refs[gots + 10 : gots + 10 + sends], refs[gots + 10 + sends :]

        def take_at(pick, at):
            values = [ref[at, :] for ref in got]
            return pick("gz", z_count, values[0], values[1] if gots > 1 else None)

        def take(pick, i):
            return take_at(pick, slice(i * rows, (i + 1) * rows))

        for c in range(1, cz - 1):
            rhs2[c] = rhs[c]
        rhs2[0] = rhs[0] + take(low_of, 4)
        rhs2[cz - 1] = rhs[cz - 1] + take(high_of, 4)
        rhs2[cz] = rhs[cz] + take(high_of, 0)
        rhs2[cz + 1] = take(high_of, 1)
        rhs2[cz + 2] = take(low_of, 1)
        rhs2[cz + 3] = rhs[cz + 3] + take(low_of, 0)
        for here, there, i in ((w, w2, 2), (xb, xb2, 5), (yb, yb2, 7)):
            for c in range(cz):
                there[c] = here[c]
            there[cz] = take(high_of, i)
            there[cz + 1] = take(high_of, i + 1)
            there[cz + 2] = take(low_of, i + 1)
            there[cz + 3] = take(low_of, i)

        lane = lane_ids(planes)

        def fill(ref, near, far, fine):
            halves = lane < cy
            first = jnp.where(halves, rhs2[:, near, :], shift_lanes(rhs2[:, far, :], cy))
            second = jnp.where(halves, w2[:, near, :], shift_lanes(w2[:, far, :], cy))
            edge = yb2[:, far, :]
            third = jnp.where(halves, xb2[:, near, :], shift_lanes(yb2[:, near, :], cy))
            third = jnp.where(lane == cy + 1, shift_lanes(edge, cy + 1), third)
            third = jnp.where(lane == LANES - 2, shift_lanes(edge, cy - 1), third)
            for i, value in enumerate((first, second, third)):
                ref[i * 16 : i * 16 + planes, :] = value
                ref[i * 16 + planes : i * 16 + 16, :] = jnp.zeros((16 - planes, LANES), F32)
            ref[48 : 48 + nz, :] = fg[:, fine, :]
            at = 9 * rows + fine
            ref[48 + nz : 49 + nz, :] = take_at(high_of, slice(at, at + 1))
            ref[49 + nz : 56 + nz, :] = jnp.zeros((7, LANES), F32)

        tail = 56 + nz

        def up(ref):
            fill(ref, cx - 1, cx - 2, nx - 1)
            ref[tail : tail + 5 * nz, :] = jnp.zeros((5 * nz, LANES), F32)

        def down(ref):
            fill(ref, 0, 1, 0)
            ref[tail : tail + 3 * nz, :] = low_x[...]
            here = fg[:, 0, :]
            lane_z = lane_ids(nz)
            row_z = row_ids(nz)
            at = 9 * rows
            below = take_at(low_of, slice(at, at + 1))
            above = take_at(high_of, slice(at, at + 1))
            around = fg[:, 1, :] + jnp.where(row_z == 0, below, shift_rows(here, 1))
            around += jnp.where(row_z == nz - 1, above, shift_rows(here, -1))
            around += jnp.where(lane_z == 0, 0.0, shift_lanes(here, 1))
            around += jnp.where(lane_z == ny - 1, 0.0, shift_lanes(here, -1))
            inverse = 1.0 / (6.0 + shift[:, 0, :])
            ref[tail + 3 * nz : tail + 4 * nz, :] = here + inverse * around
            ref[tail + 4 * nz : tail + 5 * nz, :] = inverse

        write_sides("gx", out, up, down)

    whole = (planes, rows, LANES)
    return call(
        body,
        [whole, whole, whole] + [(56 + 6 * nz, LANES)] * sends,
        "x_stage",
        scratch=[whole],
        in_specs=vmem(gots + 7),
        out_specs=vmem(3 + sends),
    )(*got, rhs, xb, yb, w, fg, low_x, node_shift)


def y_stage(got_z, got, rhs, yb, w, fg, low_y, node_shift, counts):
    planes, rows, _ = rhs.shape
    cx = rows - 8
    nz, nx, ny = fg.shape
    cy = ny // 2
    z_count, x_count, y_count = counts
    sends = 1 if y_count == 2 else 2
    n_z, gots = len(got_z), len(got)

    def body(*refs):
        gz, got = refs[:n_z], refs[n_z : n_z + gots]
        rhs, yb, w, fg, low_y, shift, rhs3, w3 = refs[n_z + gots : n_z + gots + 8]
        rest = refs[n_z + gots + 8 :]
        out, (yb3, add) = rest[:sends], rest[sends:]
        lane_p = lane_ids(planes)

        def take_at(pick, at):
            values = [ref[at, :] for ref in got]
            return pick("gx", x_count, values[0], values[1] if gots > 1 else None)

        def take(pick, i):
            return take_at(pick, slice(i * 16, i * 16 + planes))

        def z_face(pick):
            values = [ref[9 * rows : 9 * rows + nx, :] for ref in gz]
            return pick("gz", z_count, values[0], values[1] if n_z > 1 else None)

        add[...] = jnp.zeros_like(add)
        for c in range(planes):
            w3[c] = w[c]
            yb3[c] = yb[c]
        for pick, near, far, edge in ((high_of, cx, cx + 1, cx - 1), (low_of, rows - 1, rows - 2, 0)):
            first, second, third = take(pick, 0), take(pick, 1), take(pick, 2)
            other = shift_lanes(third, -cy)
            one = jnp.where((lane_p == 0) | (lane_p == cy - 1), other, 0.0)
            two = jnp.where(lane_p == 0, shift_lanes(third, -cy - 1), 0.0)
            two = jnp.where(lane_p == cy - 1, shift_lanes(third, 1 - cy), two)
            yb3[:, near, :] = one
            yb3[:, far, :] = two
            for at, value, ends in ((near, first, one), (far, shift_lanes(first, -cy), two)):
                value = jnp.where(lane_p < cy, value, 0.0)
                value += jnp.where(lane_p == cy, shift_lanes(ends, 1), 0.0)
                value += jnp.where(lane_p == LANES - 1, shift_lanes(ends, -1), 0.0)
                add[:, at, :] = value
            w3[:, near, :] = jnp.where(lane_p < cy, second, 0.0)
            w3[:, far, :] = jnp.where(lane_p < cy, shift_lanes(second, -cy), 0.0)
            add[:, edge, :] = jnp.where(lane_p < cy, third, 0.0)
        for c in range(planes):
            rhs3[c] = rhs[c] + add[c]

        lane_c = lane_ids(rows)
        lane = lane_ids(nx)
        row = row_ids(nx)
        lane8 = lane_ids(8)
        base = 5 * planes
        above = z_face(high_of)
        below = z_face(low_of)
        x_high = take_at(high_of, slice(48, 48 + nz))
        x_low = take_at(low_of, slice(48, 48 + nz))

        def line(source, fine, at):
            acc = jnp.zeros((8, LANES), F32)
            for z in range(nz):
                moved = jnp.broadcast_to(source[z : z + 1, :], (8, LANES))
                acc = jnp.where(lane8 == at + z, shift_lanes(moved, at + z - fine), acc)
            return acc

        def fill(ref, near, far, fine, tail):
            acc = jnp.zeros((rows, LANES), F32)
            jobs = ((rhs3, near), (rhs3, far), (w3, near), (w3, far), (yb3, near))
            for i, (field, at) in enumerate(jobs):
                for z in range(planes):
                    spot = i * planes + z
                    acc = jnp.where(lane_c == spot, shift_lanes(field[z], spot - at), acc)
            acc = plane(acc, nx)
            for z in range(nz):
                acc = jnp.where(lane == base + z, shift_lanes(fg[z], base + z - fine), acc)
            acc = jnp.where(lane == base + nz, shift_lanes(above, base + nz - fine), acc)
            at = base + nz + 1
            if tail is not None:
                moved = shift_lanes(tail, at)
                acc = jnp.where((lane >= at) & (lane < at + 3 * nz), moved, acc)
            ref[:nx, :] = acc
            ref[nx : nx + 8, :] = line(x_high, fine, base)
            return acc

        def up(ref):
            fill(ref, cy - 1, cy - 2, ny - 1, None)
            ref[nx + 8 :, :] = jnp.zeros((nx // 2, LANES), F32)

        def down(ref):
            acc = fill(ref, 0, 1, 0, low_y[...])
            here = jnp.where(lane < nz + 1, shift_lanes(acc, -base), 0.0)
            here = jnp.where(lane == LANES - 1, shift_lanes(below, -1), here)
            around = shift_lanes(here, 1) + shift_lanes(here, -1)
            around += jnp.where(row == 0, line(x_low, 0, 0)[:1, :], shift_rows(here, 1))
            around += jnp.where(row == nx - 1, line(x_high, 0, 0)[:1, :], shift_rows(here, -1))
            inverse = jnp.ones((nx, LANES), F32)
            for z in range(nz):
                inverse = jnp.where(lane == z, shift_lanes(6.0 + shift[z], z), inverse)
                around += jnp.where(lane == z, shift_lanes(fg[z], z - 1), 0.0)
            inverse = 1.0 / inverse
            value = here + inverse * around
            half = nx // 2
            packed = jnp.zeros((half, LANES), F32)
            for i, source in enumerate((value[:half], value[half:], inverse[:half], inverse[half:])):
                there = lane_ids(half) // nz == i
                packed = jnp.where(there, shift_lanes(source, i * nz), packed)
            ref[nx + 8 :, :] = packed

        write_sides("gy", out, up, down)

    whole = (planes, rows, LANES)
    return call(
        body,
        [whole, whole] + [(nx + 8 + nx // 2, LANES)] * sends,
        "y_stage",
        scratch=[whole, whole],
        in_specs=vmem(n_z + gots + 6),
        out_specs=vmem(2 + sends),
    )(*got_z, *got, rhs, yb, w, fg, low_y, node_shift)


def coarse_stage(got, rhs, w, after, y_count, devices):
    planes, rows, _ = rhs.shape
    cz, cx = planes - 4, rows - 8
    cy = LANES // 2
    gots = len(got)

    def body(*refs):
        got = refs[:gots]
        rhs, w, _, v1, v2, sums, tot, inv_, image_ = refs[gots:]
        values = [ref[:rows, :] for ref in got]
        second = values[1] if gots > 1 else None
        low = low_of("gy", y_count, values[0], second)
        high = high_of("gy", y_count, values[0], second)
        lane = lane_ids(rows)
        spots_r = ((cy, high, 0), (cy + 1, high, 1), (LANES - 1, low, 0), (LANES - 2, low, 1))
        spots_r += ((cy - 1, high, 4), (0, low, 4))
        for z in range(planes):
            right = rhs[z]
            for at, source, i in spots_r:
                moved = shift_lanes(source, at - (i * planes + z))
                right += jnp.where(lane == at, moved, 0.0)
            inv = w[z]
            for at, source, i in spots_r[:4]:
                moved = shift_lanes(source, at - ((i + 2) * planes + z))
                inv = jnp.where(lane == at, moved, inv)
            inv_[z] = inv
            tot[z] = right
            v1[z] = right * inv

        def near(field, z):
            here = field[z]
            total = field[(z + 1) % planes] + field[(z - 1) % planes]
            total += shift_rows(here, 1) + shift_rows(here, -1)
            return total + shift_lanes(here, 1) + shift_lanes(here, -1)

        v2[cz + 1] = jnp.zeros((rows, LANES), F32)
        v2[cz + 2] = jnp.zeros((rows, LANES), F32)
        for z in list(range(cz + 1)) + [planes - 1]:
            image = tot[z] - near(v1, z)
            if z < cz:
                image_[z] = image
            v2[z] = image * inv_[z]
        parts = [jnp.zeros((cx, LANES), F32)] * 5
        for z in range(cz):
            first, second_, right, image = v1[z], v2[z], tot[z], image_[z]
            third = image - near(v2, z)
            terms = (first * right, second_ * right, first * image, second_ * image, second_ * third)
            parts = [a + b[:cx, :] for a, b in zip(parts, terms)]
        keep = lane_ids(1) < cy
        lines = [jnp.where(keep, jnp.sum(a, axis=0, keepdims=True), 0.0) for a in parts]
        tile = jnp.concatenate(lines + [jnp.zeros((3, LANES), F32)], axis=0)
        column = jnp.sum(tile, axis=1, keepdims=True)
        spread = jnp.where(lane_ids(8) == row_ids(8), column, 0.0)
        line = jnp.sum(spread, axis=0, keepdims=True)
        sums[...] = jnp.broadcast_to(line[None], (devices, 1, LANES))

    whole = (planes, rows, LANES)
    return call(
        body,
        [whole, whole, (devices, 1, LANES)],
        "coarse_stage",
        scratch=[whole, whole, whole],
        in_specs=vmem(gots + 3),
        out_specs=vmem(3),
    )(*got, rhs, w, after)


def smooth_stage(residual, edge_diag, below, got_z, got_x, after, counts):
    _, nz, nx, ny = residual.shape
    n_z, n_x = len(got_z), len(got_x)
    rows = nx // 2 + 8

    def body(*refs):
        res, diag, lz, lx, ly = refs[:5]
        gz = refs[5 : 5 + n_z]
        gx = refs[5 + n_z : 5 + n_z + n_x]
        _, out, last, s = refs[5 + n_z + n_x :]
        lane = lane_ids(nx)
        row = row_ids(nx)
        y_low = from_below("gy", ly[...])

        def above_of(refs, axis, size, at):
            values = [ref[at, :] for ref in refs]
            return high_of(axis, size, values[0], values[1] if len(values) > 1 else None)

        acc = jnp.zeros((nx, LANES), F32)
        for k in range(3):
            for z in range(nz):
                s[z] = res[k, z] / diag[k, z]
            z_low = from_below("gz", lz[k])
            at = 9 * rows + nx + k * nx
            z_high = above_of(gz, "gz", counts[0], slice(at, at + nx))
            x_low = from_below("gx", lx[k * nz : (k + 1) * nz, :])
            at = 56 + nz + k * nz
            x_high = above_of(gx, "gx", counts[1], slice(at, at + nz))
            for z in range(nz):
                here = s[z]
                around = s[z - 1] if z > 0 else z_low
                around += s[z + 1] if z < nz - 1 else z_high
                around += jnp.where(row == 0, x_low[z : z + 1, :], shift_rows(here, 1))
                around += jnp.where(row == nx - 1, x_high[z : z + 1, :], shift_rows(here, -1))
                spot = k * nz + z
                around += jnp.where(lane == 0, shift_lanes(y_low, -spot), shift_lanes(here, 1))
                around += jnp.where(lane == LANES - 1, 0.0, shift_lanes(here, -1))
                inverse = 1.0 / diag[k, z]
                acc = jnp.where(lane == spot, shift_lanes(inverse, spot + 1), acc)
                out[k, z] = here + around * inverse
        last[...] = acc

    return call(
        body,
        [residual.shape, (nx, LANES)],
        "smooth_stage",
        scratch=[(nz, nx, ny)],
        free=(0, 1),
        in_specs=vmem(6 + n_z + n_x),
        out_specs=vmem(2),
    )(residual, edge_diag, *below, *got_z, *got_x, after)


def final_stage(sums, v1, v2, fg, node_shift, smooth, last, got_z, got_x, got_y, counts):
    planes, rows, _ = v1.shape
    cz, cx, cy = planes - 4, rows - 8, LANES // 2
    nz, nx, ny = fg.shape
    n_z, n_x, n_y = len(got_z), len(got_x), len(got_y)
    gots = n_z + n_x + n_y

    def body(*refs):
        sums, v1, v2, fg, shift, smooth, last = refs[:7]
        gz = refs[7 : 7 + n_z]
        gx = refs[7 + n_z : 7 + n_z + n_x]
        gy = refs[7 + n_z + n_x : 7 + gots]
        out, sol, dup, inter, small, lines, buf, sem = refs[7 + gots :]

        def one_side(pick, refs, axis, size, at):
            values = [ref[at, :] for ref in refs]
            return pick(axis, size, values[0], values[1] if len(values) > 1 else None)

        def both(refs, axis, size, at):
            return [one_side(pick, refs, axis, size, at) for pick in (low_of, high_of)]

        total = jnp.sum(sums[...], axis=0)
        lane1 = lane_ids(1)
        gone, gtwo, hone, hmix, htwo = [
            jnp.sum(jnp.where(lane1 == i, total, 0.0), axis=1, keepdims=True) for i in range(5)
        ]
        two = (gtwo - hmix * gone / hone) / (htwo - hmix * hmix / hone)
        one = (gone - hmix * two) / hone
        source = lax.broadcasted_iota(jnp.int32, (LANES, 2 * LANES), 0)
        target = lax.broadcasted_iota(jnp.int32, (LANES, 2 * LANES), 1)
        fine = target - LANES
        side = jnp.where(fine % 2 == 1, fine // 2 + 1, (fine // 2 + LANES - 1) % LANES)
        spread = jnp.where(jnp.where(target < LANES, target // 2, side) == source, 1.0, 0.0)
        for z in list(range(cz + 1)) + [planes - 1]:
            sol[z] = one * v1[z] + two * v2[z]
            dup[z] = jnp.dot(sol[z], spread, precision=HIGHEST, preferred_element_type=F32)

        z_at = 9 * rows
        z_low, z_high = both(gz, "gz", counts[0], slice(z_at, z_at + nx))
        z_base = one_side(high_of, gz, "gz", counts[0], slice(z_at + 4 * nx, z_at + 5 * nx))
        z_inverse = one_side(high_of, gz, "gz", counts[0], slice(z_at + 5 * nx, z_at + 6 * nx))
        x_low, x_high = both(gx, "gx", counts[1], slice(48, 48 + nz + 1))
        x_at = 56 + nz
        x_base = one_side(high_of, gx, "gx", counts[1], slice(x_at + 3 * nz, x_at + 4 * nz))
        x_inverse = one_side(high_of, gx, "gx", counts[1], slice(x_at + 4 * nz, x_at + 5 * nz))
        y_low, y_high = both(gy, "gy", counts[2], slice(0, nx))
        y_row_low, y_row_high = both(gy, "gy", counts[2], slice(nx, nx + 1))
        half = nx // 2
        y_pack = one_side(high_of, gy, "gy", counts[2], slice(nx + 8, nx + 8 + half))
        lane = lane_ids(nx)
        row = row_ids(nx)
        base = 5 * planes
        tail = base + nz + 1

        def spread_around(z):
            c, odd = z // 2, z % 2
            here = dup[c, :, :LANES]
            same = 3.0 * here + dup[c, :, LANES:]
            same += dup[(c + 1 if odd else c - 1) % planes, :, :LANES]
            slot = z % 2
            inter[slot, pl.ds(0, cx, 2), :] = (same + shift_rows(here, 1))[:cx, :]
            inter[slot, pl.ds(1, cx, 2), :] = (same + shift_rows(here, -1))[:cx, :]
            return inter[slot]

        def edges(z, guess):
            left = shift_lanes(y_low, -(base + z))
            right = shift_lanes(y_high, -(base + z) - 1)
            if guess is None:
                around = jnp.where(row == 0, x_low[z : z + 1, :], 0.0)
                around += jnp.where(row == nx - 1, x_high[z : z + 1, :], 0.0)
                around += jnp.where(lane == 0, left, 0.0)
                return around + jnp.where(lane == LANES - 1, right, 0.0)
            around = jnp.where(row == 0, x_low[z : z + 1, :], shift_rows(guess, 1))
            around += jnp.where(row == nx - 1, x_high[z : z + 1, :], shift_rows(guess, -1))
            around += jnp.where(lane == 0, left, shift_lanes(guess, 1))
            return around + jnp.where(lane == LANES - 1, right, shift_lanes(guess, -1))

        def nodal(z):
            if z == nz:
                around = spread_around(z) + edges(z, None) + fg[nz - 1]
                value = z_base + z_inverse * around
                return from_above("gz", counts[0], value)
            guess = fg[z]
            around = spread_around(z) + edges(z, guess)
            around += fg[z - 1] if z > 0 else z_low
            around += fg[z + 1] if z < nz - 1 else z_high
            return guess + around / (6.0 + shift[z])

        here = dup[:cz, cx, :LANES]
        same = 3.0 * here + dup[:cz, cx, LANES:] + dup[:cz, cx - 1, :LANES]
        small[pl.ds(0, cz, 2), :] = same + jnp.concatenate(
            [dup[planes - 1, cx : cx + 1, :LANES], here[: cz - 1]], axis=0
        )
        small[pl.ds(1, cz, 2), :] = same + dup[1 : cz + 1, cx, :LANES]
        for z in range(nz):
            left = shift_lanes(y_row_low, -(base + z))
            right = shift_lanes(y_row_high, -(base + z) - 1)
            value = jnp.where(lane1 == 0, left, 0.0)
            lines[z : z + 1, :] = jnp.where(lane1 == LANES - 1, right, value)
        x_value = x_base + x_inverse * (fg[:, nx - 1, :] + small[...] + lines[...])
        x_value = from_above("gx", counts[1], x_value)

        lane_c = lane_ids(rows)
        even = jnp.zeros((rows, LANES), F32)
        odd = jnp.zeros((rows, LANES), F32)
        own = jnp.zeros((nx, LANES), F32)
        for z in range(nz):
            c = z // 2
            here = sol[c]
            same = 3.0 * here + shift_lanes(here, 1) + sol[(c + 1 if z % 2 else c - 1) % planes]
            even = jnp.where(lane_c == z, shift_lanes(same + shift_rows(here, 1), z - cy), even)
            odd = jnp.where(lane_c == z, shift_lanes(same + shift_rows(here, -1), z - cy), odd)
            own = jnp.where(lane == z, shift_lanes(fg[z], z + 1), own)
        inter[0, pl.ds(0, cx, 2), :] = even[:cx, :]
        inter[0, pl.ds(1, cx, 2), :] = odd[:cx, :]
        y_base = jnp.concatenate([y_pack, shift_lanes(y_pack, -nz)], axis=0)
        y_inverse = jnp.concatenate(
            [shift_lanes(y_pack, -2 * nz), shift_lanes(y_pack, -3 * nz)], axis=0
        )
        y_value = y_base + y_inverse * (own + inter[0])
        y_value = from_above("gy", counts[2], y_value)
        y_fix = shift_lanes(y_high, -tail) * last[...]

        def copy(z):
            return pltpu.make_async_copy(buf.at[:, z], out.at[:, z], sem.at[z])

        value = nodal(0)
        for z in range(nz):
            after = nodal(z + 1)
            steps = [after, jnp.where(row == nx - 1, x_value[z : z + 1, :], shift_rows(value, -1))]
            steps.append(
                jnp.where(lane == LANES - 1, shift_lanes(y_value, -z - 1), shift_lanes(value, -1))
            )
            for k in range(3):
                fixed = jnp.where(lane == LANES - 1, shift_lanes(y_fix, -(k * nz + z) - 1), 0.0)
                buf[k, z] = (smooth[k, z] + fixed) + (steps[k] - value)
            copy(z).start()
            value = after
        for z in range(nz):
            copy(z).wait()

    return call(
        body,
        [smooth.shape],
        "final_stage",
        scratch=[
            (planes, rows, LANES),
            (planes, rows, 2 * LANES),
            (2, nx, LANES),
            (nz, LANES),
            (nz, LANES),
            smooth.shape,
            pltpu.SemaphoreType.DMA((nz,)),
        ],
        far_out=True,
        in_specs=vmem(7 + gots),
        out_specs=[pl.BlockSpec(memory_space=pltpu.HBM)],
    )(sums, v1, v2, fg, node_shift, smooth, last, *got_z, *got_x, *got_y)[0]


def local(residual, edge_diag, node_shift, coarse_shift):
    axes = ("gz", "gx", "gy")
    counts = tuple(lax.axis_size(a) for a in axes)
    devices = counts[0] * counts[1] * counts[2]
    part, up_z, up_x, up_y, low_z, low_x, low_y = edge_stage(residual, edge_diag)
    below = (ring(up_z, "gz", 1), ring(up_x, "gx", 1), ring(up_y, "gy", 1))
    fg, rhs, xb, yb, w, *send = nodal_stage(part, node_shift, coarse_shift, *below, low_z, counts[0])
    got_z = swap(send, "gz")
    rhs, yb, w, *send = x_stage(
        got_z, rhs, xb, yb, w, fg, low_x, node_shift, counts[0], counts[1]
    )
    got_x = swap(send, "gx")
    rhs, w, *send = y_stage(got_z, got_x, rhs, yb, w, fg, low_y, node_shift, counts)
    got_y = swap(send, "gy")
    smooth, last = smooth_stage(residual, edge_diag, below, got_z, got_x, w, counts)
    v1, v2, sums = coarse_stage(got_y, rhs, w, last, counts[2], devices)
    sums = lax.all_to_all(sums, ("gx", "gy", "gz"), 0, 0)
    return final_stage(
        sums, v1, v2, fg, node_shift, smooth, last, got_z, got_x, got_y, counts
    )


def solution(mesh):
    placed = (
        P(None, "gz", "gx", "gy"),
        P(None, "gz", "gx", "gy"),
        P("gz", "gx", "gy"),
        P("gz", "gx", "gy"),
    )
    return jax.shard_map(
        local, mesh=mesh, in_specs=placed, out_specs=P(None, "gz", "gx", "gy"), check_vma=False
    )
```

```python
import jax
import jax.numpy as jnp
from jax import lax
from jax.experimental import pallas as pl
from jax.experimental.pallas import tpu as pltpu
from jax.sharding import PartitionSpec as P


F32 = jnp.float32
HIGHEST = lax.Precision.HIGHEST
LANES = 128


def lane_ids(rows):
    return lax.broadcasted_iota(jnp.int32, (rows, LANES), 1)


def row_ids(rows):
    return lax.broadcasted_iota(jnp.int32, (rows, LANES), 0)


def shift_lanes(value, amount):
    return pltpu.roll(value, amount % LANES, 1)


def shift_rows(value, amount):
    return pltpu.roll(value, amount % value.shape[0], 0)


def low_of(axis, size, first, second):
    place = lax.axis_index(axis)
    odd = place % 2 == 1
    zero = jnp.zeros_like(first)
    if second is None:
        return jnp.where(odd, first, zero)
    return jnp.where(odd, first, jnp.where(place > 0, second, zero))


def high_of(axis, size, first, second):
    place = lax.axis_index(axis)
    even = place % 2 == 0
    zero = jnp.zeros_like(first)
    if second is None:
        return jnp.where(even, first, zero)
    return jnp.where(even, first, jnp.where(place < size - 1, second, zero))


def from_below(axis, value):
    return jnp.where(lax.axis_index(axis) > 0, value, jnp.zeros_like(value))


def from_above(axis, size, value):
    return jnp.where(lax.axis_index(axis) < size - 1, value, jnp.zeros_like(value))


def ring(value, axis, step):
    size = lax.axis_size(axis)
    return lax.ppermute(value, axis, [(i, (i + step) % size) for i in range(size)])


def swap(values, axis):
    size = lax.axis_size(axis)
    even = [(i, i ^ 1) for i in range(size)]
    out = [lax.ppermute(values[0], axis, even)]
    if len(values) > 1:
        odd = [(i, (i + 1) % size if i % 2 else (i - 1) % size) for i in range(size)]
        out.append(lax.ppermute(values[1], axis, odd))
    return out


def write_sides(axis, refs, up, down):
    even = lax.axis_index(axis) % 2 == 0

    @pl.when(even)
    def _():
        up(refs[0])
        if len(refs) > 1:
            down(refs[1])

    @pl.when(jnp.logical_not(even))
    def _():
        down(refs[0])
        if len(refs) > 1:
            up(refs[1])


def call(body, outs, scratch=(), far=(), free=(), far_out=False, **kwargs):
    kind = jax.ShapeDtypeStruct if far_out else pltpu.VMEM
    run = pl.pallas_call(
        body,
        out_shape=[kind(shape, F32) for shape in outs],
        scratch_shapes=[pltpu.VMEM(s, F32) if isinstance(s, tuple) else s for s in scratch],
        compiler_params=pltpu.CompilerParams(vmem_limit_bytes=12 * 2**20),
        **kwargs,
    )

    def apply(*args):
        spaces = [pltpu.HBM if i in far else pltpu.VMEM for i in range(len(args))]
        return run(
            *(
                a if i in free else pltpu.with_memory_space_constraint(a, space)
                for i, (a, space) in enumerate(zip(args, spaces))
            )
        )

    return apply


def vmem(count):
    return [pl.BlockSpec(memory_space=pltpu.VMEM)] * count


def edge_stage(residual, edge_diag):
    _, nz, nx, ny = residual.shape
    step = 4
    steps = nz // step

    def body(res, diag, part, up_z, up_x, up_y, low_z, low_x, low_y, last):
        block = pl.program_id(0)
        lane = lane_ids(nx)
        row = row_ids(nx)

        @pl.when(block == 0)
        def _():
            last[...] = jnp.zeros_like(last)
            up_y[...] = jnp.zeros_like(up_y)
            low_y[...] = jnp.zeros_like(low_y)

        before = last[...]
        high = up_y[...]
        low = low_y[...]
        for j in range(step):
            z = block * step + j
            s = [res[k, j] / diag[k, j] for k in range(3)]
            total = before - s[0]
            total += jnp.where(row == 0, 0.0, shift_rows(s[1], 1)) - s[1]
            total += jnp.where(lane == 0, 0.0, shift_lanes(s[2], 1)) - s[2]
            part[j] = total
            before = s[0]
            for k in range(3):
                up_x[pl.ds(k * nz + z, 1), :] = s[k][nx - 1 :, :]
                low_x[pl.ds(k * nz + z, 1), :] = s[k][:1, :]
                spot = k * nz + z
                high = jnp.where(lane == spot, pltpu.roll(s[k], spot + 1, 1), high)
                low = jnp.where(lane == spot, pltpu.roll(s[k], spot, 1), low)
            if j == 0:

                @pl.when(block == 0)
                def _():
                    for k in range(3):
                        low_z[k] = s[k]

            if j == step - 1:

                @pl.when(block == steps - 1)
                def _():
                    for k in range(3):
                        up_z[k] = s[k]

        last[...] = before
        up_y[...] = high
        low_y[...] = low

    whole = lambda *shape: pl.BlockSpec(shape, lambda i: (0,) * len(shape))
    spec = pl.BlockSpec((3, step, nx, ny), lambda i: (0, i, 0, 0))
    faces = [(3, nx, ny), (3 * nz, ny), (nx, LANES)] * 2
    return call(
        body,
        [(nz, nx, ny)] + faces,
        scratch=[(nx, ny)],
        far=(0, 1),
        grid=(steps,),
        in_specs=[spec, spec],
        out_specs=[pl.BlockSpec((step, nx, ny), lambda i: (i, 0, 0))] + [whole(*f) for f in faces],
    )(residual, edge_diag)


def plane(values, row_count):
    return jnp.concatenate([values, jnp.zeros((row_count - values.shape[0], LANES), F32)], axis=0)


def nodal_stage(part, node_shift, coarse_shift, got_z, got_x, got_y, low_z, z_count):
    nz, nx, ny = part.shape
    cz, cx, cy = nz // 2, nx // 2, ny // 2
    rows = cx + 8
    sends = 1 if z_count == 2 else 2

    def body(part, shift, coarse, gz, gx, gy, low_z, fg, rhs, xb, yb, w, *rest):
        out, (pair, s_, xl_, yl_, zl_, zh_) = rest[:sends], rest[sends:]
        lane = lane_ids(nx)
        row = row_ids(nx)
        lane_c = lane_ids(rows)
        row_c = row_ids(rows)
        below_z = from_below("gz", gz[0])
        below_y = from_below("gy", gy[...])
        fine = lax.broadcasted_iota(jnp.int32, (ny, 2 * LANES), 0)
        coarse_lane = lax.broadcasted_iota(jnp.int32, (ny, 2 * LANES), 1)
        miss = jnp.where(
            coarse_lane < LANES, fine // 2 - coarse_lane, fine - 2 * (coarse_lane - LANES)
        )
        gather = jnp.where(miss == 0, 1.0, 0.0)
        for c in range(cz):
            both = []
            for z in (2 * c, 2 * c + 1):
                total = part[z]
                if z == 0:
                    total += below_z
                total += jnp.where(row == 0, from_below("gx", gx[nz + z : nz + z + 1, :]), 0.0)
                total += jnp.where(lane == 0, shift_lanes(below_y, -(2 * nz + z)), 0.0)
                guess = total / (6.0 + shift[z])
                fg[z] = guess
                both.append(guess)
            pair[c % 2] = both[0] + both[1]
            low = pair[c % 2, pl.ds(0, cx, 2), :]
            high = pair[c % 2, pl.ds(1, cx, 2), :]
            first = fg[2 * c, pl.ds(0, cx, 2), :] + fg[2 * c, pl.ds(1, cx, 2), :]
            stacked = jnp.concatenate([low + high, low, first], axis=0)
            sums = jnp.dot(stacked, gather, precision=HIGHEST, preferred_element_type=F32)
            s = sums[:cx, :LANES]
            z_low = sums[2 * cx :, :LANES]
            s_[c] = plane(s, rows)
            yl_[c] = plane(sums[:cx, LANES:], rows)
            xl_[c] = plane(sums[cx : 2 * cx, :LANES], rows)
            zl_[c] = plane(z_low, rows)
            zh_[c] = plane(s - z_low, rows)
            w[c] = jnp.zeros((rows, LANES), F32)
            w[c, :cx, :cy] = 1.0 / (6.0 + coarse[c])
        for c in range(cz):
            s, x_low, y_low = s_[c], xl_[c], yl_[c]
            x_high = s - x_low
            y_high = s - y_low
            total = 3.0 * s
            total += shift_rows(x_low, -1) + shift_rows(x_high, 1)
            total += shift_lanes(y_low, -1) + shift_lanes(y_high, 1)
            if c > 0:
                total += zh_[c - 1]
            if c < cz - 1:
                total += zl_[c + 1]
            rhs[c] = total
            xb[c] = jnp.where(row_c < cx // 2, x_low, x_high)
            yb[c] = jnp.where(lane_c < cy // 2, y_low, y_high)
        rhs[cz] = zh_[cz - 1]
        rhs[cz + 1] = jnp.zeros((rows, LANES), F32)
        rhs[cz + 2] = jnp.zeros((rows, LANES), F32)
        rhs[cz + 3] = zl_[0]

        def fill(ref, near, far, half, face):
            planes = [rhs[near], rhs[far], w[near], w[far], half]
            planes += [xb[near], xb[far], yb[near], yb[far]]
            for i, value in enumerate(planes):
                ref[i * rows : (i + 1) * rows, :] = value
            ref[9 * rows : 9 * rows + nx, :] = face

        def tail(ref, values):
            for i, value in enumerate(values):
                at = 9 * rows + nx + i * nx
                ref[at : at + nx, :] = value

        def up(ref):
            fill(ref, cz - 1, cz - 2, zh_[cz - 1], fg[nz - 1])
            tail(ref, [jnp.zeros((nx, LANES), F32)] * 5)

        def down(ref):
            fill(ref, 0, 1, zl_[0], fg[0])
            here = fg[0]
            around = fg[1] + jnp.where(row == 0, 0.0, shift_rows(here, 1))
            around += jnp.where(row == nx - 1, 0.0, shift_rows(here, -1))
            around += jnp.where(lane == 0, 0.0, shift_lanes(here, 1))
            around += jnp.where(lane == ny - 1, 0.0, shift_lanes(here, -1))
            inverse = 1.0 / (6.0 + shift[0])
            tail(ref, [low_z[0], low_z[1], low_z[2], here + inverse * around, inverse])

        write_sides("gz", out, up, down)

    coarse = (cz, rows, LANES)
    send = (9 * rows + 6 * nx, LANES)
    return call(
        body,
        [(nz, nx, ny), (cz + 4, rows, LANES), coarse, coarse, coarse] + [send] * sends,
        scratch=[(2, nx, ny), coarse, coarse, coarse, coarse, coarse],
        in_specs=vmem(7),
        out_specs=vmem(5 + sends),
    )(part, node_shift, coarse_shift, got_z, got_x, got_y, low_z)


def x_stage(got, rhs, xb, yb, w, fg, z_count, x_count):
    planes, rows, _ = rhs.shape
    cz, cx = planes - 4, rows - 8
    nz, nx, ny = fg.shape
    cy = ny // 2
    sends = 1 if x_count == 2 else 2
    gots = len(got)
    size = -(-(3 * planes + nz + 1) // 8) * 8

    def body(*refs):
        got = refs[:gots]
        rhs, xb, yb, w, fg, rhs2, yb2, w2 = refs[gots : gots + 8]
        out, (xb2,) = refs[gots + 8 : gots + 8 + sends], refs[gots + 8 + sends :]

        def take_at(pick, at):
            values = [ref[at, :] for ref in got]
            return pick("gz", z_count, values[0], values[1] if gots > 1 else None)

        def take(pick, i):
            return take_at(pick, slice(i * rows, (i + 1) * rows))

        for c in range(1, cz - 1):
            rhs2[c] = rhs[c]
        rhs2[0] = rhs[0] + take(low_of, 4)
        rhs2[cz - 1] = rhs[cz - 1] + take(high_of, 4)
        rhs2[cz] = rhs[cz] + take(high_of, 0)
        rhs2[cz + 1] = take(high_of, 1)
        rhs2[cz + 2] = take(low_of, 1)
        rhs2[cz + 3] = rhs[cz + 3] + take(low_of, 0)
        for here, there, i in ((w, w2, 2), (xb, xb2, 5), (yb, yb2, 7)):
            for c in range(cz):
                there[c] = here[c]
            there[cz] = take(high_of, i)
            there[cz + 1] = take(high_of, i + 1)
            there[cz + 2] = take(low_of, i + 1)
            there[cz + 3] = take(low_of, i)

        lane = lane_ids(planes)

        def fill(ref, near, far, fine):
            halves = lane < cy
            first = jnp.where(halves, rhs2[:, near, :], shift_lanes(rhs2[:, far, :], cy))
            second = jnp.where(halves, w2[:, near, :], shift_lanes(w2[:, far, :], cy))
            edge = yb2[:, far, :]
            third = jnp.where(halves, xb2[:, near, :], shift_lanes(yb2[:, near, :], cy))
            third = jnp.where(lane == cy + 1, shift_lanes(edge, cy + 1), third)
            third = jnp.where(lane == LANES - 2, shift_lanes(edge, cy - 1), third)
            for i, value in enumerate((first, second, third)):
                ref[i * planes : (i + 1) * planes, :] = value
            ref[3 * planes : 3 * planes + nz, :] = fg[:, fine, :]
            at = 9 * rows + fine
            last = 3 * planes + nz
            ref[last : last + 1, :] = take_at(high_of, slice(at, at + 1))
            ref[last + 1 :, :] = jnp.zeros((size - last - 1, LANES), F32)

        def up(ref):
            fill(ref, cx - 1, cx - 2, nx - 1)

        def down(ref):
            fill(ref, 0, 1, 0)

        write_sides("gx", out, up, down)

    whole = (planes, rows, LANES)
    return call(
        body,
        [whole, whole, whole] + [(size, LANES)] * sends,
        scratch=[whole],
        in_specs=vmem(gots + 5),
        out_specs=vmem(3 + sends),
    )(*got, rhs, xb, yb, w, fg)


def x_tail(got, fg, node_shift, low_x, after, z_count):
    nz, nx, ny = fg.shape
    z_at = 9 * (nx // 2 + 8)
    gots = len(got)

    def body(*refs):
        got = refs[:gots]
        fg, shift, low_x, _, out = refs[gots:]
        lane = lane_ids(nz)
        row = row_ids(nz)

        def z_row(pick):
            values = [ref[z_at : z_at + 1, :] for ref in got]
            return pick("gz", z_count, values[0], values[1] if gots > 1 else None)

        here = fg[:, 0, :]
        around = fg[:, 1, :] + jnp.where(row == 0, z_row(low_of), shift_rows(here, 1))
        around += jnp.where(row == nz - 1, z_row(high_of), shift_rows(here, -1))
        around += jnp.where(lane == 0, 0.0, shift_lanes(here, 1))
        around += jnp.where(lane == ny - 1, 0.0, shift_lanes(here, -1))
        inverse = 1.0 / (6.0 + shift[:, 0, :])
        out[: 3 * nz, :] = low_x[...]
        out[3 * nz : 4 * nz, :] = here + inverse * around
        out[4 * nz :, :] = inverse

    return call(
        body, [(5 * nz, LANES)], in_specs=vmem(gots + 4), out_specs=vmem(1)
    )(*got, fg, node_shift, low_x, after)[0]


def part_stage(got, fg, node_shift, after, z_count):
    nz, nx, ny = fg.shape
    z_at = 9 * (nx // 2 + 8)
    gots = len(got)

    def body(*refs):
        got = refs[:gots]
        fg, shift, _, part, inv = refs[gots:]
        lane = lane_ids(nx)
        row = row_ids(nx)

        def z_face(pick):
            values = [ref[z_at : z_at + nx, :] for ref in got]
            return pick("gz", z_count, values[0], values[1] if gots > 1 else None)

        for z in range(nz):
            guess = fg[z]
            around = fg[z - 1] if z > 0 else z_face(low_of)
            around += fg[z + 1] if z < nz - 1 else z_face(high_of)
            around += jnp.where(row == 0, 0.0, shift_rows(guess, 1))
            around += jnp.where(row == nx - 1, 0.0, shift_rows(guess, -1))
            around += jnp.where(lane == 0, 0.0, shift_lanes(guess, 1))
            around += jnp.where(lane == ny - 1, 0.0, shift_lanes(guess, -1))
            inverse = 1.0 / (6.0 + shift[z])
            inv[z] = inverse
            part[z] = guess + inverse * around

    return call(
        body, [fg.shape, fg.shape], in_specs=vmem(gots + 3), out_specs=vmem(2)
    )(*got, fg, node_shift, after)


def line(source, lane, fine, at):
    acc = jnp.zeros(lane.shape, F32)
    for z in range(source.shape[0]):
        moved = jnp.broadcast_to(source[z : z + 1, :], lane.shape)
        acc = jnp.where(lane == at + z, shift_lanes(moved, at + z - fine), acc)
    return acc


def y_stage(got, rhs, yb, w, early, x_count, y_count):
    planes, rows, _ = rhs.shape
    cx = rows - 8
    nx, cy = 2 * cx, LANES // 2
    nz, half = 2 * (planes - 4), nx // 2
    sends = 1 if y_count == 2 else 2
    gots = len(got)

    def body(*refs):
        got = refs[:gots]
        rhs, yb, w, up_, down_, part, inv, _, _, rhs3, w3 = refs[gots : gots + 11]
        rest = refs[gots + 11 :]
        out, (yb3, add) = rest[:sends], rest[sends:]
        lane_p = lane_ids(planes)

        def take_at(pick, at):
            values = [ref[at, :] for ref in got]
            return pick("gx", x_count, values[0], values[1] if gots > 1 else None)

        def take(pick, i):
            return take_at(pick, slice(i * planes, (i + 1) * planes))

        add[...] = jnp.zeros_like(add)
        for c in range(planes):
            w3[c] = w[c]
            yb3[c] = yb[c]
        for pick, near, far, edge in ((high_of, cx, cx + 1, cx - 1), (low_of, rows - 1, rows - 2, 0)):
            first, second, third = take(pick, 0), take(pick, 1), take(pick, 2)
            other = shift_lanes(third, -cy)
            one = jnp.where((lane_p == 0) | (lane_p == cy - 1), other, 0.0)
            two = jnp.where(lane_p == 0, shift_lanes(third, -cy - 1), 0.0)
            two = jnp.where(lane_p == cy - 1, shift_lanes(third, 1 - cy), two)
            yb3[:, near, :] = one
            yb3[:, far, :] = two
            for at, value, ends in ((near, first, one), (far, shift_lanes(first, -cy), two)):
                value = jnp.where(lane_p < cy, value, 0.0)
                value += jnp.where(lane_p == cy, shift_lanes(ends, 1), 0.0)
                value += jnp.where(lane_p == LANES - 1, shift_lanes(ends, -1), 0.0)
                add[:, at, :] = value
            w3[:, near, :] = jnp.where(lane_p < cy, second, 0.0)
            w3[:, far, :] = jnp.where(lane_p < cy, shift_lanes(second, -cy), 0.0)
            add[:, edge, :] = jnp.where(lane_p < cy, third, 0.0)
        for c in range(planes):
            rhs3[c] = rhs[c] + add[c]

        lane_c = lane_ids(rows)
        lane8 = lane_ids(8)
        base = 5 * planes
        x_face = slice(3 * planes, 3 * planes + nz)
        x_high = take_at(high_of, x_face)

        def fill(ref, near, far, fine, early):
            acc = jnp.zeros((rows, LANES), F32)
            jobs = ((rhs3, near), (rhs3, far), (w3, near), (w3, far), (yb3, near))
            for i, (field, at) in enumerate(jobs):
                for z in range(planes):
                    spot = i * planes + z
                    acc = jnp.where(lane_c == spot, shift_lanes(field[z], spot - at), acc)
            ref[:nx, :] = plane(acc, nx) + early[...]
            ref[nx : nx + 8, :] = line(x_high, lane8, fine, base)

        def up(ref):
            fill(ref, cy - 1, cy - 2, 2 * cy - 1, up_)
            ref[nx + 8 :, :] = jnp.zeros((half, LANES), F32)

        def down(ref):
            fill(ref, 0, 1, 0, down_)
            row = row_ids(nx)
            ends = jnp.where(row == 0, line(take_at(low_of, x_face), lane8, 0, 0)[:1, :], 0.0)
            ends += jnp.where(row == nx - 1, line(x_high, lane8, 0, 0)[:1, :], 0.0)
            inverse = inv[...]
            value = part[...] + inverse * ends
            packed = jnp.zeros((half, LANES), F32)
            for i, source in enumerate((value[:half], value[half:], inverse[:half], inverse[half:])):
                there = lane_ids(half) // nz == i
                packed = jnp.where(there, shift_lanes(source, i * nz), packed)
            ref[nx + 8 :, :] = packed

        write_sides("gy", out, up, down)

    whole = (planes, rows, LANES)
    return call(
        body,
        [whole, whole] + [(nx + 8 + half, LANES)] * sends,
        scratch=[whole, whole],
        in_specs=vmem(gots + 9),
        out_specs=vmem(2 + sends),
    )(*got, rhs, yb, w, *early)


def y_early(got_z, fg, node_shift, low_y, after, planes, z_count):
    nz, nx, _ = fg.shape
    z_at = 9 * (nx // 2 + 8)
    base = 5 * planes
    n_z = len(got_z)

    def body(*refs):
        gz = refs[:n_z]
        fg, shift, low_y, _, up, down, part, inv = refs[n_z:]
        lane = lane_ids(nx)
        row = row_ids(nx)

        def side(pick):
            values = [ref[z_at : z_at + nx, :] for ref in gz]
            return pick("gz", z_count, values[0], values[1] if n_z > 1 else None)

        above = side(high_of)
        here = jnp.where(lane == nz, shift_lanes(above, nz), 0.0)
        here = jnp.where(lane == LANES - 1, shift_lanes(side(low_of), -1), here)
        high = jnp.where(lane == base + nz, shift_lanes(above, base + nz + 1), 0.0)
        inverse = jnp.ones((nx, LANES), F32)
        inner = jnp.zeros((nx, LANES), F32)
        for z in range(nz):
            guess = fg[z]
            here = jnp.where(lane == z, shift_lanes(guess, z), here)
            inner = jnp.where(lane == z, shift_lanes(guess, z - 1), inner)
            high = jnp.where(lane == base + z, shift_lanes(guess, base + z + 1), high)
            inverse = jnp.where(lane == z, shift_lanes(6.0 + shift[z], z), inverse)
        inverse = 1.0 / inverse
        around = inner + shift_lanes(here, 1) + shift_lanes(here, -1)
        around += jnp.where(row == 0, 0.0, shift_rows(here, 1))
        around += jnp.where(row == nx - 1, 0.0, shift_rows(here, -1))
        up[...] = high
        at = base + nz + 1
        low = jnp.where((lane >= base) & (lane < at), shift_lanes(here, base), 0.0)
        down[...] = jnp.where((lane >= at) & (lane < at + 3 * nz), shift_lanes(low_y[...], at), low)
        part[...] = here + inverse * around
        inv[...] = inverse

    return call(
        body, [(nx, LANES)] * 4, in_specs=vmem(n_z + 4), out_specs=vmem(4)
    )(*got_z, fg, node_shift, low_y, after)


def coarse_stage(got, rhs, w, after, y_count, devices):
    planes, rows, _ = rhs.shape
    cz, cx = planes - 4, rows - 8
    cy = LANES // 2
    gots = len(got)

    def body(*refs):
        got = refs[:gots]
        rhs, w, _, v1, v2, sums, tot, inv_, image_ = refs[gots:]
        values = [ref[:rows, :] for ref in got]
        second = values[1] if gots > 1 else None
        low = low_of("gy", y_count, values[0], second)
        high = high_of("gy", y_count, values[0], second)
        lane = lane_ids(rows)
        spots_r = ((cy, high, 0), (cy + 1, high, 1), (LANES - 1, low, 0), (LANES - 2, low, 1))
        spots_r += ((cy - 1, high, 4), (0, low, 4))
        for z in range(planes):
            right = rhs[z]
            for at, source, i in spots_r:
                moved = shift_lanes(source, at - (i * planes + z))
                right += jnp.where(lane == at, moved, 0.0)
            inv = w[z]
            for at, source, i in spots_r[:4]:
                moved = shift_lanes(source, at - ((i + 2) * planes + z))
                inv = jnp.where(lane == at, moved, inv)
            inv_[z] = inv
            tot[z] = right
            v1[z] = right * inv

        def near(field, z):
            here = field[z]
            total = field[(z + 1) % planes] + field[(z - 1) % planes]
            total += shift_rows(here, 1) + shift_rows(here, -1)
            return total + shift_lanes(here, 1) + shift_lanes(here, -1)

        v2[cz + 1] = jnp.zeros((rows, LANES), F32)
        v2[cz + 2] = jnp.zeros((rows, LANES), F32)
        for z in list(range(cz + 1)) + [planes - 1]:
            image = tot[z] - near(v1, z)
            if z < cz:
                image_[z] = image
            v2[z] = image * inv_[z]
        parts = [jnp.zeros((cx, LANES), F32)] * 5
        for z in range(cz):
            first, second_, right, image = v1[z], v2[z], tot[z], image_[z]
            third = image - near(v2, z)
            terms = (first * right, second_ * right, first * image, second_ * image, second_ * third)
            parts = [a + b[:cx, :] for a, b in zip(parts, terms)]
        keep = lane_ids(1) < cy
        lines = [jnp.where(keep, jnp.sum(a, axis=0, keepdims=True), 0.0) for a in parts]
        tile = jnp.concatenate(lines + [jnp.zeros((3, LANES), F32)], axis=0)
        column = jnp.sum(tile, axis=1, keepdims=True)
        spread = jnp.where(lane_ids(8) == row_ids(8), column, 0.0)
        line = jnp.sum(spread, axis=0, keepdims=True)
        sums[...] = jnp.broadcast_to(line[None], (devices, 1, LANES))

    whole = (planes, rows, LANES)
    return call(
        body,
        [whole, whole, (devices, 1, LANES)],
        scratch=[whole, whole, whole],
        in_specs=vmem(gots + 3),
        out_specs=vmem(3),
    )(*got, rhs, w, *after)


def smooth_stage(residual, edge_diag, below, got_z, tail_x, after, counts):
    _, nz, nx, ny = residual.shape
    n_z = len(got_z)
    rows = nx // 2 + 8

    def body(*refs):
        res, diag, lz, lx, ly = refs[:5]
        gz = refs[5 : 5 + n_z]
        gx, _, out, last, s = refs[5 + n_z :]
        lane = lane_ids(nx)
        row = row_ids(nx)
        y_low = from_below("gy", ly[...])

        def above_of(refs, axis, size, at):
            values = [ref[at, :] for ref in refs]
            return high_of(axis, size, values[0], values[1] if len(values) > 1 else None)

        acc = jnp.zeros((nx, LANES), F32)
        for k in range(3):
            for z in range(nz):
                inverse = 1.0 / diag[k, z]
                out[k, z] = inverse
                s[z] = res[k, z] * inverse
            z_low = from_below("gz", lz[k])
            at = 9 * rows + nx + k * nx
            z_high = above_of(gz, "gz", counts[0], slice(at, at + nx))
            x_low = from_below("gx", lx[k * nz : (k + 1) * nz, :])
            x_high = from_above("gx", counts[1], gx[k * nz : (k + 1) * nz, :])
            for z in range(nz):
                here = s[z]
                around = s[z - 1] if z > 0 else z_low
                around += s[z + 1] if z < nz - 1 else z_high
                around += jnp.where(row == 0, x_low[z : z + 1, :], shift_rows(here, 1))
                around += jnp.where(row == nx - 1, x_high[z : z + 1, :], shift_rows(here, -1))
                spot = k * nz + z
                around += jnp.where(lane == 0, shift_lanes(y_low, -spot), shift_lanes(here, 1))
                around += jnp.where(lane == LANES - 1, 0.0, shift_lanes(here, -1))
                inverse = out[k, z]
                acc = jnp.where(lane == spot, shift_lanes(inverse, spot + 1), acc)
                out[k, z] = here + around * inverse
        last[...] = acc

    return call(
        body,
        [residual.shape, (nx, LANES)],
        scratch=[(nz, nx, ny)],
        free=(0, 1),
        in_specs=vmem(7 + n_z),
        out_specs=vmem(2),
    )(residual, edge_diag, *below, *got_z, tail_x, after)


def final_stage(sums, v1, v2, fg, mid, smooth, last, tail_x, got_z, got_x, got_y, counts):
    planes, rows, _ = v1.shape
    cz, cx, cy = planes - 4, rows - 8, LANES // 2
    nz, nx, _ = fg.shape
    n_z, n_x, n_y = len(got_z), len(got_x), len(got_y)
    gots = n_z + n_x + n_y

    def body(*refs):
        sums, v1, v2, fg, part, inv, smooth, last, tx = refs[:9]
        gz = refs[9 : 9 + n_z]
        gx = refs[9 + n_z : 9 + n_z + n_x]
        gy = refs[9 + n_z + n_x : 9 + gots]
        out, sol, dup, inter, small, lines, buf, sem = refs[9 + gots :]

        def one_side(pick, refs, axis, size, at):
            values = [ref[at, :] for ref in refs]
            return pick(axis, size, values[0], values[1] if len(values) > 1 else None)

        def both(refs, axis, size, at):
            return [one_side(pick, refs, axis, size, at) for pick in (low_of, high_of)]

        total = jnp.sum(sums[...], axis=0)
        lane1 = lane_ids(1)
        gone, gtwo, hone, hmix, htwo = [
            jnp.sum(jnp.where(lane1 == i, total, 0.0), axis=1, keepdims=True) for i in range(5)
        ]
        two = (gtwo - hmix * gone / hone) / (htwo - hmix * hmix / hone)
        one = (gone - hmix * two) / hone
        source = lax.broadcasted_iota(jnp.int32, (LANES, 2 * LANES), 0)
        target = lax.broadcasted_iota(jnp.int32, (LANES, 2 * LANES), 1)
        fine = target - LANES
        side = jnp.where(fine % 2 == 1, fine // 2 + 1, (fine // 2 + LANES - 1) % LANES)
        spread = jnp.where(jnp.where(target < LANES, target // 2, side) == source, 1.0, 0.0)
        for z in list(range(cz + 1)) + [planes - 1]:
            sol[z] = one * v1[z] + two * v2[z]
            dup[z] = jnp.dot(sol[z], spread, precision=HIGHEST, preferred_element_type=F32)

        z_at = 9 * rows
        z_base = one_side(high_of, gz, "gz", counts[0], slice(z_at + 4 * nx, z_at + 5 * nx))
        z_inverse = one_side(high_of, gz, "gz", counts[0], slice(z_at + 5 * nx, z_at + 6 * nx))
        x_low, x_high = both(gx, "gx", counts[1], slice(3 * planes, 3 * planes + nz + 1))
        y_low, y_high = both(gy, "gy", counts[2], slice(0, nx))
        y_row_low, y_row_high = both(gy, "gy", counts[2], slice(nx, nx + 1))
        half = nx // 2
        y_pack = one_side(high_of, gy, "gy", counts[2], slice(nx + 8, nx + 8 + half))
        lane = lane_ids(nx)
        row = row_ids(nx)
        base = 5 * planes

        def spread_around(z):
            c, odd = z // 2, z % 2
            here = dup[c, :, :LANES]
            same = 3.0 * here + dup[c, :, LANES:]
            same += dup[(c + 1 if odd else c - 1) % planes, :, :LANES]
            slot = z % 2
            inter[slot, pl.ds(0, cx, 2), :] = (same + shift_rows(here, 1))[:cx, :]
            inter[slot, pl.ds(1, cx, 2), :] = (same + shift_rows(here, -1))[:cx, :]
            return inter[slot]

        def nodal(z):
            around = spread_around(z) + jnp.where(row == 0, x_low[z : z + 1, :], 0.0)
            around += jnp.where(row == nx - 1, x_high[z : z + 1, :], 0.0)
            around += jnp.where(lane == 0, shift_lanes(y_low, -(base + z)), 0.0)
            around += jnp.where(lane == LANES - 1, shift_lanes(y_high, -(base + z) - 1), 0.0)
            if z == nz:
                value = z_base + z_inverse * (around + fg[nz - 1])
                return from_above("gz", counts[0], value)
            return part[z] + inv[z] * around

        here = dup[:cz, cx, :LANES]
        same = 3.0 * here + dup[:cz, cx, LANES:] + dup[:cz, cx - 1, :LANES]
        small[pl.ds(0, cz, 2), :] = same + jnp.concatenate(
            [dup[planes - 1, cx : cx + 1, :LANES], here[: cz - 1]], axis=0
        )
        small[pl.ds(1, cz, 2), :] = same + dup[1 : cz + 1, cx, :LANES]
        for z in range(nz):
            left = shift_lanes(y_row_low, -(base + z))
            right = shift_lanes(y_row_high, -(base + z) - 1)
            value = jnp.where(lane1 == 0, left, 0.0)
            lines[z : z + 1, :] = jnp.where(lane1 == LANES - 1, right, value)
        x_value = tx[3 * nz : 4 * nz, :] + tx[4 * nz :, :] * (
            fg[:, nx - 1, :] + small[...] + lines[...]
        )
        x_value = from_above("gx", counts[1], x_value)

        lane_c = lane_ids(rows)
        even = jnp.zeros((rows, LANES), F32)
        odd = jnp.zeros((rows, LANES), F32)
        own = jnp.zeros((nx, LANES), F32)
        for z in range(nz):
            c = z // 2
            here = sol[c]
            same = 3.0 * here + shift_lanes(here, 1) + sol[(c + 1 if z % 2 else c - 1) % planes]
            even = jnp.where(lane_c == z, shift_lanes(same + shift_rows(here, 1), z - cy), even)
            odd = jnp.where(lane_c == z, shift_lanes(same + shift_rows(here, -1), z - cy), odd)
            own = jnp.where(lane == z, shift_lanes(fg[z], z + 1), own)
        inter[0, pl.ds(0, cx, 2), :] = even[:cx, :]
        inter[0, pl.ds(1, cx, 2), :] = odd[:cx, :]
        y_base = jnp.concatenate([y_pack, shift_lanes(y_pack, -nz)], axis=0)
        y_inverse = jnp.concatenate(
            [shift_lanes(y_pack, -2 * nz), shift_lanes(y_pack, -3 * nz)], axis=0
        )
        y_value = y_base + y_inverse * (own + inter[0])
        y_value = from_above("gy", counts[2], y_value)
        y_fix = shift_lanes(y_high, -(base + nz + 1)) * last[...]

        def copy(z):
            return pltpu.make_async_copy(buf.at[:, z], out.at[:, z], sem.at[z])

        value = nodal(0)
        for z in range(nz):
            after = nodal(z + 1)
            steps = [after, jnp.where(row == nx - 1, x_value[z : z + 1, :], shift_rows(value, -1))]
            steps.append(
                jnp.where(lane == LANES - 1, shift_lanes(y_value, -z - 1), shift_lanes(value, -1))
            )
            for k in range(3):
                fixed = jnp.where(lane == LANES - 1, shift_lanes(y_fix, -(k * nz + z) - 1), 0.0)
                buf[k, z] = (smooth[k, z] + fixed) + (steps[k] - value)
            copy(z).start()
            value = after
        for z in range(nz):
            copy(z).wait()

    return call(
        body,
        [smooth.shape],
        scratch=[
            (planes, rows, LANES),
            (planes, rows, 2 * LANES),
            (2, nx, LANES),
            (nz, LANES),
            (nz, LANES),
            smooth.shape,
            pltpu.SemaphoreType.DMA((nz,)),
        ],
        far_out=True,
        in_specs=vmem(9 + gots),
        out_specs=[pl.BlockSpec(memory_space=pltpu.HBM)],
    )(sums, v1, v2, fg, *mid, smooth, last, tail_x, *got_z, *got_x, *got_y)[0]


def local(residual, edge_diag, node_shift, coarse_shift):
    axes = ("gz", "gx", "gy")
    counts = tuple(lax.axis_size(a) for a in axes)
    devices = counts[0] * counts[1] * counts[2]
    part, up_z, up_x, up_y, low_z, low_x, low_y = edge_stage(residual, edge_diag)
    below = (ring(up_z, "gz", 1), ring(up_x, "gx", 1), ring(up_y, "gy", 1))
    fg, rhs, xb, yb, w, *send = nodal_stage(part, node_shift, coarse_shift, *below, low_z, counts[0])
    got_z = swap(send, "gz")
    rhs, yb, w, *send = x_stage(got_z, rhs, xb, yb, w, fg, counts[0], counts[1])
    got_x = swap(send, "gx")
    planes = rhs.shape[0]
    tail_x = x_tail(got_z, fg, node_shift, low_x, w, counts[0])
    mid = part_stage(got_z, fg, node_shift, w, counts[0])
    early = y_early(got_z, fg, node_shift, low_y, w, planes, counts[0])
    early = (*early, tail_x, mid[1])
    tail_x = ring(tail_x, "gx", -1)
    rhs, w, *send = y_stage(got_x, rhs, yb, w, early, counts[1], counts[2])
    got_y = swap(send, "gy")
    smooth, last = smooth_stage(residual, edge_diag, below, got_z, tail_x, w, counts)
    v1, v2, sums = coarse_stage(got_y, rhs, w, (last,), counts[2], devices)
    sums = lax.all_to_all(sums, ("gx", "gy", "gz"), 0, 0)
    return final_stage(sums, v1, v2, fg, mid, smooth, last, tail_x, got_z, got_x, got_y, counts)


def solution(mesh):
    placed = (
        P(None, "gz", "gx", "gy"),
        P(None, "gz", "gx", "gy"),
        P("gz", "gx", "gy"),
        P("gz", "gx", "gy"),
    )

    return jax.shard_map(
        local, mesh=mesh, in_specs=placed, out_specs=P(None, "gz", "gx", "gy"), check_vma=False
    )
```

```python
import jax
import jax.numpy as jnp
from jax import lax
from jax.experimental import pallas as pl
from jax.experimental.pallas import tpu as pltpu
from jax.sharding import PartitionSpec as P


F32 = jnp.float32
HIGHEST = lax.Precision.HIGHEST
LANES = 128


def lane_ids(rows):
    return lax.broadcasted_iota(jnp.int32, (rows, LANES), 1)


def row_ids(rows):
    return lax.broadcasted_iota(jnp.int32, (rows, LANES), 0)


def shift_lanes(value, amount):
    return pltpu.roll(value, amount % LANES, 1)


def shift_rows(value, amount):
    return pltpu.roll(value, amount % value.shape[0], 0)


def low_of(axis, size, first, second):
    place = lax.axis_index(axis)
    odd = place % 2 == 1
    zero = jnp.zeros_like(first)
    if second is None:
        return jnp.where(odd, first, zero)
    return jnp.where(odd, first, jnp.where(place > 0, second, zero))


def high_of(axis, size, first, second):
    place = lax.axis_index(axis)
    even = place % 2 == 0
    zero = jnp.zeros_like(first)
    if second is None:
        return jnp.where(even, first, zero)
    return jnp.where(even, first, jnp.where(place < size - 1, second, zero))


def from_below(axis, value):
    return jnp.where(lax.axis_index(axis) > 0, value, jnp.zeros_like(value))


def from_above(axis, size, value):
    return jnp.where(lax.axis_index(axis) < size - 1, value, jnp.zeros_like(value))


def ring(value, axis, step):
    size = lax.axis_size(axis)
    return lax.ppermute(value, axis, [(i, (i + step) % size) for i in range(size)])


def swap(values, axis):
    size = lax.axis_size(axis)
    out = [lax.ppermute(values[0], axis, [(i, i ^ 1) for i in range(size)])]
    if len(values) > 1:
        odd = [(i, (i + 1) % size if i % 2 else (i - 1) % size) for i in range(size)]
        out.append(lax.ppermute(values[1], axis, odd))
    return out


def write_sides(axis, refs, up, down):
    even = lax.axis_index(axis) % 2 == 0

    @pl.when(even)
    def _():
        up(refs[0])
        if len(refs) > 1:
            down(refs[1])

    @pl.when(jnp.logical_not(even))
    def _():
        down(refs[0])
        if len(refs) > 1:
            up(refs[1])


def call(body, outs, scratch=(), far=(), far_out=False, **kwargs):
    kind = jax.ShapeDtypeStruct if far_out else pltpu.VMEM
    run = pl.pallas_call(
        body,
        out_shape=[kind(shape, F32) for shape in outs],
        scratch_shapes=[pltpu.VMEM(s, F32) if isinstance(s, tuple) else s for s in scratch],
        compiler_params=pltpu.CompilerParams(vmem_limit_bytes=12 * 2**20),
        **kwargs,
    )

    def apply(*args):
        spaces = [pltpu.HBM if i in far else pltpu.VMEM for i in range(len(args))]
        return run(
            *(
                pltpu.with_memory_space_constraint(a, space)
                for a, space in zip(args, spaces)
            )
        )

    return apply


def vmem(count):
    return [pl.BlockSpec(memory_space=pltpu.VMEM)] * count


def edge_stage(residual, edge_diag):
    _, nz, nx, ny = residual.shape
    step = 2
    steps = nz // step

    def body(res, diag, part, up_z, up_x, up_y, low_z, low_x, low_y, scaled, inv, near, sems):
        lane = lane_ids(nx)
        row = row_ids(nx)

        def copies(block):
            at = pl.ds(block * step, step)
            return [
                pltpu.make_async_copy(source.at[:, at], target.at[:, at], sems.at[i, block])
                for i, (source, target) in enumerate(((res, near), (diag, inv)))
            ]

        for block in range(steps):
            for copy in copies(block):
                copy.start()
        before = jnp.zeros((nx, ny), F32)
        high = jnp.zeros((nx, LANES), F32)
        low = jnp.zeros((nx, LANES), F32)
        for z in range(nz):
            if z % step == 0:
                for copy in copies(z // step):
                    copy.wait()
            s = []
            for k in range(3):
                inverse = 1.0 / inv[k, z]
                inv[k, z] = inverse
                s.append(near[k, z] * inverse)
                scaled[k, z] = s[k]
            total = before - s[0]
            total += jnp.where(row == 0, 0.0, shift_rows(s[1], 1)) - s[1]
            total += jnp.where(lane == 0, 0.0, shift_lanes(s[2], 1)) - s[2]
            part[z] = total
            before = s[0]
            for k in range(3):
                spot = k * nz + z
                up_x[spot : spot + 1, :] = s[k][nx - 1 :, :]
                low_x[spot : spot + 1, :] = s[k][:1, :]
                high = jnp.where(lane == spot, shift_lanes(s[k], spot + 1), high)
                low = jnp.where(lane == spot, shift_lanes(s[k], spot), low)
                if z == 0:
                    low_z[k] = s[k]
                if z == nz - 1:
                    up_z[k] = s[k]
        up_y[...] = high
        low_y[...] = low

    faces = [(3, nx, ny), (3 * nz, ny), (nx, LANES)] * 2
    return call(
        body,
        [(nz, nx, ny)] + faces + [residual.shape] * 2,
        scratch=[residual.shape, pltpu.SemaphoreType.DMA((2, steps))],
        far=(0, 1),
        in_specs=[pl.BlockSpec(memory_space=pltpu.HBM)] * 2,
        out_specs=vmem(9),
    )(residual, edge_diag)


def plane(values, row_count):
    return jnp.concatenate([values, jnp.zeros((row_count - values.shape[0], LANES), F32)], axis=0)


def nodal_stage(part, node_shift, coarse_shift, got_z, got_x, got_y, low_z, z_count):
    nz, nx, ny = part.shape
    cz, cx, cy = nz // 2, nx // 2, ny // 2
    rows = cx + 8
    sends = 1 if z_count == 2 else 2

    def body(part, shift, coarse, gz, gx, gy, low_z, fg, rhs, xb, yb, w, *rest):
        out, (pair, s_, xl_, yl_, zl_, zh_) = rest[:sends], rest[sends:]
        lane = lane_ids(nx)
        row = row_ids(nx)
        lane_c = lane_ids(rows)
        row_c = row_ids(rows)
        below_z = from_below("gz", gz[0])
        below_y = from_below("gy", gy[...])
        fine = lax.broadcasted_iota(jnp.int32, (ny, 2 * LANES), 0)
        coarse_lane = lax.broadcasted_iota(jnp.int32, (ny, 2 * LANES), 1)
        miss = jnp.where(
            coarse_lane < LANES, fine // 2 - coarse_lane, fine - 2 * (coarse_lane - LANES)
        )
        gather = jnp.where(miss == 0, 1.0, 0.0)
        for c in range(cz):
            both = []
            for z in (2 * c, 2 * c + 1):
                total = part[z]
                if z == 0:
                    total += below_z
                total += jnp.where(row == 0, from_below("gx", gx[nz + z : nz + z + 1, :]), 0.0)
                total += jnp.where(lane == 0, shift_lanes(below_y, -(2 * nz + z)), 0.0)
                guess = total / (6.0 + shift[z])
                fg[z] = guess
                both.append(guess)
            pair[c % 2] = both[0] + both[1]
            low = pair[c % 2, pl.ds(0, cx, 2), :]
            high = pair[c % 2, pl.ds(1, cx, 2), :]
            first = fg[2 * c, pl.ds(0, cx, 2), :] + fg[2 * c, pl.ds(1, cx, 2), :]
            stacked = jnp.concatenate([low + high, low, first], axis=0)
            sums = jnp.dot(stacked, gather, precision=HIGHEST, preferred_element_type=F32)
            s = sums[:cx, :LANES]
            z_low = sums[2 * cx :, :LANES]
            s_[c] = plane(s, rows)
            yl_[c] = plane(sums[:cx, LANES:], rows)
            xl_[c] = plane(sums[cx : 2 * cx, :LANES], rows)
            zl_[c] = plane(z_low, rows)
            zh_[c] = plane(s - z_low, rows)
            w[c] = jnp.zeros((rows, LANES), F32)
            w[c, :cx, :cy] = 1.0 / (6.0 + coarse[c])
        for c in range(cz):
            s, x_low, y_low = s_[c], xl_[c], yl_[c]
            x_high = s - x_low
            y_high = s - y_low
            total = 3.0 * s
            total += shift_rows(x_low, -1) + shift_rows(x_high, 1)
            total += shift_lanes(y_low, -1) + shift_lanes(y_high, 1)
            if c > 0:
                total += zh_[c - 1]
            if c < cz - 1:
                total += zl_[c + 1]
            rhs[c] = total
            xb[c] = jnp.where(row_c < cx // 2, x_low, x_high)
            yb[c] = jnp.where(lane_c < cy // 2, y_low, y_high)
        rhs[cz] = zh_[cz - 1]
        rhs[cz + 1] = jnp.zeros((rows, LANES), F32)
        rhs[cz + 2] = jnp.zeros((rows, LANES), F32)
        rhs[cz + 3] = zl_[0]

        def fill(ref, near, far, half, face):
            planes = [rhs[near], rhs[far], w[near], w[far], half]
            planes += [xb[near], xb[far], yb[near], yb[far]]
            for i, value in enumerate(planes):
                ref[i * rows : (i + 1) * rows, :] = value
            ref[9 * rows : 9 * rows + nx, :] = face

        def tail(ref, values):
            for i, value in enumerate(values):
                at = 9 * rows + nx + i * nx
                ref[at : at + nx, :] = value

        def up(ref):
            fill(ref, cz - 1, cz - 2, zh_[cz - 1], fg[nz - 1])
            tail(ref, [jnp.zeros((nx, LANES), F32)] * 5)

        def down(ref):
            fill(ref, 0, 1, zl_[0], fg[0])
            here = fg[0]
            around = fg[1] + jnp.where(row == 0, 0.0, shift_rows(here, 1))
            around += jnp.where(row == nx - 1, 0.0, shift_rows(here, -1))
            around += jnp.where(lane == 0, 0.0, shift_lanes(here, 1))
            around += jnp.where(lane == ny - 1, 0.0, shift_lanes(here, -1))
            inverse = 1.0 / (6.0 + shift[0])
            tail(ref, [low_z[0], low_z[1], low_z[2], here + inverse * around, inverse])

        write_sides("gz", out, up, down)

    coarse = (cz, rows, LANES)
    send = (9 * rows + 6 * nx, LANES)
    return call(
        body,
        [(nz, nx, ny), (cz + 4, rows, LANES), coarse, coarse, coarse] + [send] * sends,
        scratch=[(2, nx, ny), coarse, coarse, coarse, coarse, coarse],
        in_specs=vmem(7),
        out_specs=vmem(5 + sends),
    )(part, node_shift, coarse_shift, got_z, got_x, got_y, low_z)


def x_stage(got, rhs, xb, yb, w, fg, z_count, x_count):
    planes, rows, _ = rhs.shape
    cz, cx = planes - 4, rows - 8
    nz, nx, ny = fg.shape
    cy = ny // 2
    sends = 1 if x_count == 2 else 2
    gots = len(got)
    size = -(-(3 * planes + nz + 1) // 8) * 8

    def body(*refs):
        got = refs[:gots]
        rhs, xb, yb, w, fg, rhs2, yb2, w2 = refs[gots : gots + 8]
        out, (xb2,) = refs[gots + 8 : gots + 8 + sends], refs[gots + 8 + sends :]

        def take_at(pick, at):
            values = [ref[at, :] for ref in got]
            return pick("gz", z_count, values[0], values[1] if gots > 1 else None)

        def take(pick, i):
            return take_at(pick, slice(i * rows, (i + 1) * rows))

        for c in range(1, cz - 1):
            rhs2[c] = rhs[c]
        rhs2[0] = rhs[0] + take(low_of, 4)
        rhs2[cz - 1] = rhs[cz - 1] + take(high_of, 4)
        rhs2[cz] = rhs[cz] + take(high_of, 0)
        rhs2[cz + 1] = take(high_of, 1)
        rhs2[cz + 2] = take(low_of, 1)
        rhs2[cz + 3] = rhs[cz + 3] + take(low_of, 0)
        for here, there, i in ((w, w2, 2), (xb, xb2, 5), (yb, yb2, 7)):
            for c in range(cz):
                there[c] = here[c]
            there[cz] = take(high_of, i)
            there[cz + 1] = take(high_of, i + 1)
            there[cz + 2] = take(low_of, i + 1)
            there[cz + 3] = take(low_of, i)

        lane = lane_ids(planes)

        def fill(ref, near, far, fine):
            halves = lane < cy
            first = jnp.where(halves, rhs2[:, near, :], shift_lanes(rhs2[:, far, :], cy))
            second = jnp.where(halves, w2[:, near, :], shift_lanes(w2[:, far, :], cy))
            edge = yb2[:, far, :]
            third = jnp.where(halves, xb2[:, near, :], shift_lanes(yb2[:, near, :], cy))
            third = jnp.where(lane == cy + 1, shift_lanes(edge, cy + 1), third)
            third = jnp.where(lane == LANES - 2, shift_lanes(edge, cy - 1), third)
            for i, value in enumerate((first, second, third)):
                ref[i * planes : (i + 1) * planes, :] = value
            ref[3 * planes : 3 * planes + nz, :] = fg[:, fine, :]
            at = 9 * rows + fine
            last = 3 * planes + nz
            ref[last : last + 1, :] = take_at(high_of, slice(at, at + 1))
            ref[last + 1 :, :] = jnp.zeros((size - last - 1, LANES), F32)

        def up(ref):
            fill(ref, cx - 1, cx - 2, nx - 1)

        def down(ref):
            fill(ref, 0, 1, 0)

        write_sides("gx", out, up, down)

    whole = (planes, rows, LANES)
    return call(
        body,
        [whole, whole, whole] + [(size, LANES)] * sends,
        scratch=[whole],
        in_specs=vmem(gots + 5),
        out_specs=vmem(3 + sends),
    )(*got, rhs, xb, yb, w, fg)


def x_tail(got, fg, node_shift, low_x, after, z_count):
    nz, nx, ny = fg.shape
    z_at = 9 * (nx // 2 + 8)
    gots = len(got)

    def body(*refs):
        got = refs[:gots]
        fg, shift, low_x, _, out = refs[gots:]
        lane = lane_ids(nz)
        row = row_ids(nz)

        def z_row(pick):
            values = [ref[z_at : z_at + 1, :] for ref in got]
            return pick("gz", z_count, values[0], values[1] if gots > 1 else None)

        here = fg[:, 0, :]
        around = fg[:, 1, :] + jnp.where(row == 0, z_row(low_of), shift_rows(here, 1))
        around += jnp.where(row == nz - 1, z_row(high_of), shift_rows(here, -1))
        around += jnp.where(lane == 0, 0.0, shift_lanes(here, 1))
        around += jnp.where(lane == ny - 1, 0.0, shift_lanes(here, -1))
        inverse = 1.0 / (6.0 + shift[:, 0, :])
        out[: 3 * nz, :] = low_x[...]
        out[3 * nz : 4 * nz, :] = here + inverse * around
        out[4 * nz :, :] = inverse

    return call(
        body, [(5 * nz, LANES)], in_specs=vmem(gots + 4), out_specs=vmem(1)
    )(*got, fg, node_shift, low_x, after)[0]


def part_stage(got, fg, node_shift, after, z_count):
    nz, nx, ny = fg.shape
    z_at = 9 * (nx // 2 + 8)
    gots = len(got)

    def body(*refs):
        got = refs[:gots]
        fg, shift, _, part, inv = refs[gots:]
        lane = lane_ids(nx)
        row = row_ids(nx)

        def z_face(pick):
            values = [ref[z_at : z_at + nx, :] for ref in got]
            return pick("gz", z_count, values[0], values[1] if gots > 1 else None)

        for z in range(nz):
            guess = fg[z]
            around = fg[z - 1] if z > 0 else z_face(low_of)
            around += fg[z + 1] if z < nz - 1 else z_face(high_of)
            around += jnp.where(row == 0, 0.0, shift_rows(guess, 1))
            around += jnp.where(row == nx - 1, 0.0, shift_rows(guess, -1))
            around += jnp.where(lane == 0, 0.0, shift_lanes(guess, 1))
            around += jnp.where(lane == ny - 1, 0.0, shift_lanes(guess, -1))
            inverse = 1.0 / (6.0 + shift[z])
            inv[z] = inverse
            part[z] = guess + inverse * around

    return call(
        body, [fg.shape, fg.shape], in_specs=vmem(gots + 3), out_specs=vmem(2)
    )(*got, fg, node_shift, after)


def line(source, lane, fine, at):
    acc = jnp.zeros(lane.shape, F32)
    for z in range(source.shape[0]):
        moved = jnp.broadcast_to(source[z : z + 1, :], lane.shape)
        acc = jnp.where(lane == at + z, shift_lanes(moved, at + z - fine), acc)
    return acc


def y_stage(got, rhs, yb, w, early, x_count, y_count):
    planes, rows, _ = rhs.shape
    cx = rows - 8
    nx, cy = 2 * cx, LANES // 2
    nz, half = 2 * (planes - 4), nx // 2
    sends = 1 if y_count == 2 else 2
    gots = len(got)

    def body(*refs):
        got = refs[:gots]
        rhs, yb, w, up_, down_, part, inv, _, _, rhs3, w3 = refs[gots : gots + 11]
        rest = refs[gots + 11 :]
        out, (yb3, add) = rest[:sends], rest[sends:]
        lane_p = lane_ids(planes)

        def take_at(pick, at):
            values = [ref[at, :] for ref in got]
            return pick("gx", x_count, values[0], values[1] if gots > 1 else None)

        def take(pick, i):
            return take_at(pick, slice(i * planes, (i + 1) * planes))

        add[...] = jnp.zeros_like(add)
        for c in range(planes):
            w3[c] = w[c]
            yb3[c] = yb[c]
        for pick, near, far, edge in ((high_of, cx, cx + 1, cx - 1), (low_of, rows - 1, rows - 2, 0)):
            first, second, third = take(pick, 0), take(pick, 1), take(pick, 2)
            other = shift_lanes(third, -cy)
            one = jnp.where((lane_p == 0) | (lane_p == cy - 1), other, 0.0)
            two = jnp.where(lane_p == 0, shift_lanes(third, -cy - 1), 0.0)
            two = jnp.where(lane_p == cy - 1, shift_lanes(third, 1 - cy), two)
            yb3[:, near, :] = one
            yb3[:, far, :] = two
            for at, value, ends in ((near, first, one), (far, shift_lanes(first, -cy), two)):
                value = jnp.where(lane_p < cy, value, 0.0)
                value += jnp.where(lane_p == cy, shift_lanes(ends, 1), 0.0)
                value += jnp.where(lane_p == LANES - 1, shift_lanes(ends, -1), 0.0)
                add[:, at, :] = value
            w3[:, near, :] = jnp.where(lane_p < cy, second, 0.0)
            w3[:, far, :] = jnp.where(lane_p < cy, shift_lanes(second, -cy), 0.0)
            add[:, edge, :] = jnp.where(lane_p < cy, third, 0.0)
        for c in range(planes):
            rhs3[c] = rhs[c] + add[c]

        lane_c = lane_ids(rows)
        lane8 = lane_ids(8)
        base = 5 * planes
        x_face = slice(3 * planes, 3 * planes + nz)
        x_high = take_at(high_of, x_face)

        def fill(ref, near, far, fine, early):
            acc = jnp.zeros((rows, LANES), F32)
            jobs = ((rhs3, near), (rhs3, far), (w3, near), (w3, far), (yb3, near))
            for i, (field, at) in enumerate(jobs):
                for z in range(planes):
                    spot = i * planes + z
                    acc = jnp.where(lane_c == spot, shift_lanes(field[z], spot - at), acc)
            ref[:nx, :] = plane(acc, nx) + early[...]
            ref[nx : nx + 8, :] = line(x_high, lane8, fine, base)

        def up(ref):
            fill(ref, cy - 1, cy - 2, 2 * cy - 1, up_)
            ref[nx + 8 :, :] = jnp.zeros((half, LANES), F32)

        def down(ref):
            fill(ref, 0, 1, 0, down_)
            row = row_ids(nx)
            ends = jnp.where(row == 0, line(take_at(low_of, x_face), lane8, 0, 0)[:1, :], 0.0)
            ends += jnp.where(row == nx - 1, line(x_high, lane8, 0, 0)[:1, :], 0.0)
            inverse = inv[...]
            value = part[...] + inverse * ends
            packed = jnp.zeros((half, LANES), F32)
            for i, source in enumerate((value[:half], value[half:], inverse[:half], inverse[half:])):
                there = lane_ids(half) // nz == i
                packed = jnp.where(there, shift_lanes(source, i * nz), packed)
            ref[nx + 8 :, :] = packed

        write_sides("gy", out, up, down)

    whole = (planes, rows, LANES)
    return call(
        body,
        [whole, whole] + [(nx + 8 + half, LANES)] * sends,
        scratch=[whole, whole],
        in_specs=vmem(gots + 9),
        out_specs=vmem(2 + sends),
    )(*got, rhs, yb, w, *early)


def y_early(got_z, fg, node_shift, low_y, after, planes, z_count):
    nz, nx, _ = fg.shape
    z_at = 9 * (nx // 2 + 8)
    base = 5 * planes
    n_z = len(got_z)

    def body(*refs):
        gz = refs[:n_z]
        fg, shift, low_y, _, up, down, part, inv = refs[n_z:]
        lane = lane_ids(nx)
        row = row_ids(nx)

        def side(pick):
            values = [ref[z_at : z_at + nx, :] for ref in gz]
            return pick("gz", z_count, values[0], values[1] if n_z > 1 else None)

        above = side(high_of)
        here = jnp.where(lane == nz, shift_lanes(above, nz), 0.0)
        here = jnp.where(lane == LANES - 1, shift_lanes(side(low_of), -1), here)
        high = jnp.where(lane == base + nz, shift_lanes(above, base + nz + 1), 0.0)
        inverse = jnp.ones((nx, LANES), F32)
        inner = jnp.zeros((nx, LANES), F32)
        for z in range(nz):
            guess = fg[z]
            here = jnp.where(lane == z, shift_lanes(guess, z), here)
            inner = jnp.where(lane == z, shift_lanes(guess, z - 1), inner)
            high = jnp.where(lane == base + z, shift_lanes(guess, base + z + 1), high)
            inverse = jnp.where(lane == z, shift_lanes(6.0 + shift[z], z), inverse)
        inverse = 1.0 / inverse
        around = inner + shift_lanes(here, 1) + shift_lanes(here, -1)
        around += jnp.where(row == 0, 0.0, shift_rows(here, 1))
        around += jnp.where(row == nx - 1, 0.0, shift_rows(here, -1))
        up[...] = high
        at = base + nz + 1
        low = jnp.where((lane >= base) & (lane < at), shift_lanes(here, base), 0.0)
        down[...] = jnp.where((lane >= at) & (lane < at + 3 * nz), shift_lanes(low_y[...], at), low)
        part[...] = here + inverse * around
        inv[...] = inverse

    return call(
        body, [(nx, LANES)] * 4, in_specs=vmem(n_z + 4), out_specs=vmem(4)
    )(*got_z, fg, node_shift, low_y, after)


def coarse_stage(got, rhs, w, after, y_count, devices):
    planes, rows, _ = rhs.shape
    cz, cx = planes - 4, rows - 8
    cy = LANES // 2
    gots = len(got)

    def body(*refs):
        got = refs[:gots]
        rhs, w, _, v1, v2, sums, tot, inv_, image_ = refs[gots:]
        values = [ref[:rows, :] for ref in got]
        second = values[1] if gots > 1 else None
        low = low_of("gy", y_count, values[0], second)
        high = high_of("gy", y_count, values[0], second)
        lane = lane_ids(rows)
        spots_r = ((cy, high, 0), (cy + 1, high, 1), (LANES - 1, low, 0), (LANES - 2, low, 1))
        spots_r += ((cy - 1, high, 4), (0, low, 4))
        for z in range(planes):
            right = rhs[z]
            for at, source, i in spots_r:
                moved = shift_lanes(source, at - (i * planes + z))
                right += jnp.where(lane == at, moved, 0.0)
            inv = w[z]
            for at, source, i in spots_r[:4]:
                moved = shift_lanes(source, at - ((i + 2) * planes + z))
                inv = jnp.where(lane == at, moved, inv)
            inv_[z] = inv
            tot[z] = right
            v1[z] = right * inv

        def near(field, z):
            here = field[z]
            total = field[(z + 1) % planes] + field[(z - 1) % planes]
            total += shift_rows(here, 1) + shift_rows(here, -1)
            return total + shift_lanes(here, 1) + shift_lanes(here, -1)

        v2[cz + 1] = jnp.zeros((rows, LANES), F32)
        v2[cz + 2] = jnp.zeros((rows, LANES), F32)
        for z in list(range(cz + 1)) + [planes - 1]:
            image = tot[z] - near(v1, z)
            if z < cz:
                image_[z] = image
            v2[z] = image * inv_[z]
        parts = [jnp.zeros((cx, LANES), F32)] * 5
        for z in range(cz):
            first, second_, right, image = v1[z], v2[z], tot[z], image_[z]
            third = image - near(v2, z)
            terms = (first * right, second_ * right, first * image, second_ * image, second_ * third)
            parts = [a + b[:cx, :] for a, b in zip(parts, terms)]
        keep = lane_ids(1) < cy
        lines = [jnp.where(keep, jnp.sum(a, axis=0, keepdims=True), 0.0) for a in parts]
        tile = jnp.concatenate(lines + [jnp.zeros((3, LANES), F32)], axis=0)
        column = jnp.sum(tile, axis=1, keepdims=True)
        spread = jnp.where(lane_ids(8) == row_ids(8), column, 0.0)
        line = jnp.sum(spread, axis=0, keepdims=True)
        sums[...] = jnp.broadcast_to(line[None], (devices, 1, LANES))

    whole = (planes, rows, LANES)
    return call(
        body,
        [whole, whole, (devices, 1, LANES)],
        scratch=[whole, whole, whole],
        in_specs=vmem(gots + 3),
        out_specs=vmem(3),
    )(*got, rhs, w, *after)


def smooth_stage(scaled, inverses, below, got_z, tail_x, after, counts):
    _, nz, nx, _ = scaled.shape
    n_z = len(got_z)
    rows = nx // 2 + 8

    def body(*refs):
        s, inv, lz, lx, ly = refs[:5]
        gz = refs[5 : 5 + n_z]
        gx, _, out, last = refs[5 + n_z :]
        lane = lane_ids(nx)
        row = row_ids(nx)
        y_low = from_below("gy", ly[...])

        def above_of(refs, axis, size, at):
            values = [ref[at, :] for ref in refs]
            return high_of(axis, size, values[0], values[1] if len(values) > 1 else None)

        acc = jnp.zeros((nx, LANES), F32)
        for k in range(3):
            z_low = from_below("gz", lz[k])
            at = 9 * rows + nx + k * nx
            z_high = above_of(gz, "gz", counts[0], slice(at, at + nx))
            x_low = from_below("gx", lx[k * nz : (k + 1) * nz, :])
            x_high = from_above("gx", counts[1], gx[k * nz : (k + 1) * nz, :])
            for z in range(nz):
                here = s[k, z]
                around = s[k, z - 1] if z > 0 else z_low
                around += s[k, z + 1] if z < nz - 1 else z_high
                around += jnp.where(row == 0, x_low[z : z + 1, :], shift_rows(here, 1))
                around += jnp.where(row == nx - 1, x_high[z : z + 1, :], shift_rows(here, -1))
                spot = k * nz + z
                around += jnp.where(lane == 0, shift_lanes(y_low, -spot), shift_lanes(here, 1))
                around += jnp.where(lane == LANES - 1, 0.0, shift_lanes(here, -1))
                inverse = inv[k, z]
                acc = jnp.where(lane == spot, shift_lanes(inverse, spot + 1), acc)
                out[k, z] = here + around * inverse
        last[...] = acc

    return call(
        body, [scaled.shape, (nx, LANES)], in_specs=vmem(7 + n_z), out_specs=vmem(2)
    )(scaled, inverses, *below, *got_z, tail_x, after)


def final_stage(sums, v1, v2, fg, mid, smooth, last, tail_x, got_z, got_x, got_y, counts):
    planes, rows, _ = v1.shape
    cz, cx, cy = planes - 4, rows - 8, LANES // 2
    nz, nx, _ = fg.shape
    n_z, n_x, n_y = len(got_z), len(got_x), len(got_y)
    gots = n_z + n_x + n_y

    def body(*refs):
        sums, v1, v2, fg, part, inv, smooth, last, tx = refs[:9]
        gz = refs[9 : 9 + n_z]
        gx = refs[9 + n_z : 9 + n_z + n_x]
        gy = refs[9 + n_z + n_x : 9 + gots]
        out, sol, dup, inter, small, lines, buf, sem = refs[9 + gots :]

        def one_side(pick, refs, axis, size, at):
            values = [ref[at, :] for ref in refs]
            return pick(axis, size, values[0], values[1] if len(values) > 1 else None)

        def both(refs, axis, size, at):
            return [one_side(pick, refs, axis, size, at) for pick in (low_of, high_of)]

        total = jnp.sum(sums[...], axis=0)
        lane1 = lane_ids(1)
        gone, gtwo, hone, hmix, htwo = [
            jnp.sum(jnp.where(lane1 == i, total, 0.0), axis=1, keepdims=True) for i in range(5)
        ]
        two = (gtwo - hmix * gone / hone) / (htwo - hmix * hmix / hone)
        one = (gone - hmix * two) / hone
        source = lax.broadcasted_iota(jnp.int32, (LANES, 2 * LANES), 0)
        target = lax.broadcasted_iota(jnp.int32, (LANES, 2 * LANES), 1)
        fine = target - LANES
        side = jnp.where(fine % 2 == 1, fine // 2 + 1, (fine // 2 + LANES - 1) % LANES)
        spread = jnp.where(jnp.where(target < LANES, target // 2, side) == source, 1.0, 0.0)
        for z in list(range(cz + 1)) + [planes - 1]:
            sol[z] = one * v1[z] + two * v2[z]
            dup[z] = jnp.dot(sol[z], spread, precision=HIGHEST, preferred_element_type=F32)

        z_at = 9 * rows
        z_base = one_side(high_of, gz, "gz", counts[0], slice(z_at + 4 * nx, z_at + 5 * nx))
        z_inverse = one_side(high_of, gz, "gz", counts[0], slice(z_at + 5 * nx, z_at + 6 * nx))
        x_low, x_high = both(gx, "gx", counts[1], slice(3 * planes, 3 * planes + nz + 1))
        y_low, y_high = both(gy, "gy", counts[2], slice(0, nx))
        y_row_low, y_row_high = both(gy, "gy", counts[2], slice(nx, nx + 1))
        half = nx // 2
        y_pack = one_side(high_of, gy, "gy", counts[2], slice(nx + 8, nx + 8 + half))
        lane = lane_ids(nx)
        row = row_ids(nx)
        base = 5 * planes

        def spread_around(z):
            c, odd = z // 2, z % 2
            here = dup[c, :, :LANES]
            same = 3.0 * here + dup[c, :, LANES:]
            same += dup[(c + 1 if odd else c - 1) % planes, :, :LANES]
            slot = z % 2
            inter[slot, pl.ds(0, cx, 2), :] = (same + shift_rows(here, 1))[:cx, :]
            inter[slot, pl.ds(1, cx, 2), :] = (same + shift_rows(here, -1))[:cx, :]
            return inter[slot]

        def nodal(z):
            around = spread_around(z) + jnp.where(row == 0, x_low[z : z + 1, :], 0.0)
            around += jnp.where(row == nx - 1, x_high[z : z + 1, :], 0.0)
            around += jnp.where(lane == 0, shift_lanes(y_low, -(base + z)), 0.0)
            around += jnp.where(lane == LANES - 1, shift_lanes(y_high, -(base + z) - 1), 0.0)
            if z == nz:
                value = z_base + z_inverse * (around + fg[nz - 1])
                return from_above("gz", counts[0], value)
            return part[z] + inv[z] * around

        here = dup[:cz, cx, :LANES]
        same = 3.0 * here + dup[:cz, cx, LANES:] + dup[:cz, cx - 1, :LANES]
        small[pl.ds(0, cz, 2), :] = same + jnp.concatenate(
            [dup[planes - 1, cx : cx + 1, :LANES], here[: cz - 1]], axis=0
        )
        small[pl.ds(1, cz, 2), :] = same + dup[1 : cz + 1, cx, :LANES]
        for z in range(nz):
            left = shift_lanes(y_row_low, -(base + z))
            right = shift_lanes(y_row_high, -(base + z) - 1)
            value = jnp.where(lane1 == 0, left, 0.0)
            lines[z : z + 1, :] = jnp.where(lane1 == LANES - 1, right, value)
        x_value = tx[3 * nz : 4 * nz, :] + tx[4 * nz :, :] * (
            fg[:, nx - 1, :] + small[...] + lines[...]
        )
        x_value = from_above("gx", counts[1], x_value)

        lane_c = lane_ids(rows)
        even = jnp.zeros((rows, LANES), F32)
        odd = jnp.zeros((rows, LANES), F32)
        own = jnp.zeros((nx, LANES), F32)
        for z in range(nz):
            c = z // 2
            here = sol[c]
            same = 3.0 * here + shift_lanes(here, 1) + sol[(c + 1 if z % 2 else c - 1) % planes]
            even = jnp.where(lane_c == z, shift_lanes(same + shift_rows(here, 1), z - cy), even)
            odd = jnp.where(lane_c == z, shift_lanes(same + shift_rows(here, -1), z - cy), odd)
            own = jnp.where(lane == z, shift_lanes(fg[z], z + 1), own)
        inter[0, pl.ds(0, cx, 2), :] = even[:cx, :]
        inter[0, pl.ds(1, cx, 2), :] = odd[:cx, :]
        y_base = jnp.concatenate([y_pack, shift_lanes(y_pack, -nz)], axis=0)
        y_inverse = jnp.concatenate(
            [shift_lanes(y_pack, -2 * nz), shift_lanes(y_pack, -3 * nz)], axis=0
        )
        y_value = y_base + y_inverse * (own + inter[0])
        y_value = from_above("gy", counts[2], y_value)
        y_fix = shift_lanes(y_high, -(base + nz + 1)) * last[...]

        def copy(z):
            return pltpu.make_async_copy(buf.at[:, z], out.at[:, z], sem.at[z])

        value = nodal(0)
        for z in range(nz):
            after = nodal(z + 1)
            steps = [after, jnp.where(row == nx - 1, x_value[z : z + 1, :], shift_rows(value, -1))]
            steps.append(
                jnp.where(lane == LANES - 1, shift_lanes(y_value, -z - 1), shift_lanes(value, -1))
            )
            for k in range(3):
                fixed = jnp.where(lane == LANES - 1, shift_lanes(y_fix, -(k * nz + z) - 1), 0.0)
                buf[k, z] = (smooth[k, z] + fixed) + (steps[k] - value)
            copy(z).start()
            value = after
        for z in range(nz):
            copy(z).wait()

    return call(
        body,
        [smooth.shape],
        scratch=[
            (planes, rows, LANES),
            (planes, rows, 2 * LANES),
            (2, nx, LANES),
            (nz, LANES),
            (nz, LANES),
            smooth.shape,
            pltpu.SemaphoreType.DMA((nz,)),
        ],
        far_out=True,
        in_specs=vmem(9 + gots),
        out_specs=[pl.BlockSpec(memory_space=pltpu.HBM)],
    )(sums, v1, v2, fg, *mid, smooth, last, tail_x, *got_z, *got_x, *got_y)[0]


def local(residual, edge_diag, node_shift, coarse_shift):
    axes = ("gz", "gx", "gy")
    counts = tuple(lax.axis_size(a) for a in axes)
    devices = counts[0] * counts[1] * counts[2]
    part, *faces, scaled, inverses = edge_stage(residual, edge_diag)
    up_z, up_x, up_y, low_z, low_x, low_y = faces
    below = (ring(up_z, "gz", 1), ring(up_x, "gx", 1), ring(up_y, "gy", 1))
    fg, rhs, xb, yb, w, *send = nodal_stage(part, node_shift, coarse_shift, *below, low_z, counts[0])
    got_z = swap(send, "gz")
    rhs, yb, w, *send = x_stage(got_z, rhs, xb, yb, w, fg, counts[0], counts[1])
    got_x = swap(send, "gx")
    planes = rhs.shape[0]
    tail_x = x_tail(got_z, fg, node_shift, low_x, w, counts[0])
    mid = part_stage(got_z, fg, node_shift, w, counts[0])
    early = y_early(got_z, fg, node_shift, low_y, w, planes, counts[0])
    early = (*early, tail_x, mid[1])
    tail_x = ring(tail_x, "gx", -1)
    rhs, w, *send = y_stage(got_x, rhs, yb, w, early, counts[1], counts[2])
    got_y = swap(send, "gy")
    smooth, last = smooth_stage(scaled, inverses, below, got_z, tail_x, w, counts)
    v1, v2, sums = coarse_stage(got_y, rhs, w, (last,), counts[2], devices)
    sums = lax.all_to_all(sums, ("gx", "gy", "gz"), 0, 0)
    return final_stage(sums, v1, v2, fg, mid, smooth, last, tail_x, got_z, got_x, got_y, counts)


def solution(mesh):
    placed = (
        P(None, "gz", "gx", "gy"),
        P(None, "gz", "gx", "gy"),
        P("gz", "gx", "gy"),
        P("gz", "gx", "gy"),
    )

    return jax.shard_map(
        local, mesh=mesh, in_specs=placed, out_specs=P(None, "gz", "gx", "gy"), check_vma=False
    )
```

```python
import itertools

import jax
import jax.numpy as jnp
from jax import lax
from jax.experimental import pallas as pl
from jax.experimental.pallas import tpu as pltpu
from jax.sharding import PartitionSpec as P


F32 = jnp.float32
HIGHEST = lax.Precision.HIGHEST
LANES = 128


def lane_ids(rows):
    return lax.broadcasted_iota(jnp.int32, (rows, LANES), 1)


def row_ids(rows):
    return lax.broadcasted_iota(jnp.int32, (rows, LANES), 0)


def shift_lanes(value, amount):
    return pltpu.roll(value, amount % LANES, 1)


def shift_rows(value, amount):
    return pltpu.roll(value, amount % value.shape[0], 0)


def low_of(axis, size, first, second):
    place = lax.axis_index(axis)
    odd = place % 2 == 1
    zero = jnp.zeros_like(first)
    if second is None:
        return jnp.where(odd, first, zero)
    return jnp.where(odd, first, jnp.where(place > 0, second, zero))


def high_of(axis, size, first, second):
    place = lax.axis_index(axis)
    even = place % 2 == 0
    zero = jnp.zeros_like(first)
    if second is None:
        return jnp.where(even, first, zero)
    return jnp.where(even, first, jnp.where(place < size - 1, second, zero))


def from_below(axis, value):
    return jnp.where(lax.axis_index(axis) > 0, value, jnp.zeros_like(value))


def from_above(axis, size, value):
    return jnp.where(lax.axis_index(axis) < size - 1, value, jnp.zeros_like(value))


def ring(value, axis, step):
    size = lax.axis_size(axis)
    return lax.ppermute(value, axis, [(i, (i + step) % size) for i in range(size)])


def swap(values, axis, names=None):
    size = lax.axis_size(axis)
    out = [lax.ppermute(values[0], axis, [(i, i ^ 1) for i in range(size)])]
    if len(values) == 1:
        return out
    odd = [(i + 1) % size if i % 2 else (i - 1) % size for i in range(size)]
    if names is None:
        out.append(lax.ppermute(values[1], axis, list(enumerate(odd))))
        return out
    main = names.index(axis)
    pairs = []
    sizes = [lax.axis_size(name) for name in names]
    for at in itertools.product(*(range(n) for n in sizes)):
        to = list(at)
        if at[main] in (0, size - 1):
            to[1 - main] ^= 1
        else:
            to[main] = odd[at[main]]
        pairs.append(tuple(p[0] * sizes[1] + p[1] for p in (at, to)))
    out.append(lax.ppermute(values[1], names, pairs))
    return out


def write_sides(axis, refs, up, down):
    even = lax.axis_index(axis) % 2 == 0

    @pl.when(even)
    def _():
        up(refs[0])
        if len(refs) > 1:
            down(refs[1])

    @pl.when(jnp.logical_not(even))
    def _():
        down(refs[0])
        if len(refs) > 1:
            up(refs[1])


def call(body, outs, scratch=(), far=(), far_out=False, **kwargs):
    kind = jax.ShapeDtypeStruct if far_out else pltpu.VMEM
    run = pl.pallas_call(
        body,
        out_shape=[kind(shape, F32) for shape in outs],
        scratch_shapes=[pltpu.VMEM(s, F32) if isinstance(s, tuple) else s for s in scratch],
        compiler_params=pltpu.CompilerParams(vmem_limit_bytes=12 * 2**20),
        **kwargs,
    )

    def apply(*args):
        spaces = [pltpu.HBM if i in far else pltpu.VMEM for i in range(len(args))]
        return run(
            *(
                pltpu.with_memory_space_constraint(a, space)
                for a, space in zip(args, spaces)
            )
        )

    return apply


def vmem(count):
    return [pl.BlockSpec(memory_space=pltpu.VMEM)] * count


def edge_stage(residual, edge_diag):
    _, nz, nx, ny = residual.shape
    step = 2
    steps = nz // step

    def body(res, diag, part, up_z, up_x, up_y, low_z, low_x, low_y, scaled, inv, near, sems):
        lane = lane_ids(nx)
        row = row_ids(nx)

        def copies(block):
            at = pl.ds(block * step, step)
            return [
                pltpu.make_async_copy(source.at[:, at], target.at[:, at], sems.at[i, block])
                for i, (source, target) in enumerate(((res, near), (diag, inv)))
            ]

        for block in range(steps):
            for copy in copies(block):
                copy.start()
        before = jnp.zeros((nx, ny), F32)
        high = jnp.zeros((nx, LANES), F32)
        low = jnp.zeros((nx, LANES), F32)
        for z in range(nz):
            if z % step == 0:
                for copy in copies(z // step):
                    copy.wait()
            s = []
            for k in range(3):
                inverse = 1.0 / inv[k, z]
                inv[k, z] = inverse
                s.append(near[k, z] * inverse)
                scaled[k, z] = s[k]
            total = before - s[0]
            total += jnp.where(row == 0, 0.0, shift_rows(s[1], 1)) - s[1]
            total += jnp.where(lane == 0, 0.0, shift_lanes(s[2], 1)) - s[2]
            part[z] = total
            before = s[0]
            for k in range(3):
                spot = k * nz + z
                up_x[spot : spot + 1, :] = s[k][nx - 1 :, :]
                low_x[spot : spot + 1, :] = s[k][:1, :]
                high = jnp.where(lane == spot, shift_lanes(s[k], spot + 1), high)
                low = jnp.where(lane == spot, shift_lanes(s[k], spot), low)
                if z == 0:
                    low_z[k] = s[k]
                if z == nz - 1:
                    up_z[k] = s[k]
        up_y[...] = high
        low_y[...] = low

    faces = [(3, nx, ny), (3 * nz, ny), (nx, LANES)] * 2
    return call(
        body,
        [(nz, nx, ny)] + faces + [residual.shape] * 2,
        scratch=[residual.shape, pltpu.SemaphoreType.DMA((2, steps))],
        far=(0, 1),
        in_specs=[pl.BlockSpec(memory_space=pltpu.HBM)] * 2,
        out_specs=vmem(9),
    )(residual, edge_diag)


def plane(values, row_count):
    return jnp.concatenate([values, jnp.zeros((row_count - values.shape[0], LANES), F32)], axis=0)


def nodal_stage(part, node_shift, coarse_shift, got_z, got_x, got_y, low_z, z_count):
    nz, nx, ny = part.shape
    cz, cx, cy = nz // 2, nx // 2, ny // 2
    rows = cx + 8
    sends = 1 if z_count == 2 else 2

    def body(part, shift, coarse, gz, gx, gy, low_z, fg, rhs, xb, yb, w, *rest):
        out, (pair, s_, xl_, yl_, zl_, zh_) = rest[:sends], rest[sends:]
        lane = lane_ids(nx)
        row = row_ids(nx)
        lane_c = lane_ids(rows)
        row_c = row_ids(rows)
        below_z = from_below("gz", gz[0])
        below_y = from_below("gy", gy[...])
        fine = lax.broadcasted_iota(jnp.int32, (ny, 2 * LANES), 0)
        coarse_lane = lax.broadcasted_iota(jnp.int32, (ny, 2 * LANES), 1)
        miss = jnp.where(
            coarse_lane < LANES, fine // 2 - coarse_lane, fine - 2 * (coarse_lane - LANES)
        )
        gather = jnp.where(miss == 0, 1.0, 0.0)
        for c in range(cz):
            both = []
            for z in (2 * c, 2 * c + 1):
                total = part[z]
                if z == 0:
                    total += below_z
                total += jnp.where(row == 0, from_below("gx", gx[nz + z : nz + z + 1, :]), 0.0)
                total += jnp.where(lane == 0, shift_lanes(below_y, -(2 * nz + z)), 0.0)
                guess = total / (6.0 + shift[z])
                fg[z] = guess
                both.append(guess)
            pair[c % 2] = both[0] + both[1]
            low = pair[c % 2, pl.ds(0, cx, 2), :]
            high = pair[c % 2, pl.ds(1, cx, 2), :]
            first = fg[2 * c, pl.ds(0, cx, 2), :] + fg[2 * c, pl.ds(1, cx, 2), :]
            stacked = jnp.concatenate([low + high, low, first], axis=0)
            sums = jnp.dot(stacked, gather, precision=HIGHEST, preferred_element_type=F32)
            s = sums[:cx, :LANES]
            z_low = sums[2 * cx :, :LANES]
            s_[c] = plane(s, rows)
            yl_[c] = plane(sums[:cx, LANES:], rows)
            xl_[c] = plane(sums[cx : 2 * cx, :LANES], rows)
            zl_[c] = plane(z_low, rows)
            zh_[c] = plane(s - z_low, rows)
            w[c] = jnp.zeros((rows, LANES), F32)
            w[c, :cx, :cy] = 1.0 / (6.0 + coarse[c])
        for c in range(cz):
            s, x_low, y_low = s_[c], xl_[c], yl_[c]
            x_high = s - x_low
            y_high = s - y_low
            total = 3.0 * s
            total += shift_rows(x_low, -1) + shift_rows(x_high, 1)
            total += shift_lanes(y_low, -1) + shift_lanes(y_high, 1)
            if c > 0:
                total += zh_[c - 1]
            if c < cz - 1:
                total += zl_[c + 1]
            rhs[c] = total
            xb[c] = jnp.where(row_c < cx // 2, x_low, x_high)
            yb[c] = jnp.where(lane_c < cy // 2, y_low, y_high)
        rhs[cz] = zh_[cz - 1]
        rhs[cz + 1] = jnp.zeros((rows, LANES), F32)
        rhs[cz + 2] = jnp.zeros((rows, LANES), F32)
        rhs[cz + 3] = zl_[0]

        def fill(ref, near, far, half, face):
            planes = [rhs[near], rhs[far], w[near], w[far], half]
            planes += [xb[near], xb[far], yb[near], yb[far]]
            for i, value in enumerate(planes):
                ref[i * rows : (i + 1) * rows, :] = value
            ref[9 * rows : 9 * rows + nx, :] = face

        def tail(ref, values):
            for i, value in enumerate(values):
                at = 9 * rows + nx + i * nx
                ref[at : at + nx, :] = value

        def up(ref):
            fill(ref, cz - 1, cz - 2, zh_[cz - 1], fg[nz - 1])
            tail(ref, [jnp.zeros((nx, LANES), F32)] * 5)

        def down(ref):
            fill(ref, 0, 1, zl_[0], fg[0])
            here = fg[0]
            around = fg[1] + jnp.where(row == 0, 0.0, shift_rows(here, 1))
            around += jnp.where(row == nx - 1, 0.0, shift_rows(here, -1))
            around += jnp.where(lane == 0, 0.0, shift_lanes(here, 1))
            around += jnp.where(lane == ny - 1, 0.0, shift_lanes(here, -1))
            inverse = 1.0 / (6.0 + shift[0])
            tail(ref, [low_z[0], low_z[1], low_z[2], here + inverse * around, inverse])

        write_sides("gz", out, up, down)

    coarse = (cz, rows, LANES)
    send = (9 * rows + 6 * nx, LANES)
    return call(
        body,
        [(nz, nx, ny), (cz + 4, rows, LANES), coarse, coarse, coarse] + [send] * sends,
        scratch=[(2, nx, ny), coarse, coarse, coarse, coarse, coarse],
        in_specs=vmem(7),
        out_specs=vmem(5 + sends),
    )(part, node_shift, coarse_shift, got_z, got_x, got_y, low_z)


def x_stage(got, rhs, xb, yb, w, fg, z_count, x_count):
    planes, rows, _ = rhs.shape
    cz, cx = planes - 4, rows - 8
    nz, nx, ny = fg.shape
    cy = ny // 2
    sends = 1 if x_count == 2 else 2
    gots = len(got)
    size = -(-(3 * planes + nz + 1) // 8) * 8

    def body(*refs):
        got = refs[:gots]
        rhs, xb, yb, w, fg, rhs2, yb2, w2 = refs[gots : gots + 8]
        out, (xb2,) = refs[gots + 8 : gots + 8 + sends], refs[gots + 8 + sends :]

        def take_at(pick, at):
            values = [ref[at, :] for ref in got]
            return pick("gz", z_count, values[0], values[1] if gots > 1 else None)

        def take(pick, i):
            return take_at(pick, slice(i * rows, (i + 1) * rows))

        for c in range(1, cz - 1):
            rhs2[c] = rhs[c]
        rhs2[0] = rhs[0] + take(low_of, 4)
        rhs2[cz - 1] = rhs[cz - 1] + take(high_of, 4)
        rhs2[cz] = rhs[cz] + take(high_of, 0)
        rhs2[cz + 1] = take(high_of, 1)
        rhs2[cz + 2] = take(low_of, 1)
        rhs2[cz + 3] = rhs[cz + 3] + take(low_of, 0)
        for here, there, i in ((w, w2, 2), (xb, xb2, 5), (yb, yb2, 7)):
            for c in range(cz):
                there[c] = here[c]
            there[cz] = take(high_of, i)
            there[cz + 1] = take(high_of, i + 1)
            there[cz + 2] = take(low_of, i + 1)
            there[cz + 3] = take(low_of, i)

        lane = lane_ids(planes)

        def fill(ref, near, far, fine):
            halves = lane < cy
            first = jnp.where(halves, rhs2[:, near, :], shift_lanes(rhs2[:, far, :], cy))
            second = jnp.where(halves, w2[:, near, :], shift_lanes(w2[:, far, :], cy))
            edge = yb2[:, far, :]
            third = jnp.where(halves, xb2[:, near, :], shift_lanes(yb2[:, near, :], cy))
            third = jnp.where(lane == cy + 1, shift_lanes(edge, cy + 1), third)
            third = jnp.where(lane == LANES - 2, shift_lanes(edge, cy - 1), third)
            for i, value in enumerate((first, second, third)):
                ref[i * planes : (i + 1) * planes, :] = value
            ref[3 * planes : 3 * planes + nz, :] = fg[:, fine, :]
            at = 9 * rows + fine
            last = 3 * planes + nz
            ref[last : last + 1, :] = take_at(high_of, slice(at, at + 1))
            ref[last + 1 :, :] = jnp.zeros((size - last - 1, LANES), F32)

        def up(ref):
            fill(ref, cx - 1, cx - 2, nx - 1)

        def down(ref):
            fill(ref, 0, 1, 0)

        write_sides("gx", out, up, down)

    whole = (planes, rows, LANES)
    return call(
        body,
        [whole, whole, whole] + [(size, LANES)] * sends,
        scratch=[whole],
        in_specs=vmem(gots + 5),
        out_specs=vmem(3 + sends),
    )(*got, rhs, xb, yb, w, fg)


def x_tail(got, fg, node_shift, low_x, after, z_count):
    nz, nx, ny = fg.shape
    z_at = 9 * (nx // 2 + 8)
    gots = len(got)

    def body(*refs):
        got = refs[:gots]
        fg, shift, low_x, _, out = refs[gots:]
        lane = lane_ids(nz)
        row = row_ids(nz)

        def z_row(pick):
            values = [ref[z_at : z_at + 1, :] for ref in got]
            return pick("gz", z_count, values[0], values[1] if gots > 1 else None)

        here = fg[:, 0, :]
        around = fg[:, 1, :] + jnp.where(row == 0, z_row(low_of), shift_rows(here, 1))
        around += jnp.where(row == nz - 1, z_row(high_of), shift_rows(here, -1))
        around += jnp.where(lane == 0, 0.0, shift_lanes(here, 1))
        around += jnp.where(lane == ny - 1, 0.0, shift_lanes(here, -1))
        inverse = 1.0 / (6.0 + shift[:, 0, :])
        out[: 3 * nz, :] = low_x[...]
        out[3 * nz : 4 * nz, :] = here + inverse * around
        out[4 * nz :, :] = inverse

    return call(
        body, [(5 * nz, LANES)], in_specs=vmem(gots + 4), out_specs=vmem(1)
    )(*got, fg, node_shift, low_x, after)[0]


def part_stage(got, fg, node_shift, after, z_count):
    nz, nx, ny = fg.shape
    z_at = 9 * (nx // 2 + 8)
    gots = len(got)

    def body(*refs):
        got = refs[:gots]
        fg, shift, _, part, inv = refs[gots:]
        lane = lane_ids(nx)
        row = row_ids(nx)

        def z_face(pick):
            values = [ref[z_at : z_at + nx, :] for ref in got]
            return pick("gz", z_count, values[0], values[1] if gots > 1 else None)

        for z in range(nz):
            guess = fg[z]
            around = fg[z - 1] if z > 0 else z_face(low_of)
            around += fg[z + 1] if z < nz - 1 else z_face(high_of)
            around += jnp.where(row == 0, 0.0, shift_rows(guess, 1))
            around += jnp.where(row == nx - 1, 0.0, shift_rows(guess, -1))
            around += jnp.where(lane == 0, 0.0, shift_lanes(guess, 1))
            around += jnp.where(lane == ny - 1, 0.0, shift_lanes(guess, -1))
            inverse = 1.0 / (6.0 + shift[z])
            inv[z] = inverse
            part[z] = guess + inverse * around

    return call(
        body, [fg.shape, fg.shape], in_specs=vmem(gots + 3), out_specs=vmem(2)
    )(*got, fg, node_shift, after)


def line(source, lane, fine, at):
    acc = jnp.zeros(lane.shape, F32)
    for z in range(source.shape[0]):
        moved = jnp.broadcast_to(source[z : z + 1, :], lane.shape)
        acc = jnp.where(lane == at + z, shift_lanes(moved, at + z - fine), acc)
    return acc


def y_stage(got, rhs, yb, w, early, x_count, y_count):
    planes, rows, _ = rhs.shape
    cx = rows - 8
    nx, cy = 2 * cx, LANES // 2
    nz, half = 2 * (planes - 4), nx // 2
    sends = 1 if y_count == 2 else 2
    gots = len(got)

    def body(*refs):
        got = refs[:gots]
        rhs, yb, w, up_, down_, part, inv, _, _, rhs3, w3 = refs[gots : gots + 11]
        rest = refs[gots + 11 :]
        out, (yb3, add) = rest[:sends], rest[sends:]
        lane_p = lane_ids(planes)

        def take_at(pick, at):
            values = [ref[at, :] for ref in got]
            return pick("gx", x_count, values[0], values[1] if gots > 1 else None)

        def take(pick, i):
            return take_at(pick, slice(i * planes, (i + 1) * planes))

        add[...] = jnp.zeros_like(add)
        for c in range(planes):
            w3[c] = w[c]
            yb3[c] = yb[c]
        for pick, near, far, edge in ((high_of, cx, cx + 1, cx - 1), (low_of, rows - 1, rows - 2, 0)):
            first, second, third = take(pick, 0), take(pick, 1), take(pick, 2)
            other = shift_lanes(third, -cy)
            one = jnp.where((lane_p == 0) | (lane_p == cy - 1), other, 0.0)
            two = jnp.where(lane_p == 0, shift_lanes(third, -cy - 1), 0.0)
            two = jnp.where(lane_p == cy - 1, shift_lanes(third, 1 - cy), two)
            yb3[:, near, :] = one
            yb3[:, far, :] = two
            for at, value, ends in ((near, first, one), (far, shift_lanes(first, -cy), two)):
                value = jnp.where(lane_p < cy, value, 0.0)
                value += jnp.where(lane_p == cy, shift_lanes(ends, 1), 0.0)
                value += jnp.where(lane_p == LANES - 1, shift_lanes(ends, -1), 0.0)
                add[:, at, :] = value
            w3[:, near, :] = jnp.where(lane_p < cy, second, 0.0)
            w3[:, far, :] = jnp.where(lane_p < cy, shift_lanes(second, -cy), 0.0)
            add[:, edge, :] = jnp.where(lane_p < cy, third, 0.0)
        for c in range(planes):
            rhs3[c] = rhs[c] + add[c]

        lane_c = lane_ids(rows)
        lane8 = lane_ids(8)
        base = 5 * planes
        x_face = slice(3 * planes, 3 * planes + nz)
        x_high = take_at(high_of, x_face)

        def fill(ref, near, far, fine, early):
            acc = jnp.zeros((rows, LANES), F32)
            jobs = ((rhs3, near), (rhs3, far), (w3, near), (w3, far), (yb3, near))
            for i, (field, at) in enumerate(jobs):
                for z in range(planes):
                    spot = i * planes + z
                    acc = jnp.where(lane_c == spot, shift_lanes(field[z], spot - at), acc)
            ref[:nx, :] = plane(acc, nx) + early[...]
            ref[nx : nx + 8, :] = line(x_high, lane8, fine, base)

        def up(ref):
            fill(ref, cy - 1, cy - 2, 2 * cy - 1, up_)
            ref[nx + 8 :, :] = jnp.zeros((half, LANES), F32)

        def down(ref):
            fill(ref, 0, 1, 0, down_)
            row = row_ids(nx)
            ends = jnp.where(row == 0, line(take_at(low_of, x_face), lane8, 0, 0)[:1, :], 0.0)
            ends += jnp.where(row == nx - 1, line(x_high, lane8, 0, 0)[:1, :], 0.0)
            inverse = inv[...]
            value = part[...] + inverse * ends
            packed = jnp.zeros((half, LANES), F32)
            for i, source in enumerate((value[:half], value[half:], inverse[:half], inverse[half:])):
                there = lane_ids(half) // nz == i
                packed = jnp.where(there, shift_lanes(source, i * nz), packed)
            ref[nx + 8 :, :] = packed

        write_sides("gy", out, up, down)

    whole = (planes, rows, LANES)
    return call(
        body,
        [whole, whole] + [(nx + 8 + half, LANES)] * sends,
        scratch=[whole, whole],
        in_specs=vmem(gots + 9),
        out_specs=vmem(2 + sends),
    )(*got, rhs, yb, w, *early)


def y_early(got_z, fg, node_shift, low_y, after, planes, z_count):
    nz, nx, _ = fg.shape
    z_at = 9 * (nx // 2 + 8)
    base = 5 * planes
    n_z = len(got_z)

    def body(*refs):
        gz = refs[:n_z]
        fg, shift, low_y, _, up, down, part, inv = refs[n_z:]
        lane = lane_ids(nx)
        row = row_ids(nx)

        def side(pick):
            values = [ref[z_at : z_at + nx, :] for ref in gz]
            return pick("gz", z_count, values[0], values[1] if n_z > 1 else None)

        above = side(high_of)
        here = jnp.where(lane == nz, shift_lanes(above, nz), 0.0)
        here = jnp.where(lane == LANES - 1, shift_lanes(side(low_of), -1), here)
        high = jnp.where(lane == base + nz, shift_lanes(above, base + nz + 1), 0.0)
        inverse = jnp.ones((nx, LANES), F32)
        inner = jnp.zeros((nx, LANES), F32)
        for z in range(nz):
            guess = fg[z]
            here = jnp.where(lane == z, shift_lanes(guess, z), here)
            inner = jnp.where(lane == z, shift_lanes(guess, z - 1), inner)
            high = jnp.where(lane == base + z, shift_lanes(guess, base + z + 1), high)
            inverse = jnp.where(lane == z, shift_lanes(6.0 + shift[z], z), inverse)
        inverse = 1.0 / inverse
        around = inner + shift_lanes(here, 1) + shift_lanes(here, -1)
        around += jnp.where(row == 0, 0.0, shift_rows(here, 1))
        around += jnp.where(row == nx - 1, 0.0, shift_rows(here, -1))
        up[...] = high
        at = base + nz + 1
        low = jnp.where((lane >= base) & (lane < at), shift_lanes(here, base), 0.0)
        down[...] = jnp.where((lane >= at) & (lane < at + 3 * nz), shift_lanes(low_y[...], at), low)
        part[...] = here + inverse * around
        inv[...] = inverse

    return call(
        body, [(nx, LANES)] * 4, in_specs=vmem(n_z + 4), out_specs=vmem(4)
    )(*got_z, fg, node_shift, low_y, after)


def coarse_stage(got, rhs, w, after, y_count, devices):
    planes, rows, _ = rhs.shape
    cz, cx = planes - 4, rows - 8
    cy = LANES // 2
    gots = len(got)

    def body(*refs):
        got = refs[:gots]
        rhs, w, _, v1, v2, sums, tot, inv_, image_ = refs[gots:]
        values = [ref[:rows, :] for ref in got]
        second = values[1] if gots > 1 else None
        low = low_of("gy", y_count, values[0], second)
        high = high_of("gy", y_count, values[0], second)
        lane = lane_ids(rows)
        spots_r = ((cy, high, 0), (cy + 1, high, 1), (LANES - 1, low, 0), (LANES - 2, low, 1))
        spots_r += ((cy - 1, high, 4), (0, low, 4))
        for z in range(planes):
            right = rhs[z]
            for at, source, i in spots_r:
                moved = shift_lanes(source, at - (i * planes + z))
                right += jnp.where(lane == at, moved, 0.0)
            inv = w[z]
            for at, source, i in spots_r[:4]:
                moved = shift_lanes(source, at - ((i + 2) * planes + z))
                inv = jnp.where(lane == at, moved, inv)
            inv_[z] = inv
            tot[z] = right
            v1[z] = right * inv

        def near(field, z):
            here = field[z]
            total = field[(z + 1) % planes] + field[(z - 1) % planes]
            total += shift_rows(here, 1) + shift_rows(here, -1)
            return total + shift_lanes(here, 1) + shift_lanes(here, -1)

        v2[cz + 1] = jnp.zeros((rows, LANES), F32)
        v2[cz + 2] = jnp.zeros((rows, LANES), F32)
        for z in list(range(cz + 1)) + [planes - 1]:
            image = tot[z] - near(v1, z)
            if z < cz:
                image_[z] = image
            v2[z] = image * inv_[z]
        parts = [jnp.zeros((cx, LANES), F32)] * 5
        for z in range(cz):
            first, second_, right, image = v1[z], v2[z], tot[z], image_[z]
            third = image - near(v2, z)
            terms = (first * right, second_ * right, first * image, second_ * image, second_ * third)
            parts = [a + b[:cx, :] for a, b in zip(parts, terms)]
        keep = lane_ids(1) < cy
        lines = [jnp.where(keep, jnp.sum(a, axis=0, keepdims=True), 0.0) for a in parts]
        tile = jnp.concatenate(lines + [jnp.zeros((3, LANES), F32)], axis=0)
        column = jnp.sum(tile, axis=1, keepdims=True)
        spread = jnp.where(lane_ids(8) == row_ids(8), column, 0.0)
        line = jnp.sum(spread, axis=0, keepdims=True)
        sums[...] = jnp.broadcast_to(line[None], (devices, 1, LANES))

    whole = (planes, rows, LANES)
    return call(
        body,
        [whole, whole, (devices, 1, LANES)],
        scratch=[whole, whole, whole],
        in_specs=vmem(gots + 3),
        out_specs=vmem(3),
    )(*got, rhs, w, *after)


def smooth_stage(scaled, inverses, below, got_z, tail_x, after, counts):
    _, nz, nx, _ = scaled.shape
    n_z = len(got_z)
    rows = nx // 2 + 8

    def body(*refs):
        s, inv, lz, lx, ly = refs[:5]
        gz = refs[5 : 5 + n_z]
        gx, _, out, last = refs[5 + n_z :]
        lane = lane_ids(nx)
        row = row_ids(nx)
        y_low = from_below("gy", ly[...])

        def above_of(refs, axis, size, at):
            values = [ref[at, :] for ref in refs]
            return high_of(axis, size, values[0], values[1] if len(values) > 1 else None)

        acc = jnp.zeros((nx, LANES), F32)
        for k in range(3):
            z_low = from_below("gz", lz[k])
            at = 9 * rows + nx + k * nx
            z_high = above_of(gz, "gz", counts[0], slice(at, at + nx))
            x_low = from_below("gx", lx[k * nz : (k + 1) * nz, :])
            x_high = from_above("gx", counts[1], gx[k * nz : (k + 1) * nz, :])
            for z in range(nz):
                here = s[k, z]
                around = s[k, z - 1] if z > 0 else z_low
                around += s[k, z + 1] if z < nz - 1 else z_high
                around += jnp.where(row == 0, x_low[z : z + 1, :], shift_rows(here, 1))
                around += jnp.where(row == nx - 1, x_high[z : z + 1, :], shift_rows(here, -1))
                spot = k * nz + z
                around += jnp.where(lane == 0, shift_lanes(y_low, -spot), shift_lanes(here, 1))
                around += jnp.where(lane == LANES - 1, 0.0, shift_lanes(here, -1))
                inverse = inv[k, z]
                acc = jnp.where(lane == spot, shift_lanes(inverse, spot + 1), acc)
                out[k, z] = here + around * inverse
        last[...] = acc

    return call(
        body, [scaled.shape, (nx, LANES)], in_specs=vmem(7 + n_z), out_specs=vmem(2)
    )(scaled, inverses, *below, *got_z, tail_x, after)


def final_stage(sums, v1, v2, fg, mid, smooth, last, tail_x, got_z, got_x, got_y, counts):
    planes, rows, _ = v1.shape
    cz, cx, cy = planes - 4, rows - 8, LANES // 2
    nz, nx, _ = fg.shape
    n_z, n_x, n_y = len(got_z), len(got_x), len(got_y)
    gots = n_z + n_x + n_y

    def body(*refs):
        sums, v1, v2, fg, part, inv, smooth, last, tx = refs[:9]
        gz = refs[9 : 9 + n_z]
        gx = refs[9 + n_z : 9 + n_z + n_x]
        gy = refs[9 + n_z + n_x : 9 + gots]
        out, sol, dup, inter, small, lines, buf, sem = refs[9 + gots :]

        def one_side(pick, refs, axis, size, at):
            values = [ref[at, :] for ref in refs]
            return pick(axis, size, values[0], values[1] if len(values) > 1 else None)

        def both(refs, axis, size, at):
            return [one_side(pick, refs, axis, size, at) for pick in (low_of, high_of)]

        total = jnp.sum(sums[...], axis=0)
        lane1 = lane_ids(1)
        gone, gtwo, hone, hmix, htwo = [
            jnp.sum(jnp.where(lane1 == i, total, 0.0), axis=1, keepdims=True) for i in range(5)
        ]
        two = (gtwo - hmix * gone / hone) / (htwo - hmix * hmix / hone)
        one = (gone - hmix * two) / hone
        source = lax.broadcasted_iota(jnp.int32, (LANES, 2 * LANES), 0)
        target = lax.broadcasted_iota(jnp.int32, (LANES, 2 * LANES), 1)
        fine = target - LANES
        side = jnp.where(fine % 2 == 1, fine // 2 + 1, (fine // 2 + LANES - 1) % LANES)
        spread = jnp.where(jnp.where(target < LANES, target // 2, side) == source, 1.0, 0.0)
        for z in list(range(cz + 1)) + [planes - 1]:
            sol[z] = one * v1[z] + two * v2[z]
            dup[z] = jnp.dot(sol[z], spread, precision=HIGHEST, preferred_element_type=F32)

        z_at = 9 * rows
        z_base = one_side(high_of, gz, "gz", counts[0], slice(z_at + 4 * nx, z_at + 5 * nx))
        z_inverse = one_side(high_of, gz, "gz", counts[0], slice(z_at + 5 * nx, z_at + 6 * nx))
        x_low, x_high = both(gx, "gx", counts[1], slice(3 * planes, 3 * planes + nz + 1))
        y_low, y_high = both(gy, "gy", counts[2], slice(0, nx))
        y_row_low, y_row_high = both(gy, "gy", counts[2], slice(nx, nx + 1))
        half = nx // 2
        y_pack = one_side(high_of, gy, "gy", counts[2], slice(nx + 8, nx + 8 + half))
        lane = lane_ids(nx)
        row = row_ids(nx)
        base = 5 * planes

        def spread_around(z):
            c, odd = z // 2, z % 2
            here = dup[c, :, :LANES]
            same = 3.0 * here + dup[c, :, LANES:]
            same += dup[(c + 1 if odd else c - 1) % planes, :, :LANES]
            slot = z % 2
            inter[slot, pl.ds(0, cx, 2), :] = (same + shift_rows(here, 1))[:cx, :]
            inter[slot, pl.ds(1, cx, 2), :] = (same + shift_rows(here, -1))[:cx, :]
            return inter[slot]

        def nodal(z):
            around = spread_around(z) + jnp.where(row == 0, x_low[z : z + 1, :], 0.0)
            around += jnp.where(row == nx - 1, x_high[z : z + 1, :], 0.0)
            around += jnp.where(lane == 0, shift_lanes(y_low, -(base + z)), 0.0)
            around += jnp.where(lane == LANES - 1, shift_lanes(y_high, -(base + z) - 1), 0.0)
            if z == nz:
                value = z_base + z_inverse * (around + fg[nz - 1])
                return from_above("gz", counts[0], value)
            return part[z] + inv[z] * around

        here = dup[:cz, cx, :LANES]
        same = 3.0 * here + dup[:cz, cx, LANES:] + dup[:cz, cx - 1, :LANES]
        small[pl.ds(0, cz, 2), :] = same + jnp.concatenate(
            [dup[planes - 1, cx : cx + 1, :LANES], here[: cz - 1]], axis=0
        )
        small[pl.ds(1, cz, 2), :] = same + dup[1 : cz + 1, cx, :LANES]
        for z in range(nz):
            left = shift_lanes(y_row_low, -(base + z))
            right = shift_lanes(y_row_high, -(base + z) - 1)
            value = jnp.where(lane1 == 0, left, 0.0)
            lines[z : z + 1, :] = jnp.where(lane1 == LANES - 1, right, value)
        x_value = tx[3 * nz : 4 * nz, :] + tx[4 * nz :, :] * (
            fg[:, nx - 1, :] + small[...] + lines[...]
        )
        x_value = from_above("gx", counts[1], x_value)

        lane_c = lane_ids(rows)
        even = jnp.zeros((rows, LANES), F32)
        odd = jnp.zeros((rows, LANES), F32)
        own = jnp.zeros((nx, LANES), F32)
        for z in range(nz):
            c = z // 2
            here = sol[c]
            same = 3.0 * here + shift_lanes(here, 1) + sol[(c + 1 if z % 2 else c - 1) % planes]
            even = jnp.where(lane_c == z, shift_lanes(same + shift_rows(here, 1), z - cy), even)
            odd = jnp.where(lane_c == z, shift_lanes(same + shift_rows(here, -1), z - cy), odd)
            own = jnp.where(lane == z, shift_lanes(fg[z], z + 1), own)
        inter[0, pl.ds(0, cx, 2), :] = even[:cx, :]
        inter[0, pl.ds(1, cx, 2), :] = odd[:cx, :]
        y_base = jnp.concatenate([y_pack, shift_lanes(y_pack, -nz)], axis=0)
        y_inverse = jnp.concatenate(
            [shift_lanes(y_pack, -2 * nz), shift_lanes(y_pack, -3 * nz)], axis=0
        )
        y_value = y_base + y_inverse * (own + inter[0])
        y_value = from_above("gy", counts[2], y_value)
        y_fix = shift_lanes(y_high, -(base + nz + 1)) * last[...]

        def copy(z):
            return pltpu.make_async_copy(buf.at[:, z], out.at[:, z], sem.at[z])

        value = nodal(0)
        for z in range(nz):
            after = nodal(z + 1)
            steps = [after, jnp.where(row == nx - 1, x_value[z : z + 1, :], shift_rows(value, -1))]
            steps.append(
                jnp.where(lane == LANES - 1, shift_lanes(y_value, -z - 1), shift_lanes(value, -1))
            )
            for k in range(3):
                fixed = jnp.where(lane == LANES - 1, shift_lanes(y_fix, -(k * nz + z) - 1), 0.0)
                buf[k, z] = (smooth[k, z] + fixed) + (steps[k] - value)
            copy(z).start()
            value = after
        for z in range(nz):
            copy(z).wait()

    return call(
        body,
        [smooth.shape],
        scratch=[
            (planes, rows, LANES),
            (planes, rows, 2 * LANES),
            (2, nx, LANES),
            (nz, LANES),
            (nz, LANES),
            smooth.shape,
            pltpu.SemaphoreType.DMA((nz,)),
        ],
        far_out=True,
        in_specs=vmem(9 + gots),
        out_specs=[pl.BlockSpec(memory_space=pltpu.HBM)],
    )(sums, v1, v2, fg, *mid, smooth, last, tail_x, *got_z, *got_x, *got_y)[0]


def local(residual, edge_diag, node_shift, coarse_shift):
    axes = ("gz", "gx", "gy")
    counts = tuple(lax.axis_size(a) for a in axes)
    devices = counts[0] * counts[1] * counts[2]
    part, *faces, scaled, inverses = edge_stage(residual, edge_diag)
    up_z, up_x, up_y, low_z, low_x, low_y = faces
    below = []
    for value, axis in ((up_z, "gz"), (up_x, "gx"), (up_y, "gy")):
        below.append(ring(value, axis, 1))
    fg, rhs, xb, yb, w, *send = nodal_stage(part, node_shift, coarse_shift, *below, low_z, counts[0])
    got_z = swap(send, "gz")
    rhs, yb, w, *send = x_stage(got_z, rhs, xb, yb, w, fg, counts[0], counts[1])
    got_x = swap(send, "gx", ("gx", "gy"))
    planes = rhs.shape[0]
    tail_x = x_tail(got_z, fg, node_shift, low_x, w, counts[0])
    mid = part_stage(got_z, fg, node_shift, w, counts[0])
    early = y_early(got_z, fg, node_shift, low_y, w, planes, counts[0])
    early = (*early, tail_x, mid[1])
    tail_x = ring(tail_x, "gx", -1)
    rhs, w, *send = y_stage(got_x, rhs, yb, w, early, counts[1], counts[2])
    got_y = swap(send, "gy", ("gx", "gy"))
    smooth, last = smooth_stage(scaled, inverses, below, got_z, tail_x, w, counts)
    v1, v2, sums = coarse_stage(got_y, rhs, w, (last,), counts[2], devices)
    sums = lax.all_to_all(sums, ("gx", "gy", "gz"), 0, 0)
    return final_stage(sums, v1, v2, fg, mid, smooth, last, tail_x, got_z, got_x, got_y, counts)


def solution(mesh):
    placed = (
        P(None, "gz", "gx", "gy"),
        P(None, "gz", "gx", "gy"),
        P("gz", "gx", "gy"),
        P("gz", "gx", "gy"),
    )

    return jax.shard_map(
        local, mesh=mesh, in_specs=placed, out_specs=P(None, "gz", "gx", "gy"), check_vma=False
    )
```

```python
import itertools

import jax
import jax.numpy as jnp
from jax import lax
from jax.experimental import pallas as pl
from jax.experimental.pallas import tpu as pltpu
from jax.sharding import PartitionSpec as P


F32 = jnp.float32
HIGHEST = lax.Precision.HIGHEST
LANES = 128


def lane_ids(rows):
    return lax.broadcasted_iota(jnp.int32, (rows, LANES), 1)


def row_ids(rows):
    return lax.broadcasted_iota(jnp.int32, (rows, LANES), 0)


def shift_lanes(value, amount):
    return pltpu.roll(value, amount % LANES, 1)


def shift_rows(value, amount):
    return pltpu.roll(value, amount % value.shape[0], 0)


def low_of(axis, size, first, second):
    place = lax.axis_index(axis)
    odd = place % 2 == 1
    zero = jnp.zeros_like(first)
    if second is None:
        return jnp.where(odd, first, zero)
    return jnp.where(odd, first, jnp.where(place > 0, second, zero))


def high_of(axis, size, first, second):
    place = lax.axis_index(axis)
    even = place % 2 == 0
    zero = jnp.zeros_like(first)
    if second is None:
        return jnp.where(even, first, zero)
    return jnp.where(even, first, jnp.where(place < size - 1, second, zero))


def from_below(axis, value):
    return jnp.where(lax.axis_index(axis) > 0, value, jnp.zeros_like(value))


def from_above(axis, size, value):
    return jnp.where(lax.axis_index(axis) < size - 1, value, jnp.zeros_like(value))


def ring(value, axis, step):
    size = lax.axis_size(axis)
    return lax.ppermute(value, axis, [(i, (i + step) % size) for i in range(size)])


def swap(values, axis, names=None):
    size = lax.axis_size(axis)
    out = [lax.ppermute(values[0], axis, [(i, i ^ 1) for i in range(size)])]
    if len(values) == 1:
        return out
    odd = [(i + 1) % size if i % 2 else (i - 1) % size for i in range(size)]
    if names is None:
        out.append(lax.ppermute(values[1], axis, list(enumerate(odd))))
        return out
    main = names.index(axis)
    pairs = []
    sizes = [lax.axis_size(name) for name in names]
    for at in itertools.product(*(range(n) for n in sizes)):
        to = list(at)
        if at[main] in (0, size - 1):
            to[1 - main] ^= 1
        else:
            to[main] = odd[at[main]]
        pairs.append(tuple(p[0] * sizes[1] + p[1] for p in (at, to)))
    out.append(lax.ppermute(values[1], names, pairs))
    return out


def write_sides(axis, refs, up, down):
    even = lax.axis_index(axis) % 2 == 0

    @pl.when(even)
    def _():
        up(refs[0])
        if len(refs) > 1:
            down(refs[1])

    @pl.when(jnp.logical_not(even))
    def _():
        down(refs[0])
        if len(refs) > 1:
            up(refs[1])


def call(body, outs, scratch=(), far=(), far_out=False, **kwargs):
    kind = jax.ShapeDtypeStruct if far_out else pltpu.VMEM
    run = pl.pallas_call(
        body,
        out_shape=[kind(shape, F32) for shape in outs],
        scratch_shapes=[pltpu.VMEM(s, F32) if isinstance(s, tuple) else s for s in scratch],
        compiler_params=pltpu.CompilerParams(vmem_limit_bytes=12 * 2**20),
        **kwargs,
    )

    def apply(*args):
        spaces = [pltpu.HBM if i in far else pltpu.VMEM for i in range(len(args))]
        return run(
            *(
                pltpu.with_memory_space_constraint(a, space)
                for a, space in zip(args, spaces)
            )
        )

    return apply


def vmem(count):
    return [pl.BlockSpec(memory_space=pltpu.VMEM)] * count


def edge_stage(residual, edge_diag):
    _, nz, nx, ny = residual.shape
    step = 2
    steps = nz // step

    def body(res, diag, part, up_z, up_x, up_y, low_z, low_x, low_y, scaled, inv, near, sems):
        lane = lane_ids(nx)
        row = row_ids(nx)

        def copies(block):
            at = pl.ds(block * step, step)
            return [
                pltpu.make_async_copy(source.at[:, at], target.at[:, at], sems.at[i, block])
                for i, (source, target) in enumerate(((res, near), (diag, inv)))
            ]

        for block in range(steps):
            for copy in copies(block):
                copy.start()
        before = jnp.zeros((nx, ny), F32)
        high = jnp.zeros((nx, LANES), F32)
        low = jnp.zeros((nx, LANES), F32)
        for z in range(nz):
            if z % step == 0:
                for copy in copies(z // step):
                    copy.wait()
            s = []
            for k in range(3):
                inverse = 1.0 / inv[k, z]
                inv[k, z] = inverse
                s.append(near[k, z] * inverse)
                scaled[k, z] = s[k]
            total = before - s[0]
            total += jnp.where(row == 0, 0.0, shift_rows(s[1], 1)) - s[1]
            total += jnp.where(lane == 0, 0.0, shift_lanes(s[2], 1)) - s[2]
            part[z] = total
            before = s[0]
            for k in range(3):
                spot = k * nz + z
                up_x[spot : spot + 1, :] = s[k][nx - 1 :, :]
                low_x[spot : spot + 1, :] = s[k][:1, :]
                high = jnp.where(lane == spot, shift_lanes(s[k], spot + 1), high)
                low = jnp.where(lane == spot, shift_lanes(s[k], spot), low)
                if z == 0:
                    low_z[k] = s[k]
                if z == nz - 1:
                    up_z[k] = s[k]
        up_y[...] = high
        low_y[...] = low

    faces = [(3, nx, ny), (3 * nz, ny), (nx, LANES)] * 2
    return call(
        body,
        [(nz, nx, ny)] + faces + [residual.shape] * 2,
        scratch=[residual.shape, pltpu.SemaphoreType.DMA((2, steps))],
        far=(0, 1),
        in_specs=[pl.BlockSpec(memory_space=pltpu.HBM)] * 2,
        out_specs=vmem(9),
    )(residual, edge_diag)


def plane(values, row_count):
    return jnp.concatenate([values, jnp.zeros((row_count - values.shape[0], LANES), F32)], axis=0)


def nodal_stage(part, node_shift, coarse_shift, got_z, got_x, got_y, z_count):
    nz, nx, ny = part.shape
    cz, cx, cy = nz // 2, nx // 2, ny // 2
    rows = cx + 8
    sends = 1 if z_count == 2 else 2

    def body(part, shift, coarse, gz, gx, gy, fg, rhs, xb, yb, w, *rest):
        out, (pair, s_, xl_, yl_, zl_, zh_) = rest[:sends], rest[sends:]
        lane = lane_ids(nx)
        row = row_ids(nx)
        lane_c = lane_ids(rows)
        row_c = row_ids(rows)
        below_z = from_below("gz", gz[0])
        below_y = from_below("gy", gy[...])
        fine = lax.broadcasted_iota(jnp.int32, (ny, 2 * LANES), 0)
        coarse_lane = lax.broadcasted_iota(jnp.int32, (ny, 2 * LANES), 1)
        miss = jnp.where(
            coarse_lane < LANES, fine // 2 - coarse_lane, fine - 2 * (coarse_lane - LANES)
        )
        gather = jnp.where(miss == 0, 1.0, 0.0)
        for c in range(cz):
            both = []
            for z in (2 * c, 2 * c + 1):
                total = part[z]
                if z == 0:
                    total += below_z
                total += jnp.where(row == 0, from_below("gx", gx[nz + z : nz + z + 1, :]), 0.0)
                total += jnp.where(lane == 0, shift_lanes(below_y, -(2 * nz + z)), 0.0)
                guess = total / (6.0 + shift[z])
                fg[z] = guess
                both.append(guess)
            pair[c % 2] = both[0] + both[1]
            low = pair[c % 2, pl.ds(0, cx, 2), :]
            high = pair[c % 2, pl.ds(1, cx, 2), :]
            first = fg[2 * c, pl.ds(0, cx, 2), :] + fg[2 * c, pl.ds(1, cx, 2), :]
            stacked = jnp.concatenate([low + high, low, first], axis=0)
            sums = jnp.dot(stacked, gather, precision=HIGHEST, preferred_element_type=F32)
            s = sums[:cx, :LANES]
            z_low = sums[2 * cx :, :LANES]
            s_[c] = plane(s, rows)
            yl_[c] = plane(sums[:cx, LANES:], rows)
            xl_[c] = plane(sums[cx : 2 * cx, :LANES], rows)
            zl_[c] = plane(z_low, rows)
            zh_[c] = plane(s - z_low, rows)
            w[c] = jnp.zeros((rows, LANES), F32)
            w[c, :cx, :cy] = 1.0 / (6.0 + coarse[c])
        for c in range(cz):
            s, x_low, y_low = s_[c], xl_[c], yl_[c]
            x_high = s - x_low
            y_high = s - y_low
            total = 3.0 * s
            total += shift_rows(x_low, -1) + shift_rows(x_high, 1)
            total += shift_lanes(y_low, -1) + shift_lanes(y_high, 1)
            if c > 0:
                total += zh_[c - 1]
            if c < cz - 1:
                total += zl_[c + 1]
            rhs[c] = total
            xb[c] = jnp.where(row_c < cx // 2, x_low, x_high)
            yb[c] = jnp.where(lane_c < cy // 2, y_low, y_high)
        rhs[cz] = zh_[cz - 1]
        rhs[cz + 1] = jnp.zeros((rows, LANES), F32)
        rhs[cz + 2] = jnp.zeros((rows, LANES), F32)
        rhs[cz + 3] = zl_[0]

        def fill(ref, near, far, half, face):
            planes = [rhs[near], rhs[far], w[near], w[far], half]
            planes += [xb[near], xb[far], yb[near], yb[far]]
            for i, value in enumerate(planes):
                ref[i * rows : (i + 1) * rows, :] = value
            ref[9 * rows : 9 * rows + nx, :] = face

        def up(ref):
            fill(ref, cz - 1, cz - 2, zh_[cz - 1], fg[nz - 1])

        def down(ref):
            fill(ref, 0, 1, zl_[0], fg[0])

        write_sides("gz", out, up, down)

    coarse = (cz, rows, LANES)
    send = (9 * rows + nx, LANES)
    return call(
        body,
        [(nz, nx, ny), (cz + 4, rows, LANES), coarse, coarse, coarse] + [send] * sends,
        scratch=[(2, nx, ny), coarse, coarse, coarse, coarse, coarse],
        in_specs=vmem(6),
        out_specs=vmem(5 + sends),
    )(part, node_shift, coarse_shift, got_z, got_x, got_y)


def x_stage(got, rhs, xb, yb, w, fg, z_count, x_count):
    planes, rows, _ = rhs.shape
    cz, cx = planes - 4, rows - 8
    nz, nx, ny = fg.shape
    cy = ny // 2
    sends = 1 if x_count == 2 else 2
    gots = len(got)
    size = -(-(3 * planes + nz + 1) // 8) * 8

    def body(*refs):
        got = refs[:gots]
        rhs, xb, yb, w, fg, rhs2, w2 = refs[gots : gots + 7]
        out, (xb2, yb2) = refs[gots + 7 : gots + 7 + sends], refs[gots + 7 + sends :]

        def take_at(pick, at):
            values = [ref[at, :] for ref in got]
            return pick("gz", z_count, values[0], values[1] if gots > 1 else None)

        def take(pick, i):
            return take_at(pick, slice(i * rows, (i + 1) * rows))

        for c in range(1, cz - 1):
            rhs2[c] = rhs[c]
        rhs2[0] = rhs[0] + take(low_of, 4)
        rhs2[cz - 1] = rhs[cz - 1] + take(high_of, 4)
        rhs2[cz] = rhs[cz] + take(high_of, 0)
        rhs2[cz + 1] = take(high_of, 1)
        rhs2[cz + 2] = take(low_of, 1)
        rhs2[cz + 3] = rhs[cz + 3] + take(low_of, 0)
        for here, there, i in ((w, w2, 2), (xb, xb2, 5), (yb, yb2, 7)):
            for c in range(cz):
                there[c] = here[c]
            there[cz] = take(high_of, i)
            there[cz + 1] = take(high_of, i + 1)
            there[cz + 2] = take(low_of, i + 1)
            there[cz + 3] = take(low_of, i)

        lane = lane_ids(planes)

        def fill(ref, near, far, fine):
            halves = lane < cy
            first = jnp.where(halves, rhs2[:, near, :], shift_lanes(rhs2[:, far, :], cy))
            second = jnp.where(halves, w2[:, near, :], shift_lanes(w2[:, far, :], cy))
            edge = yb2[:, far, :]
            third = jnp.where(halves, xb2[:, near, :], shift_lanes(yb2[:, near, :], cy))
            third = jnp.where(lane == cy + 1, shift_lanes(edge, cy + 1), third)
            third = jnp.where(lane == LANES - 2, shift_lanes(edge, cy - 1), third)
            for i, value in enumerate((first, second, third)):
                ref[i * planes : (i + 1) * planes, :] = value
            ref[3 * planes : 3 * planes + nz, :] = fg[:, fine, :]
            at = 9 * rows + fine
            last = 3 * planes + nz
            ref[last : last + 1, :] = take_at(high_of, slice(at, at + 1))
            ref[last + 1 :, :] = jnp.zeros((size - last - 1, LANES), F32)

        def up(ref):
            fill(ref, cx - 1, cx - 2, nx - 1)

        def down(ref):
            fill(ref, 0, 1, 0)

        write_sides("gx", out, up, down)

    whole = (planes, rows, LANES)
    return call(
        body,
        [whole, whole] + [(size, LANES)] * sends,
        scratch=[whole, whole],
        in_specs=vmem(gots + 5),
        out_specs=vmem(2 + sends),
    )(*got, rhs, xb, yb, w, fg)


def x_tail(got, fg, node_shift, low_x, after, z_count):
    nz, nx, ny = fg.shape
    z_at = 9 * (nx // 2 + 8)
    gots = len(got)

    def body(*refs):
        got = refs[:gots]
        fg, shift, low_x, _, out = refs[gots:]
        lane = lane_ids(nz)
        row = row_ids(nz)

        def z_row(pick):
            values = [ref[z_at : z_at + 1, :] for ref in got]
            return pick("gz", z_count, values[0], values[1] if gots > 1 else None)

        here = fg[:, 0, :]
        around = fg[:, 1, :] + jnp.where(row == 0, z_row(low_of), shift_rows(here, 1))
        around += jnp.where(row == nz - 1, z_row(high_of), shift_rows(here, -1))
        around += jnp.where(lane == 0, 0.0, shift_lanes(here, 1))
        around += jnp.where(lane == ny - 1, 0.0, shift_lanes(here, -1))
        inverse = 1.0 / (6.0 + shift[:, 0, :])
        out[: 3 * nz, :] = low_x[...]
        out[3 * nz : 4 * nz, :] = here + inverse * around
        out[4 * nz :, :] = inverse

    return call(
        body, [(5 * nz, LANES)], in_specs=vmem(gots + 4), out_specs=vmem(1)
    )(*got, fg, node_shift, low_x, after)[0]


def part_stage(got, fg, node_shift, low_z, after, z_count):
    nz, nx, ny = fg.shape
    z_at = 9 * (nx // 2 + 8)
    gots = len(got)

    def body(*refs):
        got = refs[:gots]
        fg, shift, low_z, _, part, inv, tail = refs[gots:]
        lane = lane_ids(nx)
        row = row_ids(nx)

        def z_face(pick):
            values = [ref[z_at : z_at + nx, :] for ref in got]
            return pick("gz", z_count, values[0], values[1] if gots > 1 else None)

        for z in range(nz):
            guess = fg[z]
            inner = fg[z + 1] if z < nz - 1 else z_face(high_of)
            inner += jnp.where(row == 0, 0.0, shift_rows(guess, 1))
            inner += jnp.where(row == nx - 1, 0.0, shift_rows(guess, -1))
            inner += jnp.where(lane == 0, 0.0, shift_lanes(guess, 1))
            inner += jnp.where(lane == ny - 1, 0.0, shift_lanes(guess, -1))
            inverse = 1.0 / (6.0 + shift[z])
            inv[z] = inverse
            part[z] = guess + inverse * (inner + (fg[z - 1] if z > 0 else z_face(low_of)))
            if z == 0:
                for k in range(3):
                    tail[k * nx : (k + 1) * nx, :] = low_z[k]
                tail[3 * nx : 4 * nx, :] = guess + inverse * inner
                tail[4 * nx :, :] = inverse

    return call(
        body, [fg.shape, fg.shape, (5 * nx, LANES)], in_specs=vmem(gots + 4), out_specs=vmem(3)
    )(*got, fg, node_shift, low_z, after)


def line(source, lane, fine, at):
    acc = jnp.zeros(lane.shape, F32)
    for z in range(source.shape[0]):
        moved = jnp.broadcast_to(source[z : z + 1, :], lane.shape)
        acc = jnp.where(lane == at + z, shift_lanes(moved, at + z - fine), acc)
    return acc


def y_stage(got, rhs, w, early, x_count, y_count):
    planes, rows, _ = rhs.shape
    cx = rows - 8
    nx, cy = 2 * cx, LANES // 2
    nz, half = 2 * (planes - 4), nx // 2
    sends = 1 if y_count == 2 else 2
    gots = len(got)

    def body(*refs):
        got = refs[:gots]
        rhs, w, up_, down_, part, inv, _, _, rhs3, w3 = refs[gots : gots + 10]
        rest = refs[gots + 10 :]
        out, (add,) = rest[:sends], rest[sends:]
        lane_p = lane_ids(planes)

        def take_at(pick, at):
            values = [ref[at, :] for ref in got]
            return pick("gx", x_count, values[0], values[1] if gots > 1 else None)

        def take(pick, i):
            return take_at(pick, slice(i * planes, (i + 1) * planes))

        add[...] = jnp.zeros_like(add)
        for c in range(planes):
            w3[c] = w[c]
        for pick, near, far, edge in ((high_of, cx, cx + 1, cx - 1), (low_of, rows - 1, rows - 2, 0)):
            first, second, third = take(pick, 0), take(pick, 1), take(pick, 2)
            other = shift_lanes(third, -cy)
            one = jnp.where((lane_p == 0) | (lane_p == cy - 1), other, 0.0)
            two = jnp.where(lane_p == 0, shift_lanes(third, -cy - 1), 0.0)
            two = jnp.where(lane_p == cy - 1, shift_lanes(third, 1 - cy), two)
            for at, value, ends in ((near, first, one), (far, shift_lanes(first, -cy), two)):
                value = jnp.where(lane_p < cy, value, 0.0)
                value += jnp.where(lane_p == cy, shift_lanes(ends, 1), 0.0)
                value += jnp.where(lane_p == LANES - 1, shift_lanes(ends, -1), 0.0)
                add[:, at, :] = value
            w3[:, near, :] = jnp.where(lane_p < cy, second, 0.0)
            w3[:, far, :] = jnp.where(lane_p < cy, shift_lanes(second, -cy), 0.0)
            add[:, edge, :] = jnp.where(lane_p < cy, third, 0.0)
        for c in range(planes):
            rhs3[c] = rhs[c] + add[c]

        lane_c = lane_ids(rows)
        lane8 = lane_ids(8)
        base = 5 * planes
        x_face = slice(3 * planes, 3 * planes + nz)
        x_high = take_at(high_of, x_face)

        def fill(ref, first, fine, early):
            acc = jnp.zeros((rows, LANES), F32)
            inner = first if first > 0 else 0
            for z in range(planes):
                for field, width, at, source in (
                    (rhs3, 3, 3 * z, first),
                    (w3, 2, 3 * planes + 2 * z, inner),
                ):
                    there = (lane_c >= at) & (lane_c < at + width)
                    acc = jnp.where(there, shift_lanes(field[z], at - source), acc)
            ref[:nx, :] = plane(acc, nx) + early[...]
            ref[nx : nx + 8, :] = line(x_high, lane8, fine, base)

        def up(ref):
            fill(ref, cy - 2, 2 * cy - 1, up_)
            ref[nx + 8 :, :] = jnp.zeros((half, LANES), F32)

        def down(ref):
            fill(ref, -1, 0, down_)
            row = row_ids(nx)
            ends = jnp.where(row == 0, line(take_at(low_of, x_face), lane8, 0, 0)[:1, :], 0.0)
            ends += jnp.where(row == nx - 1, line(x_high, lane8, 0, 0)[:1, :], 0.0)
            inverse = inv[...]
            value = part[...] + inverse * ends
            packed = jnp.zeros((half, LANES), F32)
            for i, source in enumerate((value[:half], value[half:], inverse[:half], inverse[half:])):
                there = lane_ids(half) // nz == i
                packed = jnp.where(there, shift_lanes(source, i * nz), packed)
            ref[nx + 8 :, :] = packed

        write_sides("gy", out, up, down)

    whole = (planes, rows, LANES)
    return call(
        body,
        [whole, whole] + [(nx + 8 + half, LANES)] * sends,
        scratch=[whole],
        in_specs=vmem(gots + 8),
        out_specs=vmem(2 + sends),
    )(*got, rhs, w, *early)


def y_early(got_z, fg, node_shift, low_y, after, planes, z_count):
    nz, nx, _ = fg.shape
    z_at = 9 * (nx // 2 + 8)
    base = 5 * planes
    n_z = len(got_z)

    def body(*refs):
        gz = refs[:n_z]
        fg, shift, low_y, _, up, down, part, inv = refs[n_z:]
        lane = lane_ids(nx)
        row = row_ids(nx)

        def side(pick):
            values = [ref[z_at : z_at + nx, :] for ref in gz]
            return pick("gz", z_count, values[0], values[1] if n_z > 1 else None)

        above = side(high_of)
        here = jnp.where(lane == nz, shift_lanes(above, nz), 0.0)
        here = jnp.where(lane == LANES - 1, shift_lanes(side(low_of), -1), here)
        high = jnp.where(lane == base + nz, shift_lanes(above, base + nz + 1), 0.0)
        inverse = jnp.ones((nx, LANES), F32)
        inner = jnp.zeros((nx, LANES), F32)
        for z in range(nz):
            guess = fg[z]
            here = jnp.where(lane == z, shift_lanes(guess, z), here)
            inner = jnp.where(lane == z, shift_lanes(guess, z - 1), inner)
            high = jnp.where(lane == base + z, shift_lanes(guess, base + z + 1), high)
            inverse = jnp.where(lane == z, shift_lanes(6.0 + shift[z], z), inverse)
        inverse = 1.0 / inverse
        around = inner + shift_lanes(here, 1) + shift_lanes(here, -1)
        around += jnp.where(row == 0, 0.0, shift_rows(here, 1))
        around += jnp.where(row == nx - 1, 0.0, shift_rows(here, -1))
        up[...] = high
        at = base + nz + 1
        low = jnp.where((lane >= base) & (lane < at), shift_lanes(here, base), 0.0)
        down[...] = jnp.where((lane >= at) & (lane < at + 3 * nz), shift_lanes(low_y[...], at), low)
        part[...] = here + inverse * around
        inv[...] = inverse

    return call(
        body, [(nx, LANES)] * 4, in_specs=vmem(n_z + 4), out_specs=vmem(4)
    )(*got_z, fg, node_shift, low_y, after)


def coarse_stage(got, rhs, w, after, y_count, devices):
    planes, rows, _ = rhs.shape
    cz, cx = planes - 4, rows - 8
    cy = LANES // 2
    gots = len(got)

    def body(*refs):
        got = refs[:gots]
        rhs, w, _, v1, v2, sums, tot, inv_, image_ = refs[gots:]
        values = [ref[:rows, :] for ref in got]
        second = values[1] if gots > 1 else None
        low = low_of("gy", y_count, values[0], second)
        high = high_of("gy", y_count, values[0], second)
        lane = lane_ids(rows)
        above = (lane >= cy - 1) & (lane < cy + 2)
        below = (lane >= LANES - 2) | (lane == 0)
        for z in range(planes):
            at = 3 * z
            right = jnp.where(below, shift_lanes(low, LANES - 2 - at), 0.0)
            right = rhs[z] + jnp.where(above, shift_lanes(high, cy - 1 - at), right)
            at = 3 * planes + 2 * z
            inv = jnp.where(lane >= LANES - 2, shift_lanes(low, LANES - 2 - at), w[z])
            inv = jnp.where((lane >= cy) & (lane < cy + 2), shift_lanes(high, cy - at), inv)
            inv_[z] = inv
            tot[z] = right
            v1[z] = right * inv

        def near(field, z):
            here = field[z]
            total = field[(z + 1) % planes] + field[(z - 1) % planes]
            total += shift_rows(here, 1) + shift_rows(here, -1)
            return total + shift_lanes(here, 1) + shift_lanes(here, -1)

        v2[cz + 1] = jnp.zeros((rows, LANES), F32)
        v2[cz + 2] = jnp.zeros((rows, LANES), F32)
        for z in list(range(cz + 1)) + [planes - 1]:
            image = tot[z] - near(v1, z)
            if z < cz:
                image_[z] = image
            v2[z] = image * inv_[z]
        parts = [jnp.zeros((cx, LANES), F32)] * 5
        for z in range(cz):
            first, second_, right, image = v1[z], v2[z], tot[z], image_[z]
            third = image - near(v2, z)
            terms = (first * right, second_ * right, first * image, second_ * image, second_ * third)
            parts = [a + b[:cx, :] for a, b in zip(parts, terms)]
        keep = lane_ids(1) < cy
        lines = [jnp.where(keep, jnp.sum(a, axis=0, keepdims=True), 0.0) for a in parts]
        tile = jnp.concatenate(lines + [jnp.zeros((3, LANES), F32)], axis=0)
        column = jnp.sum(tile, axis=1, keepdims=True)
        spread = jnp.where(lane_ids(8) == row_ids(8), column, 0.0)
        line = jnp.sum(spread, axis=0, keepdims=True)
        sums[...] = jnp.broadcast_to(line[None], (devices, 1, LANES))

    whole = (planes, rows, LANES)
    return call(
        body,
        [whole, whole, (devices, 1, LANES)],
        scratch=[whole, whole, whole],
        in_specs=vmem(gots + 3),
        out_specs=vmem(3),
    )(*got, rhs, w, *after)


def smooth_stage(scaled, inverses, below, tail_z, tail_x, after, counts):
    _, nz, nx, _ = scaled.shape

    def body(*refs):
        s, inv, lz, lx, ly = refs[:5]
        tz, gx, _, out, last = refs[5:]
        lane = lane_ids(nx)
        row = row_ids(nx)
        y_low = from_below("gy", ly[...])

        acc = jnp.zeros((nx, LANES), F32)
        for k in range(3):
            z_low = from_below("gz", lz[k])
            z_high = from_above("gz", counts[0], tz[k * nx : (k + 1) * nx, :])
            x_low = from_below("gx", lx[k * nz : (k + 1) * nz, :])
            x_high = from_above("gx", counts[1], gx[k * nz : (k + 1) * nz, :])
            for z in range(nz):
                here = s[k, z]
                around = s[k, z - 1] if z > 0 else z_low
                around += s[k, z + 1] if z < nz - 1 else z_high
                around += jnp.where(row == 0, x_low[z : z + 1, :], shift_rows(here, 1))
                around += jnp.where(row == nx - 1, x_high[z : z + 1, :], shift_rows(here, -1))
                spot = k * nz + z
                around += jnp.where(lane == 0, shift_lanes(y_low, -spot), shift_lanes(here, 1))
                around += jnp.where(lane == LANES - 1, 0.0, shift_lanes(here, -1))
                inverse = inv[k, z]
                acc = jnp.where(lane == spot, shift_lanes(inverse, spot + 1), acc)
                out[k, z] = here + around * inverse
        last[...] = acc

    return call(
        body, [scaled.shape, (nx, LANES)], in_specs=vmem(8), out_specs=vmem(2)
    )(scaled, inverses, *below, tail_z, tail_x, after)


def final_stage(sums, v1, v2, fg, mid, smooth, last, early, tail_z, tail_x, got_x, got_y, counts):
    planes, rows, _ = v1.shape
    cz, cx, cy = planes - 4, rows - 8, LANES // 2
    nz, nx, _ = fg.shape
    n_x, n_y = len(got_x), len(got_y)
    gots = n_x + n_y

    def body(*refs):
        sums, v1, v2, fg, part, inv, smooth, last, early, tz, tx = refs[:11]
        gx = refs[11 : 11 + n_x]
        gy = refs[11 + n_x : 11 + gots]
        out, sol, dup, inter, small, lines, buf, sem = refs[11 + gots :]

        def one_side(pick, refs, axis, size, at):
            values = [ref[at, :] for ref in refs]
            return pick(axis, size, values[0], values[1] if len(values) > 1 else None)

        def both(refs, axis, size, at):
            return [one_side(pick, refs, axis, size, at) for pick in (low_of, high_of)]

        total = jnp.sum(sums[...], axis=0)
        lane1 = lane_ids(1)
        gone, gtwo, hone, hmix, htwo = [
            jnp.sum(jnp.where(lane1 == i, total, 0.0), axis=1, keepdims=True) for i in range(5)
        ]
        two = (gtwo - hmix * gone / hone) / (htwo - hmix * hmix / hone)
        one = (gone - hmix * two) / hone
        source = lax.broadcasted_iota(jnp.int32, (LANES, 2 * LANES), 0)
        target = lax.broadcasted_iota(jnp.int32, (LANES, 2 * LANES), 1)
        fine = target - LANES
        side = jnp.where(fine % 2 == 1, fine // 2 + 1, (fine // 2 + LANES - 1) % LANES)
        spread = jnp.where(jnp.where(target < LANES, target // 2, side) == source, 1.0, 0.0)
        for z in list(range(cz + 1)) + [planes - 1]:
            sol[z] = one * v1[z] + two * v2[z]
            dup[z] = jnp.dot(sol[z], spread, precision=HIGHEST, preferred_element_type=F32)

        x_low, x_high = both(gx, "gx", counts[1], slice(3 * planes, 3 * planes + nz + 1))
        y_low, y_high = both(gy, "gy", counts[2], slice(0, nx))
        y_row_low, y_row_high = both(gy, "gy", counts[2], slice(nx, nx + 1))
        half = nx // 2
        y_pack = one_side(high_of, gy, "gy", counts[2], slice(nx + 8, nx + 8 + half))
        lane = lane_ids(nx)
        row = row_ids(nx)
        base = 5 * planes

        def spread_around(z):
            c, odd = z // 2, z % 2
            here = dup[c, :, :LANES]
            same = 3.0 * here + dup[c, :, LANES:]
            same += dup[(c + 1 if odd else c - 1) % planes, :, :LANES]
            slot = z % 2
            inter[slot, pl.ds(0, cx, 2), :] = (same + shift_rows(here, 1))[:cx, :]
            inter[slot, pl.ds(1, cx, 2), :] = (same + shift_rows(here, -1))[:cx, :]
            return inter[slot]

        def nodal(z):
            around = spread_around(z) + jnp.where(row == 0, x_low[z : z + 1, :], 0.0)
            around += jnp.where(row == nx - 1, x_high[z : z + 1, :], 0.0)
            around += jnp.where(lane == 0, shift_lanes(y_low, -(base + z)), 0.0)
            around += jnp.where(lane == LANES - 1, shift_lanes(y_high, -(base + z) - 1), 0.0)
            if z == nz:
                value = tz[3 * nx : 4 * nx, :] + tz[4 * nx :, :] * (around + fg[nz - 1])
                return from_above("gz", counts[0], value)
            return part[z] + inv[z] * around

        here = dup[:cz, cx, :LANES]
        same = 3.0 * here + dup[:cz, cx, LANES:] + dup[:cz, cx - 1, :LANES]
        small[pl.ds(0, cz, 2), :] = same + jnp.concatenate(
            [dup[planes - 1, cx : cx + 1, :LANES], here[: cz - 1]], axis=0
        )
        small[pl.ds(1, cz, 2), :] = same + dup[1 : cz + 1, cx, :LANES]
        for z in range(nz):
            left = shift_lanes(y_row_low, -(base + z))
            right = shift_lanes(y_row_high, -(base + z) - 1)
            value = jnp.where(lane1 == 0, left, 0.0)
            lines[z : z + 1, :] = jnp.where(lane1 == LANES - 1, right, value)
        x_value = tx[3 * nz : 4 * nz, :] + tx[4 * nz :, :] * (
            fg[:, nx - 1, :] + small[...] + lines[...]
        )
        x_value = from_above("gx", counts[1], x_value)

        lane_c = lane_ids(rows)
        even = jnp.zeros((rows, LANES), F32)
        odd = jnp.zeros((rows, LANES), F32)
        for z in range(nz):
            c = z // 2
            here = sol[c]
            same = 3.0 * here + shift_lanes(here, 1) + sol[(c + 1 if z % 2 else c - 1) % planes]
            even = jnp.where(lane_c == z, shift_lanes(same + shift_rows(here, 1), z - cy), even)
            odd = jnp.where(lane_c == z, shift_lanes(same + shift_rows(here, -1), z - cy), odd)
        inter[0, pl.ds(0, cx, 2), :] = even[:cx, :]
        inter[0, pl.ds(1, cx, 2), :] = odd[:cx, :]
        y_base = jnp.concatenate([y_pack, shift_lanes(y_pack, -nz)], axis=0)
        y_inverse = jnp.concatenate(
            [shift_lanes(y_pack, -2 * nz), shift_lanes(y_pack, -3 * nz)], axis=0
        )
        y_value = y_base + y_inverse * (shift_lanes(early[...], -base) + inter[0])
        y_value = from_above("gy", counts[2], y_value)
        y_fix = shift_lanes(y_high, -(base + nz + 1)) * last[...]
        y_value += shift_lanes(y_fix, -2 * nz)

        def copy(z):
            return pltpu.make_async_copy(buf.at[:, z], out.at[:, z], sem.at[z])

        value = nodal(0)
        for z in range(nz):
            after = nodal(z + 1)
            steps = [after, jnp.where(row == nx - 1, x_value[z : z + 1, :], shift_rows(value, -1))]
            steps.append(
                jnp.where(lane == LANES - 1, shift_lanes(y_value, -z - 1), shift_lanes(value, -1))
            )
            for k in range(3):
                moved = smooth[k, z]
                if k < 2:
                    fixed = shift_lanes(y_fix, -(k * nz + z) - 1)
                    moved += jnp.where(lane == LANES - 1, fixed, 0.0)
                buf[k, z] = moved + (steps[k] - value)
            copy(z).start()
            value = after
        for z in range(nz):
            copy(z).wait()

    return call(
        body,
        [smooth.shape],
        scratch=[
            (planes, rows, LANES),
            (planes, rows, 2 * LANES),
            (2, nx, LANES),
            (nz, LANES),
            (nz, LANES),
            smooth.shape,
            pltpu.SemaphoreType.DMA((nz,)),
        ],
        far_out=True,
        in_specs=vmem(11 + gots),
        out_specs=[pl.BlockSpec(memory_space=pltpu.HBM)],
    )(sums, v1, v2, fg, *mid, smooth, last, early, tail_z, tail_x, *got_x, *got_y)[0]


def local(residual, edge_diag, node_shift, coarse_shift):
    axes = ("gz", "gx", "gy")
    counts = tuple(lax.axis_size(a) for a in axes)
    devices = counts[0] * counts[1] * counts[2]
    part, *faces, scaled, inverses = edge_stage(residual, edge_diag)
    up_z, up_x, up_y, low_z, low_x, low_y = faces
    below = []
    for value, axis in ((up_z, "gz"), (up_x, "gx"), (up_y, "gy")):
        below.append(ring(value, axis, 1))
    fg, rhs, xb, yb, w, *send = nodal_stage(part, node_shift, coarse_shift, *below, counts[0])
    got_z = swap(send, "gz")
    rhs, w, *send = x_stage(got_z, rhs, xb, yb, w, fg, counts[0], counts[1])
    got_x = swap(send, "gx", ("gx", "gy"))
    planes = rhs.shape[0]
    tail_x = x_tail(got_z, fg, node_shift, low_x, w, counts[0])
    *mid, tail_z = part_stage(got_z, fg, node_shift, low_z, w, counts[0])
    early = y_early(got_z, fg, node_shift, low_y, w, planes, counts[0])
    early = (*early, tail_x, mid[1])
    tail_z = ring(tail_z, "gz", -1)
    tail_x = ring(tail_x, "gx", -1)
    rhs, w, *send = y_stage(got_x, rhs, w, early, counts[1], counts[2])
    got_y = swap(send, "gy", ("gx", "gy"))
    smooth, last = smooth_stage(scaled, inverses, below, tail_z, tail_x, w, counts)
    v1, v2, sums = coarse_stage(got_y, rhs, w, (last,), counts[2], devices)
    sums = lax.all_to_all(sums, ("gx", "gy", "gz"), 0, 0)
    early = early[0]
    return final_stage(
        sums, v1, v2, fg, mid, smooth, last, early, tail_z, tail_x, got_x, got_y, counts
    )


def solution(mesh):
    placed = (
        P(None, "gz", "gx", "gy"),
        P(None, "gz", "gx", "gy"),
        P("gz", "gx", "gy"),
        P("gz", "gx", "gy"),
    )

    return jax.shard_map(
        local, mesh=mesh, in_specs=placed, out_specs=P(None, "gz", "gx", "gy"), check_vma=False
    )
```

```python
import itertools

import jax
import jax.numpy as jnp
from jax import lax
from jax.experimental import pallas as pl
from jax.experimental.pallas import tpu as pltpu
from jax.sharding import PartitionSpec as P


F32 = jnp.float32
LANES = 128


def lane_ids(rows):
    return lax.broadcasted_iota(jnp.int32, (rows, LANES), 1)


def row_ids(rows):
    return lax.broadcasted_iota(jnp.int32, (rows, LANES), 0)


def shift_lanes(value, amount):
    return pltpu.roll(value, amount % LANES, 1)


def shift_rows(value, amount):
    return pltpu.roll(value, amount % value.shape[0], 0)


def low_of(axis, size, first, second):
    place = lax.axis_index(axis)
    odd = place % 2 == 1
    zero = jnp.zeros_like(first)
    if second is None:
        return jnp.where(odd, first, zero)
    return jnp.where(odd, first, jnp.where(place > 0, second, zero))


def high_of(axis, size, first, second):
    place = lax.axis_index(axis)
    even = place % 2 == 0
    zero = jnp.zeros_like(first)
    if second is None:
        return jnp.where(even, first, zero)
    return jnp.where(even, first, jnp.where(place < size - 1, second, zero))


def from_below(axis, value):
    return jnp.where(lax.axis_index(axis) > 0, value, jnp.zeros_like(value))


def from_above(axis, size, value):
    return jnp.where(lax.axis_index(axis) < size - 1, value, jnp.zeros_like(value))


def ring(value, axis, step):
    size = lax.axis_size(axis)
    return lax.ppermute(value, axis, [(i, (i + step) % size) for i in range(size)])


def swap(values, axis, names=None):
    size = lax.axis_size(axis)
    out = [lax.ppermute(values[0], axis, [(i, i ^ 1) for i in range(size)])]
    if len(values) == 1:
        return out
    odd = [(i + 1) % size if i % 2 else (i - 1) % size for i in range(size)]
    if names is None:
        out.append(lax.ppermute(values[1], axis, list(enumerate(odd))))
        return out
    main = names.index(axis)
    pairs = []
    sizes = [lax.axis_size(name) for name in names]
    for at in itertools.product(*(range(n) for n in sizes)):
        to = list(at)
        if at[main] in (0, size - 1):
            to[1 - main] ^= 1
        else:
            to[main] = odd[at[main]]
        pairs.append(tuple(p[0] * sizes[1] + p[1] for p in (at, to)))
    out.append(lax.ppermute(values[1], names, pairs))
    return out


def write_sides(axis, refs, up, down):
    even = lax.axis_index(axis) % 2 == 0

    @pl.when(even)
    def _():
        up(refs[0])
        if len(refs) > 1:
            down(refs[1])

    @pl.when(jnp.logical_not(even))
    def _():
        down(refs[0])
        if len(refs) > 1:
            up(refs[1])


def call(body, outs, scratch=(), far=(), far_out=False, **kwargs):
    kind = jax.ShapeDtypeStruct if far_out else pltpu.VMEM
    run = pl.pallas_call(
        body,
        out_shape=[kind(shape, F32) for shape in outs],
        scratch_shapes=[pltpu.VMEM(s, F32) if isinstance(s, tuple) else s for s in scratch],
        compiler_params=pltpu.CompilerParams(vmem_limit_bytes=12 * 2**20),
        **kwargs,
    )

    def apply(*args):
        spaces = [pltpu.HBM if i in far else pltpu.VMEM for i in range(len(args))]
        return run(
            *(
                pltpu.with_memory_space_constraint(a, space)
                for a, space in zip(args, spaces)
            )
        )

    return apply


def vmem(count):
    return [pl.BlockSpec(memory_space=pltpu.VMEM)] * count


def edge_stage(residual, edge_diag):
    _, nz, nx, ny = residual.shape
    step = 2
    steps = nz // step

    def body(res, diag, part, up_z, up_x, up_y, low_z, low_x, low_y, scaled, inv, near, sems):
        lane = lane_ids(nx)
        row = row_ids(nx)

        def copies(block):
            at = pl.ds(block * step, step)
            return [
                pltpu.make_async_copy(source.at[:, at], target.at[:, at], sems.at[i, block])
                for i, (source, target) in enumerate(((res, near), (diag, inv)))
            ]

        for block in range(steps):
            for copy in copies(block):
                copy.start()
        before = jnp.zeros((nx, ny), F32)
        high = jnp.zeros((nx, LANES), F32)
        low = jnp.zeros((nx, LANES), F32)
        for z in range(nz):
            if z % step == 0:
                for copy in copies(z // step):
                    copy.wait()
            s = []
            for k in range(3):
                inverse = 1.0 / inv[k, z]
                inv[k, z] = inverse
                s.append(near[k, z] * inverse)
                scaled[k, z] = s[k]
            total = before - s[0]
            total += jnp.where(row == 0, 0.0, shift_rows(s[1], 1)) - s[1]
            total += jnp.where(lane == 0, 0.0, shift_lanes(s[2], 1)) - s[2]
            part[z] = total
            before = s[0]
            for k in range(3):
                spot = k * nz + z
                up_x[spot : spot + 1, :] = s[k][nx - 1 :, :]
                low_x[spot : spot + 1, :] = s[k][:1, :]
                high = jnp.where(lane == spot, shift_lanes(s[k], spot + 1), high)
                low = jnp.where(lane == spot, shift_lanes(s[k], spot), low)
                if z == 0:
                    low_z[k] = s[k]
                if z == nz - 1:
                    up_z[k] = s[k]
        up_y[...] = high
        low_y[...] = low

    faces = [(3, nx, ny), (3 * nz, ny), (nx, LANES)] * 2
    return call(
        body,
        [(nz, nx, ny)] + faces + [residual.shape] * 2,
        scratch=[residual.shape, pltpu.SemaphoreType.DMA((2, steps))],
        far=(0, 1),
        in_specs=[pl.BlockSpec(memory_space=pltpu.HBM)] * 2,
        out_specs=vmem(9),
    )(residual, edge_diag)


def select_sum(values, chosen):
    first = values.astype(jnp.bfloat16)
    left = values - first.astype(F32)
    second = left.astype(jnp.bfloat16)
    third = (left - second.astype(F32)).astype(jnp.bfloat16)
    chosen = chosen.astype(jnp.bfloat16)
    both = jnp.concatenate([first, second], axis=1)
    total = jnp.dot(both, jnp.concatenate([chosen, chosen], axis=0), preferred_element_type=F32)
    return total + jnp.dot(third, chosen, preferred_element_type=F32)


def plane(values, row_count):
    return jnp.concatenate([values, jnp.zeros((row_count - values.shape[0], LANES), F32)], axis=0)


def nodal_stage(part, node_shift, coarse_shift, got_z, got_x, got_y, z_count):
    nz, nx, ny = part.shape
    cz, cx, cy = nz // 2, nx // 2, ny // 2
    rows = cx + 8
    sends = 1 if z_count == 2 else 2

    def body(part, shift, coarse, gz, gx, gy, fg, rhs, xb, yb, w, *rest):
        out, (pair, stack, s_, xl_, yl_, zl_, zh_) = rest[:sends], rest[sends:]
        lane = lane_ids(nx)
        row = row_ids(nx)
        lane_c = lane_ids(rows)
        row_c = row_ids(rows)
        below_z = from_below("gz", gz[0])
        below_y = from_below("gy", gy[...])
        fine = lax.broadcasted_iota(jnp.int32, (ny, 2 * LANES), 0)
        coarse_lane = lax.broadcasted_iota(jnp.int32, (ny, 2 * LANES), 1)
        miss = jnp.where(
            coarse_lane < LANES, fine // 2 - coarse_lane, fine - 2 * (coarse_lane - LANES)
        )
        gather = jnp.where(miss == 0, 1.0, 0.0)
        for c in range(cz):
            both = []
            for z in (2 * c, 2 * c + 1):
                total = part[z]
                if z == 0:
                    total += below_z
                total += jnp.where(row == 0, from_below("gx", gx[nz + z : nz + z + 1, :]), 0.0)
                total += jnp.where(lane == 0, shift_lanes(below_y, -(2 * nz + z)), 0.0)
                guess = total / (6.0 + shift[z])
                fg[z] = guess
                both.append(guess)
            pair[c % 2] = both[0] + both[1]
            low = pair[c % 2, pl.ds(0, cx, 2), :]
            high = pair[c % 2, pl.ds(1, cx, 2), :]
            first = fg[2 * c, pl.ds(0, cx, 2), :] + fg[2 * c, pl.ds(1, cx, 2), :]
            stack[c, :cx, :] = low + high
            stack[c, cx : 2 * cx, :] = low
            stack[c, 2 * cx :, :] = first
        every = select_sum(stack[...].reshape(3 * cx * cz, LANES), gather)
        for c in range(cz):
            sums = every[3 * cx * c : 3 * cx * (c + 1)]
            s = sums[:cx, :LANES]
            z_low = sums[2 * cx :, :LANES]
            s_[c] = plane(s, rows)
            yl_[c] = plane(sums[:cx, LANES:], rows)
            xl_[c] = plane(sums[cx : 2 * cx, :LANES], rows)
            zl_[c] = plane(z_low, rows)
            zh_[c] = plane(s - z_low, rows)
            w[c] = jnp.zeros((rows, LANES), F32)
            w[c, :cx, :cy] = 1.0 / (6.0 + coarse[c])
        for c in range(cz):
            s, x_low, y_low = s_[c], xl_[c], yl_[c]
            x_high = s - x_low
            y_high = s - y_low
            total = 3.0 * s
            total += shift_rows(x_low, -1) + shift_rows(x_high, 1)
            total += shift_lanes(y_low, -1) + shift_lanes(y_high, 1)
            if c > 0:
                total += zh_[c - 1]
            if c < cz - 1:
                total += zl_[c + 1]
            rhs[c] = total
            xb[c] = jnp.where(row_c < cx // 2, x_low, x_high)
            yb[c] = jnp.where(lane_c < cy // 2, y_low, y_high)
        rhs[cz] = zh_[cz - 1]
        rhs[cz + 1] = jnp.zeros((rows, LANES), F32)
        rhs[cz + 2] = jnp.zeros((rows, LANES), F32)
        rhs[cz + 3] = zl_[0]

        def fill(ref, near, far, half, face):
            planes = [rhs[near], rhs[far], w[near], w[far], half]
            planes += [xb[near], xb[far], yb[near], yb[far]]
            for i, value in enumerate(planes):
                ref[i * rows : (i + 1) * rows, :] = value
            ref[9 * rows : 9 * rows + nx, :] = face

        def up(ref):
            fill(ref, cz - 1, cz - 2, zh_[cz - 1], fg[nz - 1])

        def down(ref):
            fill(ref, 0, 1, zl_[0], fg[0])

        write_sides("gz", out, up, down)

    coarse = (cz, rows, LANES)
    send = (9 * rows + nx, LANES)
    return call(
        body,
        [(nz, nx, ny), (cz + 4, rows, LANES), coarse, coarse, coarse] + [send] * sends,
        scratch=[(2, nx, ny), (cz, 3 * cx, LANES), coarse, coarse, coarse, coarse, coarse],
        in_specs=vmem(6),
        out_specs=vmem(5 + sends),
    )(part, node_shift, coarse_shift, got_z, got_x, got_y)


def x_stage(got, rhs, xb, yb, w, fg, z_count, x_count):
    planes, rows, _ = rhs.shape
    cz, cx = planes - 4, rows - 8
    nz, nx, ny = fg.shape
    cy = ny // 2
    sends = 1 if x_count == 2 else 2
    gots = len(got)
    size = -(-(3 * planes + nz + 1) // 8) * 8

    def body(*refs):
        got = refs[:gots]
        rhs, xb, yb, w, fg, rhs2, w2 = refs[gots : gots + 7]
        out, (xb2, yb2) = refs[gots + 7 : gots + 7 + sends], refs[gots + 7 + sends :]

        def take_at(pick, at):
            values = [ref[at, :] for ref in got]
            return pick("gz", z_count, values[0], values[1] if gots > 1 else None)

        def take(pick, i):
            return take_at(pick, slice(i * rows, (i + 1) * rows))

        for c in range(1, cz - 1):
            rhs2[c] = rhs[c]
        rhs2[0] = rhs[0] + take(low_of, 4)
        rhs2[cz - 1] = rhs[cz - 1] + take(high_of, 4)
        rhs2[cz] = rhs[cz] + take(high_of, 0)
        rhs2[cz + 1] = take(high_of, 1)
        rhs2[cz + 2] = take(low_of, 1)
        rhs2[cz + 3] = rhs[cz + 3] + take(low_of, 0)
        for here, there, i in ((w, w2, 2), (xb, xb2, 5), (yb, yb2, 7)):
            for c in range(cz):
                there[c] = here[c]
            there[cz] = take(high_of, i)
            there[cz + 1] = take(high_of, i + 1)
            there[cz + 2] = take(low_of, i + 1)
            there[cz + 3] = take(low_of, i)

        lane = lane_ids(planes)

        def fill(ref, near, far, fine):
            halves = lane < cy
            first = jnp.where(halves, rhs2[:, near, :], shift_lanes(rhs2[:, far, :], cy))
            second = jnp.where(halves, w2[:, near, :], shift_lanes(w2[:, far, :], cy))
            edge = yb2[:, far, :]
            third = jnp.where(halves, xb2[:, near, :], shift_lanes(yb2[:, near, :], cy))
            third = jnp.where(lane == cy + 1, shift_lanes(edge, cy + 1), third)
            third = jnp.where(lane == LANES - 2, shift_lanes(edge, cy - 1), third)
            for i, value in enumerate((first, second, third)):
                ref[i * planes : (i + 1) * planes, :] = value
            ref[3 * planes : 3 * planes + nz, :] = fg[:, fine, :]
            at = 9 * rows + fine
            last = 3 * planes + nz
            ref[last : last + 1, :] = take_at(high_of, slice(at, at + 1))
            ref[last + 1 :, :] = jnp.zeros((size - last - 1, LANES), F32)

        def up(ref):
            fill(ref, cx - 1, cx - 2, nx - 1)

        def down(ref):
            fill(ref, 0, 1, 0)

        write_sides("gx", out, up, down)

    whole = (planes, rows, LANES)
    return call(
        body,
        [whole, whole] + [(size, LANES)] * sends,
        scratch=[whole, whole],
        in_specs=vmem(gots + 5),
        out_specs=vmem(2 + sends),
    )(*got, rhs, xb, yb, w, fg)


def x_tail(got, fg, node_shift, low_x, after, z_count):
    nz, nx, ny = fg.shape
    z_at = 9 * (nx // 2 + 8)
    gots = len(got)

    def body(*refs):
        got = refs[:gots]
        fg, shift, low_x, _, out = refs[gots:]
        lane = lane_ids(nz)
        row = row_ids(nz)

        def z_row(pick):
            values = [ref[z_at : z_at + 1, :] for ref in got]
            return pick("gz", z_count, values[0], values[1] if gots > 1 else None)

        here = fg[:, 0, :]
        around = fg[:, 1, :] + jnp.where(row == 0, z_row(low_of), shift_rows(here, 1))
        around += jnp.where(row == nz - 1, z_row(high_of), shift_rows(here, -1))
        around += jnp.where(lane == 0, 0.0, shift_lanes(here, 1))
        around += jnp.where(lane == ny - 1, 0.0, shift_lanes(here, -1))
        inverse = 1.0 / (6.0 + shift[:, 0, :])
        out[: 3 * nz, :] = low_x[...]
        out[3 * nz : 4 * nz, :] = here + inverse * around
        out[4 * nz :, :] = inverse

    return call(
        body, [(5 * nz, LANES)], in_specs=vmem(gots + 4), out_specs=vmem(1)
    )(*got, fg, node_shift, low_x, after)[0]


def part_stage(got, fg, node_shift, low_z, after, z_count):
    nz, nx, ny = fg.shape
    z_at = 9 * (nx // 2 + 8)
    gots = len(got)

    def body(*refs):
        got = refs[:gots]
        fg, shift, low_z, _, part, inv, tail = refs[gots:]
        lane = lane_ids(nx)
        row = row_ids(nx)

        def z_face(pick):
            values = [ref[z_at : z_at + nx, :] for ref in got]
            return pick("gz", z_count, values[0], values[1] if gots > 1 else None)

        for z in range(nz):
            guess = fg[z]
            inner = fg[z + 1] if z < nz - 1 else z_face(high_of)
            inner += jnp.where(row == 0, 0.0, shift_rows(guess, 1))
            inner += jnp.where(row == nx - 1, 0.0, shift_rows(guess, -1))
            inner += jnp.where(lane == 0, 0.0, shift_lanes(guess, 1))
            inner += jnp.where(lane == ny - 1, 0.0, shift_lanes(guess, -1))
            inverse = 1.0 / (6.0 + shift[z])
            inv[z] = inverse
            part[z] = guess + inverse * (inner + (fg[z - 1] if z > 0 else z_face(low_of)))
            if z == 0:
                for k in range(3):
                    tail[k * nx : (k + 1) * nx, :] = low_z[k]
                tail[3 * nx : 4 * nx, :] = guess + inverse * inner
                tail[4 * nx :, :] = inverse

    return call(
        body, [fg.shape, fg.shape, (5 * nx, LANES)], in_specs=vmem(gots + 4), out_specs=vmem(3)
    )(*got, fg, node_shift, low_z, after)


def line(source, lane, fine, at):
    acc = jnp.zeros(lane.shape, F32)
    for z in range(source.shape[0]):
        moved = jnp.broadcast_to(source[z : z + 1, :], lane.shape)
        acc = jnp.where(lane == at + z, shift_lanes(moved, at + z - fine), acc)
    return acc


def y_stage(got, rhs, w, early, x_count, y_count):
    planes, rows, _ = rhs.shape
    cx = rows - 8
    nx, cy = 2 * cx, LANES // 2
    nz, half = 2 * (planes - 4), nx // 2
    sends = 1 if y_count == 2 else 2
    gots = len(got)

    def body(*refs):
        got = refs[:gots]
        rhs, w, up_, down_, part, inv, _, _, rhs3, w3 = refs[gots : gots + 10]
        rest = refs[gots + 10 :]
        out, (add,) = rest[:sends], rest[sends:]
        lane_p = lane_ids(planes)

        def take_at(pick, at):
            values = [ref[at, :] for ref in got]
            return pick("gx", x_count, values[0], values[1] if gots > 1 else None)

        def take(pick, i):
            return take_at(pick, slice(i * planes, (i + 1) * planes))

        add[...] = jnp.zeros_like(add)
        for c in range(planes):
            w3[c] = w[c]
        for pick, near, far, edge in ((high_of, cx, cx + 1, cx - 1), (low_of, rows - 1, rows - 2, 0)):
            first, second, third = take(pick, 0), take(pick, 1), take(pick, 2)
            other = shift_lanes(third, -cy)
            one = jnp.where((lane_p == 0) | (lane_p == cy - 1), other, 0.0)
            two = jnp.where(lane_p == 0, shift_lanes(third, -cy - 1), 0.0)
            two = jnp.where(lane_p == cy - 1, shift_lanes(third, 1 - cy), two)
            for at, value, ends in ((near, first, one), (far, shift_lanes(first, -cy), two)):
                value = jnp.where(lane_p < cy, value, 0.0)
                value += jnp.where(lane_p == cy, shift_lanes(ends, 1), 0.0)
                value += jnp.where(lane_p == LANES - 1, shift_lanes(ends, -1), 0.0)
                add[:, at, :] = value
            w3[:, near, :] = jnp.where(lane_p < cy, second, 0.0)
            w3[:, far, :] = jnp.where(lane_p < cy, shift_lanes(second, -cy), 0.0)
            add[:, edge, :] = jnp.where(lane_p < cy, third, 0.0)
        for c in range(planes):
            rhs3[c] = rhs[c] + add[c]

        lane_c = lane_ids(rows)
        lane8 = lane_ids(8)
        base = 5 * planes
        x_face = slice(3 * planes, 3 * planes + nz)
        x_high = take_at(high_of, x_face)

        def fill(ref, first, fine, early):
            acc = jnp.zeros((rows, LANES), F32)
            inner = first if first > 0 else 0
            for z in range(planes):
                for field, width, at, source in (
                    (rhs3, 3, 3 * z, first),
                    (w3, 2, 3 * planes + 2 * z, inner),
                ):
                    there = (lane_c >= at) & (lane_c < at + width)
                    acc = jnp.where(there, shift_lanes(field[z], at - source), acc)
            ref[:nx, :] = plane(acc, nx) + early[...]
            ref[nx : nx + 8, :] = line(x_high, lane8, fine, base)

        def up(ref):
            fill(ref, cy - 2, 2 * cy - 1, up_)
            ref[nx + 8 :, :] = jnp.zeros((half, LANES), F32)

        def down(ref):
            fill(ref, -1, 0, down_)
            row = row_ids(nx)
            ends = jnp.where(row == 0, line(take_at(low_of, x_face), lane8, 0, 0)[:1, :], 0.0)
            ends += jnp.where(row == nx - 1, line(x_high, lane8, 0, 0)[:1, :], 0.0)
            inverse = inv[...]
            value = part[...] + inverse * ends
            packed = jnp.zeros((half, LANES), F32)
            for i, source in enumerate((value[:half], value[half:], inverse[:half], inverse[half:])):
                there = lane_ids(half) // nz == i
                packed = jnp.where(there, shift_lanes(source, i * nz), packed)
            ref[nx + 8 :, :] = packed

        write_sides("gy", out, up, down)

    whole = (planes, rows, LANES)
    return call(
        body,
        [whole, whole] + [(nx + 8 + half, LANES)] * sends,
        scratch=[whole],
        in_specs=vmem(gots + 8),
        out_specs=vmem(2 + sends),
    )(*got, rhs, w, *early)


def y_early(got_z, fg, node_shift, low_y, after, planes, z_count):
    nz, nx, _ = fg.shape
    z_at = 9 * (nx // 2 + 8)
    base = 5 * planes
    n_z = len(got_z)

    def body(*refs):
        gz = refs[:n_z]
        fg, shift, low_y, _, up, down, part, inv = refs[n_z:]
        lane = lane_ids(nx)
        row = row_ids(nx)

        def side(pick):
            values = [ref[z_at : z_at + nx, :] for ref in gz]
            return pick("gz", z_count, values[0], values[1] if n_z > 1 else None)

        above = side(high_of)
        here = jnp.where(lane == nz, shift_lanes(above, nz), 0.0)
        here = jnp.where(lane == LANES - 1, shift_lanes(side(low_of), -1), here)
        high = jnp.where(lane == base + nz, shift_lanes(above, base + nz + 1), 0.0)
        inverse = jnp.ones((nx, LANES), F32)
        inner = jnp.zeros((nx, LANES), F32)
        for z in range(nz):
            guess = fg[z]
            here = jnp.where(lane == z, shift_lanes(guess, z), here)
            inner = jnp.where(lane == z, shift_lanes(guess, z - 1), inner)
            high = jnp.where(lane == base + z, shift_lanes(guess, base + z + 1), high)
            inverse = jnp.where(lane == z, shift_lanes(6.0 + shift[z], z), inverse)
        inverse = 1.0 / inverse
        around = inner + shift_lanes(here, 1) + shift_lanes(here, -1)
        around += jnp.where(row == 0, 0.0, shift_rows(here, 1))
        around += jnp.where(row == nx - 1, 0.0, shift_rows(here, -1))
        up[...] = high
        at = base + nz + 1
        low = jnp.where((lane >= base) & (lane < at), shift_lanes(here, base), 0.0)
        down[...] = jnp.where((lane >= at) & (lane < at + 3 * nz), shift_lanes(low_y[...], at), low)
        part[...] = here + inverse * around
        inv[...] = inverse

    return call(
        body, [(nx, LANES)] * 4, in_specs=vmem(n_z + 4), out_specs=vmem(4)
    )(*got_z, fg, node_shift, low_y, after)


def coarse_stage(got, rhs, w, after, y_count, devices):
    planes, rows, _ = rhs.shape
    cz, cx = planes - 4, rows - 8
    cy = LANES // 2
    gots = len(got)

    def body(*refs):
        got = refs[:gots]
        rhs, w, _, v1, v2, sums, tot, inv_, image_ = refs[gots:]
        values = [ref[:rows, :] for ref in got]
        second = values[1] if gots > 1 else None
        low = low_of("gy", y_count, values[0], second)
        high = high_of("gy", y_count, values[0], second)
        lane = lane_ids(rows)
        above = (lane >= cy - 1) & (lane < cy + 2)
        below = (lane >= LANES - 2) | (lane == 0)
        for z in range(planes):
            at = 3 * z
            right = jnp.where(below, shift_lanes(low, LANES - 2 - at), 0.0)
            right = rhs[z] + jnp.where(above, shift_lanes(high, cy - 1 - at), right)
            at = 3 * planes + 2 * z
            inv = jnp.where(lane >= LANES - 2, shift_lanes(low, LANES - 2 - at), w[z])
            inv = jnp.where((lane >= cy) & (lane < cy + 2), shift_lanes(high, cy - at), inv)
            inv_[z] = inv
            tot[z] = right
            v1[z] = right * inv

        def near(field, z):
            here = field[z]
            total = field[(z + 1) % planes] + field[(z - 1) % planes]
            total += shift_rows(here, 1) + shift_rows(here, -1)
            return total + shift_lanes(here, 1) + shift_lanes(here, -1)

        v2[cz + 1] = jnp.zeros((rows, LANES), F32)
        v2[cz + 2] = jnp.zeros((rows, LANES), F32)
        for z in list(range(cz + 1)) + [planes - 1]:
            image = tot[z] - near(v1, z)
            if z < cz:
                image_[z] = image
            v2[z] = image * inv_[z]
        parts = [jnp.zeros((cx, LANES), F32)] * 5
        for z in range(cz):
            first, second_, right, image = v1[z], v2[z], tot[z], image_[z]
            third = image - near(v2, z)
            terms = (first * right, second_ * right, first * image, second_ * image, second_ * third)
            parts = [a + b[:cx, :] for a, b in zip(parts, terms)]
        keep = lane_ids(1) < cy
        lines = [jnp.where(keep, jnp.sum(a, axis=0, keepdims=True), 0.0) for a in parts]
        tile = jnp.concatenate(lines + [jnp.zeros((3, LANES), F32)], axis=0)
        column = jnp.sum(tile, axis=1, keepdims=True)
        spread = jnp.where(lane_ids(8) == row_ids(8), column, 0.0)
        line = jnp.sum(spread, axis=0, keepdims=True)
        sums[...] = jnp.broadcast_to(line[None], (devices, 1, LANES))

    whole = (planes, rows, LANES)
    return call(
        body,
        [whole, whole, (devices, 1, LANES)],
        scratch=[whole, whole, whole],
        in_specs=vmem(gots + 3),
        out_specs=vmem(3),
    )(*got, rhs, w, *after)


def smooth_stage(scaled, inverses, below, tail_z, tail_x, after, counts):
    _, nz, nx, _ = scaled.shape

    def body(*refs):
        s, inv, lz, lx, ly = refs[:5]
        tz, gx, _, out, last = refs[5:]
        lane = lane_ids(nx)
        row = row_ids(nx)
        y_low = from_below("gy", ly[...])

        acc = jnp.zeros((nx, LANES), F32)
        for k in range(3):
            z_low = from_below("gz", lz[k])
            z_high = from_above("gz", counts[0], tz[k * nx : (k + 1) * nx, :])
            x_low = from_below("gx", lx[k * nz : (k + 1) * nz, :])
            x_high = from_above("gx", counts[1], gx[k * nz : (k + 1) * nz, :])
            for z in range(nz):
                here = s[k, z]
                around = s[k, z - 1] if z > 0 else z_low
                around += s[k, z + 1] if z < nz - 1 else z_high
                around += jnp.where(row == 0, x_low[z : z + 1, :], shift_rows(here, 1))
                around += jnp.where(row == nx - 1, x_high[z : z + 1, :], shift_rows(here, -1))
                spot = k * nz + z
                around += jnp.where(lane == 0, shift_lanes(y_low, -spot), shift_lanes(here, 1))
                around += jnp.where(lane == LANES - 1, 0.0, shift_lanes(here, -1))
                inverse = inv[k, z]
                acc = jnp.where(lane == spot, shift_lanes(inverse, spot + 1), acc)
                out[k, z] = here + around * inverse
        last[...] = acc

    return call(
        body, [scaled.shape, (nx, LANES)], in_specs=vmem(8), out_specs=vmem(2)
    )(scaled, inverses, *below, tail_z, tail_x, after)


def final_stage(sums, v1, v2, fg, mid, smooth, last, early, tail_z, tail_x, got_x, got_y, counts):
    planes, rows, _ = v1.shape
    cz, cx, cy = planes - 4, rows - 8, LANES // 2
    nz, nx, _ = fg.shape
    n_x, n_y = len(got_x), len(got_y)
    gots = n_x + n_y

    def body(*refs):
        sums, v1, v2, fg, part, inv, smooth, last, early, tz, tx = refs[:11]
        gx = refs[11 : 11 + n_x]
        gy = refs[11 + n_x : 11 + gots]
        out, sol, dup, inter, small, lines, buf, sem = refs[11 + gots :]

        def one_side(pick, refs, axis, size, at):
            values = [ref[at, :] for ref in refs]
            return pick(axis, size, values[0], values[1] if len(values) > 1 else None)

        def both(refs, axis, size, at):
            return [one_side(pick, refs, axis, size, at) for pick in (low_of, high_of)]

        total = jnp.sum(sums[...], axis=0)
        lane1 = lane_ids(1)
        gone, gtwo, hone, hmix, htwo = [
            jnp.sum(jnp.where(lane1 == i, total, 0.0), axis=1, keepdims=True) for i in range(5)
        ]
        two = (gtwo - hmix * gone / hone) / (htwo - hmix * hmix / hone)
        one = (gone - hmix * two) / hone
        source = lax.broadcasted_iota(jnp.int32, (LANES, 2 * LANES), 0)
        target = lax.broadcasted_iota(jnp.int32, (LANES, 2 * LANES), 1)
        fine = target - LANES
        side = jnp.where(fine % 2 == 1, fine // 2 + 1, (fine // 2 + LANES - 1) % LANES)
        spread = jnp.where(jnp.where(target < LANES, target // 2, side) == source, 1.0, 0.0)
        for z in range(planes):
            sol[z] = one * v1[z] + two * v2[z]
        every = select_sum(sol[...].reshape(planes * rows, LANES), spread)
        dup[...] = every.reshape(planes, rows, 2 * LANES)

        x_low, x_high = both(gx, "gx", counts[1], slice(3 * planes, 3 * planes + nz + 1))
        y_low, y_high = both(gy, "gy", counts[2], slice(0, nx))
        y_row_low, y_row_high = both(gy, "gy", counts[2], slice(nx, nx + 1))
        half = nx // 2
        y_pack = one_side(high_of, gy, "gy", counts[2], slice(nx + 8, nx + 8 + half))
        lane = lane_ids(nx)
        row = row_ids(nx)
        base = 5 * planes

        def spread_around(z):
            c, odd = z // 2, z % 2
            here = dup[c, :, :LANES]
            same = 3.0 * here + dup[c, :, LANES:]
            same += dup[(c + 1 if odd else c - 1) % planes, :, :LANES]
            slot = z % 2
            inter[slot, pl.ds(0, cx, 2), :] = (same + shift_rows(here, 1))[:cx, :]
            inter[slot, pl.ds(1, cx, 2), :] = (same + shift_rows(here, -1))[:cx, :]
            return inter[slot]

        def nodal(z):
            around = spread_around(z) + jnp.where(row == 0, x_low[z : z + 1, :], 0.0)
            around += jnp.where(row == nx - 1, x_high[z : z + 1, :], 0.0)
            around += jnp.where(lane == 0, shift_lanes(y_low, -(base + z)), 0.0)
            around += jnp.where(lane == LANES - 1, shift_lanes(y_high, -(base + z) - 1), 0.0)
            if z == nz:
                value = tz[3 * nx : 4 * nx, :] + tz[4 * nx :, :] * (around + fg[nz - 1])
                return from_above("gz", counts[0], value)
            return part[z] + inv[z] * around

        here = dup[:cz, cx, :LANES]
        same = 3.0 * here + dup[:cz, cx, LANES:] + dup[:cz, cx - 1, :LANES]
        small[pl.ds(0, cz, 2), :] = same + jnp.concatenate(
            [dup[planes - 1, cx : cx + 1, :LANES], here[: cz - 1]], axis=0
        )
        small[pl.ds(1, cz, 2), :] = same + dup[1 : cz + 1, cx, :LANES]
        for z in range(nz):
            left = shift_lanes(y_row_low, -(base + z))
            right = shift_lanes(y_row_high, -(base + z) - 1)
            value = jnp.where(lane1 == 0, left, 0.0)
            lines[z : z + 1, :] = jnp.where(lane1 == LANES - 1, right, value)
        x_value = tx[3 * nz : 4 * nz, :] + tx[4 * nz :, :] * (
            fg[:, nx - 1, :] + small[...] + lines[...]
        )
        x_value = from_above("gx", counts[1], x_value)

        lane_c = lane_ids(rows)
        even = jnp.zeros((rows, LANES), F32)
        odd = jnp.zeros((rows, LANES), F32)
        for z in range(nz):
            c = z // 2
            here = sol[c]
            same = 3.0 * here + shift_lanes(here, 1) + sol[(c + 1 if z % 2 else c - 1) % planes]
            even = jnp.where(lane_c == z, shift_lanes(same + shift_rows(here, 1), z - cy), even)
            odd = jnp.where(lane_c == z, shift_lanes(same + shift_rows(here, -1), z - cy), odd)
        inter[0, pl.ds(0, cx, 2), :] = even[:cx, :]
        inter[0, pl.ds(1, cx, 2), :] = odd[:cx, :]
        y_base = jnp.concatenate([y_pack, shift_lanes(y_pack, -nz)], axis=0)
        y_inverse = jnp.concatenate(
            [shift_lanes(y_pack, -2 * nz), shift_lanes(y_pack, -3 * nz)], axis=0
        )
        y_value = y_base + y_inverse * (shift_lanes(early[...], -base) + inter[0])
        y_value = from_above("gy", counts[2], y_value)
        y_fix = shift_lanes(y_high, -(base + nz + 1)) * last[...]
        y_value += shift_lanes(y_fix, -2 * nz)

        def copy(z):
            return pltpu.make_async_copy(buf.at[:, z], out.at[:, z], sem.at[z])

        value = nodal(0)
        for z in range(nz):
            after = nodal(z + 1)
            steps = [after, jnp.where(row == nx - 1, x_value[z : z + 1, :], shift_rows(value, -1))]
            steps.append(
                jnp.where(lane == LANES - 1, shift_lanes(y_value, -z - 1), shift_lanes(value, -1))
            )
            for k in range(3):
                moved = smooth[k, z]
                if k < 2:
                    fixed = shift_lanes(y_fix, -(k * nz + z) - 1)
                    moved += jnp.where(lane == LANES - 1, fixed, 0.0)
                buf[k, z] = moved + (steps[k] - value)
            copy(z).start()
            value = after
        for z in range(nz):
            copy(z).wait()

    return call(
        body,
        [smooth.shape],
        scratch=[
            (planes, rows, LANES),
            (planes, rows, 2 * LANES),
            (2, nx, LANES),
            (nz, LANES),
            (nz, LANES),
            smooth.shape,
            pltpu.SemaphoreType.DMA((nz,)),
        ],
        far_out=True,
        in_specs=vmem(11 + gots),
        out_specs=[pl.BlockSpec(memory_space=pltpu.HBM)],
    )(sums, v1, v2, fg, *mid, smooth, last, early, tail_z, tail_x, *got_x, *got_y)[0]


def local(residual, edge_diag, node_shift, coarse_shift):
    axes = ("gz", "gx", "gy")
    counts = tuple(lax.axis_size(a) for a in axes)
    devices = counts[0] * counts[1] * counts[2]
    part, *faces, scaled, inverses = edge_stage(residual, edge_diag)
    up_z, up_x, up_y, low_z, low_x, low_y = faces
    below = []
    for value, axis in ((up_z, "gz"), (up_x, "gx"), (up_y, "gy")):
        below.append(ring(value, axis, 1))
    fg, rhs, xb, yb, w, *send = nodal_stage(part, node_shift, coarse_shift, *below, counts[0])
    got_z = swap(send, "gz")
    rhs, w, *send = x_stage(got_z, rhs, xb, yb, w, fg, counts[0], counts[1])
    got_x = swap(send, "gx", ("gx", "gy"))
    planes = rhs.shape[0]
    tail_x = x_tail(got_z, fg, node_shift, low_x, w, counts[0])
    *mid, tail_z = part_stage(got_z, fg, node_shift, low_z, w, counts[0])
    early = y_early(got_z, fg, node_shift, low_y, w, planes, counts[0])
    early = (*early, tail_x, mid[1])
    tail_z = ring(tail_z, "gz", -1)
    tail_x = ring(tail_x, "gx", -1)
    rhs, w, *send = y_stage(got_x, rhs, w, early, counts[1], counts[2])
    got_y = swap(send, "gy", ("gx", "gy"))
    smooth, last = smooth_stage(scaled, inverses, below, tail_z, tail_x, w, counts)
    v1, v2, sums = coarse_stage(got_y, rhs, w, (last,), counts[2], devices)
    sums = lax.all_to_all(sums, ("gx", "gy", "gz"), 0, 0)
    early = early[0]
    return final_stage(
        sums, v1, v2, fg, mid, smooth, last, early, tail_z, tail_x, got_x, got_y, counts
    )


def solution(mesh):
    placed = (
        P(None, "gz", "gx", "gy"),
        P(None, "gz", "gx", "gy"),
        P("gz", "gx", "gy"),
        P("gz", "gx", "gy"),
    )

    return jax.shard_map(
        local, mesh=mesh, in_specs=placed, out_specs=P(None, "gz", "gx", "gy"), check_vma=False
    )
```

```python
import itertools

import jax
import jax.numpy as jnp
from jax import lax
from jax.experimental import pallas as pl
from jax.experimental.pallas import tpu as pltpu
from jax.sharding import PartitionSpec as P


F32 = jnp.float32
LANES = 128


def lane_ids(rows):
    return lax.broadcasted_iota(jnp.int32, (rows, LANES), 1)


def row_ids(rows):
    return lax.broadcasted_iota(jnp.int32, (rows, LANES), 0)


def shift_lanes(value, amount):
    return pltpu.roll(value, amount % LANES, 1)


def shift_rows(value, amount):
    return pltpu.roll(value, amount % value.shape[0], 0)


def low_of(axis, size, first, second):
    place = lax.axis_index(axis)
    odd = place % 2 == 1
    zero = jnp.zeros_like(first)
    if second is None:
        return jnp.where(odd, first, zero)
    return jnp.where(odd, first, jnp.where(place > 0, second, zero))


def high_of(axis, size, first, second):
    place = lax.axis_index(axis)
    even = place % 2 == 0
    zero = jnp.zeros_like(first)
    if second is None:
        return jnp.where(even, first, zero)
    return jnp.where(even, first, jnp.where(place < size - 1, second, zero))


def from_below(axis, value):
    return jnp.where(lax.axis_index(axis) > 0, value, jnp.zeros_like(value))


def from_above(axis, size, value):
    return jnp.where(lax.axis_index(axis) < size - 1, value, jnp.zeros_like(value))


def ring(value, axis, step):
    size = lax.axis_size(axis)
    return lax.ppermute(value, axis, [(i, (i + step) % size) for i in range(size)])


def swap(values, axis, names=None):
    size = lax.axis_size(axis)
    out = [lax.ppermute(values[0], axis, [(i, i ^ 1) for i in range(size)])]
    if len(values) == 1:
        return out
    odd = [(i + 1) % size if i % 2 else (i - 1) % size for i in range(size)]
    if names is None:
        out.append(lax.ppermute(values[1], axis, list(enumerate(odd))))
        return out
    main = names.index(axis)
    pairs = []
    sizes = [lax.axis_size(name) for name in names]
    for at in itertools.product(*(range(n) for n in sizes)):
        to = list(at)
        if at[main] in (0, size - 1):
            to[1 - main] ^= 1
        else:
            to[main] = odd[at[main]]
        pairs.append(tuple(p[0] * sizes[1] + p[1] for p in (at, to)))
    out.append(lax.ppermute(values[1], names, pairs))
    return out


def write_sides(axis, refs, up, down):
    even = lax.axis_index(axis) % 2 == 0

    @pl.when(even)
    def _():
        up(refs[0])
        if len(refs) > 1:
            down(refs[1])

    @pl.when(jnp.logical_not(even))
    def _():
        down(refs[0])
        if len(refs) > 1:
            up(refs[1])


def call(body, outs, scratch=(), far=(), far_out=False, **kwargs):
    kind = jax.ShapeDtypeStruct if far_out else pltpu.VMEM
    run = pl.pallas_call(
        body,
        out_shape=[kind(shape, F32) for shape in outs],
        scratch_shapes=[pltpu.VMEM(s, F32) if isinstance(s, tuple) else s for s in scratch],
        compiler_params=pltpu.CompilerParams(vmem_limit_bytes=12 * 2**20),
        **kwargs,
    )

    def apply(*args):
        spaces = [pltpu.HBM if i in far else pltpu.VMEM for i in range(len(args))]
        return run(
            *(
                pltpu.with_memory_space_constraint(a, space)
                for a, space in zip(args, spaces)
            )
        )

    return apply


def vmem(count):
    return [pl.BlockSpec(memory_space=pltpu.VMEM)] * count


def edge_stage(residual, edge_diag):
    _, nz, nx, ny = residual.shape
    step = 2
    steps = nz // step

    def body(res, diag, part, up_z, up_x, up_y, low_z, low_x, low_y, scaled, inv, near, sems):
        lane = lane_ids(nx)
        row = row_ids(nx)

        def copies(block):
            at = pl.ds(block * step, step)
            return [
                pltpu.make_async_copy(source.at[:, at], target.at[:, at], sems.at[i, block])
                for i, (source, target) in enumerate(((res, near), (diag, inv)))
            ]

        for block in range(steps):
            for copy in copies(block):
                copy.start()
        before = jnp.zeros((nx, ny), F32)
        high = jnp.zeros((nx, LANES), F32)
        low = jnp.zeros((nx, LANES), F32)
        for z in range(nz):
            if z % step == 0:
                for copy in copies(z // step):
                    copy.wait()
            s = []
            for k in range(3):
                inverse = 1.0 / inv[k, z]
                inv[k, z] = inverse
                s.append(near[k, z] * inverse)
                scaled[k, z] = s[k]
            total = before - s[0]
            total += jnp.where(row == 0, 0.0, shift_rows(s[1], 1)) - s[1]
            total += jnp.where(lane == 0, 0.0, shift_lanes(s[2], 1)) - s[2]
            part[z] = total
            before = s[0]
            for k in range(3):
                spot = k * nz + z
                up_x[spot : spot + 1, :] = s[k][nx - 1 :, :]
                low_x[spot : spot + 1, :] = s[k][:1, :]
                high = jnp.where(lane == spot, shift_lanes(s[k], spot + 1), high)
                low = jnp.where(lane == spot, shift_lanes(s[k], spot), low)
                if z == 0:
                    low_z[k] = s[k]
                if z == nz - 1:
                    up_z[k] = s[k]
        up_y[...] = high
        low_y[...] = low

    faces = [(3, nx, ny), (3 * nz, ny), (nx, LANES)] * 2
    return call(
        body,
        [(nz, nx, ny)] + faces + [residual.shape] * 2,
        scratch=[residual.shape, pltpu.SemaphoreType.DMA((2, steps))],
        far=(0, 1),
        in_specs=[pl.BlockSpec(memory_space=pltpu.HBM)] * 2,
        out_specs=vmem(9),
    )(residual, edge_diag)


def select_sum(values, chosen):
    first = values.astype(jnp.bfloat16)
    left = values - first.astype(F32)
    second = left.astype(jnp.bfloat16)
    third = (left - second.astype(F32)).astype(jnp.bfloat16)
    chosen = chosen.astype(jnp.bfloat16)
    both = jnp.concatenate([first, second], axis=1)
    total = jnp.dot(both, jnp.concatenate([chosen, chosen], axis=0), preferred_element_type=F32)
    return total + jnp.dot(third, chosen, preferred_element_type=F32)


def plane(values, row_count):
    return jnp.concatenate([values, jnp.zeros((row_count - values.shape[0], LANES), F32)], axis=0)


def nodal_stage(part, node_shift, coarse_shift, got_z, got_x, got_y, z_count):
    nz, nx, ny = part.shape
    cz, cx, cy = nz // 2, nx // 2, ny // 2
    rows = cx + 8
    sends = 1 if z_count == 2 else 2

    def body(part, shift, coarse, gz, gx, gy, fg, rhs, xb, yb, w, *rest):
        out, (pair, stack, s_, xl_, yl_, zl_, zh_) = rest[:sends], rest[sends:]
        lane = lane_ids(nx)
        row = row_ids(nx)
        lane_c = lane_ids(rows)
        row_c = row_ids(rows)
        below_z = from_below("gz", gz[0])
        below_y = from_below("gy", gy[...])
        fine = lax.broadcasted_iota(jnp.int32, (ny, 2 * LANES), 0)
        coarse_lane = lax.broadcasted_iota(jnp.int32, (ny, 2 * LANES), 1)
        miss = jnp.where(
            coarse_lane < LANES, fine // 2 - coarse_lane, fine - 2 * (coarse_lane - LANES)
        )
        gather = jnp.where(miss == 0, 1.0, 0.0)
        for c in range(cz):
            both = []
            for z in (2 * c, 2 * c + 1):
                total = part[z]
                if z == 0:
                    total += below_z
                total += jnp.where(row == 0, from_below("gx", gx[nz + z : nz + z + 1, :]), 0.0)
                total += jnp.where(lane == 0, shift_lanes(below_y, -(2 * nz + z)), 0.0)
                guess = total / (6.0 + shift[z])
                fg[z] = guess
                both.append(guess)
            pair[c % 2] = both[0] + both[1]
            low = pair[c % 2, pl.ds(0, cx, 2), :]
            high = pair[c % 2, pl.ds(1, cx, 2), :]
            first = fg[2 * c, pl.ds(0, cx, 2), :] + fg[2 * c, pl.ds(1, cx, 2), :]
            stack[c, :cx, :] = low + high
            stack[c, cx : 2 * cx, :] = low
            stack[c, 2 * cx :, :] = first
        every = select_sum(stack[...].reshape(3 * cx * cz, LANES), gather)
        for c in range(cz):
            sums = every[3 * cx * c : 3 * cx * (c + 1)]
            s = sums[:cx, :LANES]
            z_low = sums[2 * cx :, :LANES]
            s_[c] = plane(s, rows)
            yl_[c] = plane(sums[:cx, LANES:], rows)
            xl_[c] = plane(sums[cx : 2 * cx, :LANES], rows)
            zl_[c] = plane(z_low, rows)
            zh_[c] = plane(s - z_low, rows)
            w[c] = jnp.zeros((rows, LANES), F32)
            w[c, :cx, :cy] = 1.0 / (6.0 + coarse[c])
        for c in range(cz):
            s, x_low, y_low = s_[c], xl_[c], yl_[c]
            x_high = s - x_low
            y_high = s - y_low
            total = 3.0 * s
            total += shift_rows(x_low, -1) + shift_rows(x_high, 1)
            total += shift_lanes(y_low, -1) + shift_lanes(y_high, 1)
            if c > 0:
                total += zh_[c - 1]
            if c < cz - 1:
                total += zl_[c + 1]
            rhs[c] = total
            xb[c] = jnp.where(row_c < cx // 2, x_low, x_high)
            yb[c] = jnp.where(lane_c < cy // 2, y_low, y_high)
        rhs[cz] = zh_[cz - 1]
        rhs[cz + 1] = jnp.zeros((rows, LANES), F32)
        rhs[cz + 2] = jnp.zeros((rows, LANES), F32)
        rhs[cz + 3] = zl_[0]

        def fill(ref, near, far, half, face):
            planes = [rhs[near], rhs[far], w[near], w[far], half]
            planes += [xb[near], xb[far], yb[near], yb[far]]
            for i, value in enumerate(planes):
                ref[i * rows : (i + 1) * rows, :] = value
            ref[9 * rows : 9 * rows + nx, :] = face

        def up(ref):
            fill(ref, cz - 1, cz - 2, zh_[cz - 1], fg[nz - 1])

        def down(ref):
            fill(ref, 0, 1, zl_[0], fg[0])

        write_sides("gz", out, up, down)

    coarse = (cz, rows, LANES)
    send = (9 * rows + nx, LANES)
    return call(
        body,
        [(nz, nx, ny), (cz + 4, rows, LANES), coarse, coarse, coarse] + [send] * sends,
        scratch=[(2, nx, ny), (cz, 3 * cx, LANES), coarse, coarse, coarse, coarse, coarse],
        in_specs=vmem(6),
        out_specs=vmem(5 + sends),
    )(part, node_shift, coarse_shift, got_z, got_x, got_y)


def x_stage(got, rhs, xb, yb, w, fg, z_count, x_count):
    planes, rows, _ = rhs.shape
    cz, cx = planes - 4, rows - 8
    nz, nx, ny = fg.shape
    cy = ny // 2
    sends = 1 if x_count == 2 else 2
    gots = len(got)
    size = -(-(3 * planes + nz + 1) // 8) * 8

    def body(*refs):
        got = refs[:gots]
        rhs, xb, yb, w, fg, rhs2, w2 = refs[gots : gots + 7]
        out, (xb2, yb2) = refs[gots + 7 : gots + 7 + sends], refs[gots + 7 + sends :]

        def take_at(pick, at):
            values = [ref[at, :] for ref in got]
            return pick("gz", z_count, values[0], values[1] if gots > 1 else None)

        def take(pick, i):
            return take_at(pick, slice(i * rows, (i + 1) * rows))

        for c in range(1, cz - 1):
            rhs2[c] = rhs[c]
        rhs2[0] = rhs[0] + take(low_of, 4)
        rhs2[cz - 1] = rhs[cz - 1] + take(high_of, 4)
        rhs2[cz] = rhs[cz] + take(high_of, 0)
        rhs2[cz + 1] = take(high_of, 1)
        rhs2[cz + 2] = take(low_of, 1)
        rhs2[cz + 3] = rhs[cz + 3] + take(low_of, 0)
        for here, there, i in ((w, w2, 2), (xb, xb2, 5), (yb, yb2, 7)):
            for c in range(cz):
                there[c] = here[c]
            there[cz] = take(high_of, i)
            there[cz + 1] = take(high_of, i + 1)
            there[cz + 2] = take(low_of, i + 1)
            there[cz + 3] = take(low_of, i)

        lane = lane_ids(planes)

        def fill(ref, near, far, fine):
            halves = lane < cy
            first = jnp.where(halves, rhs2[:, near, :], shift_lanes(rhs2[:, far, :], cy))
            second = jnp.where(halves, w2[:, near, :], shift_lanes(w2[:, far, :], cy))
            edge = yb2[:, far, :]
            third = jnp.where(halves, xb2[:, near, :], shift_lanes(yb2[:, near, :], cy))
            third = jnp.where(lane == cy + 1, shift_lanes(edge, cy + 1), third)
            third = jnp.where(lane == LANES - 2, shift_lanes(edge, cy - 1), third)
            for i, value in enumerate((first, second, third)):
                ref[i * planes : (i + 1) * planes, :] = value
            ref[3 * planes : 3 * planes + nz, :] = fg[:, fine, :]
            at = 9 * rows + fine
            last = 3 * planes + nz
            ref[last : last + 1, :] = take_at(high_of, slice(at, at + 1))
            ref[last + 1 :, :] = jnp.zeros((size - last - 1, LANES), F32)

        def up(ref):
            fill(ref, cx - 1, cx - 2, nx - 1)

        def down(ref):
            fill(ref, 0, 1, 0)

        write_sides("gx", out, up, down)

    whole = (planes, rows, LANES)
    return call(
        body,
        [whole, whole] + [(size, LANES)] * sends,
        scratch=[whole, whole],
        in_specs=vmem(gots + 5),
        out_specs=vmem(2 + sends),
    )(*got, rhs, xb, yb, w, fg)


def x_tail(got, fg, node_shift, low_x, after, z_count):
    nz, nx, ny = fg.shape
    z_at = 9 * (nx // 2 + 8)
    gots = len(got)

    def body(*refs):
        got = refs[:gots]
        fg, shift, low_x, _, out = refs[gots:]
        lane = lane_ids(nz)
        row = row_ids(nz)

        def z_row(pick):
            values = [ref[z_at : z_at + 1, :] for ref in got]
            return pick("gz", z_count, values[0], values[1] if gots > 1 else None)

        here = fg[:, 0, :]
        around = fg[:, 1, :] + jnp.where(row == 0, z_row(low_of), shift_rows(here, 1))
        around += jnp.where(row == nz - 1, z_row(high_of), shift_rows(here, -1))
        around += jnp.where(lane == 0, 0.0, shift_lanes(here, 1))
        around += jnp.where(lane == ny - 1, 0.0, shift_lanes(here, -1))
        inverse = 1.0 / (6.0 + shift[:, 0, :])
        out[: 3 * nz, :] = low_x[...]
        out[3 * nz : 4 * nz, :] = here + inverse * around
        out[4 * nz :, :] = inverse

    return call(
        body, [(5 * nz, LANES)], in_specs=vmem(gots + 4), out_specs=vmem(1)
    )(*got, fg, node_shift, low_x, after)[0]


def part_stage(got, fg, node_shift, low_z, after, z_count):
    nz, nx, ny = fg.shape
    z_at = 9 * (nx // 2 + 8)
    gots = len(got)

    def body(*refs):
        got = refs[:gots]
        fg, shift, low_z, _, part, inv, tail = refs[gots:]
        lane = lane_ids(nx)
        row = row_ids(nx)

        def z_face(pick):
            values = [ref[z_at : z_at + nx, :] for ref in got]
            return pick("gz", z_count, values[0], values[1] if gots > 1 else None)

        for z in range(nz):
            guess = fg[z]
            inner = fg[z + 1] if z < nz - 1 else z_face(high_of)
            inner += jnp.where(row == 0, 0.0, shift_rows(guess, 1))
            inner += jnp.where(row == nx - 1, 0.0, shift_rows(guess, -1))
            inner += jnp.where(lane == 0, 0.0, shift_lanes(guess, 1))
            inner += jnp.where(lane == ny - 1, 0.0, shift_lanes(guess, -1))
            inverse = 1.0 / (6.0 + shift[z])
            inv[z] = inverse
            part[z] = guess + inverse * (inner + (fg[z - 1] if z > 0 else z_face(low_of)))
            if z == 0:
                for k in range(3):
                    tail[k * nx : (k + 1) * nx, :] = low_z[k]
                tail[3 * nx : 4 * nx, :] = guess + inverse * inner
                tail[4 * nx :, :] = inverse

    return call(
        body, [fg.shape, fg.shape, (5 * nx, LANES)], in_specs=vmem(gots + 4), out_specs=vmem(3)
    )(*got, fg, node_shift, low_z, after)


def fold_row(rows):
    return (rows + 8) // 16 * 8


def line(source, lane, fine, at):
    acc = jnp.zeros(lane.shape, F32)
    for z in range(source.shape[0]):
        moved = jnp.broadcast_to(source[z : z + 1, :], lane.shape)
        acc = jnp.where(lane == at + z, shift_lanes(moved, at + z - fine), acc)
    return acc


def y_stage(got, rhs, w, early, x_count, y_count):
    planes, rows, _ = rhs.shape
    cx = rows - 8
    nx, cy = 2 * cx, LANES // 2
    nz, half, cut = 2 * (planes - 4), nx // 2, fold_row(rows)
    sends = 1 if y_count == 2 else 2
    gots = len(got)

    def body(*refs):
        got = refs[:gots]
        rhs, w, up_, down_, part, inv, _, _, _, rhs3, w3 = refs[gots : gots + 11]
        rest = refs[gots + 11 :]
        out, (add,) = rest[:sends], rest[sends:]
        lane_p = lane_ids(planes)

        def take_at(pick, at):
            values = [ref[at, :] for ref in got]
            return pick("gx", x_count, values[0], values[1] if gots > 1 else None)

        def take(pick, i):
            return take_at(pick, slice(i * planes, (i + 1) * planes))

        add[...] = jnp.zeros_like(add)
        for c in range(planes):
            w3[c] = w[c]
        for pick, near, far, edge in ((high_of, cx, cx + 1, cx - 1), (low_of, rows - 1, rows - 2, 0)):
            first, second, third = take(pick, 0), take(pick, 1), take(pick, 2)
            other = shift_lanes(third, -cy)
            one = jnp.where((lane_p == 0) | (lane_p == cy - 1), other, 0.0)
            two = jnp.where(lane_p == 0, shift_lanes(third, -cy - 1), 0.0)
            two = jnp.where(lane_p == cy - 1, shift_lanes(third, 1 - cy), two)
            for at, value, ends in ((near, first, one), (far, shift_lanes(first, -cy), two)):
                value = jnp.where(lane_p < cy, value, 0.0)
                value += jnp.where(lane_p == cy, shift_lanes(ends, 1), 0.0)
                value += jnp.where(lane_p == LANES - 1, shift_lanes(ends, -1), 0.0)
                add[:, at, :] = value
            w3[:, near, :] = jnp.where(lane_p < cy, second, 0.0)
            w3[:, far, :] = jnp.where(lane_p < cy, shift_lanes(second, -cy), 0.0)
            add[:, edge, :] = jnp.where(lane_p < cy, third, 0.0)
        for c in range(planes):
            rhs3[c] = rhs[c] + add[c]

        lane_c = lane_ids(rows)
        lane8 = lane_ids(8)
        base = 5 * planes
        x_face = slice(3 * planes, 3 * planes + nz)
        x_high = take_at(high_of, x_face)

        def fill(ref, first, fine, early):
            acc = jnp.zeros((rows, LANES), F32)
            inner = first if first > 0 else 0
            for z in range(planes):
                for field, width, at, source in (
                    (rhs3, 3, 3 * z, first),
                    (w3, 2, 3 * planes + 2 * z, inner),
                ):
                    there = (lane_c >= at) & (lane_c < at + width)
                    acc = jnp.where(there, shift_lanes(field[z], at - source), acc)
            ref[:cut, :] = acc[:cut]
            ref[: rows - cut, :] += shift_lanes(acc[cut:], base)
            ref[cut - 8 : cut, :] += line(x_high, lane8, fine, base)
            ref[cut:, :] = early

        def up(ref):
            fill(ref, cy - 2, 2 * cy - 1, up_[...])

        def down(ref):
            row = row_ids(nx)
            ends = jnp.where(row == 0, line(take_at(low_of, x_face), lane8, 0, 0)[:1, :], 0.0)
            ends += jnp.where(row == nx - 1, line(x_high, lane8, 0, 0)[:1, :], 0.0)
            inverse = inv[...]
            value = part[...] + inverse * ends
            packed = down_[...]
            for i, source in (
                (1, value[:half]),
                (2, inverse[:half]),
                (4, value[half:]),
                (5, inverse[half:]),
            ):
                there = lane_ids(half) // nz == i
                packed = jnp.where(there, shift_lanes(source, i * nz), packed)
            fill(ref, -1, 0, packed)

        write_sides("gy", out, up, down)

    whole = (planes, rows, LANES)
    return call(
        body,
        [whole, whole] + [(cut + half, LANES)] * sends,
        scratch=[whole],
        in_specs=vmem(gots + 9),
        out_specs=vmem(2 + sends),
    )(*got, rhs, w, *early)


def y_early(got_z, fg, node_shift, after, z_count):
    nz, nx, _ = fg.shape
    z_at = 9 * (nx // 2 + 8)
    n_z = len(got_z)

    def body(*refs):
        gz = refs[:n_z]
        fg, shift, _, up, down, part, inv, last = refs[n_z:]
        lane = lane_ids(nx)
        row = row_ids(nx)

        def side(pick):
            values = [ref[z_at : z_at + nx, :] for ref in gz]
            return pick("gz", z_count, values[0], values[1] if n_z > 1 else None)

        above = side(high_of)
        here = jnp.where(lane == nz, shift_lanes(above, nz), 0.0)
        here = jnp.where(lane == LANES - 1, shift_lanes(side(low_of), -1), here)
        high = jnp.where(lane == nz, shift_lanes(above, nz + 1), 0.0)
        inverse = jnp.ones((nx, LANES), F32)
        inner = jnp.zeros((nx, LANES), F32)
        for z in range(nz):
            guess = fg[z]
            here = jnp.where(lane == z, shift_lanes(guess, z), here)
            inner = jnp.where(lane == z, shift_lanes(guess, z - 1), inner)
            high = jnp.where(lane == z, shift_lanes(guess, z + 1), high)
            inverse = jnp.where(lane == z, shift_lanes(6.0 + shift[z], z), inverse)
        inverse = 1.0 / inverse
        around = inner + shift_lanes(here, 1) + shift_lanes(here, -1)
        around += jnp.where(row == 0, 0.0, shift_rows(here, 1))
        around += jnp.where(row == nx - 1, 0.0, shift_rows(here, -1))
        last[...] = high
        half = nx // 2
        lane_h = lane_ids(half)

        def fold(value):
            first, second = value[:half], value[half:]
            block = jnp.where(lane_h < nz, first, 0.0)
            there = (lane_h >= 3 * nz) & (lane_h < 4 * nz)
            block = jnp.where(there, shift_lanes(second, 3 * nz), block)
            block = jnp.where(lane_h == 6 * nz, shift_lanes(first, 5 * nz), block)
            return jnp.where(lane_h == 6 * nz + 1, shift_lanes(second, 5 * nz + 1), block)

        up[...] = fold(high)
        down[...] = fold(here)
        part[...] = here + inverse * around
        inv[...] = inverse

    return call(
        body, [(nx // 2, LANES)] * 2 + [(nx, LANES)] * 3, in_specs=vmem(n_z + 3), out_specs=vmem(5)
    )(*got_z, fg, node_shift, after)


def coarse_stage(got, rhs, w, after, y_count, devices):
    planes, rows, _ = rhs.shape
    cz, cx = planes - 4, rows - 8
    cy = LANES // 2
    gots = len(got)

    def body(*refs):
        got = refs[:gots]
        rhs, w, _, v1, v2, sums, tot, inv_, image_ = refs[gots:]
        cut = fold_row(rows)
        tail = [shift_lanes(ref[: rows - cut, :], -5 * planes) for ref in got]
        values = [jnp.concatenate([ref[:cut, :], t], axis=0) for ref, t in zip(got, tail)]
        second = values[1] if gots > 1 else None
        low = low_of("gy", y_count, values[0], second)
        high = high_of("gy", y_count, values[0], second)
        lane = lane_ids(rows)
        above = (lane >= cy - 1) & (lane < cy + 2)
        below = (lane >= LANES - 2) | (lane == 0)
        for z in range(planes):
            at = 3 * z
            right = jnp.where(below, shift_lanes(low, LANES - 2 - at), 0.0)
            right = rhs[z] + jnp.where(above, shift_lanes(high, cy - 1 - at), right)
            at = 3 * planes + 2 * z
            inv = jnp.where(lane >= LANES - 2, shift_lanes(low, LANES - 2 - at), w[z])
            inv = jnp.where((lane >= cy) & (lane < cy + 2), shift_lanes(high, cy - at), inv)
            inv_[z] = inv
            tot[z] = right
            v1[z] = right * inv

        def near(field, z):
            here = field[z]
            total = field[(z + 1) % planes] + field[(z - 1) % planes]
            total += shift_rows(here, 1) + shift_rows(here, -1)
            return total + shift_lanes(here, 1) + shift_lanes(here, -1)

        v2[cz + 1] = jnp.zeros((rows, LANES), F32)
        v2[cz + 2] = jnp.zeros((rows, LANES), F32)
        for z in list(range(cz + 1)) + [planes - 1]:
            image = tot[z] - near(v1, z)
            if z < cz:
                image_[z] = image
            v2[z] = image * inv_[z]
        parts = [jnp.zeros((cx, LANES), F32)] * 5
        for z in range(cz):
            first, second_, right, image = v1[z], v2[z], tot[z], image_[z]
            third = image - near(v2, z)
            terms = (first * right, second_ * right, first * image, second_ * image, second_ * third)
            parts = [a + b[:cx, :] for a, b in zip(parts, terms)]
        keep = lane_ids(1) < cy
        lines = [jnp.where(keep, jnp.sum(a, axis=0, keepdims=True), 0.0) for a in parts]
        tile = jnp.concatenate(lines + [jnp.zeros((3, LANES), F32)], axis=0)
        column = jnp.sum(tile, axis=1, keepdims=True)
        spread = jnp.where(lane_ids(8) == row_ids(8), column, 0.0)
        line = jnp.sum(spread, axis=0, keepdims=True)
        sums[...] = jnp.broadcast_to(line[None], (devices, 1, LANES))

    whole = (planes, rows, LANES)
    return call(
        body,
        [whole, whole, (devices, 1, LANES)],
        scratch=[whole, whole, whole],
        in_specs=vmem(gots + 3),
        out_specs=vmem(3),
    )(*got, rhs, w, *after)


def smooth_stage(scaled, inverses, below, tail_z, tail_x, tail_y, after, counts):
    _, nz, nx, _ = scaled.shape

    def body(*refs):
        s, inv, lz, lx, ly = refs[:5]
        tz, gx, ty, _, out = refs[5:]
        lane = lane_ids(nx)
        row = row_ids(nx)
        y_low = from_below("gy", ly[...])

        y_high = from_above("gy", counts[2], ty[...])
        for k in range(3):
            z_low = from_below("gz", lz[k])
            z_high = from_above("gz", counts[0], tz[k * nx : (k + 1) * nx, :])
            x_low = from_below("gx", lx[k * nz : (k + 1) * nz, :])
            x_high = from_above("gx", counts[1], gx[k * nz : (k + 1) * nz, :])
            for z in range(nz):
                here = s[k, z]
                around = s[k, z - 1] if z > 0 else z_low
                around += s[k, z + 1] if z < nz - 1 else z_high
                around += jnp.where(row == 0, x_low[z : z + 1, :], shift_rows(here, 1))
                around += jnp.where(row == nx - 1, x_high[z : z + 1, :], shift_rows(here, -1))
                spot = k * nz + z
                around += jnp.where(lane == 0, shift_lanes(y_low, -spot), shift_lanes(here, 1))
                right = shift_lanes(y_high, -spot - 1)
                around += jnp.where(lane == LANES - 1, right, shift_lanes(here, -1))
                out[k, z] = here + around * inv[k, z]

    return call(
        body, [scaled.shape], in_specs=vmem(9), out_specs=vmem(1)
    )(scaled, inverses, *below, tail_z, tail_x, tail_y, after)[0]


def final_stage(sums, v1, v2, fg, mid, smooth, early, tail_z, tail_x, got_x, got_y, counts):
    planes, rows, _ = v1.shape
    cz, cx, cy = planes - 4, rows - 8, LANES // 2
    nz, nx, _ = fg.shape
    n_x, n_y = len(got_x), len(got_y)
    gots = n_x + n_y

    def body(*refs):
        sums, v1, v2, fg, part, inv, smooth, early, tz, tx = refs[:10]
        gx = refs[10 : 10 + n_x]
        gy = refs[10 + n_x : 10 + gots]
        out, sol, dup, inter, small, lines, buf, sem = refs[10 + gots :]

        def one_side(pick, refs, axis, size, at):
            values = [ref[at, :] for ref in refs]
            return pick(axis, size, values[0], values[1] if len(values) > 1 else None)

        def both(refs, axis, size, at):
            return [one_side(pick, refs, axis, size, at) for pick in (low_of, high_of)]

        total = jnp.sum(sums[...], axis=0)
        lane1 = lane_ids(1)
        gone, gtwo, hone, hmix, htwo = [
            jnp.sum(jnp.where(lane1 == i, total, 0.0), axis=1, keepdims=True) for i in range(5)
        ]
        two = (gtwo - hmix * gone / hone) / (htwo - hmix * hmix / hone)
        one = (gone - hmix * two) / hone
        source = lax.broadcasted_iota(jnp.int32, (LANES, 2 * LANES), 0)
        target = lax.broadcasted_iota(jnp.int32, (LANES, 2 * LANES), 1)
        fine = target - LANES
        side = jnp.where(fine % 2 == 1, fine // 2 + 1, (fine // 2 + LANES - 1) % LANES)
        spread = jnp.where(jnp.where(target < LANES, target // 2, side) == source, 1.0, 0.0)
        for z in range(planes):
            sol[z] = one * v1[z] + two * v2[z]
        every = select_sum(sol[...].reshape(planes * rows, LANES), spread)
        dup[...] = every.reshape(planes, rows, 2 * LANES)

        x_low, x_high = both(gx, "gx", counts[1], slice(3 * planes, 3 * planes + nz + 1))
        half, cut = nx // 2, fold_row(rows)
        y_row_low, y_row_high = both(gy, "gy", counts[2], slice(cut - 8, cut - 7))
        y_packs = both(gy, "gy", counts[2], slice(cut, cut + half))
        lane_h = lane_ids(half)

        def unfold(pack):
            first = jnp.where(lane_h < nz, pack, shift_lanes(pack, -5 * nz))
            second = shift_lanes(pack, -5 * nz - 1)
            second = jnp.where(lane_h < nz, shift_lanes(pack, -3 * nz), second)
            return jnp.concatenate([first, second], axis=0)

        y_low, y_high = [unfold(pack) for pack in y_packs]
        y_pack = y_packs[1]
        lane = lane_ids(nx)
        row = row_ids(nx)
        base = 5 * planes

        def spread_around(z):
            c, odd = z // 2, z % 2
            here = dup[c, :, :LANES]
            same = 3.0 * here + dup[c, :, LANES:]
            same += dup[(c + 1 if odd else c - 1) % planes, :, :LANES]
            slot = z % 2
            inter[slot, pl.ds(0, cx, 2), :] = (same + shift_rows(here, 1))[:cx, :]
            inter[slot, pl.ds(1, cx, 2), :] = (same + shift_rows(here, -1))[:cx, :]
            return inter[slot]

        def nodal(z):
            around = spread_around(z) + jnp.where(row == 0, x_low[z : z + 1, :], 0.0)
            around += jnp.where(row == nx - 1, x_high[z : z + 1, :], 0.0)
            around += jnp.where(lane == 0, shift_lanes(y_low, -z), 0.0)
            around += jnp.where(lane == LANES - 1, shift_lanes(y_high, -z - 1), 0.0)
            if z == nz:
                value = tz[3 * nx : 4 * nx, :] + tz[4 * nx :, :] * (around + fg[nz - 1])
                return from_above("gz", counts[0], value)
            return part[z] + inv[z] * around

        here = dup[:cz, cx, :LANES]
        same = 3.0 * here + dup[:cz, cx, LANES:] + dup[:cz, cx - 1, :LANES]
        small[pl.ds(0, cz, 2), :] = same + jnp.concatenate(
            [dup[planes - 1, cx : cx + 1, :LANES], here[: cz - 1]], axis=0
        )
        small[pl.ds(1, cz, 2), :] = same + dup[1 : cz + 1, cx, :LANES]
        for z in range(nz):
            left = shift_lanes(y_row_low, -(base + z))
            right = shift_lanes(y_row_high, -(base + z) - 1)
            value = jnp.where(lane1 == 0, left, 0.0)
            lines[z : z + 1, :] = jnp.where(lane1 == LANES - 1, right, value)
        x_value = tx[3 * nz : 4 * nz, :] + tx[4 * nz :, :] * (
            fg[:, nx - 1, :] + small[...] + lines[...]
        )
        x_value = from_above("gx", counts[1], x_value)

        lane_c = lane_ids(rows)
        even = jnp.zeros((rows, LANES), F32)
        odd = jnp.zeros((rows, LANES), F32)
        for z in range(nz):
            c = z // 2
            here = sol[c]
            same = 3.0 * here + shift_lanes(here, 1) + sol[(c + 1 if z % 2 else c - 1) % planes]
            even = jnp.where(lane_c == z, shift_lanes(same + shift_rows(here, 1), z - cy), even)
            odd = jnp.where(lane_c == z, shift_lanes(same + shift_rows(here, -1), z - cy), odd)
        inter[0, pl.ds(0, cx, 2), :] = even[:cx, :]
        inter[0, pl.ds(1, cx, 2), :] = odd[:cx, :]
        y_base = jnp.concatenate(
            [shift_lanes(y_pack, -nz), shift_lanes(y_pack, -4 * nz)], axis=0
        )
        y_inverse = jnp.concatenate(
            [shift_lanes(y_pack, -2 * nz), shift_lanes(y_pack, -5 * nz)], axis=0
        )
        y_value = y_base + y_inverse * (early[...] + inter[0])
        y_value = from_above("gy", counts[2], y_value)

        def copy(z):
            return pltpu.make_async_copy(buf.at[:, z], out.at[:, z], sem.at[z])

        value = nodal(0)
        for z in range(nz):
            after = nodal(z + 1)
            steps = [after, jnp.where(row == nx - 1, x_value[z : z + 1, :], shift_rows(value, -1))]
            steps.append(
                jnp.where(lane == LANES - 1, shift_lanes(y_value, -z - 1), shift_lanes(value, -1))
            )
            for k in range(3):
                buf[k, z] = smooth[k, z] + (steps[k] - value)
            copy(z).start()
            value = after
        for z in range(nz):
            copy(z).wait()

    return call(
        body,
        [smooth.shape],
        scratch=[
            (planes, rows, LANES),
            (planes, rows, 2 * LANES),
            (2, nx, LANES),
            (nz, LANES),
            (nz, LANES),
            smooth.shape,
            pltpu.SemaphoreType.DMA((nz,)),
        ],
        far_out=True,
        in_specs=vmem(10 + gots),
        out_specs=[pl.BlockSpec(memory_space=pltpu.HBM)],
    )(sums, v1, v2, fg, *mid, smooth, early, tail_z, tail_x, *got_x, *got_y)[0]


def local(residual, edge_diag, node_shift, coarse_shift):
    axes = ("gz", "gx", "gy")
    counts = tuple(lax.axis_size(a) for a in axes)
    devices = counts[0] * counts[1] * counts[2]
    part, *faces, scaled, inverses = edge_stage(residual, edge_diag)
    up_z, up_x, up_y, low_z, low_x, low_y = faces
    below = []
    for value, axis in ((up_z, "gz"), (up_x, "gx"), (up_y, "gy")):
        below.append(ring(value, axis, 1))
    tail_y = ring(low_y, "gy", -1)
    fg, rhs, xb, yb, w, *send = nodal_stage(part, node_shift, coarse_shift, *below, counts[0])
    got_z = swap(send, "gz")
    rhs, w, *send = x_stage(got_z, rhs, xb, yb, w, fg, counts[0], counts[1])
    got_x = swap(send, "gx", ("gx", "gy"))
    tail_x = x_tail(got_z, fg, node_shift, low_x, w, counts[0])
    *mid, tail_z = part_stage(got_z, fg, node_shift, low_z, w, counts[0])
    early = y_early(got_z, fg, node_shift, w, counts[0])
    early = (*early, tail_x, mid[1])
    tail_z = ring(tail_z, "gz", -1)
    tail_x = ring(tail_x, "gx", -1)
    rhs, w, *send = y_stage(got_x, rhs, w, early, counts[1], counts[2])
    got_y = swap(send, "gy", ("gx", "gy"))
    smooth = smooth_stage(scaled, inverses, below, tail_z, tail_x, tail_y, w, counts)
    v1, v2, sums = coarse_stage(got_y, rhs, w, (smooth,), counts[2], devices)
    sums = lax.all_to_all(sums, ("gx", "gy", "gz"), 0, 0)
    early = early[4]
    return final_stage(
        sums, v1, v2, fg, mid, smooth, early, tail_z, tail_x, got_x, got_y, counts
    )


def solution(mesh):
    placed = (
        P(None, "gz", "gx", "gy"),
        P(None, "gz", "gx", "gy"),
        P("gz", "gx", "gy"),
        P("gz", "gx", "gy"),
    )

    return jax.shard_map(
        local, mesh=mesh, in_specs=placed, out_specs=P(None, "gz", "gx", "gy"), check_vma=False
    )
```

```python
import itertools

import jax
import jax.numpy as jnp
from jax import lax
from jax.experimental import pallas as pl
from jax.experimental.pallas import tpu as pltpu
from jax.sharding import PartitionSpec as P


F32 = jnp.float32
LANES = 128


def lane_ids(rows):
    return lax.broadcasted_iota(jnp.int32, (rows, LANES), 1)


def row_ids(rows):
    return lax.broadcasted_iota(jnp.int32, (rows, LANES), 0)


def shift_lanes(value, amount):
    return pltpu.roll(value, amount % LANES, 1)


def shift_rows(value, amount):
    return pltpu.roll(value, amount % value.shape[0], 0)


def low_of(axis, size, first, second):
    place = lax.axis_index(axis)
    odd = place % 2 == 1
    zero = jnp.zeros_like(first)
    if second is None:
        return jnp.where(odd, first, zero)
    return jnp.where(odd, first, jnp.where(place > 0, second, zero))


def high_of(axis, size, first, second):
    place = lax.axis_index(axis)
    even = place % 2 == 0
    zero = jnp.zeros_like(first)
    if second is None:
        return jnp.where(even, first, zero)
    return jnp.where(even, first, jnp.where(place < size - 1, second, zero))


def from_below(axis, value):
    return jnp.where(lax.axis_index(axis) > 0, value, jnp.zeros_like(value))


def from_above(axis, size, value):
    return jnp.where(lax.axis_index(axis) < size - 1, value, jnp.zeros_like(value))


def ring(value, axis, step):
    size = lax.axis_size(axis)
    return lax.ppermute(value, axis, [(i, (i + step) % size) for i in range(size)])


def swap(values, axis, names=None):
    size = lax.axis_size(axis)
    out = [lax.ppermute(values[0], axis, [(i, i ^ 1) for i in range(size)])]
    if len(values) == 1:
        return out
    odd = [(i + 1) % size if i % 2 else (i - 1) % size for i in range(size)]
    if names is None:
        out.append(lax.ppermute(values[1], axis, list(enumerate(odd))))
        return out
    main = names.index(axis)
    pairs = []
    sizes = [lax.axis_size(name) for name in names]
    for at in itertools.product(*(range(n) for n in sizes)):
        to = list(at)
        if at[main] in (0, size - 1):
            to[1 - main] ^= 1
        else:
            to[main] = odd[at[main]]
        pairs.append(tuple(p[0] * sizes[1] + p[1] for p in (at, to)))
    out.append(lax.ppermute(values[1], names, pairs))
    return out


def write_sides(axis, refs, up, down):
    even = lax.axis_index(axis) % 2 == 0

    @pl.when(even)
    def _():
        up(refs[0])
        if len(refs) > 1:
            down(refs[1])

    @pl.when(jnp.logical_not(even))
    def _():
        down(refs[0])
        if len(refs) > 1:
            up(refs[1])


def call(body, outs, scratch=(), far=(), far_out=False, **kwargs):
    kind = jax.ShapeDtypeStruct if far_out else pltpu.VMEM
    run = pl.pallas_call(
        body,
        out_shape=[kind(shape, F32) for shape in outs],
        scratch_shapes=[pltpu.VMEM(s, F32) if isinstance(s, tuple) else s for s in scratch],
        compiler_params=pltpu.CompilerParams(vmem_limit_bytes=12 * 2**20),
        **kwargs,
    )

    def apply(*args):
        spaces = [pltpu.HBM if i in far else pltpu.VMEM for i in range(len(args))]
        return run(
            *(
                pltpu.with_memory_space_constraint(a, space)
                for a, space in zip(args, spaces)
            )
        )

    return apply


def vmem(count):
    return [pl.BlockSpec(memory_space=pltpu.VMEM)] * count


def edge_stage(residual, edge_diag):
    _, nz, nx, ny = residual.shape
    step = 4
    steps = nz // step

    def body(res, diag, part, up_z, up_x, up_y, low_z, low_x, low_y, scaled, inv, near, sems):
        lane = lane_ids(nx)
        row = row_ids(nx)

        def copies(block):
            at = pl.ds(block * step, step)
            return [
                pltpu.make_async_copy(source.at[:, at], target.at[:, at], sems.at[i, block])
                for i, (source, target) in enumerate(((res, near), (diag, inv)))
            ]

        for block in range(steps):
            for copy in copies(block):
                copy.start()
        before = jnp.zeros((nx, ny), F32)
        high = jnp.zeros((nx, LANES), F32)
        low = jnp.zeros((nx, LANES), F32)
        for z in range(nz):
            if z % step == 0:
                for copy in copies(z // step):
                    copy.wait()
            s = []
            for k in range(3):
                inverse = 1.0 / inv[k, z]
                inv[k, z] = inverse
                s.append(near[k, z] * inverse)
                scaled[k, z] = s[k]
            total = before - s[0]
            total += jnp.where(row == 0, 0.0, shift_rows(s[1], 1)) - s[1]
            total += jnp.where(lane == 0, 0.0, shift_lanes(s[2], 1)) - s[2]
            part[z] = total
            before = s[0]
            for k in range(3):
                spot = k * nz + z
                up_x[spot : spot + 1, :] = s[k][nx - 1 :, :]
                low_x[spot : spot + 1, :] = s[k][:1, :]
                high = jnp.where(lane == spot, shift_lanes(s[k], spot + 1), high)
                low = jnp.where(lane == spot, shift_lanes(s[k], spot), low)
                if z == 0:
                    low_z[k] = s[k]
                if z == nz - 1:
                    up_z[k] = s[k]
        up_y[...] = high
        low_y[...] = low

    faces = [(3, nx, ny), (3 * nz, ny), (nx, LANES)] * 2
    return call(
        body,
        [(nz, nx, ny)] + faces + [residual.shape] * 2,
        scratch=[residual.shape, pltpu.SemaphoreType.DMA((2, steps))],
        far=(0, 1),
        in_specs=[pl.BlockSpec(memory_space=pltpu.HBM)] * 2,
        out_specs=vmem(9),
    )(residual, edge_diag)


def select_sum(values, chosen):
    first = values.astype(jnp.bfloat16)
    left = values - first.astype(F32)
    second = left.astype(jnp.bfloat16)
    third = (left - second.astype(F32)).astype(jnp.bfloat16)
    chosen = chosen.astype(jnp.bfloat16)
    both = jnp.concatenate([first, second], axis=1)
    total = jnp.dot(both, jnp.concatenate([chosen, chosen], axis=0), preferred_element_type=F32)
    return total + jnp.dot(third, chosen, preferred_element_type=F32)


def plane(values, row_count):
    return jnp.concatenate([values, jnp.zeros((row_count - values.shape[0], LANES), F32)], axis=0)


def nodal_stage(part, node_shift, coarse_shift, got_z, got_x, got_y, z_count):
    nz, nx, ny = part.shape
    cz, cx, cy = nz // 2, nx // 2, ny // 2
    rows = cx + 8
    sends = 1 if z_count == 2 else 2

    def body(part, shift, coarse, gz, gx, gy, fg, rhs, xb, yb, w, *rest):
        out, (pair, stack, s_, xl_, yl_, zl_, zh_) = rest[:sends], rest[sends:]
        lane = lane_ids(nx)
        row = row_ids(nx)
        lane_c = lane_ids(rows)
        row_c = row_ids(rows)
        below_z = from_below("gz", gz[0])
        below_y = from_below("gy", gy[...])
        fine = lax.broadcasted_iota(jnp.int32, (ny, 2 * LANES), 0)
        coarse_lane = lax.broadcasted_iota(jnp.int32, (ny, 2 * LANES), 1)
        miss = jnp.where(
            coarse_lane < LANES, fine // 2 - coarse_lane, fine - 2 * (coarse_lane - LANES)
        )
        gather = jnp.where(miss == 0, 1.0, 0.0)
        for c in range(cz):
            both = []
            for z in (2 * c, 2 * c + 1):
                total = part[z]
                if z == 0:
                    total += below_z
                total += jnp.where(row == 0, from_below("gx", gx[nz + z : nz + z + 1, :]), 0.0)
                total += jnp.where(lane == 0, shift_lanes(below_y, -(2 * nz + z)), 0.0)
                guess = total / (6.0 + shift[z])
                fg[z] = guess
                both.append(guess)
            pair[c % 2] = both[0] + both[1]
            low = pair[c % 2, pl.ds(0, cx, 2), :]
            high = pair[c % 2, pl.ds(1, cx, 2), :]
            first = fg[2 * c, pl.ds(0, cx, 2), :] + fg[2 * c, pl.ds(1, cx, 2), :]
            stack[c, :cx, :] = low + high
            stack[c, cx : 2 * cx, :] = low
            stack[c, 2 * cx :, :] = first
        every = select_sum(stack[...].reshape(3 * cx * cz, LANES), gather)
        for c in range(cz):
            sums = every[3 * cx * c : 3 * cx * (c + 1)]
            s = sums[:cx, :LANES]
            z_low = sums[2 * cx :, :LANES]
            s_[c] = plane(s, rows)
            yl_[c] = plane(sums[:cx, LANES:], rows)
            xl_[c] = plane(sums[cx : 2 * cx, :LANES], rows)
            zl_[c] = plane(z_low, rows)
            zh_[c] = plane(s - z_low, rows)
            w[c] = jnp.zeros((rows, LANES), F32)
            w[c, :cx, :cy] = 1.0 / (6.0 + coarse[c])
        for c in range(cz):
            s, x_low, y_low = s_[c], xl_[c], yl_[c]
            x_high = s - x_low
            y_high = s - y_low
            total = 3.0 * s
            total += shift_rows(x_low, -1) + shift_rows(x_high, 1)
            total += shift_lanes(y_low, -1) + shift_lanes(y_high, 1)
            if c > 0:
                total += zh_[c - 1]
            if c < cz - 1:
                total += zl_[c + 1]
            rhs[c] = total
            xb[c] = jnp.where(row_c < cx // 2, x_low, x_high)
            yb[c] = jnp.where(lane_c < cy // 2, y_low, y_high)
        rhs[cz] = zh_[cz - 1]
        rhs[cz + 1] = jnp.zeros((rows, LANES), F32)
        rhs[cz + 2] = jnp.zeros((rows, LANES), F32)
        rhs[cz + 3] = zl_[0]

        def fill(ref, near, far, half, face):
            planes = [rhs[near], rhs[far], w[near], w[far], half]
            planes += [xb[near], xb[far], yb[near], yb[far]]
            for i, value in enumerate(planes):
                ref[i * rows : (i + 1) * rows, :] = value
            ref[9 * rows : 9 * rows + nx, :] = face

        def up(ref):
            fill(ref, cz - 1, cz - 2, zh_[cz - 1], fg[nz - 1])

        def down(ref):
            fill(ref, 0, 1, zl_[0], fg[0])

        write_sides("gz", out, up, down)

    coarse = (cz, rows, LANES)
    send = (9 * rows + nx, LANES)
    return call(
        body,
        [(nz, nx, ny), (cz + 4, rows, LANES), coarse, coarse, coarse] + [send] * sends,
        scratch=[(2, nx, ny), (cz, 3 * cx, LANES), coarse, coarse, coarse, coarse, coarse],
        in_specs=vmem(6),
        out_specs=vmem(5 + sends),
    )(part, node_shift, coarse_shift, got_z, got_x, got_y)


def x_stage(got, rhs, xb, yb, w, fg, after, z_count, x_count):
    planes, rows, _ = rhs.shape
    cz, cx = planes - 4, rows - 8
    nz, nx, ny = fg.shape
    cy = ny // 2
    sends = 1 if x_count == 2 else 2
    gots = len(got)
    size = -(-(3 * planes + nz + 1) // 8) * 8

    def body(*refs):
        got = refs[:gots]
        rhs, xb, yb, w, fg, _, _, rhs2, w2 = refs[gots : gots + 9]
        out, (xb2, yb2) = refs[gots + 9 : gots + 9 + sends], refs[gots + 9 + sends :]

        def take_at(pick, at):
            values = [ref[at, :] for ref in got]
            return pick("gz", z_count, values[0], values[1] if gots > 1 else None)

        def take(pick, i):
            return take_at(pick, slice(i * rows, (i + 1) * rows))

        for c in range(1, cz - 1):
            rhs2[c] = rhs[c]
        rhs2[0] = rhs[0] + take(low_of, 4)
        rhs2[cz - 1] = rhs[cz - 1] + take(high_of, 4)
        rhs2[cz] = rhs[cz] + take(high_of, 0)
        rhs2[cz + 1] = take(high_of, 1)
        rhs2[cz + 2] = take(low_of, 1)
        rhs2[cz + 3] = rhs[cz + 3] + take(low_of, 0)
        for here, there, i in ((w, w2, 2), (xb, xb2, 5), (yb, yb2, 7)):
            for c in range(cz):
                there[c] = here[c]
            there[cz] = take(high_of, i)
            there[cz + 1] = take(high_of, i + 1)
            there[cz + 2] = take(low_of, i + 1)
            there[cz + 3] = take(low_of, i)

        lane = lane_ids(planes)

        def fill(ref, near, far, fine):
            halves = lane < cy
            first = jnp.where(halves, rhs2[:, near, :], shift_lanes(rhs2[:, far, :], cy))
            second = jnp.where(halves, w2[:, near, :], shift_lanes(w2[:, far, :], cy))
            edge = yb2[:, far, :]
            third = jnp.where(halves, xb2[:, near, :], shift_lanes(yb2[:, near, :], cy))
            third = jnp.where(lane == cy + 1, shift_lanes(edge, cy + 1), third)
            third = jnp.where(lane == LANES - 2, shift_lanes(edge, cy - 1), third)
            for i, value in enumerate((first, second, third)):
                ref[i * planes : (i + 1) * planes, :] = value
            ref[3 * planes : 3 * planes + nz, :] = fg[:, fine, :]
            at = 9 * rows + fine
            last = 3 * planes + nz
            ref[last : last + 1, :] = take_at(high_of, slice(at, at + 1))
            ref[last + 1 :, :] = jnp.zeros((size - last - 1, LANES), F32)

        def up(ref):
            fill(ref, cx - 1, cx - 2, nx - 1)

        def down(ref):
            fill(ref, 0, 1, 0)

        write_sides("gx", out, up, down)

    whole = (planes, rows, LANES)
    return call(
        body,
        [whole, whole] + [(size, LANES)] * sends,
        scratch=[whole, whole],
        in_specs=vmem(gots + 7),
        out_specs=vmem(2 + sends),
    )(*got, rhs, xb, yb, w, fg, *after)


def x_tail(got, fg, node_shift, low_x, after, z_count):
    nz, nx, ny = fg.shape
    z_at = 9 * (nx // 2 + 8)
    gots = len(got)

    def body(*refs):
        got = refs[:gots]
        fg, shift, low_x, _, out = refs[gots:]
        lane = lane_ids(nz)
        row = row_ids(nz)

        def z_row(pick):
            values = [ref[z_at : z_at + 1, :] for ref in got]
            return pick("gz", z_count, values[0], values[1] if gots > 1 else None)

        here = fg[:, 0, :]
        around = fg[:, 1, :] + jnp.where(row == 0, z_row(low_of), shift_rows(here, 1))
        around += jnp.where(row == nz - 1, z_row(high_of), shift_rows(here, -1))
        around += jnp.where(lane == 0, 0.0, shift_lanes(here, 1))
        around += jnp.where(lane == ny - 1, 0.0, shift_lanes(here, -1))
        inverse = 1.0 / (6.0 + shift[:, 0, :])
        out[: 3 * nz, :] = low_x[...]
        out[3 * nz : 4 * nz, :] = here + inverse * around
        out[4 * nz :, :] = inverse

    return call(
        body, [(5 * nz, LANES)], in_specs=vmem(gots + 4), out_specs=vmem(1)
    )(*got, fg, node_shift, low_x, after)[0]


def part_stage(fg, node_shift, low_z):
    nz, nx, ny = fg.shape

    def body(fg, shift, low_z, part, inv, tail):
        lane = lane_ids(nx)
        row = row_ids(nx)
        zero = jnp.zeros((nx, ny), F32)
        for z in range(nz):
            guess = fg[z]
            inner = fg[z + 1] if z < nz - 1 else zero
            inner += jnp.where(row == 0, 0.0, shift_rows(guess, 1))
            inner += jnp.where(row == nx - 1, 0.0, shift_rows(guess, -1))
            inner += jnp.where(lane == 0, 0.0, shift_lanes(guess, 1))
            inner += jnp.where(lane == ny - 1, 0.0, shift_lanes(guess, -1))
            inverse = 1.0 / (6.0 + shift[z])
            inv[z] = inverse
            part[z] = guess + inverse * (inner + (fg[z - 1] if z > 0 else zero))
            if z == 0:
                for k in range(3):
                    tail[k * nx : (k + 1) * nx, :] = low_z[k]
                tail[3 * nx : 4 * nx, :] = guess + inverse * inner
                tail[4 * nx :, :] = inverse

    return call(
        body, [fg.shape, fg.shape, (5 * nx, LANES)], in_specs=vmem(3), out_specs=vmem(3)
    )(fg, node_shift, low_z)


def fold_row(rows):
    return (rows + 8) // 16 * 8


def line(source, lane, fine, at):
    acc = jnp.zeros(lane.shape, F32)
    for z in range(source.shape[0]):
        moved = jnp.broadcast_to(source[z : z + 1, :], lane.shape)
        acc = jnp.where(lane == at + z, shift_lanes(moved, at + z - fine), acc)
    return acc


def y_stage(got, rhs, w, early, x_count, y_count):
    planes, rows, _ = rhs.shape
    cx = rows - 8
    nx, cy = 2 * cx, LANES // 2
    nz, half, cut = 2 * (planes - 4), nx // 2, fold_row(rows)
    sends = 1 if y_count == 2 else 2
    gots = len(got)

    def body(*refs):
        got = refs[:gots]
        rhs, w, up_, down_, part, inv, _, rhs3, w3 = refs[gots : gots + 9]
        rest = refs[gots + 9 :]
        out, (add,) = rest[:sends], rest[sends:]
        lane_p = lane_ids(planes)

        def take_at(pick, at):
            values = [ref[at, :] for ref in got]
            return pick("gx", x_count, values[0], values[1] if gots > 1 else None)

        def take(pick, i):
            return take_at(pick, slice(i * planes, (i + 1) * planes))

        add[...] = jnp.zeros_like(add)
        for c in range(planes):
            w3[c] = w[c]
        for pick, near, far, edge in ((high_of, cx, cx + 1, cx - 1), (low_of, rows - 1, rows - 2, 0)):
            first, second, third = take(pick, 0), take(pick, 1), take(pick, 2)
            other = shift_lanes(third, -cy)
            one = jnp.where((lane_p == 0) | (lane_p == cy - 1), other, 0.0)
            two = jnp.where(lane_p == 0, shift_lanes(third, -cy - 1), 0.0)
            two = jnp.where(lane_p == cy - 1, shift_lanes(third, 1 - cy), two)
            for at, value, ends in ((near, first, one), (far, shift_lanes(first, -cy), two)):
                value = jnp.where(lane_p < cy, value, 0.0)
                value += jnp.where(lane_p == cy, shift_lanes(ends, 1), 0.0)
                value += jnp.where(lane_p == LANES - 1, shift_lanes(ends, -1), 0.0)
                add[:, at, :] = value
            w3[:, near, :] = jnp.where(lane_p < cy, second, 0.0)
            w3[:, far, :] = jnp.where(lane_p < cy, shift_lanes(second, -cy), 0.0)
            add[:, edge, :] = jnp.where(lane_p < cy, third, 0.0)
        for c in range(planes):
            rhs3[c] = rhs[c] + add[c]

        lane_c = lane_ids(rows)
        lane8 = lane_ids(8)
        base = 5 * planes
        x_face = slice(3 * planes, 3 * planes + nz)
        x_high = take_at(high_of, x_face)

        def fill(ref, first, fine, early):
            acc = jnp.zeros((rows, LANES), F32)
            inner = first if first > 0 else 0
            for z in range(planes):
                for field, width, at, source in (
                    (rhs3, 3, 3 * z, first),
                    (w3, 2, 3 * planes + 2 * z, inner),
                ):
                    there = (lane_c >= at) & (lane_c < at + width)
                    acc = jnp.where(there, shift_lanes(field[z], at - source), acc)
            ref[:cut, :] = acc[:cut]
            ref[: rows - cut, :] += shift_lanes(acc[cut:], base)
            ref[cut - 8 : cut, :] += line(x_high, lane8, fine, base)
            ref[cut:, :] = early

        def up(ref):
            fill(ref, cy - 2, 2 * cy - 1, up_[...])

        def down(ref):
            row = row_ids(nx)
            ends = jnp.where(row == 0, line(take_at(low_of, x_face), lane8, 0, 0)[:1, :], 0.0)
            ends += jnp.where(row == nx - 1, line(x_high, lane8, 0, 0)[:1, :], 0.0)
            inverse = inv[...]
            value = part[...] + inverse * ends
            packed = down_[...]
            for i, source in (
                (1, value[:half]),
                (2, inverse[:half]),
                (4, value[half:]),
                (5, inverse[half:]),
            ):
                there = lane_ids(half) // nz == i
                packed = jnp.where(there, shift_lanes(source, i * nz), packed)
            fill(ref, -1, 0, packed)

        write_sides("gy", out, up, down)

    whole = (planes, rows, LANES)
    return call(
        body,
        [whole, whole] + [(cut + half, LANES)] * sends,
        scratch=[whole],
        in_specs=vmem(gots + 7),
        out_specs=vmem(2 + sends),
    )(*got, rhs, w, *early)


def y_columns(fg, node_shift):
    nz, nx, _ = fg.shape

    def body(fg, shift, here_, inner_, high_, inv):
        lane = lane_ids(nx)
        zero = jnp.zeros((nx, LANES), F32)
        here, inner, high, inverse = zero, zero, zero, zero + 1.0
        for z in range(nz):
            guess = fg[z]
            here = jnp.where(lane == z, shift_lanes(guess, z), here)
            inner = jnp.where(lane == z, shift_lanes(guess, z - 1), inner)
            high = jnp.where(lane == z, shift_lanes(guess, z + 1), high)
            inverse = jnp.where(lane == z, shift_lanes(6.0 + shift[z], z), inverse)
        here_[...] = here
        inner_[...] = inner
        high_[...] = high
        inv[...] = 1.0 / inverse

    return call(body, [(nx, LANES)] * 4, in_specs=vmem(2), out_specs=vmem(4))(fg, node_shift)


def y_early(got_z, columns, after, nz, z_count):
    nx = columns[0].shape[0]
    z_at = 9 * (nx // 2 + 8)
    n_z = len(got_z)

    def body(*refs):
        gz = refs[:n_z]
        here_, inner, high_, inv, _, up, down, part, last = refs[n_z:]
        lane = lane_ids(nx)
        row = row_ids(nx)

        def side(pick):
            values = [ref[z_at : z_at + nx, :] for ref in gz]
            return pick("gz", z_count, values[0], values[1] if n_z > 1 else None)

        above = side(high_of)
        here = jnp.where(lane == nz, shift_lanes(above, nz), here_[...])
        here = jnp.where(lane == LANES - 1, shift_lanes(side(low_of), -1), here)
        high = jnp.where(lane == nz, shift_lanes(above, nz + 1), high_[...])
        inverse = inv[...]
        around = inner[...] + shift_lanes(here, 1) + shift_lanes(here, -1)
        around += jnp.where(row == 0, 0.0, shift_rows(here, 1))
        around += jnp.where(row == nx - 1, 0.0, shift_rows(here, -1))
        last[...] = high
        half = nx // 2
        lane_h = lane_ids(half)

        def fold(value):
            first, second = value[:half], value[half:]
            block = jnp.where(lane_h < nz, first, 0.0)
            there = (lane_h >= 3 * nz) & (lane_h < 4 * nz)
            block = jnp.where(there, shift_lanes(second, 3 * nz), block)
            block = jnp.where(lane_h == 6 * nz, shift_lanes(first, 5 * nz), block)
            return jnp.where(lane_h == 6 * nz + 1, shift_lanes(second, 5 * nz + 1), block)

        up[...] = fold(high)
        down[...] = fold(here)
        part[...] = here + inverse * around

    return call(
        body, [(nx // 2, LANES)] * 2 + [(nx, LANES)] * 2, in_specs=vmem(n_z + 5), out_specs=vmem(4)
    )(*got_z, *columns, after)


def coarse_stage(got, rhs, w, after, y_count, devices):
    planes, rows, _ = rhs.shape
    cz, cx = planes - 4, rows - 8
    cy = LANES // 2
    gots = len(got)

    def body(*refs):
        got = refs[:gots]
        rhs, w, _, v1, v2, sums, tot, inv_, image_ = refs[gots:]
        cut = fold_row(rows)
        tail = [shift_lanes(ref[: rows - cut, :], -5 * planes) for ref in got]
        values = [jnp.concatenate([ref[:cut, :], t], axis=0) for ref, t in zip(got, tail)]
        second = values[1] if gots > 1 else None
        low = low_of("gy", y_count, values[0], second)
        high = high_of("gy", y_count, values[0], second)
        lane = lane_ids(rows)
        above = (lane >= cy - 1) & (lane < cy + 2)
        below = (lane >= LANES - 2) | (lane == 0)
        for z in range(planes):
            at = 3 * z
            right = jnp.where(below, shift_lanes(low, LANES - 2 - at), 0.0)
            right = rhs[z] + jnp.where(above, shift_lanes(high, cy - 1 - at), right)
            at = 3 * planes + 2 * z
            inv = jnp.where(lane >= LANES - 2, shift_lanes(low, LANES - 2 - at), w[z])
            inv = jnp.where((lane >= cy) & (lane < cy + 2), shift_lanes(high, cy - at), inv)
            inv_[z] = inv
            tot[z] = right
            v1[z] = right * inv

        def near(field, z):
            here = field[z]
            total = field[(z + 1) % planes] + field[(z - 1) % planes]
            total += shift_rows(here, 1) + shift_rows(here, -1)
            return total + shift_lanes(here, 1) + shift_lanes(here, -1)

        v2[cz + 1] = jnp.zeros((rows, LANES), F32)
        v2[cz + 2] = jnp.zeros((rows, LANES), F32)
        for z in list(range(cz + 1)) + [planes - 1]:
            image = tot[z] - near(v1, z)
            if z < cz:
                image_[z] = image
            v2[z] = image * inv_[z]
        parts = [jnp.zeros((cx, LANES), F32)] * 5
        for z in range(cz):
            first, second_, right, image = v1[z], v2[z], tot[z], image_[z]
            third = image - near(v2, z)
            terms = (first * right, second_ * right, first * image, second_ * image, second_ * third)
            parts = [a + b[:cx, :] for a, b in zip(parts, terms)]
        keep = lane_ids(1) < cy
        lines = [jnp.where(keep, jnp.sum(a, axis=0, keepdims=True), 0.0) for a in parts]
        tile = jnp.concatenate(lines + [jnp.zeros((3, LANES), F32)], axis=0)
        column = jnp.sum(tile, axis=1, keepdims=True)
        spread = jnp.where(lane_ids(8) == row_ids(8), column, 0.0)
        line = jnp.sum(spread, axis=0, keepdims=True)
        sums[...] = jnp.broadcast_to(line[None], (devices, 1, LANES))

    whole = (planes, rows, LANES)
    return call(
        body,
        [whole, whole, (devices, 1, LANES)],
        scratch=[whole, whole, whole],
        in_specs=vmem(gots + 3),
        out_specs=vmem(3),
    )(*got, rhs, w, *after)


def smooth_stage(scaled, inverses, below, tail_z, tail_x, tail_y, after, counts):
    _, nz, nx, _ = scaled.shape

    def body(*refs):
        s, inv, lz, lx, ly = refs[:5]
        tz, gx, ty, _, out = refs[5:]
        lane = lane_ids(nx)
        row = row_ids(nx)
        y_low = from_below("gy", ly[...])

        y_high = from_above("gy", counts[2], ty[...])
        for k in range(3):
            z_low = from_below("gz", lz[k])
            z_high = from_above("gz", counts[0], tz[k * nx : (k + 1) * nx, :])
            x_low = from_below("gx", lx[k * nz : (k + 1) * nz, :])
            x_high = from_above("gx", counts[1], gx[k * nz : (k + 1) * nz, :])
            for z in range(nz):
                here = s[k, z]
                around = s[k, z - 1] if z > 0 else z_low
                around += s[k, z + 1] if z < nz - 1 else z_high
                around += jnp.where(row == 0, x_low[z : z + 1, :], shift_rows(here, 1))
                around += jnp.where(row == nx - 1, x_high[z : z + 1, :], shift_rows(here, -1))
                spot = k * nz + z
                around += jnp.where(lane == 0, shift_lanes(y_low, -spot), shift_lanes(here, 1))
                right = shift_lanes(y_high, -spot - 1)
                around += jnp.where(lane == LANES - 1, right, shift_lanes(here, -1))
                out[k, z] = here + around * inv[k, z]

    return call(
        body, [scaled.shape], in_specs=vmem(9), out_specs=vmem(1)
    )(scaled, inverses, *below, tail_z, tail_x, tail_y, after)[0]


def final_stage(sums, v1, v2, fg, mid, smooth, early, tail_z, tail_x, got_z, got_x, got_y, counts):
    planes, rows, _ = v1.shape
    cz, cx, cy = planes - 4, rows - 8, LANES // 2
    nz, nx, _ = fg.shape
    step = 2
    n_z, n_x, n_y = len(got_z), len(got_x), len(got_y)
    gots = n_z + n_x + n_y

    def body(*refs):
        sums, v1, v2, fg, part, inv, smooth, early, tz, tx = refs[:10]
        gz = refs[10 : 10 + n_z]
        gx = refs[10 + n_z : 10 + n_z + n_x]
        gy = refs[10 + n_z + n_x : 10 + gots]
        out, sol, dup, inter, small, lines, buf, sem = refs[10 + gots :]

        def one_side(pick, refs, axis, size, at):
            values = [ref[at, :] for ref in refs]
            return pick(axis, size, values[0], values[1] if len(values) > 1 else None)

        def both(refs, axis, size, at):
            return [one_side(pick, refs, axis, size, at) for pick in (low_of, high_of)]

        total = jnp.sum(sums[...], axis=0)
        lane1 = lane_ids(1)
        gone, gtwo, hone, hmix, htwo = [
            jnp.sum(jnp.where(lane1 == i, total, 0.0), axis=1, keepdims=True) for i in range(5)
        ]
        two = (gtwo - hmix * gone / hone) / (htwo - hmix * hmix / hone)
        one = (gone - hmix * two) / hone
        source = lax.broadcasted_iota(jnp.int32, (LANES, 2 * LANES), 0)
        target = lax.broadcasted_iota(jnp.int32, (LANES, 2 * LANES), 1)
        fine = target - LANES
        side = jnp.where(fine % 2 == 1, fine // 2 + 1, (fine // 2 + LANES - 1) % LANES)
        spread = jnp.where(jnp.where(target < LANES, target // 2, side) == source, 1.0, 0.0)
        for z in range(planes):
            sol[z] = one * v1[z] + two * v2[z]
        every = select_sum(sol[...].reshape(planes * rows, LANES), spread)
        dup[...] = every.reshape(planes, rows, 2 * LANES)

        z_low, z_high = both(gz, "gz", counts[0], slice(9 * rows, 9 * rows + nx))
        x_low, x_high = both(gx, "gx", counts[1], slice(3 * planes, 3 * planes + nz + 1))
        half, cut = nx // 2, fold_row(rows)
        y_row_low, y_row_high = both(gy, "gy", counts[2], slice(cut - 8, cut - 7))
        y_packs = both(gy, "gy", counts[2], slice(cut, cut + half))
        lane_h = lane_ids(half)

        def unfold(pack):
            first = jnp.where(lane_h < nz, pack, shift_lanes(pack, -5 * nz))
            second = shift_lanes(pack, -5 * nz - 1)
            second = jnp.where(lane_h < nz, shift_lanes(pack, -3 * nz), second)
            return jnp.concatenate([first, second], axis=0)

        y_low, y_high = [unfold(pack) for pack in y_packs]
        y_pack = y_packs[1]
        lane = lane_ids(nx)
        row = row_ids(nx)
        base = 5 * planes

        def spread_around(z):
            c, odd = z // 2, z % 2
            here = dup[c, :, :LANES]
            same = 3.0 * here + dup[c, :, LANES:]
            same += dup[(c + 1 if odd else c - 1) % planes, :, :LANES]
            slot = z % 2
            inter[slot, pl.ds(0, cx, 2), :] = (same + shift_rows(here, 1))[:cx, :]
            inter[slot, pl.ds(1, cx, 2), :] = (same + shift_rows(here, -1))[:cx, :]
            return inter[slot]

        def nodal(z):
            around = spread_around(z) + jnp.where(row == 0, x_low[z : z + 1, :], 0.0)
            around += jnp.where(row == nx - 1, x_high[z : z + 1, :], 0.0)
            around += jnp.where(lane == 0, shift_lanes(y_low, -z), 0.0)
            around += jnp.where(lane == LANES - 1, shift_lanes(y_high, -z - 1), 0.0)
            if z == nz:
                value = tz[3 * nx : 4 * nx, :] + tz[4 * nx :, :] * (around + fg[nz - 1])
                return from_above("gz", counts[0], value)
            if z == 0:
                around += z_low
            if z == nz - 1:
                around += z_high
            return part[z] + inv[z] * around

        here = dup[:cz, cx, :LANES]
        same = 3.0 * here + dup[:cz, cx, LANES:] + dup[:cz, cx - 1, :LANES]
        small[pl.ds(0, cz, 2), :] = same + jnp.concatenate(
            [dup[planes - 1, cx : cx + 1, :LANES], here[: cz - 1]], axis=0
        )
        small[pl.ds(1, cz, 2), :] = same + dup[1 : cz + 1, cx, :LANES]
        for z in range(nz):
            left = shift_lanes(y_row_low, -(base + z))
            right = shift_lanes(y_row_high, -(base + z) - 1)
            value = jnp.where(lane1 == 0, left, 0.0)
            lines[z : z + 1, :] = jnp.where(lane1 == LANES - 1, right, value)
        x_value = tx[3 * nz : 4 * nz, :] + tx[4 * nz :, :] * (
            fg[:, nx - 1, :] + small[...] + lines[...]
        )
        x_value = from_above("gx", counts[1], x_value)

        lane_c = lane_ids(rows)
        even = jnp.zeros((rows, LANES), F32)
        odd = jnp.zeros((rows, LANES), F32)
        for z in range(nz):
            c = z // 2
            here = sol[c]
            same = 3.0 * here + shift_lanes(here, 1) + sol[(c + 1 if z % 2 else c - 1) % planes]
            even = jnp.where(lane_c == z, shift_lanes(same + shift_rows(here, 1), z - cy), even)
            odd = jnp.where(lane_c == z, shift_lanes(same + shift_rows(here, -1), z - cy), odd)
        inter[0, pl.ds(0, cx, 2), :] = even[:cx, :]
        inter[0, pl.ds(1, cx, 2), :] = odd[:cx, :]
        y_base = jnp.concatenate(
            [shift_lanes(y_pack, -nz), shift_lanes(y_pack, -4 * nz)], axis=0
        )
        y_inverse = jnp.concatenate(
            [shift_lanes(y_pack, -2 * nz), shift_lanes(y_pack, -5 * nz)], axis=0
        )
        y_value = y_base + y_inverse * (early[...] + inter[0])
        y_value = from_above("gy", counts[2], y_value)

        def copy(block):
            at = pl.ds(block * step, step)
            return pltpu.make_async_copy(buf.at[:, at], out.at[:, at], sem.at[block])

        value = nodal(0)
        for z in range(nz):
            after = nodal(z + 1)
            steps = [after, jnp.where(row == nx - 1, x_value[z : z + 1, :], shift_rows(value, -1))]
            steps.append(
                jnp.where(lane == LANES - 1, shift_lanes(y_value, -z - 1), shift_lanes(value, -1))
            )
            for k in range(3):
                buf[k, z] = smooth[k, z] + (steps[k] - value)
            if z % step == step - 1:
                copy(z // step).start()
            value = after
        for block in range(nz // step):
            copy(block).wait()

    return call(
        body,
        [smooth.shape],
        scratch=[
            (planes, rows, LANES),
            (planes, rows, 2 * LANES),
            (2, nx, LANES),
            (nz, LANES),
            (nz, LANES),
            smooth.shape,
            pltpu.SemaphoreType.DMA((nz // step,)),
        ],
        far_out=True,
        in_specs=vmem(10 + gots),
        out_specs=[pl.BlockSpec(memory_space=pltpu.HBM)],
    )(sums, v1, v2, fg, *mid, smooth, early, tail_z, tail_x, *got_z, *got_x, *got_y)[0]


def local(residual, edge_diag, node_shift, coarse_shift):
    axes = ("gz", "gx", "gy")
    counts = tuple(lax.axis_size(a) for a in axes)
    devices = counts[0] * counts[1] * counts[2]
    part, *faces, scaled, inverses = edge_stage(residual, edge_diag)
    up_z, up_x, up_y, low_z, low_x, low_y = faces
    below = []
    for value, axis in ((up_z, "gz"), (up_x, "gx"), (up_y, "gy")):
        below.append(ring(value, axis, 1))
    tail_y = ring(low_y, "gy", -1)
    fg, rhs, xb, yb, w, *send = nodal_stage(part, node_shift, coarse_shift, *below, counts[0])
    got_z = swap(send, "gz")
    *mid, tail_z = part_stage(fg, node_shift, low_z)
    columns = y_columns(fg, node_shift)
    after = (mid[1], columns[0])
    rhs, w, *send = x_stage(got_z, rhs, xb, yb, w, fg, after, counts[0], counts[1])
    got_x = swap(send, "gx", ("gx", "gz"))
    tail_x = x_tail(got_z, fg, node_shift, low_x, w, counts[0])
    *early, last = y_early(got_z, columns, w, fg.shape[0], counts[0])
    early = (*early, columns[3], tail_x)
    tail_z = ring(tail_z, "gz", -1)
    tail_x = ring(tail_x, "gx", -1)
    rhs, w, *send = y_stage(got_x, rhs, w, early, counts[1], counts[2])
    got_y = swap(send, "gy", ("gy", "gz"))
    smooth = smooth_stage(scaled, inverses, below, tail_z, tail_x, tail_y, w, counts)
    v1, v2, sums = coarse_stage(got_y, rhs, w, (smooth,), counts[2], devices)
    sums = lax.all_to_all(sums, ("gx", "gy", "gz"), 0, 0)
    return final_stage(
        sums, v1, v2, fg, mid, smooth, last, tail_z, tail_x, got_z, got_x, got_y, counts
    )


def solution(mesh):
    placed = (
        P(None, "gz", "gx", "gy"),
        P(None, "gz", "gx", "gy"),
        P("gz", "gx", "gy"),
        P("gz", "gx", "gy"),
    )

    return jax.shard_map(
        local, mesh=mesh, in_specs=placed, out_specs=P(None, "gz", "gx", "gy"), check_vma=False
    )
```

```python
import itertools

import jax
import jax.numpy as jnp
from jax import lax
from jax.experimental import pallas as pl
from jax.experimental.pallas import tpu as pltpu
from jax.sharding import PartitionSpec as P


F32 = jnp.float32
LANES = 128


def lane_ids(rows):
    return lax.broadcasted_iota(jnp.int32, (rows, LANES), 1)


def row_ids(rows):
    return lax.broadcasted_iota(jnp.int32, (rows, LANES), 0)


def shift_lanes(value, amount):
    return pltpu.roll(value, amount % LANES, 1)


def shift_rows(value, amount):
    return pltpu.roll(value, amount % value.shape[0], 0)


def low_of(axis, size, first, second):
    place = lax.axis_index(axis)
    odd = place % 2 == 1
    zero = jnp.zeros_like(first)
    if second is None:
        return jnp.where(odd, first, zero)
    return jnp.where(odd, first, jnp.where(place > 0, second, zero))


def high_of(axis, size, first, second):
    place = lax.axis_index(axis)
    even = place % 2 == 0
    zero = jnp.zeros_like(first)
    if second is None:
        return jnp.where(even, first, zero)
    return jnp.where(even, first, jnp.where(place < size - 1, second, zero))


def from_below(axis, value):
    return jnp.where(lax.axis_index(axis) > 0, value, jnp.zeros_like(value))


def from_above(axis, size, value):
    return jnp.where(lax.axis_index(axis) < size - 1, value, jnp.zeros_like(value))


def ring(value, axis, step):
    size = lax.axis_size(axis)
    return lax.ppermute(value, axis, [(i, (i + step) % size) for i in range(size)])


def swap(values, axis, names=None):
    size = lax.axis_size(axis)
    out = [lax.ppermute(values[0], axis, [(i, i ^ 1) for i in range(size)])]
    if len(values) == 1:
        return out
    odd = [(i + 1) % size if i % 2 else (i - 1) % size for i in range(size)]
    if names is None:
        out.append(lax.ppermute(values[1], axis, list(enumerate(odd))))
        return out
    main = names.index(axis)
    pairs = []
    sizes = [lax.axis_size(name) for name in names]
    for at in itertools.product(*(range(n) for n in sizes)):
        to = list(at)
        if at[main] in (0, size - 1):
            to[1 - main] ^= 1
        else:
            to[main] = odd[at[main]]
        pairs.append(tuple(p[0] * sizes[1] + p[1] for p in (at, to)))
    out.append(lax.ppermute(values[1], names, pairs))
    return out


def write_sides(axis, refs, up, down):
    even = lax.axis_index(axis) % 2 == 0

    @pl.when(even)
    def _():
        up(refs[0])
        if len(refs) > 1:
            down(refs[1])

    @pl.when(jnp.logical_not(even))
    def _():
        down(refs[0])
        if len(refs) > 1:
            up(refs[1])


def call(body, outs, scratch=(), far=(), far_out=False, **kwargs):
    kind = jax.ShapeDtypeStruct if far_out else pltpu.VMEM
    run = pl.pallas_call(
        body,
        out_shape=[kind(shape, F32) for shape in outs],
        scratch_shapes=[pltpu.VMEM(s, F32) if isinstance(s, tuple) else s for s in scratch],
        compiler_params=pltpu.CompilerParams(vmem_limit_bytes=12 * 2**20),
        **kwargs,
    )

    def apply(*args):
        spaces = [pltpu.HBM if i in far else pltpu.VMEM for i in range(len(args))]
        return run(
            *(
                pltpu.with_memory_space_constraint(a, space)
                for a, space in zip(args, spaces)
            )
        )

    return apply


def vmem(count):
    return [pl.BlockSpec(memory_space=pltpu.VMEM)] * count


def edge_stage(residual, edge_diag):
    _, nz, nx, ny = residual.shape
    step = 4
    steps = nz // step

    def body(res, diag, part, up_z, up_x, up_y, low_z, low_x, low_y, scaled, inv, near, sems):
        lane = lane_ids(nx)
        row = row_ids(nx)

        def copies(block):
            at = pl.ds(block * step, step)
            return [
                pltpu.make_async_copy(source.at[:, at], target.at[:, at], sems.at[i, block])
                for i, (source, target) in enumerate(((res, near), (diag, inv)))
            ]

        for block in range(steps):
            for copy in copies(block):
                copy.start()
        before = jnp.zeros((nx, ny), F32)
        high = jnp.zeros((nx, LANES), F32)
        low = jnp.zeros((nx, LANES), F32)
        for z in range(nz):
            if z % step == 0:
                for copy in copies(z // step):
                    copy.wait()
            s = []
            for k in range(3):
                inverse = 1.0 / inv[k, z]
                inv[k, z] = inverse
                s.append(near[k, z] * inverse)
                scaled[k, z] = s[k]
            total = before - s[0]
            total += jnp.where(row == 0, 0.0, shift_rows(s[1], 1)) - s[1]
            total += jnp.where(lane == 0, 0.0, shift_lanes(s[2], 1)) - s[2]
            part[z] = total
            before = s[0]
            for k in range(3):
                spot = k * nz + z
                up_x[spot : spot + 1, :] = s[k][nx - 1 :, :]
                low_x[spot : spot + 1, :] = s[k][:1, :]
                high = jnp.where(lane == 2 * spot + 1, shift_lanes(s[k], 2 * spot + 2), high)
                low = jnp.where(lane == 2 * spot, shift_lanes(s[k], 2 * spot), low)
                if z == 0:
                    low_z[k] = s[k]
                if z == nz - 1:
                    up_z[k] = s[k]
        up_y[...] = high
        low_y[...] = low

    faces = [(3, nx, ny), (3 * nz, ny), (nx, LANES)] * 2
    return call(
        body,
        [(nz, nx, ny)] + faces + [residual.shape] * 2,
        scratch=[residual.shape, pltpu.SemaphoreType.DMA((2, steps))],
        far=(0, 1),
        in_specs=[pl.BlockSpec(memory_space=pltpu.HBM)] * 2,
        out_specs=vmem(9),
    )(residual, edge_diag)


def select_sum(values, chosen):
    first = values.astype(jnp.bfloat16)
    left = values - first.astype(F32)
    second = left.astype(jnp.bfloat16)
    third = (left - second.astype(F32)).astype(jnp.bfloat16)
    chosen = chosen.astype(jnp.bfloat16)
    both = jnp.concatenate([first, second], axis=1)
    total = jnp.dot(both, jnp.concatenate([chosen, chosen], axis=0), preferred_element_type=F32)
    return total + jnp.dot(third, chosen, preferred_element_type=F32)


def plane(values, row_count):
    return jnp.concatenate([values, jnp.zeros((row_count - values.shape[0], LANES), F32)], axis=0)


def nodal_stage(part, node_shift, coarse_shift, got_z, got_x, got_y, z_count):
    nz, nx, ny = part.shape
    cz, cx, cy = nz // 2, nx // 2, ny // 2
    rows = cx + 8
    sends = 1 if z_count == 2 else 2

    def body(part, shift, coarse, gz, gx, gy, fg, rhs, xb, yb, w, *rest):
        out, (pair, stack, s_, xl_, yl_, zl_, zh_) = rest[:sends], rest[sends:]
        lane = lane_ids(nx)
        row = row_ids(nx)
        lane_c = lane_ids(rows)
        row_c = row_ids(rows)
        below_z = from_below("gz", gz[0])
        below_y = from_below("gy", gy[...])
        fine = lax.broadcasted_iota(jnp.int32, (ny, 2 * LANES), 0)
        coarse_lane = lax.broadcasted_iota(jnp.int32, (ny, 2 * LANES), 1)
        miss = jnp.where(
            coarse_lane < LANES, fine // 2 - coarse_lane, fine - 2 * (coarse_lane - LANES)
        )
        gather = jnp.where(miss == 0, 1.0, 0.0)
        for c in range(cz):
            both = []
            for z in (2 * c, 2 * c + 1):
                total = part[z]
                if z == 0:
                    total += below_z
                total += jnp.where(row == 0, from_below("gx", gx[nz + z : nz + z + 1, :]), 0.0)
                total += jnp.where(lane == 0, shift_lanes(below_y, -(4 * nz + 2 * z + 1)), 0.0)
                guess = total / (6.0 + shift[z])
                fg[z] = guess
                both.append(guess)
            pair[c % 2] = both[0] + both[1]
            low = pair[c % 2, pl.ds(0, cx, 2), :]
            high = pair[c % 2, pl.ds(1, cx, 2), :]
            first = fg[2 * c, pl.ds(0, cx, 2), :] + fg[2 * c, pl.ds(1, cx, 2), :]
            stack[c, :cx, :] = low + high
            stack[c, cx : 2 * cx, :] = low
            stack[c, 2 * cx :, :] = first
        every = select_sum(stack[...].reshape(3 * cx * cz, LANES), gather)
        for c in range(cz):
            sums = every[3 * cx * c : 3 * cx * (c + 1)]
            s = sums[:cx, :LANES]
            z_low = sums[2 * cx :, :LANES]
            s_[c] = plane(s, rows)
            yl_[c] = plane(sums[:cx, LANES:], rows)
            xl_[c] = plane(sums[cx : 2 * cx, :LANES], rows)
            zl_[c] = plane(z_low, rows)
            zh_[c] = plane(s - z_low, rows)
            w[c] = jnp.zeros((rows, LANES), F32)
            w[c, :cx, :cy] = 1.0 / (6.0 + coarse[c])
        for c in range(cz):
            s, x_low, y_low = s_[c], xl_[c], yl_[c]
            x_high = s - x_low
            y_high = s - y_low
            total = 3.0 * s
            total += shift_rows(x_low, -1) + shift_rows(x_high, 1)
            total += shift_lanes(y_low, -1) + shift_lanes(y_high, 1)
            if c > 0:
                total += zh_[c - 1]
            if c < cz - 1:
                total += zl_[c + 1]
            rhs[c] = total
            xb[c] = jnp.where(row_c < cx // 2, x_low, x_high)
            yb[c] = jnp.where(lane_c < cy // 2, y_low, y_high)
        rhs[cz] = zh_[cz - 1]
        rhs[cz + 1] = jnp.zeros((rows, LANES), F32)
        rhs[cz + 2] = jnp.zeros((rows, LANES), F32)
        rhs[cz + 3] = zl_[0]

        def fill(ref, near, far, half, face):
            planes = [rhs[near], rhs[far], w[near], w[far], half]
            planes += [xb[near], xb[far], yb[near], yb[far]]
            for i, value in enumerate(planes):
                ref[i * rows : (i + 1) * rows, :] = value
            ref[9 * rows : 9 * rows + nx, :] = face

        def up(ref):
            fill(ref, cz - 1, cz - 2, zh_[cz - 1], fg[nz - 1])

        def down(ref):
            fill(ref, 0, 1, zl_[0], fg[0])

        write_sides("gz", out, up, down)

    coarse = (cz, rows, LANES)
    send = (9 * rows + nx, LANES)
    return call(
        body,
        [(nz, nx, ny), (cz + 4, rows, LANES), coarse, coarse, coarse] + [send] * sends,
        scratch=[(2, nx, ny), (cz, 3 * cx, LANES), coarse, coarse, coarse, coarse, coarse],
        in_specs=vmem(6),
        out_specs=vmem(5 + sends),
    )(part, node_shift, coarse_shift, got_z, got_x, got_y)


def x_stage(got, rhs, xb, yb, w, fg, after, z_count, x_count):
    planes, rows, _ = rhs.shape
    cz, cx = planes - 4, rows - 8
    nz, nx, ny = fg.shape
    cy = ny // 2
    sends = 1 if x_count == 2 else 2
    gots = len(got)
    size = -(-(3 * planes + nz + 1) // 8) * 8

    def body(*refs):
        got = refs[:gots]
        rhs, xb, yb, w, fg, _, _, rhs2, w2 = refs[gots : gots + 9]
        out, (xb2, yb2) = refs[gots + 9 : gots + 9 + sends], refs[gots + 9 + sends :]

        def take_at(pick, at):
            values = [ref[at, :] for ref in got]
            return pick("gz", z_count, values[0], values[1] if gots > 1 else None)

        def take(pick, i):
            return take_at(pick, slice(i * rows, (i + 1) * rows))

        for c in range(1, cz - 1):
            rhs2[c] = rhs[c]
        rhs2[0] = rhs[0] + take(low_of, 4)
        rhs2[cz - 1] = rhs[cz - 1] + take(high_of, 4)
        rhs2[cz] = rhs[cz] + take(high_of, 0)
        rhs2[cz + 1] = take(high_of, 1)
        rhs2[cz + 2] = take(low_of, 1)
        rhs2[cz + 3] = rhs[cz + 3] + take(low_of, 0)
        for here, there, i in ((w, w2, 2), (xb, xb2, 5), (yb, yb2, 7)):
            for c in range(cz):
                there[c] = here[c]
            there[cz] = take(high_of, i)
            there[cz + 1] = take(high_of, i + 1)
            there[cz + 2] = take(low_of, i + 1)
            there[cz + 3] = take(low_of, i)

        lane = lane_ids(planes)

        def fill(ref, near, far, fine):
            halves = lane < cy
            first = jnp.where(halves, rhs2[:, near, :], shift_lanes(rhs2[:, far, :], cy))
            second = jnp.where(halves, w2[:, near, :], shift_lanes(w2[:, far, :], cy))
            edge = yb2[:, far, :]
            third = jnp.where(halves, xb2[:, near, :], shift_lanes(yb2[:, near, :], cy))
            third = jnp.where(lane == cy + 1, shift_lanes(edge, cy + 1), third)
            third = jnp.where(lane == LANES - 2, shift_lanes(edge, cy - 1), third)
            for i, value in enumerate((first, second, third)):
                ref[i * planes : (i + 1) * planes, :] = value
            ref[3 * planes : 3 * planes + nz, :] = fg[:, fine, :]
            at = 9 * rows + fine
            last = 3 * planes + nz
            ref[last : last + 1, :] = take_at(high_of, slice(at, at + 1))
            ref[last + 1 :, :] = jnp.zeros((size - last - 1, LANES), F32)

        def up(ref):
            fill(ref, cx - 1, cx - 2, nx - 1)

        def down(ref):
            fill(ref, 0, 1, 0)

        write_sides("gx", out, up, down)

    whole = (planes, rows, LANES)
    return call(
        body,
        [whole, whole] + [(size, LANES)] * sends,
        scratch=[whole, whole],
        in_specs=vmem(gots + 7),
        out_specs=vmem(2 + sends),
    )(*got, rhs, xb, yb, w, fg, *after)


def x_tail(got, fg, node_shift, low_x, after, z_count):
    nz, nx, ny = fg.shape
    z_at = 9 * (nx // 2 + 8)
    gots = len(got)

    def body(*refs):
        got = refs[:gots]
        fg, shift, low_x, _, out = refs[gots:]
        lane = lane_ids(nz)
        row = row_ids(nz)

        def z_row(pick):
            values = [ref[z_at : z_at + 1, :] for ref in got]
            return pick("gz", z_count, values[0], values[1] if gots > 1 else None)

        here = fg[:, 0, :]
        around = fg[:, 1, :] + jnp.where(row == 0, z_row(low_of), shift_rows(here, 1))
        around += jnp.where(row == nz - 1, z_row(high_of), shift_rows(here, -1))
        around += jnp.where(lane == 0, 0.0, shift_lanes(here, 1))
        around += jnp.where(lane == ny - 1, 0.0, shift_lanes(here, -1))
        inverse = 1.0 / (6.0 + shift[:, 0, :])
        out[: 3 * nz, :] = low_x[...]
        out[3 * nz : 4 * nz, :] = here + inverse * around
        out[4 * nz :, :] = inverse

    return call(
        body, [(5 * nz, LANES)], in_specs=vmem(gots + 4), out_specs=vmem(1)
    )(*got, fg, node_shift, low_x, after)[0]


def part_stage(fg, node_shift, low_z):
    nz, nx, ny = fg.shape

    def body(fg, shift, low_z, part, inv, tail):
        lane = lane_ids(nx)
        row = row_ids(nx)
        zero = jnp.zeros((nx, ny), F32)
        for z in range(nz):
            guess = fg[z]
            inner = fg[z + 1] if z < nz - 1 else zero
            inner += jnp.where(row == 0, 0.0, shift_rows(guess, 1))
            inner += jnp.where(row == nx - 1, 0.0, shift_rows(guess, -1))
            inner += jnp.where(lane == 0, 0.0, shift_lanes(guess, 1))
            inner += jnp.where(lane == ny - 1, 0.0, shift_lanes(guess, -1))
            inverse = 1.0 / (6.0 + shift[z])
            inv[z] = inverse
            part[z] = guess + inverse * (inner + (fg[z - 1] if z > 0 else zero))
            if z == 0:
                for k in range(3):
                    tail[k * nx : (k + 1) * nx, :] = low_z[k]
                tail[3 * nx : 4 * nx, :] = guess + inverse * inner
                tail[4 * nx :, :] = inverse

    return call(
        body, [fg.shape, fg.shape, (5 * nx, LANES)], in_specs=vmem(3), out_specs=vmem(3)
    )(fg, node_shift, low_z)


def fold_row(rows):
    return (rows + 8) // 16 * 8


def line(source, lane, fine, at):
    acc = jnp.zeros(lane.shape, F32)
    for z in range(source.shape[0]):
        moved = jnp.broadcast_to(source[z : z + 1, :], lane.shape)
        acc = jnp.where(lane == at + z, shift_lanes(moved, at + z - fine), acc)
    return acc


def y_stage(got, rhs, w, early, x_count, y_count):
    planes, rows, _ = rhs.shape
    cx = rows - 8
    nx, cy = 2 * cx, LANES // 2
    nz, half, cut = 2 * (planes - 4), nx // 2, fold_row(rows)
    sends = 1 if y_count == 2 else 2
    gots = len(got)

    def body(*refs):
        got = refs[:gots]
        rhs, w, up_, down_, part, inv, _, rhs3, w3 = refs[gots : gots + 9]
        rest = refs[gots + 9 :]
        out = rest
        lane_p = lane_ids(planes)

        def take_at(pick, at):
            values = [ref[at, :] for ref in got]
            return pick("gx", x_count, values[0], values[1] if gots > 1 else None)

        def take(pick, i):
            return take_at(pick, slice(i * planes, (i + 1) * planes))

        for c in range(planes):
            w3[c] = w[c]
            rhs3[c] = rhs[c]
        for pick, near, far, edge in ((high_of, cx, cx + 1, cx - 1), (low_of, rows - 1, rows - 2, 0)):
            first, second, third = take(pick, 0), take(pick, 1), take(pick, 2)
            other = shift_lanes(third, -cy)
            one = jnp.where((lane_p == 0) | (lane_p == cy - 1), other, 0.0)
            two = jnp.where(lane_p == 0, shift_lanes(third, -cy - 1), 0.0)
            two = jnp.where(lane_p == cy - 1, shift_lanes(third, 1 - cy), two)
            for at, value, ends in ((near, first, one), (far, shift_lanes(first, -cy), two)):
                value = jnp.where(lane_p < cy, value, 0.0)
                value += jnp.where(lane_p == cy, shift_lanes(ends, 1), 0.0)
                value += jnp.where(lane_p == LANES - 1, shift_lanes(ends, -1), 0.0)
                rhs3[:, at, :] += value
            w3[:, near, :] = jnp.where(lane_p < cy, second, 0.0)
            w3[:, far, :] = jnp.where(lane_p < cy, shift_lanes(second, -cy), 0.0)
            rhs3[:, edge, :] += jnp.where(lane_p < cy, third, 0.0)

        lane_c = lane_ids(rows)
        lane8 = lane_ids(8)
        base = 5 * planes
        x_face = slice(3 * planes, 3 * planes + nz)
        x_high = take_at(high_of, x_face)

        def fill(ref, first, fine, early):
            acc = jnp.zeros((rows, LANES), F32)
            inner = first if first > 0 else 0
            for z in range(planes):
                for field, width, at, source in (
                    (rhs3, 3, 3 * z, first),
                    (w3, 2, 3 * planes + 2 * z, inner),
                ):
                    there = (lane_c >= at) & (lane_c < at + width)
                    acc = jnp.where(there, shift_lanes(field[z], at - source), acc)
            ref[:cut, :] = acc[:cut]
            ref[: rows - cut, :] += shift_lanes(acc[cut:], base)
            ref[cut - 8 : cut, :] += line(x_high, lane8, fine, base)
            ref[cut:, :] = early

        def up(ref):
            fill(ref, cy - 2, 2 * cy - 1, up_[...])

        def down(ref):
            row = row_ids(nx)
            ends = jnp.where(row == 0, line(take_at(low_of, x_face), lane8, 0, 0)[:1, :], 0.0)
            ends += jnp.where(row == nx - 1, line(x_high, lane8, 0, 0)[:1, :], 0.0)
            inverse = inv[...]
            value = part[...] + inverse * ends
            packed = down_[...]
            for i, source in (
                (1, value[:half]),
                (2, inverse[:half]),
                (4, value[half:]),
                (5, inverse[half:]),
            ):
                there = lane_ids(half) // nz == i
                packed = jnp.where(there, shift_lanes(source, i * nz), packed)
            fill(ref, -1, 0, packed)

        write_sides("gy", out, up, down)

    whole = (planes, rows, LANES)
    return call(
        body,
        [whole, whole] + [(cut + half, LANES)] * sends,
        in_specs=vmem(gots + 7),
        out_specs=vmem(2 + sends),
    )(*got, rhs, w, *early)


def y_columns(fg, node_shift):
    nz, nx, _ = fg.shape

    def body(fg, shift, here_, inner_, high_, inv):
        lane = lane_ids(nx)
        zero = jnp.zeros((nx, LANES), F32)
        here, inner, high, inverse = zero, zero, zero, zero + 1.0
        for z in range(nz):
            guess = fg[z]
            here = jnp.where(lane == z, shift_lanes(guess, z), here)
            inner = jnp.where(lane == z, shift_lanes(guess, z - 1), inner)
            high = jnp.where(lane == z, shift_lanes(guess, z + 1), high)
            inverse = jnp.where(lane == z, shift_lanes(6.0 + shift[z], z), inverse)
        here_[...] = here
        inner_[...] = inner
        high_[...] = high
        inv[...] = 1.0 / inverse

    return call(body, [(nx, LANES)] * 4, in_specs=vmem(2), out_specs=vmem(4))(fg, node_shift)


def y_early(got_z, columns, after, nz, z_count):
    nx = columns[0].shape[0]
    z_at = 9 * (nx // 2 + 8)
    n_z = len(got_z)

    def body(*refs):
        gz = refs[:n_z]
        here_, inner, high_, inv, _, up, down, part, last = refs[n_z:]
        lane = lane_ids(nx)
        row = row_ids(nx)

        def side(pick):
            values = [ref[z_at : z_at + nx, :] for ref in gz]
            return pick("gz", z_count, values[0], values[1] if n_z > 1 else None)

        above = side(high_of)
        here = jnp.where(lane == nz, shift_lanes(above, nz), here_[...])
        here = jnp.where(lane == LANES - 1, shift_lanes(side(low_of), -1), here)
        high = jnp.where(lane == nz, shift_lanes(above, nz + 1), high_[...])
        inverse = inv[...]
        around = inner[...] + shift_lanes(here, 1) + shift_lanes(here, -1)
        around += jnp.where(row == 0, 0.0, shift_rows(here, 1))
        around += jnp.where(row == nx - 1, 0.0, shift_rows(here, -1))
        last[...] = high
        half = nx // 2
        lane_h = lane_ids(half)

        def fold(value):
            first, second = value[:half], value[half:]
            block = jnp.where(lane_h < nz, first, 0.0)
            there = (lane_h >= 3 * nz) & (lane_h < 4 * nz)
            block = jnp.where(there, shift_lanes(second, 3 * nz), block)
            block = jnp.where(lane_h == 6 * nz, shift_lanes(first, 5 * nz), block)
            return jnp.where(lane_h == 6 * nz + 1, shift_lanes(second, 5 * nz + 1), block)

        up[...] = fold(high)
        down[...] = fold(here)
        part[...] = here + inverse * around

    return call(
        body, [(nx // 2, LANES)] * 2 + [(nx, LANES)] * 2, in_specs=vmem(n_z + 5), out_specs=vmem(4)
    )(*got_z, *columns, after)


def coarse_stage(got, rhs, w, after, y_count, devices):
    planes, rows, _ = rhs.shape
    cz, cx = planes - 4, rows - 8
    cy = LANES // 2
    gots = len(got)

    def body(*refs):
        got = refs[:gots]
        rhs, w, _, v1, v2, sums, tot, inv_, image_ = refs[gots:]
        cut = fold_row(rows)
        tail = [shift_lanes(ref[: rows - cut, :], -5 * planes) for ref in got]
        values = [jnp.concatenate([ref[:cut, :], t], axis=0) for ref, t in zip(got, tail)]
        second = values[1] if gots > 1 else None
        low = low_of("gy", y_count, values[0], second)
        high = high_of("gy", y_count, values[0], second)
        lane = lane_ids(rows)
        above = (lane >= cy - 1) & (lane < cy + 2)
        below = (lane >= LANES - 2) | (lane == 0)
        for z in range(planes):
            at = 3 * z
            right = jnp.where(below, shift_lanes(low, LANES - 2 - at), 0.0)
            right = rhs[z] + jnp.where(above, shift_lanes(high, cy - 1 - at), right)
            at = 3 * planes + 2 * z
            inv = jnp.where(lane >= LANES - 2, shift_lanes(low, LANES - 2 - at), w[z])
            inv = jnp.where((lane >= cy) & (lane < cy + 2), shift_lanes(high, cy - at), inv)
            inv_[z] = inv
            tot[z] = right
            v1[z] = right * inv

        def near(field, z):
            here = field[z]
            total = field[(z + 1) % planes] + field[(z - 1) % planes]
            total += shift_rows(here, 1) + shift_rows(here, -1)
            return total + shift_lanes(here, 1) + shift_lanes(here, -1)

        v2[cz + 1] = jnp.zeros((rows, LANES), F32)
        v2[cz + 2] = jnp.zeros((rows, LANES), F32)
        for z in list(range(cz + 1)) + [planes - 1]:
            image = tot[z] - near(v1, z)
            if z < cz:
                image_[z] = image
            v2[z] = image * inv_[z]
        parts = [jnp.zeros((cx, LANES), F32)] * 5
        for z in range(cz):
            first, second_, right, image = v1[z], v2[z], tot[z], image_[z]
            third = image - near(v2, z)
            terms = (first * right, second_ * right, first * image, second_ * image, second_ * third)
            parts = [a + b[:cx, :] for a, b in zip(parts, terms)]
        keep = lane_ids(1) < cy
        lines = [jnp.where(keep, jnp.sum(a, axis=0, keepdims=True), 0.0) for a in parts]
        tile = jnp.concatenate(lines + [jnp.zeros((3, LANES), F32)], axis=0)
        column = jnp.sum(tile, axis=1, keepdims=True)
        spread = jnp.where(lane_ids(8) == row_ids(8), column, 0.0)
        line = jnp.sum(spread, axis=0, keepdims=True)
        sums[...] = jnp.broadcast_to(line[None], (devices, 1, LANES))

    whole = (planes, rows, LANES)
    return call(
        body,
        [whole, whole, (devices, 1, LANES)],
        scratch=[whole, whole, whole],
        in_specs=vmem(gots + 3),
        out_specs=vmem(3),
    )(*got, rhs, w, *after)


def smooth_stage(scaled, inverses, below, tail_z, tail_x, tail_y, after, counts):
    _, nz, nx, _ = scaled.shape

    def body(*refs):
        s, inv, lz, lx, ly = refs[:5]
        tz, gx, ty, _, out = refs[5:]
        lane = lane_ids(nx)
        row = row_ids(nx)

        ends = from_below("gy", ly[...]) + from_above("gy", counts[2], ty[...])
        for k in range(3):
            z_low = from_below("gz", lz[k])
            z_high = from_above("gz", counts[0], tz[k * nx : (k + 1) * nx, :])
            x_low = from_below("gx", lx[k * nz : (k + 1) * nz, :])
            x_high = from_above("gx", counts[1], gx[k * nz : (k + 1) * nz, :])
            for z in range(nz):
                here = s[k, z]
                around = s[k, z - 1] if z > 0 else z_low
                around += s[k, z + 1] if z < nz - 1 else z_high
                around += jnp.where(row == 0, x_low[z : z + 1, :], shift_rows(here, 1))
                around += jnp.where(row == nx - 1, x_high[z : z + 1, :], shift_rows(here, -1))
                spot = k * nz + z
                end = shift_lanes(ends, LANES - 1 - 2 * spot)
                around += jnp.where(lane == 0, end, shift_lanes(here, 1))
                around += jnp.where(lane == LANES - 1, end, shift_lanes(here, -1))
                out[k, z] = here + around * inv[k, z]

    return call(
        body, [scaled.shape], in_specs=vmem(9), out_specs=vmem(1)
    )(scaled, inverses, *below, tail_z, tail_x, tail_y, after)[0]


def final_stage(sums, v1, v2, fg, mid, smooth, early, tail_z, tail_x, got_z, got_x, got_y, counts):
    planes, rows, _ = v1.shape
    cz, cx, cy = planes - 4, rows - 8, LANES // 2
    nz, nx, _ = fg.shape
    step = 2
    n_z, n_x, n_y = len(got_z), len(got_x), len(got_y)
    gots = n_z + n_x + n_y

    def body(*refs):
        sums, v1, v2, fg, part, inv, smooth, early, tz, tx = refs[:10]
        gz = refs[10 : 10 + n_z]
        gx = refs[10 + n_z : 10 + n_z + n_x]
        gy = refs[10 + n_z + n_x : 10 + gots]
        out, sol, dup, inter, small, lines, buf, sem = refs[10 + gots :]

        def one_side(pick, refs, axis, size, at):
            values = [ref[at, :] for ref in refs]
            return pick(axis, size, values[0], values[1] if len(values) > 1 else None)

        def both(refs, axis, size, at):
            return [one_side(pick, refs, axis, size, at) for pick in (low_of, high_of)]

        total = jnp.sum(sums[...], axis=0)
        lane1 = lane_ids(1)
        gone, gtwo, hone, hmix, htwo = [
            jnp.sum(jnp.where(lane1 == i, total, 0.0), axis=1, keepdims=True) for i in range(5)
        ]
        two = (gtwo - hmix * gone / hone) / (htwo - hmix * hmix / hone)
        one = (gone - hmix * two) / hone
        source = lax.broadcasted_iota(jnp.int32, (LANES, 2 * LANES), 0)
        target = lax.broadcasted_iota(jnp.int32, (LANES, 2 * LANES), 1)
        fine = target - LANES
        side = jnp.where(fine % 2 == 1, fine // 2 + 1, (fine // 2 + LANES - 1) % LANES)
        spread = jnp.where(jnp.where(target < LANES, target // 2, side) == source, 1.0, 0.0)
        for z in range(planes):
            sol[z] = one * v1[z] + two * v2[z]
        every = select_sum(sol[...].reshape(planes * rows, LANES), spread)
        dup[...] = every.reshape(planes, rows, 2 * LANES)

        z_low, z_high = both(gz, "gz", counts[0], slice(9 * rows, 9 * rows + nx))
        x_low, x_high = both(gx, "gx", counts[1], slice(3 * planes, 3 * planes + nz + 1))
        half, cut = nx // 2, fold_row(rows)
        y_row_low, y_row_high = both(gy, "gy", counts[2], slice(cut - 8, cut - 7))
        y_packs = both(gy, "gy", counts[2], slice(cut, cut + half))
        lane_h = lane_ids(half)

        def unfold(pack):
            first = jnp.where(lane_h < nz, pack, shift_lanes(pack, -5 * nz))
            second = shift_lanes(pack, -5 * nz - 1)
            second = jnp.where(lane_h < nz, shift_lanes(pack, -3 * nz), second)
            return jnp.concatenate([first, second], axis=0)

        y_low, y_high = [unfold(pack) for pack in y_packs]
        y_pack = y_packs[1]
        lane = lane_ids(nx)
        row = row_ids(nx)
        base = 5 * planes

        def spread_around(z):
            c, odd = z // 2, z % 2
            here = dup[c, :, :LANES]
            same = 3.0 * here + dup[c, :, LANES:]
            same += dup[(c + 1 if odd else c - 1) % planes, :, :LANES]
            slot = z % 2
            inter[slot, pl.ds(0, cx, 2), :] = (same + shift_rows(here, 1))[:cx, :]
            inter[slot, pl.ds(1, cx, 2), :] = (same + shift_rows(here, -1))[:cx, :]
            return inter[slot]

        def nodal(z):
            around = spread_around(z) + jnp.where(row == 0, x_low[z : z + 1, :], 0.0)
            around += jnp.where(row == nx - 1, x_high[z : z + 1, :], 0.0)
            around += jnp.where(lane == 0, shift_lanes(y_low, -z), 0.0)
            around += jnp.where(lane == LANES - 1, shift_lanes(y_high, -z - 1), 0.0)
            if z == nz:
                value = tz[3 * nx : 4 * nx, :] + tz[4 * nx :, :] * (around + fg[nz - 1])
                return from_above("gz", counts[0], value)
            if z == 0:
                around += z_low
            if z == nz - 1:
                around += z_high
            return part[z] + inv[z] * around

        here = dup[:cz, cx, :LANES]
        same = 3.0 * here + dup[:cz, cx, LANES:] + dup[:cz, cx - 1, :LANES]
        small[pl.ds(0, cz, 2), :] = same + jnp.concatenate(
            [dup[planes - 1, cx : cx + 1, :LANES], here[: cz - 1]], axis=0
        )
        small[pl.ds(1, cz, 2), :] = same + dup[1 : cz + 1, cx, :LANES]
        for z in range(nz):
            left = shift_lanes(y_row_low, -(base + z))
            right = shift_lanes(y_row_high, -(base + z) - 1)
            value = jnp.where(lane1 == 0, left, 0.0)
            lines[z : z + 1, :] = jnp.where(lane1 == LANES - 1, right, value)
        x_value = tx[3 * nz : 4 * nz, :] + tx[4 * nz :, :] * (
            fg[:, nx - 1, :] + small[...] + lines[...]
        )
        x_value = from_above("gx", counts[1], x_value)

        lane_c = lane_ids(rows)
        middle = jnp.zeros((rows, LANES), F32)
        inward = jnp.zeros((rows, LANES), F32)
        beside = jnp.zeros((rows, LANES), F32)
        for z in range(nz):
            c = z // 2
            here = sol[c]
            same = 3.0 * here + sol[(c + 1 if z % 2 else c - 1) % planes]
            middle = jnp.where(lane_c == z, shift_lanes(same, z - cy), middle)
            inward = jnp.where(lane_c == z, shift_lanes(here, z - cy + 1), inward)
            beside = jnp.where(lane_c == z, shift_lanes(here, z - cy), beside)
        middle += inward
        even = middle + shift_rows(beside, 1)
        odd = middle + shift_rows(beside, -1)
        inter[0, pl.ds(0, cx, 2), :] = even[:cx, :]
        inter[0, pl.ds(1, cx, 2), :] = odd[:cx, :]
        y_base = jnp.concatenate(
            [shift_lanes(y_pack, -nz), shift_lanes(y_pack, -4 * nz)], axis=0
        )
        y_inverse = jnp.concatenate(
            [shift_lanes(y_pack, -2 * nz), shift_lanes(y_pack, -5 * nz)], axis=0
        )
        y_value = y_base + y_inverse * (early[...] + inter[0])
        y_value = from_above("gy", counts[2], y_value)

        def copy(block):
            at = pl.ds(block * step, step)
            return pltpu.make_async_copy(buf.at[:, at], out.at[:, at], sem.at[block])

        value = nodal(0)
        for z in range(nz):
            after = nodal(z + 1)
            steps = [after, jnp.where(row == nx - 1, x_value[z : z + 1, :], shift_rows(value, -1))]
            steps.append(
                jnp.where(lane == LANES - 1, shift_lanes(y_value, -z - 1), shift_lanes(value, -1))
            )
            for k in range(3):
                buf[k, z] = smooth[k, z] + (steps[k] - value)
            if z % step == step - 1:
                copy(z // step).start()
            value = after
        for block in range(nz // step):
            copy(block).wait()

    return call(
        body,
        [smooth.shape],
        scratch=[
            (planes, rows, LANES),
            (planes, rows, 2 * LANES),
            (2, nx, LANES),
            (nz, LANES),
            (nz, LANES),
            smooth.shape,
            pltpu.SemaphoreType.DMA((nz // step,)),
        ],
        far_out=True,
        in_specs=vmem(10 + gots),
        out_specs=[pl.BlockSpec(memory_space=pltpu.HBM)],
    )(sums, v1, v2, fg, *mid, smooth, early, tail_z, tail_x, *got_z, *got_x, *got_y)[0]


def local(residual, edge_diag, node_shift, coarse_shift):
    axes = ("gz", "gx", "gy")
    counts = tuple(lax.axis_size(a) for a in axes)
    devices = counts[0] * counts[1] * counts[2]
    part, *faces, scaled, inverses = edge_stage(residual, edge_diag)
    up_z, up_x, up_y, low_z, low_x, low_y = faces
    below = []
    for value, axis in ((up_z, "gz"), (up_x, "gx"), (up_y, "gy")):
        below.append(ring(value, axis, 1))
    tail_y = ring(low_y, "gy", -1)
    fg, rhs, xb, yb, w, *send = nodal_stage(part, node_shift, coarse_shift, *below, counts[0])
    got_z = swap(send, "gz")
    *mid, tail_z = part_stage(fg, node_shift, low_z)
    columns = y_columns(fg, node_shift)
    after = (mid[1], columns[0])
    rhs, w, *send = x_stage(got_z, rhs, xb, yb, w, fg, after, counts[0], counts[1])
    got_x = swap(send, "gx", ("gx", "gz"))
    tail_x = x_tail(got_z, fg, node_shift, low_x, w, counts[0])
    *early, last = y_early(got_z, columns, w, fg.shape[0], counts[0])
    early = (*early, columns[3], tail_x)
    tail_z = ring(tail_z, "gz", -1)
    tail_x = ring(tail_x, "gx", -1)
    rhs, w, *send = y_stage(got_x, rhs, w, early, counts[1], counts[2])
    got_y = swap(send, "gy", ("gy", "gz"))
    smooth = smooth_stage(scaled, inverses, below, tail_z, tail_x, tail_y, w, counts)
    v1, v2, sums = coarse_stage(got_y, rhs, w, (smooth,), counts[2], devices)
    sums = lax.all_to_all(sums, ("gx", "gy", "gz"), 0, 0)
    return final_stage(
        sums, v1, v2, fg, mid, smooth, last, tail_z, tail_x, got_z, got_x, got_y, counts
    )


def solution(mesh):
    placed = (
        P(None, "gz", "gx", "gy"),
        P(None, "gz", "gx", "gy"),
        P("gz", "gx", "gy"),
        P("gz", "gx", "gy"),
    )

    return jax.shard_map(
        local, mesh=mesh, in_specs=placed, out_specs=P(None, "gz", "gx", "gy"), check_vma=False
    )
```

```python
import itertools

import jax
import jax.numpy as jnp
from jax import lax
from jax.experimental import pallas as pl
from jax.experimental.pallas import tpu as pltpu
from jax.sharding import PartitionSpec as P


F32 = jnp.float32
LANES = 128


def lane_ids(rows):
    return lax.broadcasted_iota(jnp.int32, (rows, LANES), 1)


def row_ids(rows):
    return lax.broadcasted_iota(jnp.int32, (rows, LANES), 0)


def shift_lanes(value, amount):
    return pltpu.roll(value, amount % LANES, 1)


def shift_rows(value, amount):
    return pltpu.roll(value, amount % value.shape[0], 0)


def low_of(axis, size, first, second):
    place = lax.axis_index(axis)
    odd = place % 2 == 1
    zero = jnp.zeros_like(first)
    if second is None:
        return jnp.where(odd, first, zero)
    return jnp.where(odd, first, jnp.where(place > 0, second, zero))


def high_of(axis, size, first, second):
    place = lax.axis_index(axis)
    even = place % 2 == 0
    zero = jnp.zeros_like(first)
    if second is None:
        return jnp.where(even, first, zero)
    return jnp.where(even, first, jnp.where(place < size - 1, second, zero))


def from_below(axis, value):
    return jnp.where(lax.axis_index(axis) > 0, value, jnp.zeros_like(value))


def from_above(axis, size, value):
    return jnp.where(lax.axis_index(axis) < size - 1, value, jnp.zeros_like(value))


def ring(value, axis, step):
    size = lax.axis_size(axis)
    return lax.ppermute(value, axis, [(i, (i + step) % size) for i in range(size)])


def swap(values, axis, names=None):
    size = lax.axis_size(axis)
    out = [lax.ppermute(values[0], axis, [(i, i ^ 1) for i in range(size)])]
    if len(values) == 1:
        return out
    odd = [(i + 1) % size if i % 2 else (i - 1) % size for i in range(size)]
    if names is None:
        out.append(lax.ppermute(values[1], axis, list(enumerate(odd))))
        return out
    main = names.index(axis)
    pairs = []
    sizes = [lax.axis_size(name) for name in names]
    for at in itertools.product(*(range(n) for n in sizes)):
        to = list(at)
        if at[main] in (0, size - 1):
            to[1 - main] ^= 1
        else:
            to[main] = odd[at[main]]
        pairs.append(tuple(p[0] * sizes[1] + p[1] for p in (at, to)))
    out.append(lax.ppermute(values[1], names, pairs))
    return out


def write_sides(axis, refs, up, down):
    even = lax.axis_index(axis) % 2 == 0

    @pl.when(even)
    def _():
        up(refs[0])
        if len(refs) > 1:
            down(refs[1])

    @pl.when(jnp.logical_not(even))
    def _():
        down(refs[0])
        if len(refs) > 1:
            up(refs[1])


def call(body, outs, scratch=(), far=(), far_out=False, **kwargs):
    kind = jax.ShapeDtypeStruct if far_out else pltpu.VMEM
    run = pl.pallas_call(
        body,
        out_shape=[kind(shape, F32) for shape in outs],
        scratch_shapes=[pltpu.VMEM(s, F32) if isinstance(s, tuple) else s for s in scratch],
        compiler_params=pltpu.CompilerParams(vmem_limit_bytes=12 * 2**20),
        **kwargs,
    )

    def apply(*args):
        spaces = [pltpu.HBM if i in far else pltpu.VMEM for i in range(len(args))]
        return run(
            *(
                pltpu.with_memory_space_constraint(a, space)
                for a, space in zip(args, spaces)
            )
        )

    return apply


def vmem(count):
    return [pl.BlockSpec(memory_space=pltpu.VMEM)] * count


def edge_stage(residual, edge_diag):
    _, nz, nx, ny = residual.shape
    step = 4
    steps = nz // step

    def body(res, diag, part, up_z, up_x, up_y, low_z, low_x, low_y, scaled, inv, near, sems):
        lane = lane_ids(nx)
        row = row_ids(nx)

        def copies(block):
            at = pl.ds(block * step, step)
            return [
                pltpu.make_async_copy(source.at[:, at], target.at[:, at], sems.at[i, block])
                for i, (source, target) in enumerate(((res, near), (diag, inv)))
            ]

        for block in range(steps):
            for copy in copies(block):
                copy.start()
        before = jnp.zeros((nx, ny), F32)
        high = jnp.zeros((nx, LANES), F32)
        low = jnp.zeros((nx, LANES), F32)
        for z in range(nz):
            if z % step == 0:
                for copy in copies(z // step):
                    copy.wait()
            s = []
            for k in range(3):
                inverse = 1.0 / inv[k, z]
                inv[k, z] = inverse
                s.append(near[k, z] * inverse)
                scaled[k, z] = s[k]
            total = before - s[0]
            total += jnp.where(row == 0, 0.0, shift_rows(s[1], 1)) - s[1]
            total += jnp.where(lane == 0, 0.0, shift_lanes(s[2], 1)) - s[2]
            part[z] = total
            before = s[0]
            for k in range(3):
                spot = k * nz + z
                up_x[spot : spot + 1, :] = s[k][nx - 1 :, :]
                low_x[spot : spot + 1, :] = s[k][:1, :]
                high = jnp.where(lane == 2 * spot + 1, shift_lanes(s[k], 2 * spot + 2), high)
                low = jnp.where(lane == 2 * spot, shift_lanes(s[k], 2 * spot), low)
                if z == 0:
                    low_z[k] = s[k]
                if z == nz - 1:
                    up_z[k] = s[k]
        up_y[...] = high
        low_y[...] = low

    faces = [(3, nx, ny), (3 * nz, ny), (nx, LANES)] * 2
    return call(
        body,
        [(nz, nx, ny)] + faces + [residual.shape] * 2,
        scratch=[residual.shape, pltpu.SemaphoreType.DMA((2, steps))],
        far=(0, 1),
        in_specs=[pl.BlockSpec(memory_space=pltpu.HBM)] * 2,
        out_specs=vmem(9),
    )(residual, edge_diag)


def select_sum(values, chosen):
    first = values.astype(jnp.bfloat16)
    left = values - first.astype(F32)
    second = left.astype(jnp.bfloat16)
    third = (left - second.astype(F32)).astype(jnp.bfloat16)
    chosen = chosen.astype(jnp.bfloat16)
    both = jnp.concatenate([first, second], axis=1)
    total = jnp.dot(both, jnp.concatenate([chosen, chosen], axis=0), preferred_element_type=F32)
    return total + jnp.dot(third, chosen, preferred_element_type=F32)


def plane(values, row_count):
    return jnp.concatenate([values, jnp.zeros((row_count - values.shape[0], LANES), F32)], axis=0)


def nodal_stage(part, node_shift, coarse_shift, got_z, got_x, got_y, z_count):
    nz, nx, ny = part.shape
    cz, cx, cy = nz // 2, nx // 2, ny // 2
    rows = cx + 8
    sends = 1 if z_count == 2 else 2

    def body(part, shift, coarse, gz, gx, gy, fg, rhs, xb, yb, w, *rest):
        out, (pair, stack, s_, xl_, yl_, zl_, zh_) = rest[:sends], rest[sends:]
        lane = lane_ids(nx)
        row = row_ids(nx)
        lane_c = lane_ids(rows)
        row_c = row_ids(rows)
        below_z = from_below("gz", gz[0])
        below_x = from_below("gx", gx[nz : 2 * nz, :])
        below_y = from_below("gy", gy[...])
        fine = lax.broadcasted_iota(jnp.int32, (ny, 2 * LANES), 0)
        coarse_lane = lax.broadcasted_iota(jnp.int32, (ny, 2 * LANES), 1)
        miss = jnp.where(
            coarse_lane < LANES, fine // 2 - coarse_lane, fine - 2 * (coarse_lane - LANES)
        )
        gather = jnp.where(miss == 0, 1.0, 0.0)
        for c in range(cz):
            both = []
            for z in (2 * c, 2 * c + 1):
                total = part[z]
                if z == 0:
                    total += below_z
                total += jnp.where(row == 0, below_x[z : z + 1, :], 0.0)
                total += jnp.where(lane == 0, shift_lanes(below_y, -(4 * nz + 2 * z + 1)), 0.0)
                guess = total / (6.0 + shift[z])
                fg[z] = guess
                both.append(guess)
            pair[c % 2] = both[0] + both[1]
            low = pair[c % 2, pl.ds(0, cx, 2), :]
            high = pair[c % 2, pl.ds(1, cx, 2), :]
            first = fg[2 * c, pl.ds(0, cx, 2), :] + fg[2 * c, pl.ds(1, cx, 2), :]
            stack[c, :cx, :] = low + high
            stack[c, cx : 2 * cx, :] = low
            stack[c, 2 * cx :, :] = first
        every = select_sum(stack[...].reshape(3 * cx * cz, LANES), gather)
        for c in range(cz):
            sums = every[3 * cx * c : 3 * cx * (c + 1)]
            s = sums[:cx, :LANES]
            z_low = sums[2 * cx :, :LANES]
            s_[c] = plane(s, rows)
            yl_[c] = plane(sums[:cx, LANES:], rows)
            xl_[c] = plane(sums[cx : 2 * cx, :LANES], rows)
            zl_[c] = plane(z_low, rows)
            zh_[c] = plane(s - z_low, rows)
            w[c] = jnp.zeros((rows, LANES), F32)
            w[c, :cx, :cy] = 1.0 / (6.0 + coarse[c])
        for c in range(cz):
            s, x_low, y_low = s_[c], xl_[c], yl_[c]
            x_high = s - x_low
            y_high = s - y_low
            total = 3.0 * s
            total += shift_rows(x_low, -1) + shift_rows(x_high, 1)
            total += shift_lanes(y_low, -1) + shift_lanes(y_high, 1)
            if c > 0:
                total += zh_[c - 1]
            if c < cz - 1:
                total += zl_[c + 1]
            rhs[c] = total
            xb[c] = jnp.where(row_c < cx // 2, x_low, x_high)
            yb[c] = jnp.where(lane_c < cy // 2, y_low, y_high)
        rhs[cz] = zh_[cz - 1]
        rhs[cz + 1] = jnp.zeros((rows, LANES), F32)
        rhs[cz + 2] = jnp.zeros((rows, LANES), F32)
        rhs[cz + 3] = zl_[0]

        def fill(ref, near, far, half, face):
            planes = [rhs[near], rhs[far], w[near], w[far], half]
            planes += [xb[near], xb[far], yb[near], yb[far]]
            for i, value in enumerate(planes):
                ref[i * rows : (i + 1) * rows, :] = value
            ref[9 * rows : 9 * rows + nx, :] = face

        def up(ref):
            fill(ref, cz - 1, cz - 2, zh_[cz - 1], fg[nz - 1])

        def down(ref):
            fill(ref, 0, 1, zl_[0], fg[0])

        write_sides("gz", out, up, down)

    coarse = (cz, rows, LANES)
    send = (9 * rows + nx, LANES)
    return call(
        body,
        [(nz, nx, ny), (cz + 4, rows, LANES), coarse, coarse, coarse] + [send] * sends,
        scratch=[(2, nx, ny), (cz, 3 * cx, LANES), coarse, coarse, coarse, coarse, coarse],
        in_specs=vmem(6),
        out_specs=vmem(5 + sends),
    )(part, node_shift, coarse_shift, got_z, got_x, got_y)


def x_stage(got, rhs, xb, yb, w, fg, after, z_count, x_count):
    planes, rows, _ = rhs.shape
    cz, cx = planes - 4, rows - 8
    nz, nx, ny = fg.shape
    cy = ny // 2
    sends = 1 if x_count == 2 else 2
    gots = len(got)
    size = -(-(3 * planes + nz + 1) // 8) * 8

    def body(*refs):
        got = refs[:gots]
        rhs, xb, yb, w, fg, _, _, rhs2, w2 = refs[gots : gots + 9]
        out, (xb2, yb2) = refs[gots + 9 : gots + 9 + sends], refs[gots + 9 + sends :]

        def take_at(pick, at):
            values = [ref[at, :] for ref in got]
            return pick("gz", z_count, values[0], values[1] if gots > 1 else None)

        def take(pick, i):
            return take_at(pick, slice(i * rows, (i + 1) * rows))

        for c in range(1, cz - 1):
            rhs2[c] = rhs[c]
        rhs2[0] = rhs[0] + take(low_of, 4)
        rhs2[cz - 1] = rhs[cz - 1] + take(high_of, 4)
        rhs2[cz] = rhs[cz] + take(high_of, 0)
        rhs2[cz + 1] = take(high_of, 1)
        rhs2[cz + 2] = take(low_of, 1)
        rhs2[cz + 3] = rhs[cz + 3] + take(low_of, 0)
        for here, there, i in ((w, w2, 2), (xb, xb2, 5), (yb, yb2, 7)):
            for c in range(cz):
                there[c] = here[c]
            there[cz] = take(high_of, i)
            there[cz + 1] = take(high_of, i + 1)
            there[cz + 2] = take(low_of, i + 1)
            there[cz + 3] = take(low_of, i)

        lane = lane_ids(planes)

        def fill(ref, near, far, fine):
            halves = lane < cy
            first = jnp.where(halves, rhs2[:, near, :], shift_lanes(rhs2[:, far, :], cy))
            second = jnp.where(halves, w2[:, near, :], shift_lanes(w2[:, far, :], cy))
            edge = yb2[:, far, :]
            third = jnp.where(halves, xb2[:, near, :], shift_lanes(yb2[:, near, :], cy))
            third = jnp.where(lane == cy + 1, shift_lanes(edge, cy + 1), third)
            third = jnp.where(lane == LANES - 2, shift_lanes(edge, cy - 1), third)
            for i, value in enumerate((first, second, third)):
                ref[i * planes : (i + 1) * planes, :] = value
            ref[3 * planes : 3 * planes + nz, :] = fg[:, fine, :]
            at = 9 * rows + fine
            last = 3 * planes + nz
            ref[last : last + 1, :] = take_at(high_of, slice(at, at + 1))
            ref[last + 1 :, :] = jnp.zeros((size - last - 1, LANES), F32)

        def up(ref):
            fill(ref, cx - 1, cx - 2, nx - 1)

        def down(ref):
            fill(ref, 0, 1, 0)

        write_sides("gx", out, up, down)

    whole = (planes, rows, LANES)
    return call(
        body,
        [whole, whole] + [(size, LANES)] * sends,
        scratch=[whole, whole],
        in_specs=vmem(gots + 7),
        out_specs=vmem(2 + sends),
    )(*got, rhs, xb, yb, w, fg, *after)


def x_tail(got, fg, node_shift, low_x, after, z_count):
    nz, nx, ny = fg.shape
    z_at = 9 * (nx // 2 + 8)
    gots = len(got)

    def body(*refs):
        got = refs[:gots]
        fg, shift, low_x, _, out = refs[gots:]
        lane = lane_ids(nz)
        row = row_ids(nz)

        def z_row(pick):
            values = [ref[z_at : z_at + 1, :] for ref in got]
            return pick("gz", z_count, values[0], values[1] if gots > 1 else None)

        here = fg[:, 0, :]
        around = fg[:, 1, :] + jnp.where(row == 0, z_row(low_of), shift_rows(here, 1))
        around += jnp.where(row == nz - 1, z_row(high_of), shift_rows(here, -1))
        around += jnp.where(lane == 0, 0.0, shift_lanes(here, 1))
        around += jnp.where(lane == ny - 1, 0.0, shift_lanes(here, -1))
        inverse = 1.0 / (6.0 + shift[:, 0, :])
        out[: 3 * nz, :] = low_x[...]
        out[3 * nz : 4 * nz, :] = here + inverse * around
        out[4 * nz :, :] = inverse

    return call(
        body, [(5 * nz, LANES)], in_specs=vmem(gots + 4), out_specs=vmem(1)
    )(*got, fg, node_shift, low_x, after)[0]


def part_stage(fg, node_shift, low_z):
    nz, nx, ny = fg.shape

    def body(fg, shift, low_z, part, inv, tail):
        lane = lane_ids(nx)
        row = row_ids(nx)
        zero = jnp.zeros((nx, ny), F32)
        for z in range(nz):
            guess = fg[z]
            inner = fg[z + 1] if z < nz - 1 else zero
            inner += jnp.where(row == 0, 0.0, shift_rows(guess, 1))
            inner += jnp.where(row == nx - 1, 0.0, shift_rows(guess, -1))
            inner += jnp.where(lane == 0, 0.0, shift_lanes(guess, 1))
            inner += jnp.where(lane == ny - 1, 0.0, shift_lanes(guess, -1))
            inverse = 1.0 / (6.0 + shift[z])
            inv[z] = inverse
            part[z] = guess + inverse * (inner + (fg[z - 1] if z > 0 else zero))
            if z == 0:
                for k in range(3):
                    tail[k * nx : (k + 1) * nx, :] = low_z[k]
                tail[3 * nx : 4 * nx, :] = guess + inverse * inner
                tail[4 * nx :, :] = inverse

    return call(
        body, [fg.shape, fg.shape, (5 * nx, LANES)], in_specs=vmem(3), out_specs=vmem(3)
    )(fg, node_shift, low_z)


def fold_row(rows):
    return (rows + 8) // 16 * 8


def line(source, fine, at):
    count = source.shape[0]
    spread = jnp.broadcast_to(source[:, fine : fine + 1], (count, LANES))
    own = lane_ids(count) - at == row_ids(count)
    return jnp.sum(jnp.where(own, spread, 0.0), axis=0, keepdims=True)


def y_stage(got, rhs, w, early, x_count, y_count):
    planes, rows, _ = rhs.shape
    cx = rows - 8
    nx, cy = 2 * cx, LANES // 2
    nz, half, cut = 2 * (planes - 4), nx // 2, fold_row(rows)
    sends = 1 if y_count == 2 else 2
    gots = len(got)

    def body(*refs):
        got = refs[:gots]
        rhs, w, up_, down_, part, inv, _, rhs3, w3 = refs[gots : gots + 9]
        rest = refs[gots + 9 :]
        out = rest
        lane_p = lane_ids(planes)

        def take_at(pick, at):
            values = [ref[at, :] for ref in got]
            return pick("gx", x_count, values[0], values[1] if gots > 1 else None)

        def take(pick, i):
            return take_at(pick, slice(i * planes, (i + 1) * planes))

        for c in range(planes):
            w3[c] = w[c]
            rhs3[c] = rhs[c]
        for pick, near, far, edge in ((high_of, cx, cx + 1, cx - 1), (low_of, rows - 1, rows - 2, 0)):
            first, second, third = take(pick, 0), take(pick, 1), take(pick, 2)
            other = shift_lanes(third, -cy)
            one = jnp.where((lane_p == 0) | (lane_p == cy - 1), other, 0.0)
            two = jnp.where(lane_p == 0, shift_lanes(third, -cy - 1), 0.0)
            two = jnp.where(lane_p == cy - 1, shift_lanes(third, 1 - cy), two)
            for at, value, ends in ((near, first, one), (far, shift_lanes(first, -cy), two)):
                value = jnp.where(lane_p < cy, value, 0.0)
                value += jnp.where(lane_p == cy, shift_lanes(ends, 1), 0.0)
                value += jnp.where(lane_p == LANES - 1, shift_lanes(ends, -1), 0.0)
                rhs3[:, at, :] += value
            w3[:, near, :] = jnp.where(lane_p < cy, second, 0.0)
            w3[:, far, :] = jnp.where(lane_p < cy, shift_lanes(second, -cy), 0.0)
            rhs3[:, edge, :] += jnp.where(lane_p < cy, third, 0.0)

        lane_c = lane_ids(rows)
        base = 5 * planes
        x_face = slice(3 * planes, 3 * planes + nz)
        x_high = take_at(high_of, x_face)

        def fill(ref, first, fine, early):
            acc = jnp.zeros((rows, LANES), F32)
            inner = first if first > 0 else 0
            for z in range(planes):
                for field, width, at, source in (
                    (rhs3, 3, 3 * z, first),
                    (w3, 2, 3 * planes + 2 * z, inner),
                ):
                    there = (lane_c >= at) & (lane_c < at + width)
                    acc = jnp.where(there, shift_lanes(field[z], at - source), acc)
            ref[:cut, :] = acc[:cut]
            ref[: rows - cut, :] += shift_lanes(acc[cut:], base)
            ref[cut - 8 : cut, :] += line(x_high, fine, base)
            ref[cut:, :] = early

        def up(ref):
            fill(ref, cy - 2, 2 * cy - 1, up_[...])

        def down(ref):
            row = row_ids(nx)
            ends = jnp.where(row == 0, line(take_at(low_of, x_face), 0, 0), 0.0)
            ends += jnp.where(row == nx - 1, line(x_high, 0, 0), 0.0)
            inverse = inv[...]
            value = part[...] + inverse * ends
            packed = down_[...]
            for i, source in (
                (1, value[:half]),
                (2, inverse[:half]),
                (4, value[half:]),
                (5, inverse[half:]),
            ):
                there = lane_ids(half) // nz == i
                packed = jnp.where(there, shift_lanes(source, i * nz), packed)
            fill(ref, -1, 0, packed)

        write_sides("gy", out, up, down)

    whole = (planes, rows, LANES)
    return call(
        body,
        [whole, whole] + [(cut + half, LANES)] * sends,
        in_specs=vmem(gots + 7),
        out_specs=vmem(2 + sends),
    )(*got, rhs, w, *early)


def y_columns(fg, node_shift):
    nz, nx, _ = fg.shape

    def body(fg, shift, here_, inner_, high_, inv):
        lane = lane_ids(nx)
        zero = jnp.zeros((nx, LANES), F32)
        here, inner, high, inverse = zero, zero, zero, zero + 1.0
        for z in range(nz):
            guess = fg[z]
            here = jnp.where(lane == z, shift_lanes(guess, z), here)
            inner = jnp.where(lane == z, shift_lanes(guess, z - 1), inner)
            high = jnp.where(lane == z, shift_lanes(guess, z + 1), high)
            inverse = jnp.where(lane == z, shift_lanes(6.0 + shift[z], z), inverse)
        here_[...] = here
        inner_[...] = inner
        high_[...] = high
        inv[...] = 1.0 / inverse

    return call(body, [(nx, LANES)] * 4, in_specs=vmem(2), out_specs=vmem(4))(fg, node_shift)


def y_early(got_z, columns, after, nz, z_count):
    nx = columns[0].shape[0]
    z_at = 9 * (nx // 2 + 8)
    n_z = len(got_z)

    def body(*refs):
        gz = refs[:n_z]
        here_, inner, high_, inv, _, up, down, part, last = refs[n_z:]
        lane = lane_ids(nx)
        row = row_ids(nx)

        def side(pick):
            values = [ref[z_at : z_at + nx, :] for ref in gz]
            return pick("gz", z_count, values[0], values[1] if n_z > 1 else None)

        above = side(high_of)
        here = jnp.where(lane == nz, shift_lanes(above, nz), here_[...])
        here = jnp.where(lane == LANES - 1, shift_lanes(side(low_of), -1), here)
        high = jnp.where(lane == nz, shift_lanes(above, nz + 1), high_[...])
        inverse = inv[...]
        around = inner[...] + shift_lanes(here, 1) + shift_lanes(here, -1)
        around += jnp.where(row == 0, 0.0, shift_rows(here, 1))
        around += jnp.where(row == nx - 1, 0.0, shift_rows(here, -1))
        last[...] = high
        half = nx // 2
        lane_h = lane_ids(half)

        def fold(value):
            first, second = value[:half], value[half:]
            block = jnp.where(lane_h < nz, first, 0.0)
            there = (lane_h >= 3 * nz) & (lane_h < 4 * nz)
            block = jnp.where(there, shift_lanes(second, 3 * nz), block)
            block = jnp.where(lane_h == 6 * nz, shift_lanes(first, 5 * nz), block)
            return jnp.where(lane_h == 6 * nz + 1, shift_lanes(second, 5 * nz + 1), block)

        up[...] = fold(high)
        down[...] = fold(here)
        part[...] = here + inverse * around

    return call(
        body, [(nx // 2, LANES)] * 2 + [(nx, LANES)] * 2, in_specs=vmem(n_z + 5), out_specs=vmem(4)
    )(*got_z, *columns, after)


def coarse_stage(got, rhs, w, after, y_count, devices):
    planes, rows, _ = rhs.shape
    cz, cx = planes - 4, rows - 8
    cy = LANES // 2
    gots = len(got)

    def body(*refs):
        got = refs[:gots]
        rhs, w, _, v1, v2, sums, tot, inv_, image_ = refs[gots:]
        cut = fold_row(rows)
        tail = [shift_lanes(ref[: rows - cut, :], -5 * planes) for ref in got]
        values = [jnp.concatenate([ref[:cut, :], t], axis=0) for ref, t in zip(got, tail)]
        second = values[1] if gots > 1 else None
        low = low_of("gy", y_count, values[0], second)
        high = high_of("gy", y_count, values[0], second)
        lane = lane_ids(rows)
        above = (lane >= cy - 1) & (lane < cy + 2)
        below = (lane >= LANES - 2) | (lane == 0)
        for z in range(planes):
            at = 3 * z
            right = jnp.where(below, shift_lanes(low, LANES - 2 - at), 0.0)
            right = rhs[z] + jnp.where(above, shift_lanes(high, cy - 1 - at), right)
            at = 3 * planes + 2 * z
            inv = jnp.where(lane >= LANES - 2, shift_lanes(low, LANES - 2 - at), w[z])
            inv = jnp.where((lane >= cy) & (lane < cy + 2), shift_lanes(high, cy - at), inv)
            inv_[z] = inv
            tot[z] = right
            v1[z] = right * inv

        def near(field, z):
            here = field[z]
            total = field[(z + 1) % planes] + field[(z - 1) % planes]
            total += shift_rows(here, 1) + shift_rows(here, -1)
            return total + shift_lanes(here, 1) + shift_lanes(here, -1)

        v2[cz + 1] = jnp.zeros((rows, LANES), F32)
        v2[cz + 2] = jnp.zeros((rows, LANES), F32)
        for z in list(range(cz + 1)) + [planes - 1]:
            image = tot[z] - near(v1, z)
            if z < cz:
                image_[z] = image
            v2[z] = image * inv_[z]
        parts = [jnp.zeros((cx, LANES), F32)] * 5
        for z in range(cz):
            first, second_, right, image = v1[z], v2[z], tot[z], image_[z]
            third = image - near(v2, z)
            terms = (first * right, second_ * right, first * image, second_ * image, second_ * third)
            parts = [a + b[:cx, :] for a, b in zip(parts, terms)]
        keep = lane_ids(1) < cy
        lines = [jnp.where(keep, jnp.sum(a, axis=0, keepdims=True), 0.0) for a in parts]
        tile = jnp.concatenate(lines + [jnp.zeros((3, LANES), F32)], axis=0)
        column = jnp.sum(tile, axis=1, keepdims=True)
        spread = jnp.where(lane_ids(8) == row_ids(8), column, 0.0)
        line = jnp.sum(spread, axis=0, keepdims=True)
        sums[...] = jnp.broadcast_to(line[None], (devices, 1, LANES))

    whole = (planes, rows, LANES)
    return call(
        body,
        [whole, whole, (devices, 1, LANES)],
        scratch=[whole, whole, whole],
        in_specs=vmem(gots + 3),
        out_specs=vmem(3),
    )(*got, rhs, w, *after)


def smooth_stage(scaled, inverses, below, tail_z, tail_x, tail_y, after, counts):
    _, nz, nx, _ = scaled.shape

    def body(*refs):
        s, inv, lz, lx, ly = refs[:5]
        tz, gx, ty, _, out = refs[5:]
        lane = lane_ids(nx)
        row = row_ids(nx)

        ends = from_below("gy", ly[...]) + from_above("gy", counts[2], ty[...])
        for k in range(3):
            z_low = from_below("gz", lz[k])
            z_high = from_above("gz", counts[0], tz[k * nx : (k + 1) * nx, :])
            x_low = from_below("gx", lx[k * nz : (k + 1) * nz, :])
            x_high = from_above("gx", counts[1], gx[k * nz : (k + 1) * nz, :])
            for z in range(nz):
                here = s[k, z]
                around = s[k, z - 1] if z > 0 else z_low
                around += s[k, z + 1] if z < nz - 1 else z_high
                around += jnp.where(row == 0, x_low[z : z + 1, :], shift_rows(here, 1))
                around += jnp.where(row == nx - 1, x_high[z : z + 1, :], shift_rows(here, -1))
                spot = k * nz + z
                end = shift_lanes(ends, LANES - 1 - 2 * spot)
                around += jnp.where(lane == 0, end, shift_lanes(here, 1))
                around += jnp.where(lane == LANES - 1, end, shift_lanes(here, -1))
                out[k, z] = here + around * inv[k, z]

    return call(
        body, [scaled.shape], in_specs=vmem(9), out_specs=vmem(1)
    )(scaled, inverses, *below, tail_z, tail_x, tail_y, after)[0]


def final_stage(sums, v1, v2, fg, mid, smooth, early, tail_z, tail_x, got_z, got_x, got_y, counts):
    planes, rows, _ = v1.shape
    cz, cx, cy = planes - 4, rows - 8, LANES // 2
    nz, nx, _ = fg.shape
    step = 2
    n_z, n_x, n_y = len(got_z), len(got_x), len(got_y)
    gots = n_z + n_x + n_y

    def body(*refs):
        sums, v1, v2, fg, part, inv, smooth, early, tz, tx = refs[:10]
        gz = refs[10 : 10 + n_z]
        gx = refs[10 + n_z : 10 + n_z + n_x]
        gy = refs[10 + n_z + n_x : 10 + gots]
        out, sol, dup, inter, small, lines, buf, sem = refs[10 + gots :]

        def one_side(pick, refs, axis, size, at):
            values = [ref[at, :] for ref in refs]
            return pick(axis, size, values[0], values[1] if len(values) > 1 else None)

        def both(refs, axis, size, at):
            return [one_side(pick, refs, axis, size, at) for pick in (low_of, high_of)]

        total = jnp.sum(sums[...], axis=0)
        lane1 = lane_ids(1)
        gone, gtwo, hone, hmix, htwo = [
            jnp.sum(jnp.where(lane1 == i, total, 0.0), axis=1, keepdims=True) for i in range(5)
        ]
        two = (gtwo - hmix * gone / hone) / (htwo - hmix * hmix / hone)
        one = (gone - hmix * two) / hone
        source = lax.broadcasted_iota(jnp.int32, (LANES, 2 * LANES), 0)
        target = lax.broadcasted_iota(jnp.int32, (LANES, 2 * LANES), 1)
        fine = target - LANES
        side = jnp.where(fine % 2 == 1, fine // 2 + 1, (fine // 2 + LANES - 1) % LANES)
        spread = jnp.where(jnp.where(target < LANES, target // 2, side) == source, 1.0, 0.0)
        for z in range(planes):
            sol[z] = one * v1[z] + two * v2[z]
        every = select_sum(sol[...].reshape(planes * rows, LANES), spread)
        dup[...] = every.reshape(planes, rows, 2 * LANES)

        z_low, z_high = both(gz, "gz", counts[0], slice(9 * rows, 9 * rows + nx))
        x_low, x_high = both(gx, "gx", counts[1], slice(3 * planes, 3 * planes + nz + 1))
        half, cut = nx // 2, fold_row(rows)
        y_row_low, y_row_high = both(gy, "gy", counts[2], slice(cut - 8, cut - 7))
        y_packs = both(gy, "gy", counts[2], slice(cut, cut + half))
        lane_h = lane_ids(half)

        def unfold(pack):
            first = jnp.where(lane_h < nz, pack, shift_lanes(pack, -5 * nz))
            second = shift_lanes(pack, -5 * nz - 1)
            second = jnp.where(lane_h < nz, shift_lanes(pack, -3 * nz), second)
            return jnp.concatenate([first, second], axis=0)

        y_low, y_high = [unfold(pack) for pack in y_packs]
        y_pack = y_packs[1]
        lane = lane_ids(nx)
        row = row_ids(nx)
        base = 5 * planes

        def spread_around(z):
            c, odd = z // 2, z % 2
            here = dup[c, :, :LANES]
            same = 3.0 * here + dup[c, :, LANES:]
            same += dup[(c + 1 if odd else c - 1) % planes, :, :LANES]
            slot = z % 2
            inter[slot, pl.ds(0, cx, 2), :] = (same + shift_rows(here, 1))[:cx, :]
            inter[slot, pl.ds(1, cx, 2), :] = (same + shift_rows(here, -1))[:cx, :]
            return inter[slot]

        def nodal(z):
            around = spread_around(z) + jnp.where(row == 0, x_low[z : z + 1, :], 0.0)
            around += jnp.where(row == nx - 1, x_high[z : z + 1, :], 0.0)
            around += jnp.where(lane == 0, shift_lanes(y_low, -z), 0.0)
            around += jnp.where(lane == LANES - 1, shift_lanes(y_high, -z - 1), 0.0)
            if z == nz:
                value = tz[3 * nx : 4 * nx, :] + tz[4 * nx :, :] * (around + fg[nz - 1])
                return from_above("gz", counts[0], value)
            if z == 0:
                around += z_low
            if z == nz - 1:
                around += z_high
            return part[z] + inv[z] * around

        here = dup[:cz, cx, :LANES]
        same = 3.0 * here + dup[:cz, cx, LANES:] + dup[:cz, cx - 1, :LANES]
        small[pl.ds(0, cz, 2), :] = same + jnp.concatenate(
            [dup[planes - 1, cx : cx + 1, :LANES], here[: cz - 1]], axis=0
        )
        small[pl.ds(1, cz, 2), :] = same + dup[1 : cz + 1, cx, :LANES]
        for z in range(nz):
            left = shift_lanes(y_row_low, -(base + z))
            right = shift_lanes(y_row_high, -(base + z) - 1)
            value = jnp.where(lane1 == 0, left, 0.0)
            lines[z : z + 1, :] = jnp.where(lane1 == LANES - 1, right, value)
        x_value = tx[3 * nz : 4 * nz, :] + tx[4 * nz :, :] * (
            fg[:, nx - 1, :] + small[...] + lines[...]
        )
        x_value = from_above("gx", counts[1], x_value)

        lane_c = lane_ids(rows)
        middle = jnp.zeros((rows, LANES), F32)
        inward = jnp.zeros((rows, LANES), F32)
        beside = jnp.zeros((rows, LANES), F32)
        for z in range(nz):
            c = z // 2
            here = sol[c]
            same = 3.0 * here + sol[(c + 1 if z % 2 else c - 1) % planes]
            middle = jnp.where(lane_c == z, shift_lanes(same, z - cy), middle)
            inward = jnp.where(lane_c == z, shift_lanes(here, z - cy + 1), inward)
            beside = jnp.where(lane_c == z, shift_lanes(here, z - cy), beside)
        middle += inward
        even = middle + shift_rows(beside, 1)
        odd = middle + shift_rows(beside, -1)
        inter[0, pl.ds(0, cx, 2), :] = even[:cx, :]
        inter[0, pl.ds(1, cx, 2), :] = odd[:cx, :]
        y_base = jnp.concatenate(
            [shift_lanes(y_pack, -nz), shift_lanes(y_pack, -4 * nz)], axis=0
        )
        y_inverse = jnp.concatenate(
            [shift_lanes(y_pack, -2 * nz), shift_lanes(y_pack, -5 * nz)], axis=0
        )
        y_value = y_base + y_inverse * (early[...] + inter[0])
        y_value = from_above("gy", counts[2], y_value)

        def copy(block):
            at = pl.ds(block * step, step)
            return pltpu.make_async_copy(buf.at[:, at], out.at[:, at], sem.at[block])

        value = nodal(0)
        for z in range(nz):
            after = nodal(z + 1)
            steps = [after, jnp.where(row == nx - 1, x_value[z : z + 1, :], shift_rows(value, -1))]
            steps.append(
                jnp.where(lane == LANES - 1, shift_lanes(y_value, -z - 1), shift_lanes(value, -1))
            )
            for k in range(3):
                buf[k, z] = smooth[k, z] + (steps[k] - value)
            if z % step == step - 1:
                copy(z // step).start()
            value = after
        for block in range(nz // step):
            copy(block).wait()

    return call(
        body,
        [smooth.shape],
        scratch=[
            (planes, rows, LANES),
            (planes, rows, 2 * LANES),
            (2, nx, LANES),
            (nz, LANES),
            (nz, LANES),
            smooth.shape,
            pltpu.SemaphoreType.DMA((nz // step,)),
        ],
        far_out=True,
        in_specs=vmem(10 + gots),
        out_specs=[pl.BlockSpec(memory_space=pltpu.HBM)],
    )(sums, v1, v2, fg, *mid, smooth, early, tail_z, tail_x, *got_z, *got_x, *got_y)[0]


def local(residual, edge_diag, node_shift, coarse_shift):
    axes = ("gz", "gx", "gy")
    counts = tuple(lax.axis_size(a) for a in axes)
    devices = counts[0] * counts[1] * counts[2]
    part, *faces, scaled, inverses = edge_stage(residual, edge_diag)
    up_z, up_x, up_y, low_z, low_x, low_y = faces
    below = []
    for value, axis in ((up_z, "gz"), (up_x, "gx"), (up_y, "gy")):
        below.append(ring(value, axis, 1))
    tail_y = ring(low_y, "gy", -1)
    fg, rhs, xb, yb, w, *send = nodal_stage(part, node_shift, coarse_shift, *below, counts[0])
    got_z = swap(send, "gz")
    *mid, tail_z = part_stage(fg, node_shift, low_z)
    columns = y_columns(fg, node_shift)
    after = (mid[1], columns[0])
    rhs, w, *send = x_stage(got_z, rhs, xb, yb, w, fg, after, counts[0], counts[1])
    got_x = swap(send, "gx", ("gx", "gz"))
    tail_x = x_tail(got_z, fg, node_shift, low_x, w, counts[0])
    *early, last = y_early(got_z, columns, w, fg.shape[0], counts[0])
    early = (*early, columns[3], tail_x)
    tail_z = ring(tail_z, "gz", -1)
    tail_x = ring(tail_x, "gx", -1)
    rhs, w, *send = y_stage(got_x, rhs, w, early, counts[1], counts[2])
    got_y = swap(send, "gy", ("gy", "gz"))
    smooth = smooth_stage(scaled, inverses, below, tail_z, tail_x, tail_y, w, counts)
    v1, v2, sums = coarse_stage(got_y, rhs, w, (smooth,), counts[2], devices)
    sums = lax.all_to_all(sums, ("gx", "gy", "gz"), 0, 0)
    return final_stage(
        sums, v1, v2, fg, mid, smooth, last, tail_z, tail_x, got_z, got_x, got_y, counts
    )


def solution(mesh):
    placed = (
        P(None, "gz", "gx", "gy"),
        P(None, "gz", "gx", "gy"),
        P("gz", "gx", "gy"),
        P("gz", "gx", "gy"),
    )

    return jax.shard_map(
        local, mesh=mesh, in_specs=placed, out_specs=P(None, "gz", "gx", "gy"), check_vma=False
    )
```
